128 devices in a mesh: dp: 4 (over z), w: 4 (over y), h: 8 (over x, core).
Axes of the slice: x: 4, y: 4, z: 4, core: 2. Of those that a mesh axis runs over, the one named last changes fastest.
Arguments:
- field: float32 [12, 256, 128, 256], P('dp', None, 'h', 'w')
- target: float32 [12, 256, 128, 256], P('dp', None, 'h', 'w')
- lat_weight: float32 [128], P('h')
- leg_fwd: float32 [64, 64, 128], P('w', None, 'h')
- leg_inv: float32 [64, 64, 128], P('w', None, 'h')
- spec_w: float32 [2, 64, 256, 256], replicated
- w_in: bfloat16 [256, 512], replicated
- w_out: bfloat16 [512, 256], replicated
Outputs:
- output 1: float32 [], replicated
- output 2: float32 [12, 256, 128, 256], P('dp', None, 'h', 'w')
- output 3: float32 [2, 64, 256, 256], P(None, 'h')
- output 4: float32 [256, 512], replicated
- output 5: float32 [512, 256], replicated
All inputs are finite; a program needn't handle non-finite values.
Results may differ from the reference program's by a relative error of at most 0.00130349.
Values sent between devices are 32-bit elements.
A program may use at most 1 GiB of HBM per device.

```python
import functools
import jax
import jax.numpy as jnp
from jax import lax

BATCH = 12
CHANNELS = 256
NLAT = 128
NLON = 256
LMAX = 64
NORM_EPS = 1e-5
TOTAL = BATCH * CHANNELS * NLAT * NLON


def setup_inputs(seed: int = 0) -> dict:
    keys = jax.random.split(jax.random.key(seed), 12)
    lat_angle = (jnp.arange(NLAT, dtype=jnp.float32) + 0.5) * (jnp.pi / NLAT) - 0.5 * jnp.pi
    lon_angle = jnp.arange(NLON, dtype=jnp.float32) * (2.0 * jnp.pi / NLON)
    grid_shape = (BATCH, CHANNELS, NLAT, NLON)
    chan_mean = jax.random.normal(keys[0], (1, CHANNELS, 1, 1))
    chan_scale = 0.5 + jax.random.uniform(keys[1], (1, CHANNELS, 1, 1))
    wave_amp = jax.random.normal(keys[2], (BATCH, CHANNELS, 1, 1))
    wave_phase = 2.0 * jnp.pi * jax.random.uniform(keys[3], (BATCH, CHANNELS, 1, 1))
    wave = wave_amp * jnp.sin(2.0 * lat_angle)[:, None] * jnp.cos(lon_angle + wave_phase)
    field = chan_mean + chan_scale * (jax.random.normal(keys[4], grid_shape) + wave)
    target = chan_mean + 0.7 * jax.random.normal(keys[5], grid_shape)
    lat_weight = jnp.cos(lat_angle) * (0.5 + jax.random.uniform(keys[6], (NLAT,)))
    degrees = jnp.arange(LMAX)
    tri_mask = (degrees[None, :, None] >= degrees[:, None, None]).astype(jnp.float32)
    leg_fwd = jax.random.normal(keys[7], (LMAX, LMAX, NLAT)) * tri_mask * (NLAT ** -0.5)
    leg_inv = jax.random.normal(keys[8], (LMAX, LMAX, NLAT)) * tri_mask * ((2.0 / LMAX) ** 0.5)
    spec_w = jax.random.normal(keys[9], (2, LMAX, CHANNELS, CHANNELS)) * ((2.0 * CHANNELS) ** -0.5)
    w_in = jax.random.normal(keys[10], (CHANNELS, 2 * CHANNELS)) * (CHANNELS ** -0.5)
    w_out = jax.random.normal(keys[11], (2 * CHANNELS, CHANNELS)) * ((2.0 * CHANNELS) ** -0.5)
    return {"field": field.astype(jnp.float32), "target": target.astype(jnp.float32), "lat_weight": lat_weight.astype(jnp.float32), "leg_fwd": leg_fwd.astype(jnp.float32), "leg_inv": leg_inv.astype(jnp.float32), "spec_w": spec_w.astype(jnp.float32), "w_in": w_in.astype(jnp.bfloat16), "w_out": w_out.astype(jnp.bfloat16)}


def as_bf16_value(values):
    return values + lax.stop_gradient(values.astype(jnp.bfloat16).astype(jnp.float32) - values)


def sample_energy(sample, lat_weight, leg_fwd, leg_inv, spec_w, w_in, w_out):
    field, target = sample
    chan_mean = jnp.mean(field, axis=(1, 2), keepdims=True)
    centred = field - chan_mean
    variance = jnp.mean(centred * centred, axis=(1, 2), keepdims=True)
    normed = centred * lax.rsqrt(variance + NORM_EPS)
    lon_spec = jnp.fft.rfft(normed, axis=2, norm="ortho")[:, :, :LMAX]
    coef_re = jnp.einsum("mlt,ctm->clm", leg_fwd, lon_spec.real)
    coef_im = jnp.einsum("mlt,ctm->clm", leg_fwd, lon_spec.imag)
    mix_re = jnp.einsum("ilm,lio->olm", coef_re, spec_w[0]) - jnp.einsum("ilm,lio->olm", coef_im, spec_w[1])
    mix_im = jnp.einsum("ilm,lio->olm", coef_re, spec_w[1]) + jnp.einsum("ilm,lio->olm", coef_im, spec_w[0])
    back_re = jnp.einsum("mlt,clm->ctm", leg_inv, mix_re)
    back_im = jnp.einsum("mlt,clm->ctm", leg_inv, mix_im)
    back_spec = jnp.pad(lax.complex(back_re, back_im), ((0, 0), (0, 0), (0, NLON // 2 + 1 - LMAX)))
    y_grid = jnp.fft.irfft(back_spec, n=NLON, axis=2, norm="ortho")
    hidden = jnp.einsum("ctp,cf->ftp", as_bf16_value(y_grid), w_in)
    activation = as_bf16_value(jax.nn.gelu(hidden))
    mlp_out = jnp.einsum("ftp,fc->ctp", activation, w_out)
    residual = field + y_grid + mlp_out - target
    return 0.5 * jnp.sum(lat_weight[:, None] * residual * residual)


def total_energy(field, spec_w, w_in, w_out, target, lat_weight, leg_fwd, leg_inv):
    body = jax.checkpoint(functools.partial(sample_energy, lat_weight=lat_weight, leg_fwd=leg_fwd, leg_inv=leg_inv, spec_w=spec_w, w_in=w_in, w_out=w_out))
    return jnp.sum(lax.map(body, (field, target)))


def reference(field, target, lat_weight, leg_fwd, leg_inv, spec_w, w_in, w_out):
    energy_fn = functools.partial(total_energy, target=target, lat_weight=lat_weight, leg_fwd=leg_fwd, leg_inv=leg_inv)
    energy, pullback = jax.vjp(energy_fn, field, spec_w, w_in.astype(jnp.float32), w_out.astype(jnp.float32))
    grad_field, grad_spec, grad_w_in, grad_w_out = pullback(jnp.ones_like(energy))
    loss = 2.0 * energy / TOTAL
    return (loss, grad_field, grad_spec, grad_w_in, grad_w_out)
```

```python
import functools
import jax
import jax.numpy as jnp
import numpy as np
from jax import lax
from jax.sharding import PartitionSpec as P

NORM_EPS = 1e-5
PRECISE = lax.Precision.HIGHEST


def mm(form, a, b):
    return jnp.einsum(form, a, b, precision=PRECISE, preferred_element_type=jnp.float32)


def dft_tables(lon_count, num_modes):
    modes, lons = np.arange(num_modes), np.arange(lon_count)
    angle = 2.0 * np.pi * ((modes[:, None] * lons[None, :]) % lon_count) / lon_count
    scale = lon_count ** -0.5
    fwd = np.stack([np.cos(angle), -np.sin(angle)], 0) * scale
    weight = np.where(modes == 0, 1.0, 2.0)[None, :, None]
    inv = fwd * weight

    def rows(table):
        table = table.reshape(2, num_modes // 4, 4, lon_count).transpose(1, 0, 2, 3)
        return table.reshape(2 * num_modes, lon_count).astype(np.float32)

    return rows(fwd), rows(inv)


def solution(mesh):
    dp_size = mesh.shape["dp"]
    w_size = mesh.shape["w"]
    h_size = mesh.shape["h"]
    grid_axes = ("h", "w")
    all_axes = ("dp", "h", "w")
    xs = h_size // 2

    def swap(pieces, axes):
        return lax.all_to_all(pieces, axes, 0, 0, tiled=True)

    def local_step(field, target, lat_weight, leg_fwd, leg_inv, spec_w, w_in, w_out):
        nb, nc, nt, npl = field.shape
        nlon = npl * w_size
        tq = nt // w_size
        nm = leg_fwd.shape[0] * w_size
        ng = nm // 4
        half = nc // 2
        ndev = h_size * w_size
        nlat = nt * h_size
        nl = leg_fwd.shape[1]
        l_own = nl // ndev
        grid_points = nlat * nlon
        total_points = nb * dp_size * nc * grid_points
        hi, wi = lax.axis_index("h"), lax.axis_index("w")
        fwd_np, inv_np = dft_tables(nlon, nm)
        f_tab, g_tab = jnp.asarray(fwd_np), jnp.asarray(inv_np)

        x = field.transpose(0, 2, 3, 1)
        tgt = target.transpose(0, 2, 3, 1)

        def to_rows(v):
            v = v.reshape(nb, w_size, tq, npl, nc).transpose(1, 0, 2, 3, 4)
            v = swap(v, "w")
            return v.transpose(1, 2, 0, 3, 4).reshape(nb, tq, nlon, nc)

        def from_rows(v):
            v = v.reshape(nb, tq, w_size, npl, nc).transpose(2, 0, 1, 3, 4)
            v = swap(v, "w")
            return v.transpose(1, 0, 2, 3, 4).reshape(nb, nt, npl, nc)

        loc_mean = jnp.mean(x, axis=(1, 2))
        loc_m2 = jnp.sum((x - loc_mean[:, None, None, :]) ** 2, axis=(1, 2))
        stats = lax.all_gather(jnp.stack([loc_mean, loc_m2]), grid_axes)
        mu = jnp.mean(stats[:, 0], axis=0)
        m2 = jnp.sum(stats[:, 1], axis=0) + (nt * npl) * jnp.sum((stats[:, 0] - mu) ** 2, axis=0)
        inv_std = lax.rsqrt(m2 / grid_points + NORM_EPS)
        lane0 = (hi % 2) * half
        mu_h = lax.dynamic_slice_in_dim(mu, lane0, half, 1)
        std_h = lax.dynamic_slice_in_dim(inv_std, lane0, half, 1)

        def tab(leg):
            v = leg.transpose(0, 2, 1).reshape(xs, 4, nt, nl)
            v = jnp.repeat(v, 2, axis=0)
            v = swap(v, "h")
            return v.transpose(1, 0, 2, 3).reshape(4, nlat, nl)

        p_t, q_t = tab(leg_fwd), tab(leg_inv)

        def spread(v):
            v = v.reshape(nb, tq, w_size, xs, 8, 2, half).transpose(3, 5, 2, 0, 1, 4, 6)
            v = v.reshape(ndev, nb, tq, 8, half)
            v = swap(v, grid_axes)
            return v.transpose(1, 0, 2, 3, 4).reshape(nb, nlat, 8, half)

        def gather(v):
            v = v.reshape(nb, ndev, tq, 8, half).transpose(1, 0, 2, 3, 4)
            v = swap(v, grid_axes)
            v = v.reshape(xs, 2, w_size, nb, tq, 8, half).transpose(3, 4, 2, 0, 5, 1, 6)
            return v.reshape(nb, tq, ng * 8, nc)

        def to_owner(v):
            v = v.reshape(ndev, l_own, nb, 8, half)
            v = swap(v, grid_axes)
            v = v.reshape(xs, 2, w_size, l_own, nb, 8, half).transpose(3, 4, 2, 0, 5, 1, 6)
            return v.reshape(l_own, nb, ng, 2, 4, nc)

        def from_owner(v):
            v = v.reshape(l_own, nb, w_size, xs, 8, 2, half).transpose(3, 5, 2, 0, 1, 4, 6)
            v = v.reshape(ndev, l_own, nb, 8, half)
            v = swap(v, grid_axes)
            return v.reshape(nl, nb, 2, 4, half)

        def leg_down(tab_t, v):
            v = v.reshape(nb, nlat, 2, 4, half)
            return mm("mtl,btrmc->lbrmc", tab_t, v)

        def leg_up(tab_t, v):
            return mm("mtl,lbrmc->btrmc", tab_t, v).reshape(nb, nlat, 8, half)

        x2 = to_rows(x)
        t2 = to_rows(tgt)
        spec = mm("rp,btpc->btrc", f_tab, x2)
        sp = spread(spec)
        has0 = jnp.where((hi // 2 == 0) & (wi == 0), jnp.float32(nlon ** 0.5), 0.0)
        corr = jnp.zeros((8, 1), jnp.float32).at[0, 0].set(1.0) * has0
        sp = sp - corr[None, None] * mu_h[:, None, None, :]
        a_loc = leg_down(p_t, sp) * std_h[None, :, None, None, :]
        a = to_owner(a_loc)
        me = hi * w_size + wi
        ker = lax.dynamic_slice_in_dim(spec_w, me * l_own, l_own, 1)
        kr, ki = ker[0], ker[1]
        b1 = mm("lbgrmi,lio->lbgrmo", a, kr)
        b2 = mm("lbgrmi,lio->lbgrmo", a, ki)
        sgn = jnp.asarray(np.array([-1.0, 1.0], np.float32))[:, None, None]
        mixed = b1 + sgn * b2[:, :, :, ::-1]
        back = gather(leg_up(q_t, from_owner(mixed)))
        y = mm("rp,btrc->btpc", g_tab, back)
        y_bf = y.astype(jnp.bfloat16)
        hid = jnp.einsum("btpc,cf->btpf", y_bf, w_in, preferred_element_type=jnp.float32)
        act, gelu_pull = jax.vjp(jax.nn.gelu, hid)
        act_bf = act.astype(jnp.bfloat16)
        out = jnp.einsum("btpf,fc->btpc", act_bf, w_out, preferred_element_type=jnp.float32)
        resid = x2 + y + out - t2
        q4 = lax.dynamic_slice_in_dim(lat_weight, wi * tq, tq, 0)
        d_out = q4[None, :, None, None] * resid
        loss = lax.psum(jnp.sum(d_out * resid), all_axes) / total_points
        d_out_bf = d_out.astype(jnp.bfloat16)
        g_out = lax.psum(jnp.einsum("btpf,btpc->fc", act_bf, d_out_bf, preferred_element_type=jnp.float32), all_axes)
        d_act = jnp.einsum("btpc,fc->btpf", d_out_bf, w_out, preferred_element_type=jnp.float32)
        d_hid = gelu_pull(d_act)[0].astype(jnp.bfloat16)
        g_in = lax.psum(jnp.einsum("btpc,btpf->cf", y_bf, d_hid, preferred_element_type=jnp.float32), all_axes)
        d_y = d_out + jnp.einsum("btpf,cf->btpc", d_hid, w_in, preferred_element_type=jnp.float32)
        d_back = spread(mm("rp,btpc->btrc", g_tab, d_y))
        d_mixed = to_owner(leg_down(q_t, d_back))
        d1 = mm("lbgrmo,lio->lbgrmi", d_mixed, kr)
        d2 = mm("lbgrmo,lio->lbgrmi", d_mixed, ki)
        d_a = d1 - sgn * d2[:, :, :, ::-1]
        rot = -sgn * d_mixed[:, :, :, ::-1]
        gr = mm("lbgrmi,lbgrmo->lio", a, d_mixed)
        gi = mm("lbgrmi,lbgrmo->lio", a, rot)
        grad_spec = lax.psum(jnp.stack([gr, gi]), "dp")
        grad_spec = lax.all_gather(grad_spec, "w", axis=1, tiled=True)
        d_sp = leg_up(p_t, from_owner(d_a))
        s1_h = has0 * jnp.sum(d_sp[:, :, 0], axis=1)
        s1 = lax.dynamic_update_slice_in_dim(jnp.zeros((nb, nc), jnp.float32), s1_h, lane0, 1)
        s2 = jnp.sum(d_a * a, axis=(0, 2, 3, 4))
        bstat = lax.psum(jnp.stack([s1, s2]), grid_axes) / grid_points
        d_n = mm("rp,btrc->btpc", f_tab, gather(d_sp))
        row = lambda v: v[:, None, None, :]
        normed = (x2 - row(mu)) * row(inv_std)
        d_x = d_out + row(inv_std) * (d_n - row(bstat[0]) - normed * row(bstat[1]))
        d_field = from_rows(d_x).transpose(0, 3, 1, 2)
        return loss, d_field, grad_spec, g_in, g_out

    grid_spec = P("dp", None, "h", "w")
    table_spec = P("w", None, "h")
    kernel_spec = P(None, "h", None, None)
    return jax.shard_map(local_step, mesh=mesh, in_specs=(grid_spec, grid_spec, P("h"), table_spec, table_spec, P(), P(), P()), out_specs=(P(), grid_spec, kernel_spec, P(), P()), check_vma=False)
```

```python
import functools
import jax
import jax.numpy as jnp
import numpy as np
from jax import lax
from jax.experimental import pallas as pl
from jax.experimental.pallas import tpu as pltpu
from jax.sharding import PartitionSpec as P

NORM_EPS = 1e-5
PRECISE = lax.Precision.HIGHEST
MESH = pl.DeviceIdType.MESH
F32 = jnp.float32


def mm(form, a, b):
    return jnp.einsum(form, a, b, precision=PRECISE, preferred_element_type=F32)


def dot(a, b):
    return jnp.dot(a, b, precision=PRECISE, preferred_element_type=F32)


def dft_tables(lon_count, num_modes):
    modes, lons = np.arange(num_modes), np.arange(lon_count)
    angle = 2.0 * np.pi * ((modes[:, None] * lons[None, :]) % lon_count) / lon_count
    fwd = np.stack([np.cos(angle), -np.sin(angle)], 0) * lon_count ** -0.5
    inv = fwd * np.where(modes == 0, 1.0, 2.0)[None, :, None]

    def rows(table):
        table = table.reshape(2, num_modes // 4, 4, lon_count).transpose(1, 0, 2, 3)
        return table.reshape(2 * num_modes, lon_count).astype(np.float32)

    return rows(fwd), rows(inv)


class Plane:
    def __init__(self, h_size, w_size):
        self.h_size, self.w_size = h_size, w_size
        self.h, self.w = lax.axis_index("h"), lax.axis_index("w")
        self.me = self.h * w_size + self.w
        self.group = self.w * (h_size // 2) + self.h // 2
        self.half = self.h % 2

    def barrier(self):
        sem = pltpu.get_barrier_semaphore()
        count = self.h_size * self.w_size

        def body(k, _):
            h, w = self.peer(k)
            pl.semaphore_signal(sem, inc=1, device_id={"h": h, "w": w}, device_id_type=MESH)
            return 0

        lax.fori_loop(1, count, body, 0)
        pl.semaphore_wait(sem, count - 1)

    def peer(self, k):
        return (self.h + k // self.w_size) % self.h_size, (self.w + k % self.w_size) % self.w_size

    def each(self, refs):
        src, dst, _, recv = refs(self.h, self.w, self.me, self.group, self.half)
        pltpu.make_async_copy(src, dst, recv).start()

        def body(k, _):
            h, w = self.peer(k)
            src, dst, send, recv = refs(h, w, h * self.w_size + w, w * (self.h_size // 2) + h // 2, h % 2)
            pltpu.make_async_remote_copy(src_ref=src, dst_ref=dst, send_sem=send, recv_sem=recv,
                                         device_id={"h": h, "w": w}, device_id_type=MESH).start()
            return 0

        lax.fori_loop(1, self.h_size * self.w_size, body, 0)


def drain(ref, sem):
    pltpu.make_async_copy(ref, ref, sem).wait()


def rows_at(i, n):
    return pl.ds(pl.multiple_of(i * n, n), n)


def lanes_at(half):
    return pl.ds(pl.multiple_of(half * 128, 128), 128)


def forward_kernel(h_size, w_size, x, tgt, leg_p, leg_q, spec_w, f_tab,
                   x2_out, t2_out, a_out, y_out, st_out, p_out, q_out,
                   xr, tr, xs, sr, als, ar, bs, br, ys, yr, st_s, st, pt, qt, ker,
                   sem_x, sem_s, sem_a, sem_b, sem_y, sem_m, sem_t):
    pn = Plane(h_size, w_size)
    nb = x.shape[0]
    tq = x.shape[1] // w_size
    npl = x.shape[2]
    l_own = als.shape[1] // 8 // (h_size * w_size)
    load_k = pltpu.make_async_copy(spec_w.at[:, pl.ds(pn.me * l_own, l_own)], ker, sem_m.at[0])
    load_k.start()
    pn.barrier()

    def send_rows(src, dst, b, sem):
        pltpu.make_async_copy(src.at[b, rows_at(pn.w, tq)], dst.at[b, :, rows_at(pn.w, npl)], sem.at[1, b]).start()
        for step in (1, 3, 2):
            w = (pn.w + step) % w_size
            pltpu.make_async_remote_copy(src_ref=src.at[b, rows_at(w, tq)], dst_ref=dst.at[b, :, rows_at(pn.w, npl)],
                                         send_sem=sem.at[0, b], recv_sem=sem.at[1, b],
                                         device_id={"w": w}, device_id_type=MESH).start()

    def send_table(src, dst, k):
        pltpu.make_async_copy(src.at[rows_at(pn.h // 2, 4)], dst.at[:, rows_at(pn.h, src.shape[1])], sem_t.at[1, k]).start()

        def body(step, _):
            h = (pn.h + step) % h_size
            pltpu.make_async_remote_copy(src_ref=src.at[rows_at(h // 2, 4)], dst_ref=dst.at[:, rows_at(pn.h, src.shape[1])],
                                         send_sem=sem_t.at[0, k], recv_sem=sem_t.at[1, k],
                                         device_id={"h": h}, device_id_type=MESH).start()
            return 0
        lax.fori_loop(1, h_size, body, 0)

    for b in range(nb):
        send_rows(x, xr, b, sem_x)
    send_table(leg_p, pt, 0)
    send_table(leg_q, qt, 1)

    for b in range(nb):
        drain(xr.at[b], sem_x.at[1, b])

        def spec(t, total, b=b):
            rows = xr[b, t]
            out = dot(f_tab[...], rows).reshape(-1, 8, rows.shape[1])
            for hf in range(2):
                xs[:, hf, b, rows_at(t, 8), :] = out[:, :, hf * 128:(hf + 1) * 128]
            return total + jnp.sum(rows, axis=0, keepdims=True)

        total = lax.fori_loop(0, tq, spec, jnp.zeros((1, xr.shape[3]), F32))
        pn.each(lambda h, w, lin, g, hf, b=b: (xs.at[g, hf, b], sr.at[b, rows_at(pn.me, 8 * tq)], sem_s.at[0, b], sem_s.at[1, b]))
        mean = total / (tq * xr.shape[2])

        def spread2(t, total, b=b, mean=mean):
            d = xr[b, t] - mean
            return total + jnp.sum(d * d, axis=0, keepdims=True)

        m2 = lax.fori_loop(0, tq, spread2, jnp.zeros((1, xr.shape[3]), F32))
        st_s[2 * b:2 * b + 1, :] = mean
        st_s[2 * b + 1:2 * b + 2, :] = m2
    st_s[2 * nb:, :] = jnp.zeros_like(st_s[2 * nb:, :])
    pn.each(lambda h, w, lin, g, hf: (st_s, st.at[pn.me], sem_m.at[1], sem_m.at[2]))
    for b in range(nb):
        send_rows(tgt, tr, b, sem_y.at[2])

    drain(pt, sem_t.at[1, 0])
    drain(qt, sem_t.at[1, 1])
    first = pn.group == 0

    for b in range(nb):
        drain(sr.at[b], sem_s.at[1, b])
        for mi in range(4):
            parts = []
            for ri in range(2):
                part = sr[b, pl.ds(ri * 4 + mi, sr.shape[1] // 8, stride=8), :]
                if mi == 0 and ri == 0:
                    part = part - jnp.where(first, jnp.mean(part, axis=0, keepdims=True), 0.0)
                parts.append(part)
            out = dot(pt[mi].T, jnp.concatenate(parts, axis=1))
            for ri in range(2):
                als[b, pl.ds(ri * 4 + mi, out.shape[0], stride=8), :] = out[:, ri * 128:(ri + 1) * 128]
        pn.each(lambda h, w, lin, g, hf, b=b: (als.at[b, rows_at(lin, 8 * l_own)], ar.at[b, pn.group, :, lanes_at(pn.half)],
                                               sem_a.at[0, b], sem_a.at[1, b]))

    load_k.wait()
    drain(st, sem_m.at[2])
    count = xr.shape[1] * xr.shape[2]
    mean_d = st[...]
    mu = jnp.mean(mean_d, axis=0)
    dev = mean_d - mu[None]
    dev2 = jnp.sum(dev * dev, axis=0)
    m2 = jnp.sum(mean_d, axis=0)
    row_sign = jnp.where(lax.broadcasted_iota(jnp.int32, (1, 8, 1), 1) < 4, -1.0, 1.0)
    ones = jnp.zeros((8, xr.shape[3]), F32)
    st_out[...] = ones
    for b in range(nb):
        var = (m2[2 * b + 1:2 * b + 2] + count * dev2[2 * b:2 * b + 1]) / (count * h_size * w_size)
        scale = lax.rsqrt(var + NORM_EPS)
        st_out[2 * b:2 * b + 1, :] = mu[2 * b:2 * b + 1]
        st_out[2 * b + 1:2 * b + 2, :] = scale
        drain(ar.at[b], sem_a.at[1, b])
        for l in range(l_own):
            a = ar[b, :, l * 8:(l + 1) * 8, :] * scale[None]
            ar[b, :, l * 8:(l + 1) * 8, :] = a
            a = a.reshape(-1, a.shape[2])
            own = dot(a, ker[0, l])
            other = dot(a, ker[1, l]).reshape(-1, 8, a.shape[1])
            other = jnp.concatenate([other[:, 4:], other[:, :4]], axis=1)
            out = own.reshape(-1, 8, a.shape[1]) + row_sign * other
            for hf in range(2):
                bs[b, :, hf, l * 8:(l + 1) * 8, :] = out[:, :, hf * 128:(hf + 1) * 128]
        pn.each(lambda h, w, lin, g, hf, b=b: (bs.at[b, g, hf], br.at[b, rows_at(pn.me, 8 * l_own)], sem_b.at[0, b], sem_b.at[1, b]))

    for b in range(nb):
        drain(br.at[b], sem_b.at[1, b])
        for mi in range(4):
            parts = [br[b, pl.ds(ri * 4 + mi, br.shape[1] // 8, stride=8), :] for ri in range(2)]
            out = dot(qt[mi], jnp.concatenate(parts, axis=1))
            for ri in range(2):
                ys[b, pl.ds(ri * 4 + mi, out.shape[0], stride=8), :] = out[:, ri * 128:(ri + 1) * 128]
        pn.each(lambda h, w, lin, g, hf, b=b: (ys.at[b, rows_at(lin, 8 * tq)], yr.at[b, pn.group, :, lanes_at(pn.half)],
                                               sem_y.at[0, 0, b], sem_y.at[0, 1, b]))
    for b in range(nb):
        drain(yr.at[b], sem_y.at[0, 1, b])
    for b in range(nb):
        drain(tr.at[b], sem_y.at[2, 1, b])
    outs = [(xr, x2_out), (tr, t2_out), (ar, a_out), (yr, y_out), (pt, p_out), (qt, q_out)]
    for i, (src, dst) in enumerate(outs):
        pltpu.make_async_copy(src, dst, sem_y.at[1, i // nb, i % nb]).start()
    for i, (src, dst) in enumerate(outs):
        pltpu.make_async_copy(src, dst, sem_y.at[1, i // nb, i % nb]).wait()
    others = h_size * w_size - 1
    for b in range(nb):
        drain(x.at[b, pl.ds(0, (w_size - 1) * tq)], sem_x.at[0, b])
        drain(tgt.at[b, pl.ds(0, (w_size - 1) * tq)], sem_y.at[2, 0, b])
        drain(sr.at[b, pl.ds(0, others * 8 * tq)], sem_s.at[0, b])
        drain(als.at[b, pl.ds(0, others * 8 * l_own)], sem_a.at[0, b])
        drain(br.at[b, pl.ds(0, others * 8 * l_own)], sem_b.at[0, b])
        drain(ys.at[b, pl.ds(0, others * 8 * tq)], sem_y.at[0, 0, b])
    drain(st.at[pl.ds(0, others)], sem_m.at[1])
    for k, tab in enumerate((pt, qt)):
        drain(tab.at[:, pl.ds(0, tab.shape[1] // h_size * (h_size - 1))], sem_t.at[0, k])


def solution(mesh):
    dp_size = mesh.shape["dp"]
    w_size = mesh.shape["w"]
    h_size = mesh.shape["h"]
    grid_axes = ("h", "w")
    all_axes = ("dp", "h", "w")
    xs_ = h_size // 2

    def swap(pieces, axes):
        return lax.all_to_all(pieces, axes, 0, 0, tiled=True)

    def local_step(field, target, lat_weight, leg_fwd, leg_inv, spec_w, w_in, w_out):
        nb, nc, nt, npl = field.shape
        nlon = npl * w_size
        tq = nt // w_size
        nm = leg_fwd.shape[0] * w_size
        ng = nm // 4
        half = nc // 2
        ndev = h_size * w_size
        nlat = nt * h_size
        nl = leg_fwd.shape[1]
        l_own = nl // ndev
        grid_points = nlat * nlon
        total_points = nb * dp_size * nc * grid_points
        hi, wi = lax.axis_index("h"), lax.axis_index("w")
        fwd_np, inv_np = dft_tables(nlon, nm)
        f_tab, g_tab = jnp.asarray(fwd_np), jnp.asarray(inv_np)

        x = field.transpose(0, 2, 3, 1)
        tgt = target.transpose(0, 2, 3, 1)

        def from_rows(v):
            v = v.reshape(nb, tq, w_size, npl, nc).transpose(2, 0, 1, 3, 4)
            v = swap(v, "w")
            return v.transpose(1, 0, 2, 3, 4).reshape(nb, nt, npl, nc)

        any_spec = pl.BlockSpec(memory_space=pl.ANY)
        vmem_spec = pl.BlockSpec(memory_space=pltpu.VMEM)
        sds = lambda *s: jax.ShapeDtypeStruct(s, F32)
        vm = lambda *s: pltpu.VMEM(s, F32)
        x2, t2, a, back, stv, p_t, q_t = pl.pallas_call(
            functools.partial(forward_kernel, h_size, w_size),
            name="forward",
            out_shape=[sds(nb, tq, nlon, nc), sds(nb, tq, nlon, nc), sds(nb, ng, 8 * l_own, nc), sds(nb, ng, 8 * tq, nc),
                       sds(8, nc), sds(4, nlat, nl), sds(4, nlat, nl)],
            in_specs=[any_spec] * 5 + [vmem_spec],
            out_specs=[any_spec] * 4 + [vmem_spec] + [any_spec] * 2,
            scratch_shapes=[
                vm(nb, tq, nlon, nc), vm(nb, tq, nlon, nc), vm(ng, 2, nb, 8 * tq, half), vm(nb, 8 * nlat, half),
                vm(nb, 8 * nl, half), vm(nb, ng, 8 * l_own, nc), vm(nb, ng, 2, 8 * l_own, half), vm(nb, 8 * nl, half),
                vm(nb, 8 * nlat, half), vm(nb, ng, 8 * tq, nc), vm(8, nc), vm(ndev, 8, nc), vm(4, nlat, nl), vm(4, nlat, nl),
                vm(2, l_own, nc, nc),
                pltpu.SemaphoreType.DMA((2, nb)), pltpu.SemaphoreType.DMA((2, nb)), pltpu.SemaphoreType.DMA((2, nb)),
                pltpu.SemaphoreType.DMA((2, nb)), pltpu.SemaphoreType.DMA((3, 2, nb)), pltpu.SemaphoreType.DMA((3,)),
                pltpu.SemaphoreType.DMA((2, 2)),
            ],
            compiler_params=pltpu.CompilerParams(collective_id=0, has_side_effects=True, vmem_limit_bytes=60 * 1024 * 1024),
        )(x, tgt, leg_fwd.transpose(0, 2, 1), leg_inv.transpose(0, 2, 1), spec_w, f_tab)
        mu, inv_std = stv[0:2 * nb:2], stv[1:2 * nb:2]
        a = a.reshape(nb, ng, l_own, 2, 4, nc).transpose(2, 0, 1, 3, 4, 5)
        back = back.reshape(nb, ng, tq, 8, nc).transpose(0, 2, 1, 3, 4).reshape(nb, tq, ng * 8, nc)
        lane0 = (hi % 2) * half

        def spread(v):
            v = v.reshape(nb, tq, w_size, xs_, 8, 2, half).transpose(3, 5, 2, 0, 1, 4, 6)
            v = v.reshape(ndev, nb, tq, 8, half)
            v = swap(v, grid_axes)
            return v.transpose(1, 0, 2, 3, 4).reshape(nb, nlat, 8, half)

        def gather(v):
            v = v.reshape(nb, ndev, tq, 8, half).transpose(1, 0, 2, 3, 4)
            v = swap(v, grid_axes)
            v = v.reshape(xs_, 2, w_size, nb, tq, 8, half).transpose(3, 4, 2, 0, 5, 1, 6)
            return v.reshape(nb, tq, ng * 8, nc)

        def to_owner(v):
            v = v.reshape(ndev, l_own, nb, 8, half)
            v = swap(v, grid_axes)
            v = v.reshape(xs_, 2, w_size, l_own, nb, 8, half).transpose(3, 4, 2, 0, 5, 1, 6)
            return v.reshape(l_own, nb, ng, 2, 4, nc)

        def from_owner(v):
            v = v.reshape(l_own, nb, w_size, xs_, 8, 2, half).transpose(3, 5, 2, 0, 1, 4, 6)
            v = v.reshape(ndev, l_own, nb, 8, half)
            v = swap(v, grid_axes)
            return v.reshape(nl, nb, 2, 4, half)

        def leg_down(tab_t, v):
            v = v.reshape(nb, nlat, 2, 4, half)
            return mm("mtl,btrmc->lbrmc", tab_t, v)

        def leg_up(tab_t, v):
            return mm("mtl,lbrmc->btrmc", tab_t, v).reshape(nb, nlat, 8, half)

        has0 = jnp.where((hi // 2 == 0) & (wi == 0), jnp.float32(nlon ** 0.5), 0.0)
        me = hi * w_size + wi
        ker = lax.dynamic_slice_in_dim(spec_w, me * l_own, l_own, 1)
        kr, ki = ker[0], ker[1]
        sgn = jnp.asarray(np.array([-1.0, 1.0], np.float32))[:, None, None]
        y = mm("rp,btrc->btpc", g_tab, back)
        y_bf = y.astype(jnp.bfloat16)
        hid = jnp.einsum("btpc,cf->btpf", y_bf, w_in, preferred_element_type=F32)
        act, gelu_pull = jax.vjp(jax.nn.gelu, hid)
        act_bf = act.astype(jnp.bfloat16)
        out = jnp.einsum("btpf,fc->btpc", act_bf, w_out, preferred_element_type=F32)
        resid = x2 + y + out - t2
        q4 = lax.dynamic_slice_in_dim(lat_weight, wi * tq, tq, 0)
        d_out = q4[None, :, None, None] * resid
        loss = lax.psum(jnp.sum(d_out * resid), all_axes) / total_points
        d_out_bf = d_out.astype(jnp.bfloat16)
        g_out = lax.psum(jnp.einsum("btpf,btpc->fc", act_bf, d_out_bf, preferred_element_type=F32), all_axes)
        d_act = jnp.einsum("btpc,fc->btpf", d_out_bf, w_out, preferred_element_type=F32)
        d_hid = gelu_pull(d_act)[0].astype(jnp.bfloat16)
        g_in = lax.psum(jnp.einsum("btpc,btpf->cf", y_bf, d_hid, preferred_element_type=F32), all_axes)
        d_y = d_out + jnp.einsum("btpf,cf->btpc", d_hid, w_in, preferred_element_type=F32)
        d_back = spread(mm("rp,btpc->btrc", g_tab, d_y))
        d_mixed = to_owner(leg_down(q_t, d_back))
        d1 = mm("lbgrmo,lio->lbgrmi", d_mixed, kr)
        d2 = mm("lbgrmo,lio->lbgrmi", d_mixed, ki)
        d_a = d1 - sgn * d2[:, :, :, ::-1]
        rot = -sgn * d_mixed[:, :, :, ::-1]
        gr = mm("lbgrmi,lbgrmo->lio", a, d_mixed)
        gi = mm("lbgrmi,lbgrmo->lio", a, rot)
        grad_spec = lax.psum(jnp.stack([gr, gi]), "dp")
        grad_spec = lax.all_gather(grad_spec, "w", axis=1, tiled=True)
        d_sp = leg_up(p_t, from_owner(d_a))
        s1_h = has0 * jnp.sum(d_sp[:, :, 0], axis=1)
        s1 = lax.dynamic_update_slice_in_dim(jnp.zeros((nb, nc), F32), s1_h, lane0, 1)
        s2 = jnp.sum(d_a * a, axis=(0, 2, 3, 4))
        bstat = lax.psum(jnp.stack([s1, s2]), grid_axes) / grid_points
        d_n = mm("rp,btrc->btpc", f_tab, gather(d_sp))
        row = lambda v: v[:, None, None, :]
        normed = (x2 - row(mu)) * row(inv_std)
        d_x = d_out + row(inv_std) * (d_n - row(bstat[0]) - normed * row(bstat[1]))
        d_field = from_rows(d_x).transpose(0, 3, 1, 2)
        return loss, d_field, grad_spec, g_in, g_out

    grid_spec = P("dp", None, "h", "w")
    table_spec = P("w", None, "h")
    kernel_spec = P(None, "h", None, None)
    return jax.shard_map(local_step, mesh=mesh, in_specs=(grid_spec, grid_spec, P("h"), table_spec, table_spec, P(), P(), P()), out_specs=(P(), grid_spec, kernel_spec, P(), P()), check_vma=False)
```

```python
import functools
import jax
import jax.numpy as jnp
import numpy as np
from jax import lax
from jax.experimental import pallas as pl
from jax.experimental.pallas import tpu as pltpu
from jax.sharding import PartitionSpec as P

NORM_EPS = 1e-5
PRECISE = lax.Precision.HIGHEST
MESH = pl.DeviceIdType.MESH
F32 = jnp.float32
BF16 = jnp.bfloat16
GELU_C = float(np.sqrt(2.0 / np.pi))
GELU_A = 0.044715
NN = (((1,), (0,)), ((), ()))
NT = (((1,), (1,)), ((), ()))
TN = (((0,), (0,)), ((), ()))


def dot(a, b, dims=NN):
    return lax.dot_general(a, b, dims, precision=PRECISE, preferred_element_type=F32)


def bdot(a, b, dims=NN):
    return lax.dot_general(a, b, dims, preferred_element_type=F32)


def dft_tables(lon_count, num_modes):
    modes, lons = np.arange(num_modes), np.arange(lon_count)
    angle = 2.0 * np.pi * ((modes[:, None] * lons[None, :]) % lon_count) / lon_count
    fwd = np.stack([np.cos(angle), -np.sin(angle)], 0) * lon_count ** -0.5
    inv = fwd * np.where(modes == 0, 1.0, 2.0)[None, :, None]

    def rows(table):
        table = table.reshape(2, num_modes // 4, 4, lon_count).transpose(1, 0, 2, 3)
        return table.reshape(2 * num_modes, lon_count).astype(np.float32)

    return rows(fwd), rows(inv)


def drain(ref, sem):
    pltpu.make_async_copy(ref, ref, sem).wait()


def rows_at(i, n):
    return pl.ds(pl.multiple_of(i * n, n), n)


def lanes_at(half):
    return pl.ds(pl.multiple_of(half * 128, 128), 128)


def push(src, dst, sems, device):
    pltpu.make_async_remote_copy(src_ref=src, dst_ref=dst, send_sem=sems.at[0], recv_sem=sems.at[1],
                                 device_id=device, device_id_type=MESH).start()


def keep(src, dst, sems):
    pltpu.make_async_copy(src, dst, sems.at[1]).start()


def swap_parts(v):
    return jnp.concatenate([v[:, 4:], v[:, :4]], axis=1)


def block_kernel(sizes, total_points,
                 x, tgt, leg_p, leg_q, spec_w, lat, w1, w2, f_tab, g_tab, ft_tab, gt_tab,
                 dx_out, gs_out, gin_out, gout_out, loss_out,
                 xr, tr, xs, sr, als, ar, bs, br, ys, yr, dout, dsr, dar, dbr, dyr,
                 st_s, st, st2_s, st2, pt, qt, ptt, qtt, ker,
                 gw, gw_z, gw_zs, gw_h, gw_hs, gw_w, gw_ws, gw_w2, gw_h2, gw_f,
                 ls, ls_z, ls_zs, ls_h, ls_hs, ls_w, gsp, gs_z, gs_sum, gs_w,
                 sem_x, sem_t, sem_s, sem_a, sem_b, sem_y, sem_ds, sem_da, sem_db, sem_dy, sem_o,
                 sem_st, sem_tab, sem_k, sem_gw, sem_ls, sem_gs, sem_fin):
    dp_size, h_size, w_size = sizes
    dp, h, w = lax.axis_index("dp"), lax.axis_index("h"), lax.axis_index("w")
    ndev = h_size * w_size
    me = h * w_size + w
    group_of = lambda h, w: (h // 2) * w_size + w
    group, half = group_of(h, w), h % 2
    nb, nt, npl, nc = x.shape
    tq = nt // w_size
    nlon = npl * w_size
    nlat = nt * h_size
    l_own = als.shape[1] // 8 // ndev
    first = group == 0

    load_k = pltpu.make_async_copy(spec_w.at[:, pl.ds(me * l_own, l_own)], ker, sem_k.at[0])
    load_k.start()

    def peer(k):
        return (h + k // w_size) % h_size, (w + k % w_size) % w_size

    barrier = pltpu.get_barrier_semaphore()

    def meet(k, _):
        h2, w2_ = peer(k)
        pl.semaphore_signal(barrier, inc=1, device_id={"h": h2, "w": w2_}, device_id_type=MESH)
        return 0

    def meet_dp(k, _):
        pl.semaphore_signal(barrier, inc=1, device_id={"dp": (dp + k) % dp_size}, device_id_type=MESH)
        return 0

    lax.fori_loop(1, ndev, meet, 0)
    lax.fori_loop(1, dp_size, meet_dp, 0)
    pl.semaphore_wait(barrier, ndev - 1 + dp_size - 1)

    def plane(refs, sems):
        src, dst = refs(me, group, half)
        keep(src, dst, sems)

        def body(k, _):
            h2, w2_ = peer(k)
            src, dst = refs(h2 * w_size + w2_, group_of(h2, w2_), h2 % 2)
            push(src, dst, sems, {"h": h2, "w": w2_})
            return 0

        lax.fori_loop(1, ndev, body, 0)

    def along(axis, size, index, refs, sems):
        src, dst = refs(index)
        keep(src, dst, sems)

        def body(k, _):
            other = (index + k) % size
            src, dst = refs(other)
            push(src, dst, sems, {axis: other})
            return 0

        lax.fori_loop(1, size, body, 0)

    def send_rows(src, dst, b, sem):
        along("w", w_size, w, lambda o: (src.at[b, rows_at(o, tq)], dst.at[b, :, rows_at(w, npl)]), sem.at[b])

    def send_table(src, dst, sems):
        for c in range(2):
            for w2_ in range(w_size):
                h2 = 2 * w + c
                a, z = src.at[w2_ * 4:(w2_ + 1) * 4], dst.at[:, rows_at(h, nt)]
                mine = jnp.logical_and(h2 == h, w == w2_)

                @pl.when(mine)
                def _():
                    keep(a, z, sems)

                @pl.when(jnp.logical_not(mine))
                def _():
                    push(a, z, sems, {"h": h2, "w": w2_})

    def send_spread(b, dst, sem):
        plane(lambda lin, g, hf: (xs.at[g, hf, b], dst.at[b, rows_at(me, 8 * tq)]), sem.at[b])

    def send_owner(b, dst, sem):
        plane(lambda lin, g, hf: (als.at[b, rows_at(lin, 8 * l_own)], dst.at[b, group, :, lanes_at(half)]), sem.at[b])

    def send_back(b, dst, sem):
        plane(lambda lin, g, hf: (bs.at[b, g, hf], dst.at[b, rows_at(me, 8 * l_own)]), sem.at[b])

    def send_gather(b, dst, sem):
        plane(lambda lin, g, hf: (ys.at[b, rows_at(lin, 8 * tq)], dst.at[b, group, :, lanes_at(half)]), sem.at[b])

    def put_spec(b, t, out):
        out = out.reshape(-1, 8, nc)
        for hf in range(2):
            xs[:, hf, b, rows_at(t, 8), :] = out[:, :, hf * 128:(hf + 1) * 128]

    def leg_down(b, tab, src, fix):
        for mi in range(4):
            parts = []
            for ri in range(2):
                part = src[b, pl.ds(ri * 4 + mi, nlat, stride=8), :]
                if fix and mi == 0 and ri == 0:
                    part = part - jnp.where(first, jnp.mean(part, axis=0, keepdims=True), 0.0)
                parts.append(part)
            out = dot(tab[mi], jnp.concatenate(parts, axis=1))
            for ri in range(2):
                als[b, pl.ds(ri * 4 + mi, out.shape[0], stride=8), :] = out[:, ri * 128:(ri + 1) * 128]

    def leg_up(b, tab, src, fix):
        for mi in range(4):
            parts = [src[b, pl.ds(ri * 4 + mi, src.shape[1] // 8, stride=8), :] for ri in range(2)]
            out = dot(tab[mi], jnp.concatenate(parts, axis=1))
            for ri in range(2):
                part = out[:, ri * 128:(ri + 1) * 128]
                if fix and mi == 0 and ri == 0:
                    part = part - jnp.where(first, jnp.mean(part, axis=0, keepdims=True), 0.0)
                ys[b, pl.ds(ri * 4 + mi, nlat, stride=8), :] = part

    def put_back(b, l, out):
        for hf in range(2):
            bs[b, :, hf, l * 8:(l + 1) * 8, :] = out[:, :, hf * 128:(hf + 1) * 128]

    for b in range(nb):
        send_rows(x, xr, b, sem_x)
    send_table(leg_p, pt, sem_tab.at[0])
    send_table(leg_q, qt, sem_tab.at[1])
    st_s[...] = jnp.zeros_like(st_s)
    st2_s[...] = jnp.zeros_like(st2_s)
    gw[...] = jnp.zeros_like(gw)
    ls[...] = jnp.zeros_like(ls)

    for b in range(nb):
        drain(xr.at[b], sem_x.at[b, 1])

        def spec(t, total, b=b):
            rows = xr[b, t]
            put_spec(b, t, dot(f_tab[...], rows))
            return total + jnp.sum(rows, axis=0, keepdims=True)

        total = lax.fori_loop(0, tq, spec, jnp.zeros((1, nc), F32))
        send_spread(b, sr, sem_s)
        mean = total / (tq * nlon)

        def spread2(t, total, b=b, mean=mean):
            d = xr[b, t] - mean
            return total + jnp.sum(d * d, axis=0, keepdims=True)

        st_s[2 * b:2 * b + 1, :] = mean
        st_s[2 * b + 1:2 * b + 2, :] = lax.fori_loop(0, tq, spread2, jnp.zeros((1, nc), F32))
    plane(lambda lin, g, hf: (st_s, st.at[me]), sem_st.at[0])

    for tab, tabt, k in ((pt, ptt, 0), (qt, qtt, 1)):
        drain(tab, sem_tab.at[k, 1])
        for mi in range(4):
            tabt[mi] = tab[mi].T

    for b in range(nb):
        drain(sr.at[b], sem_s.at[b, 1])
        leg_down(b, ptt, sr, True)
        send_owner(b, ar, sem_a)
    send_rows(tgt, tr, 0, sem_t)

    load_k.wait()
    drain(st, sem_st.at[0, 1])
    stats = st[...]
    mu = jnp.mean(stats, axis=0)
    dev = stats - mu[None]
    dev2 = jnp.sum(dev * dev, axis=0)
    m2 = jnp.sum(stats, axis=0)
    count = tq * nlon
    row_sign = jnp.where(lax.broadcasted_iota(jnp.int32, (1, 8, 1), 1) < 4, -1.0, 1.0)
    scales, means = [], []
    for b in range(nb):
        var = (m2[2 * b + 1:2 * b + 2] + count * dev2[2 * b:2 * b + 1]) / (count * ndev)
        scales.append(lax.rsqrt(var + NORM_EPS))
        means.append(mu[2 * b:2 * b + 1])
    for b in range(nb):
        drain(ar.at[b], sem_a.at[b, 1])
        for l in range(l_own):
            a = ar[b, :, l * 8:(l + 1) * 8, :] * scales[b][None]
            ar[b, :, l * 8:(l + 1) * 8, :] = a
            a = a.reshape(-1, nc)
            own = dot(a, ker[0, l]).reshape(-1, 8, nc)
            other = dot(a, ker[1, l]).reshape(-1, 8, nc)
            put_back(b, l, own + row_sign * swap_parts(other))
        send_back(b, br, sem_b)
    send_rows(tgt, tr, 1, sem_t)

    for b in range(nb):
        drain(br.at[b], sem_b.at[b, 1])
        leg_up(b, qt, br, False)
        send_gather(b, yr, sem_y)
    for b in range(2, nb):
        send_rows(tgt, tr, b, sem_t)

    for b in range(nb):
        drain(yr.at[b], sem_y.at[b, 1])
        drain(tr.at[b], sem_t.at[b, 1])
        drain(sr.at[b, pl.ds(0, (ndev - 1) * 8 * tq)], sem_s.at[b, 0])

        def point(t, _, b=b):
            y = dot(gt_tab[...], yr[b, :, rows_at(t, 8), :].reshape(-1, nc))
            yb = y.astype(BF16)
            hid = bdot(yb, w1[...])
            th = jnp.tanh(GELU_C * (hid + GELU_A * (hid * hid * hid)))
            act = (hid * (0.5 * (1.0 + th))).astype(BF16)
            resid = xr[b, t] + y + bdot(act, w2[...]) - tr[b, t]
            d = lat[w * tq + t] * resid
            ls[...] += jnp.sum((d * resid).reshape(-1, 8, nc), axis=0)
            dout[b, t] = d
            db = d.astype(BF16)
            gw[2 * nc:, :] += bdot(act, db, TN)
            slope = 0.5 * (1.0 + th) + (0.5 * GELU_C) * hid * (1.0 - th * th) * (1.0 + (3.0 * GELU_A) * (hid * hid))
            dh = (bdot(db, w2[...], NT) * slope).astype(BF16)
            gin = bdot(yb, dh, TN)
            gw[:nc, :] += gin[:, :nc]
            gw[nc:2 * nc, :] += gin[:, nc:]
            dy = d + bdot(dh, w1[...], NT)
            put_spec(b, t, dot(g_tab[...], dy))
            return 0

        lax.fori_loop(0, tq, point, 0)
        send_spread(b, dsr, sem_ds)

    n_z, n_h, n_w = gw_zs.shape[0], gw_hs.shape[0], gw_ws.shape[0]
    along("dp", dp_size, dp, lambda o: (gw.at[rows_at(o, n_z)], gw_z.at[dp]), sem_gw.at[0])
    along("dp", dp_size, dp, lambda o: (ls, ls_z.at[dp]), sem_ls.at[0])

    for b in range(nb):
        drain(dsr.at[b], sem_ds.at[b, 1])
        drain(als.at[b, pl.ds(0, (ndev - 1) * 8 * l_own)], sem_a.at[b, 0])
        leg_down(b, qtt, dsr, False)
        send_owner(b, dar, sem_da)

    drain(gw_z, sem_gw.at[0, 1])
    drain(ls_z, sem_ls.at[0, 1])
    gw_zs[...] = jnp.sum(gw_z[...], axis=0)
    ls_zs[...] = jnp.sum(ls_z[...], axis=0)
    along("h", h_size, h, lambda o: (gw_zs.at[rows_at(o, n_h)], gw_h.at[h]), sem_gw.at[1])
    along("h", h_size, h, lambda o: (ls_zs, ls_h.at[h]), sem_ls.at[1])

    for b in range(nb):
        drain(dar.at[b], sem_da.at[b, 1])
        drain(br.at[b, pl.ds(0, (ndev - 1) * 8 * l_own)], sem_b.at[b, 0])
        s2 = jnp.zeros((1, nc), F32)
        for l in range(l_own):
            d = dar[b, :, l * 8:(l + 1) * 8, :].reshape(-1, nc)
            own = dot(d, ker[0, l], NT).reshape(-1, 8, nc)
            other = dot(d, ker[1, l], NT).reshape(-1, 8, nc)
            da = own - row_sign * swap_parts(other)
            put_back(b, l, da)
            s2 = s2 + jnp.sum((da * ar[b, :, l * 8:(l + 1) * 8, :]).reshape(-1, nc), axis=0, keepdims=True)
        send_back(b, dbr, sem_db)
        st2_s[b:b + 1, :] = s2
    plane(lambda lin, g, hf: (st2_s, st2.at[me]), sem_st.at[1])

    for l in range(l_own):
        a = ar[:, :, l * 8:(l + 1) * 8, :].reshape(-1, nc)
        d3 = dar[:, :, l * 8:(l + 1) * 8, :].reshape(-1, 8, nc)
        gsp[2 * l] = dot(a, d3.reshape(-1, nc), TN)
        gsp[2 * l + 1] = dot(a, (-row_sign * swap_parts(d3)).reshape(-1, nc), TN)
    along("dp", dp_size, dp, lambda o: (gsp.at[o], gs_z.at[dp]), sem_gs.at[0])

    drain(gw_h, sem_gw.at[1, 1])
    drain(ls_h, sem_ls.at[1, 1])
    gw_hs[...] = jnp.sum(gw_h[...], axis=0)
    ls_hs[...] = jnp.sum(ls_h[...], axis=0)
    along("w", w_size, w, lambda o: (gw_hs.at[rows_at(o, n_w)], gw_w.at[w]), sem_gw.at[2])
    along("w", w_size, w, lambda o: (ls_hs, ls_w.at[w]), sem_ls.at[2])

    for b in range(nb):
        drain(dbr.at[b], sem_db.at[b, 1])
        drain(ys.at[b, pl.ds(0, (ndev - 1) * 8 * tq)], sem_y.at[b, 0])
        leg_up(b, pt, dbr, True)
        send_gather(b, dyr, sem_dy)

    drain(gs_z, sem_gs.at[0, 1])
    gs_sum[...] = jnp.sum(gs_z[...], axis=0)
    along("w", w_size, w, lambda o: (gs_sum, gs_w.at[w]), sem_gs.at[1])
    drain(gw_w, sem_gw.at[2, 1])
    drain(ls_w, sem_ls.at[2, 1])
    gw_ws[...] = jnp.sum(gw_w[...], axis=0)
    loss_out[...] = jnp.sum(ls_w[...], keepdims=True).reshape(1, 1) / total_points
    along("w", w_size, w, lambda o: (gw_ws, gw_w2.at[rows_at(w, n_w)]), sem_gw.at[3])

    drain(st2, sem_st.at[1, 1])
    proj = jnp.sum(st2[...], axis=0) / (count * ndev)
    for b in range(nb):
        drain(dyr.at[b], sem_dy.at[b, 1])

        def finish(t, _, b=b):
            dn = dot(ft_tab[...], dyr[b, :, rows_at(t, 8), :].reshape(-1, nc))
            normed = (xr[b, t] - means[b]) * scales[b]
            dout[b, t] = dout[b, t] + scales[b] * (dn - normed * proj[b:b + 1])
            return 0

        lax.fori_loop(0, tq, finish, 0)
        along("w", w_size, w, lambda o, b=b: (dout.at[b, :, rows_at(o, npl)], dx_out.at[b, rows_at(w, tq)]), sem_o.at[b])

    drain(gs_w, sem_gs.at[1, 1])
    slot = dp // 2
    part = dp % 2
    for o in range(w_size):
        along("dp", dp_size, dp, lambda k, o=o: (gs_w.at[o], gs_out.at[part, l_own * o + slot]), sem_gs.at[2])
    drain(gw_w2, sem_gw.at[3, 1])
    along("h", h_size, h, lambda o: (gw_w2, gw_h2.at[rows_at(h, n_h)]), sem_gw.at[4])
    drain(gw_h2, sem_gw.at[4, 1])
    along("dp", dp_size, dp, lambda o: (gw_h2, gw_f.at[rows_at(dp, n_z)]), sem_gw.at[5])
    drain(gw_f, sem_gw.at[5, 1])
    fin = [(gw_f.at[:nc], gin_out.at[:, :nc]), (gw_f.at[nc:2 * nc], gin_out.at[:, nc:]), (gw_f.at[2 * nc:], gout_out)]
    fin = [pltpu.make_async_copy(s, d, sem_fin.at[i]) for i, (s, d) in enumerate(fin)]
    for c in fin:
        c.start()

    drain(gs_out, sem_gs.at[2, 1])
    for b in range(nb):
        drain(dx_out.at[b], sem_o.at[b, 1])
    for c in fin:
        c.wait()
    rest = ndev - 1
    for b in range(nb):
        drain(x.at[b, pl.ds(0, (w_size - 1) * tq)], sem_x.at[b, 0])
        drain(tgt.at[b, pl.ds(0, (w_size - 1) * tq)], sem_t.at[b, 0])
        drain(dsr.at[b, pl.ds(0, rest * 8 * tq)], sem_ds.at[b, 0])
        drain(als.at[b, pl.ds(0, rest * 8 * l_own)], sem_da.at[b, 0])
        drain(dbr.at[b, pl.ds(0, rest * 8 * l_own)], sem_db.at[b, 0])
        drain(ys.at[b, pl.ds(0, rest * 8 * tq)], sem_dy.at[b, 0])
        drain(dx_out.at[b, pl.ds(0, (w_size - 1) * tq)], sem_o.at[b, 0])
    drain(st.at[pl.ds(0, rest)], sem_st.at[0, 0])
    drain(st2.at[pl.ds(0, rest)], sem_st.at[1, 0])
    for k, tab in enumerate((pt, qt)):
        @pl.when(h // 2 == w)
        def _():
            drain(tab.at[:, pl.ds(0, nlat - nt)], sem_tab.at[k, 0])

        @pl.when(h // 2 != w)
        def _():
            drain(tab, sem_tab.at[k, 0])
    for i, (ref, loss_ref, n) in enumerate(((gw_z, ls_z, dp_size), (gw_h, ls_h, h_size), (gw_w, ls_w, w_size))):
        drain(ref.at[pl.ds(0, n - 1)], sem_gw.at[i, 0])
        drain(loss_ref.at[pl.ds(0, n - 1)], sem_ls.at[i, 0])
    for i, (ref, n, m) in enumerate(((gw_w2, w_size, n_w), (gw_h2, h_size, n_h), (gw_f, dp_size, n_z))):
        drain(ref.at[pl.ds(0, (n - 1) * m)], sem_gw.at[3 + i, 0])
    drain(gs_z.at[pl.ds(0, dp_size - 1)], sem_gs.at[0, 0])
    drain(gs_w.at[pl.ds(0, w_size - 1)], sem_gs.at[1, 0])
    for i in range(dp_size - 1):
        drain(gs_w, sem_gs.at[2, 0])


def solution(mesh):
    dp_size, w_size, h_size = mesh.shape["dp"], mesh.shape["w"], mesh.shape["h"]

    def local_step(field, target, lat_weight, leg_fwd, leg_inv, spec_w, w_in, w_out):
        nb, nc, nt, npl = field.shape
        nlon = npl * w_size
        tq = nt // w_size
        nm = leg_fwd.shape[0] * w_size
        ng = nm // 4
        half = nc // 2
        ndev = h_size * w_size
        nlat = nt * h_size
        nl = leg_fwd.shape[1]
        lo = nl // ndev
        total_points = nb * dp_size * nc * nlat * nlon
        fwd_np, inv_np = dft_tables(nlon, nm)
        any_spec = pl.BlockSpec(memory_space=pl.ANY)
        vmem_spec = pl.BlockSpec(memory_space=pltpu.VMEM)
        sds = lambda *s: jax.ShapeDtypeStruct(s, F32)
        vm = lambda *s: pltpu.VMEM(s, F32)
        dma = lambda *s: pltpu.SemaphoreType.DMA(s)
        rows = 2 * nc + w_out.shape[0]
        n_z, n_h, n_w = rows // dp_size, rows // dp_size // h_size, rows // dp_size // h_size // w_size
        spread, owner, back, gather = vm(nb, 8 * nlat, half), vm(nb, ng, 8 * lo, nc), vm(nb, 8 * nl, half), vm(nb, ng, 8 * tq, nc)
        grid = vm(nb, tq, nlon, nc)
        d_x, g_spec, g_in, g_out, loss = pl.pallas_call(
            functools.partial(block_kernel, (dp_size, h_size, w_size), total_points),
            name="block",
            out_shape=[sds(nb, nt, npl, nc), sds(2, lo * w_size, nc, nc), sds(nc, 2 * nc), sds(2 * nc, nc), sds(1, 1)],
            in_specs=[any_spec] * 5 + [pl.BlockSpec(memory_space=pltpu.SMEM)] + [vmem_spec] * 6,
            out_specs=[any_spec] * 4 + [vmem_spec],
            scratch_shapes=[
                grid, grid, vm(ng, 2, nb, 8 * tq, half), spread, vm(nb, 8 * nl, half), owner, vm(nb, ng, 2, 8 * lo, half), back,
                vm(nb, 8 * nlat, half), gather, grid, spread, owner, back, gather,
                vm(8, nc), vm(ndev, 8, nc), vm(8, nc), vm(ndev, 8, nc), vm(4, nlat, nl), vm(4, nlat, nl), vm(4, nl, nlat), vm(4, nl, nlat),
                vm(2, lo, nc, nc),
                vm(rows, nc), vm(dp_size, n_z, nc), vm(n_z, nc), vm(h_size, n_h, nc), vm(n_h, nc), vm(w_size, n_w, nc), vm(n_w, nc),
                vm(n_h, nc), vm(n_z, nc), vm(rows, nc),
                vm(8, nc), vm(dp_size, 8, nc), vm(8, nc), vm(h_size, 8, nc), vm(8, nc), vm(w_size, 8, nc),
                vm(2 * lo, nc, nc), vm(dp_size, nc, nc), vm(nc, nc), vm(w_size, nc, nc),
            ] + [dma(nb, 2)] * 11 + [dma(2, 2), dma(2, 2), dma(1), dma(6, 2), dma(3, 2), dma(3, 2), dma(3)],
            compiler_params=pltpu.CompilerParams(collective_id=0, has_side_effects=True, vmem_limit_bytes=62 * 1024 * 1024),
        )(field.transpose(0, 2, 3, 1), target.transpose(0, 2, 3, 1), leg_fwd.transpose(0, 2, 1), leg_inv.transpose(0, 2, 1),
          spec_w, lat_weight, w_in, w_out, jnp.asarray(fwd_np), jnp.asarray(inv_np), jnp.asarray(fwd_np.T.copy()), jnp.asarray(inv_np.T.copy()))
        return loss.reshape(()), d_x.transpose(0, 3, 1, 2), g_spec, g_in, g_out

    grid_spec = P("dp", None, "h", "w")
    table_spec = P("w", None, "h")
    kernel_spec = P(None, "h", None, None)
    return jax.shard_map(local_step, mesh=mesh, in_specs=(grid_spec, grid_spec, P("h"), table_spec, table_spec, P(), P(), P()), out_specs=(P(), grid_spec, kernel_spec, P(), P()), check_vma=False)
```

```python
import functools
import jax
import jax.numpy as jnp
import numpy as np
from jax import lax
from jax.experimental import pallas as pl
from jax.experimental.pallas import tpu as pltpu
from jax.sharding import PartitionSpec as P

NORM_EPS = 1e-5
PRECISE = lax.Precision.HIGHEST
MESH = pl.DeviceIdType.MESH
F32 = jnp.float32
BF16 = jnp.bfloat16
GELU_C = float(np.sqrt(2.0 / np.pi))
GELU_A = 0.044715
NN = (((1,), (0,)), ((), ()))
NT = (((1,), (1,)), ((), ()))
TN = (((0,), (0,)), ((), ()))


def dot(a, b, dims=NN):
    return lax.dot_general(a, b, dims, precision=PRECISE, preferred_element_type=F32)


def bdot(a, b, dims=NN):
    return lax.dot_general(a, b, dims, preferred_element_type=F32)


def dft_tables(lon_count, num_modes):
    modes, lons = np.arange(num_modes), np.arange(lon_count)
    angle = 2.0 * np.pi * ((modes[:, None] * lons[None, :]) % lon_count) / lon_count
    fwd = np.stack([np.cos(angle), -np.sin(angle)], 0) * lon_count ** -0.5
    inv = fwd * np.where(modes == 0, 1.0, 2.0)[None, :, None]

    def rows(table):
        table = table.reshape(2, num_modes // 4, 4, lon_count).transpose(1, 0, 2, 3)
        return table.reshape(2 * num_modes, lon_count).astype(np.float32)

    return rows(fwd), rows(inv)


def drain(ref, sem):
    pltpu.make_async_copy(ref, ref, sem).wait()


def rows_at(i, n):
    return pl.ds(pl.multiple_of(i * n, n), n)


def lanes_at(half):
    return pl.ds(pl.multiple_of(half * 128, 128), 128)


def push(src, dst, sems, device):
    pltpu.make_async_remote_copy(src_ref=src, dst_ref=dst, send_sem=sems.at[0], recv_sem=sems.at[1],
                                 device_id=device, device_id_type=MESH).start()


def keep(src, dst, sems):
    pltpu.make_async_copy(src, dst, sems.at[1]).start()


def swap_parts(v):
    return jnp.concatenate([v[:, 4:], v[:, :4]], axis=1)


def block_kernel(sizes, total_points, stop,
                 x, tgt, leg_p, leg_q, spec_w, lat, w1, w2, f_tab, g_tab, ft_tab, gt_tab,
                 dx_out, gs_out, gin_out, gout_out, loss_out,
                 xr, tr, xs, sr, als, ar, bs, br, ys, yr, dout, dsr, dar, dbr, dyr,
                 st_s, st, st2_s, st2, pt, qt, ptt, qtt, ker,
                 gw, gw_z, gw_zs, gw_h, gw_hs, gw_w, gw_ws, gw_w2, gw_h2, gw_f,
                 ls, ls_z, ls_zs, ls_h, ls_hs, ls_w, gsp, gs_z, gs_sum, gs_w,
                 sem_x, sem_t, sem_s, sem_a, sem_b, sem_y, sem_ds, sem_da, sem_db, sem_dy, sem_o,
                 sem_st, sem_tab, sem_k, sem_gw, sem_ls, sem_gs, sem_gf, sem_fin):
    dp_size, h_size, w_size = sizes
    dp, h, w = lax.axis_index("dp"), lax.axis_index("h"), lax.axis_index("w")
    ndev = h_size * w_size
    me = h * w_size + w
    group_of = lambda h, w: (h // 2) * w_size + w
    group, half = group_of(h, w), h % 2
    nb, nt, npl, nc = x.shape
    tq = nt // w_size
    nlon = npl * w_size
    nlat = nt * h_size
    l_own = als.shape[1] // 8 // ndev
    first = group == 0
    rest = ndev - 1
    unsent = {}

    def peer(k):
        return (h + k // w_size) % h_size, (w + k % w_size) % w_size

    barrier = pltpu.get_barrier_semaphore()

    def meet(k, _):
        h2, w2_ = peer(k)
        pl.semaphore_signal(barrier, inc=1, device_id={"h": h2, "w": w2_}, device_id_type=MESH)
        return 0

    def meet_dp(k, _):
        pl.semaphore_signal(barrier, inc=1, device_id={"dp": (dp + k) % dp_size}, device_id_type=MESH)
        return 0

    lax.fori_loop(1, ndev, meet, 0)
    lax.fori_loop(1, dp_size, meet_dp, 0)
    load_k = pltpu.make_async_copy(spec_w.at[:, pl.ds(me * l_own, l_own)], ker, sem_k.at[0])
    load_k.start()
    for ref in (ar, br, dar, dbr, st_s, st2_s, gw, ls):
        ref[...] = jnp.zeros_like(ref)
    pl.semaphore_wait(barrier, ndev - 1 + dp_size - 1)

    def plane(refs, sems, size, key=None):
        src, dst = refs(me, group, half)
        keep(src, dst, sems)

        def body(k, _):
            h2, w2_ = peer(k)
            src, dst = refs(h2 * w_size + w2_, group_of(h2, w2_), h2 % 2)
            push(src, dst, sems, {"h": h2, "w": w2_})
            return 0

        lax.fori_loop(1, ndev, body, 0)
        unsent.setdefault(key, []).append(lambda: drain(size, sems.at[0]))

    def along(axis, size, index, refs, sems, sent=None):
        src, dst = refs(index)
        keep(src, dst, sems)

        def body(k, _):
            other = (index + k) % size
            src, dst = refs(other)
            push(src, dst, sems, {axis: other})
            return 0

        lax.fori_loop(1, size, body, 0)
        if sent is not None:
            unsent.setdefault(None, []).append(lambda: drain(sent, sems.at[0]))

    def holds(lin, g):
        return (lin + 1) * l_own > 4 * g

    def some(refs, sems, used, count, counts, key):
        src, dst = refs(me, group, half)

        @pl.when(used(me, group))
        def _():
            keep(src, dst, sems)

        def body(k, _):
            h2, w2_ = peer(k)
            lin, g = h2 * w_size + w2_, group_of(h2, w2_)

            @pl.when(used(lin, g))
            def _():
                src, dst = refs(lin, g, h2 % 2)
                push(src, dst, sems, {"h": h2, "w": w2_})
            return 0

        lax.fori_loop(1, ndev, body, 0)
        sent = count - jnp.where(used(me, group), 1, 0)
        unsent.setdefault(key, []).append(lambda: take(piece, sems.at[0], sent, sorted({n - i for n in counts for i in (0, 1)} - {0})))

    def take(one, sem, count, counts):
        for n in counts:
            @pl.when(count == n)
            def _():
                drain(als.at[0, pl.ds(0, n * one)], sem)

    n_groups = ((me + 1) * l_own + 3) // 4
    n_owners = ndev - (4 * group) // l_own
    piece = 8 * l_own
    all_groups = [2 * n for n in range(1, (ndev * l_own + 3) // 4 + 1)]
    all_owners = [ndev - (4 * g) // l_own for g in range(h_size // 2 * w_size)]

    def send_rows(src, dst, b, sem):
        along("w", w_size, w, lambda o: (src.at[b, rows_at(o, tq)], dst.at[b, :, rows_at(w, npl)]), sem.at[b],
              x.at[b, pl.ds(0, (w_size - 1) * tq)])

    def send_table(src, dst, sems):
        for c in range(2):
            for w2_ in range(w_size):
                h2 = 2 * w + c
                a, z = src.at[w2_ * 4:(w2_ + 1) * 4], dst.at[:, rows_at(h, nt)]
                mine = jnp.logical_and(h2 == h, w == w2_)

                @pl.when(mine)
                def _():
                    keep(a, z, sems)

                @pl.when(jnp.logical_not(mine))
                def _():
                    push(a, z, sems, {"h": h2, "w": w2_})

        def sent():
            @pl.when(h // 2 == w)
            def _():
                drain(dst.at[:, pl.ds(0, nlat - nt)], sems.at[0])

            @pl.when(h // 2 != w)
            def _():
                drain(dst, sems.at[0])

        unsent.setdefault(None, []).append(sent)

    def send_spread(b, dst, sem):
        plane(lambda lin, g, hf: (xs.at[g, hf, b], dst.at[b, rows_at(me, 8 * tq)]), sem.at[b], dst.at[b, pl.ds(0, rest * 8 * tq)], ("xs", b))

    def send_owner(b, dst, sem):
        some(lambda lin, g, hf: (als.at[b, rows_at(lin, 8 * l_own)], dst.at[b, group, :, lanes_at(half)]), sem.at[b],
             lambda lin, g: holds(lin, group), n_owners, all_owners, ("als", b))

    def got_owner(b, dst, sem):
        take(piece, sem.at[b, 1], 2 * n_groups, all_groups)

    def send_back(b, dst, sem):
        some(lambda lin, g, hf: (bs.at[b, g, hf], dst.at[b, rows_at(me, 8 * l_own)]), sem.at[b],
             lambda lin, g: holds(me, g), 2 * n_groups, all_groups, ("bs", b))

    def got_back(b, dst, sem):
        take(piece, sem.at[b, 1], n_owners, all_owners)

    def send_gather(b, dst, sem):
        plane(lambda lin, g, hf: (ys.at[b, rows_at(lin, 8 * tq)], dst.at[b, group, :, lanes_at(half)]), sem.at[b],
              ys.at[b, pl.ds(0, rest * 8 * tq)], ("ys", b))

    def settle(*keys):
        for key in keys or list(unsent):
            for wait in unsent.pop(key, []):
                wait()

    def put_spec(b, t, out):
        out = out.reshape(-1, 8, nc)
        for hf in range(2):
            xs[:, hf, b, rows_at(t, 8), :] = out[:, :, hf * 128:(hf + 1) * 128]

    def leg_down(b, tab, src, fix):
        settle(("als", b))
        for mi in range(4):
            parts = []
            for ri in range(2):
                part = src[b, pl.ds(ri * 4 + mi, nlat, stride=8), :]
                if fix and mi == 0 and ri == 0:
                    part = part - jnp.where(first, jnp.mean(part, axis=0, keepdims=True), 0.0)
                parts.append(part)
            out = dot(tab[mi], jnp.concatenate(parts, axis=1))
            for ri in range(2):
                als[b, pl.ds(ri * 4 + mi, out.shape[0], stride=8), :] = out[:, ri * 128:(ri + 1) * 128]

    def leg_up(b, tab, src, fix):
        settle(("ys", b))
        for mi in range(4):
            parts = [src[b, pl.ds(ri * 4 + mi, src.shape[1] // 8, stride=8), :] for ri in range(2)]
            out = dot(tab[mi], jnp.concatenate(parts, axis=1))
            for ri in range(2):
                part = out[:, ri * 128:(ri + 1) * 128]
                if fix and mi == 0 and ri == 0:
                    part = part - jnp.where(first, jnp.mean(part, axis=0, keepdims=True), 0.0)
                ys[b, pl.ds(ri * 4 + mi, nlat, stride=8), :] = part

    def put_back(b, l, out):
        for hf in range(2):
            bs[b, :, hf, l * 8:(l + 1) * 8, :] = out[:, :, hf * 128:(hf + 1) * 128]

    def end(*recvs):
        for r in recvs:
            r()
        settle()

    for b in range(nb):
        send_rows(x, xr, b, sem_x)
    send_table(leg_p, pt, sem_tab.at[0])
    send_table(leg_q, qt, sem_tab.at[1])

    for b in range(nb):
        drain(xr.at[b], sem_x.at[b, 1])

        def spec(t, total, b=b):
            rows = xr[b, t]
            put_spec(b, t, dot(f_tab[...], rows))
            return total + jnp.sum(rows, axis=0, keepdims=True)

        total = lax.fori_loop(0, tq, spec, jnp.zeros((1, nc), F32))
        send_spread(b, sr, sem_s)
        mean = total / (tq * nlon)

        def spread2(t, total, b=b, mean=mean):
            d = xr[b, t] - mean
            return total + jnp.sum(d * d, axis=0, keepdims=True)

        st_s[2 * b:2 * b + 1, :] = mean
        st_s[2 * b + 1:2 * b + 2, :] = lax.fori_loop(0, tq, spread2, jnp.zeros((1, nc), F32))
    plane(lambda lin, g, hf: (st_s, st.at[me]), sem_st.at[0], st.at[pl.ds(0, rest)])

    for tab, tabt, k in ((pt, ptt, 0), (qt, qtt, 1)):
        drain(tab, sem_tab.at[k, 1])
        for mi in range(4):
            tabt[mi] = tab[mi].T
    if stop == 1:
        return end(load_k.wait, lambda: drain(st, sem_st.at[0, 1]), *[lambda b=b: drain(sr.at[b], sem_s.at[b, 1]) for b in range(nb)])

    for b in range(nb):
        drain(sr.at[b], sem_s.at[b, 1])
        leg_down(b, ptt, sr, True)
        send_owner(b, ar, sem_a)
    if stop == 2:
        return end(load_k.wait, lambda: drain(st, sem_st.at[0, 1]), *[lambda b=b: got_owner(b, ar, sem_a) for b in range(nb)])
    send_rows(tgt, tr, 0, sem_t)

    load_k.wait()
    drain(st, sem_st.at[0, 1])
    stats = st[...]
    mu = jnp.mean(stats, axis=0)
    dev = stats - mu[None]
    dev2 = jnp.sum(dev * dev, axis=0)
    m2 = jnp.sum(stats, axis=0)
    count = tq * nlon
    row_sign = jnp.where(lax.broadcasted_iota(jnp.int32, (1, 8, 1), 1) < 4, -1.0, 1.0)
    scales, means = [], []
    for b in range(nb):
        var = (m2[2 * b + 1:2 * b + 2] + count * dev2[2 * b:2 * b + 1]) / (count * ndev)
        scales.append(lax.rsqrt(var + NORM_EPS))
        means.append(mu[2 * b:2 * b + 1])
    for b in range(nb):
        got_owner(b, ar, sem_a)
        for l in range(l_own):
            a = ar[b, :, l * 8:(l + 1) * 8, :] * scales[b][None]
            ar[b, :, l * 8:(l + 1) * 8, :] = a
            a = a.reshape(-1, nc)
            own = dot(a, ker[0, l]).reshape(-1, 8, nc)
            other = dot(a, ker[1, l]).reshape(-1, 8, nc)
            put_back(b, l, own + row_sign * swap_parts(other))
        send_back(b, br, sem_b)
    if stop == 3:
        return end(lambda: drain(tr.at[0], sem_t.at[0, 1]), *[lambda b=b: got_back(b, br, sem_b) for b in range(nb)])
    send_rows(tgt, tr, 1, sem_t)

    for b in range(nb):
        got_back(b, br, sem_b)
        leg_up(b, qt, br, False)
        send_gather(b, yr, sem_y)
    for b in range(2, nb):
        send_rows(tgt, tr, b, sem_t)
    if stop == 4:
        return end(*[lambda b=b: drain(tr.at[b], sem_t.at[b, 1]) for b in range(nb)], *[lambda b=b: drain(yr.at[b], sem_y.at[b, 1]) for b in range(nb)])

    for b in range(nb):
        drain(yr.at[b], sem_y.at[b, 1])
        drain(tr.at[b], sem_t.at[b, 1])
        settle(("xs", b))

        def point(t, _, b=b):
            y = dot(gt_tab[...], yr[b, :, rows_at(t, 8), :].reshape(-1, nc))
            yb = y.astype(BF16)
            hid = bdot(yb, w1[...])
            th = jnp.tanh(GELU_C * (hid + GELU_A * (hid * hid * hid)))
            act = (hid * (0.5 * (1.0 + th))).astype(BF16)
            resid = xr[b, t] + y + bdot(act, w2[...]) - tr[b, t]
            d = lat[w * tq + t] * resid
            ls[...] += jnp.sum((d * resid).reshape(-1, 8, nc), axis=0)
            dout[b, t] = d
            db = d.astype(BF16)
            gw[2 * nc:, :] += bdot(act, db, TN)
            slope = 0.5 * (1.0 + th) + (0.5 * GELU_C) * hid * (1.0 - th * th) * (1.0 + (3.0 * GELU_A) * (hid * hid))
            dh = (bdot(db, w2[...], NT) * slope).astype(BF16)
            gin = bdot(yb, dh, TN)
            gw[:nc, :] += gin[:, :nc]
            gw[nc:2 * nc, :] += gin[:, nc:]
            dy = d + bdot(dh, w1[...], NT)
            put_spec(b, t, dot(g_tab[...], dy))
            return 0

        lax.fori_loop(0, tq, point, 0)
        send_spread(b, dsr, sem_ds)

    n_z, n_h, n_w = gw_zs.shape[0], gw_hs.shape[0], gw_ws.shape[0]
    along("dp", dp_size, dp, lambda o: (gw.at[rows_at(o, n_z)], gw_z.at[dp]), sem_gw.at[0], gw_z.at[pl.ds(0, dp_size - 1)])
    along("dp", dp_size, dp, lambda o: (ls, ls_z.at[dp]), sem_ls.at[0], ls_z.at[pl.ds(0, dp_size - 1)])
    gw1 = [lambda: drain(gw_z, sem_gw.at[0, 1]), lambda: drain(ls_z, sem_ls.at[0, 1])]
    if stop == 5:
        return end(*gw1, *[lambda b=b: drain(dsr.at[b], sem_ds.at[b, 1]) for b in range(nb)])

    for b in range(nb):
        drain(dsr.at[b], sem_ds.at[b, 1])
        leg_down(b, qtt, dsr, False)
        send_owner(b, dar, sem_da)
    if stop == 6:
        return end(*gw1, *[lambda b=b: got_owner(b, dar, sem_da) for b in range(nb)])

    for r in gw1:
        r()
    gw_zs[...] = jnp.sum(gw_z[...], axis=0)
    ls_zs[...] = jnp.sum(ls_z[...], axis=0)
    along("h", h_size, h, lambda o: (gw_zs.at[rows_at(o, n_h)], gw_h.at[h]), sem_gw.at[1], gw_h.at[pl.ds(0, h_size - 1)])
    along("h", h_size, h, lambda o: (ls_zs, ls_h.at[h]), sem_ls.at[1], ls_h.at[pl.ds(0, h_size - 1)])
    gw2 = [lambda: drain(gw_h, sem_gw.at[1, 1]), lambda: drain(ls_h, sem_ls.at[1, 1])]

    for b in range(nb):
        got_owner(b, dar, sem_da)
        settle(("bs", b))
        s2 = jnp.zeros((1, nc), F32)
        for l in range(l_own):
            d = dar[b, :, l * 8:(l + 1) * 8, :].reshape(-1, nc)
            own = dot(d, ker[0, l], NT).reshape(-1, 8, nc)
            other = dot(d, ker[1, l], NT).reshape(-1, 8, nc)
            da = own - row_sign * swap_parts(other)
            put_back(b, l, da)
            s2 = s2 + jnp.sum((da * ar[b, :, l * 8:(l + 1) * 8, :]).reshape(-1, nc), axis=0, keepdims=True)
        send_back(b, dbr, sem_db)
        st2_s[b:b + 1, :] = s2
    plane(lambda lin, g, hf: (st2_s, st2.at[me]), sem_st.at[1], st2.at[pl.ds(0, rest)])
    if stop == 7:
        return end(*gw2, lambda: drain(st2, sem_st.at[1, 1]), *[lambda b=b: got_back(b, dbr, sem_db) for b in range(nb)])

    for l in range(l_own):
        a = ar[:, :, l * 8:(l + 1) * 8, :].reshape(-1, nc)
        d3 = dar[:, :, l * 8:(l + 1) * 8, :].reshape(-1, 8, nc)
        gsp[2 * l] = dot(a, d3.reshape(-1, nc), TN)
        gsp[2 * l + 1] = dot(a, (-row_sign * swap_parts(d3)).reshape(-1, nc), TN)
    along("dp", dp_size, dp, lambda o: (gsp.at[o], gs_z.at[dp]), sem_gs.at[0], gs_z.at[pl.ds(0, dp_size - 1)])

    for r in gw2:
        r()
    gw_hs[...] = jnp.sum(gw_h[...], axis=0)
    ls_hs[...] = jnp.sum(ls_h[...], axis=0)
    along("w", w_size, w, lambda o: (gw_hs.at[rows_at(o, n_w)], gw_w.at[w]), sem_gw.at[2], gw_w.at[pl.ds(0, w_size - 1)])
    along("w", w_size, w, lambda o: (ls_hs, ls_w.at[w]), sem_ls.at[2], ls_w.at[pl.ds(0, w_size - 1)])
    gw3 = [lambda: drain(gw_w, sem_gw.at[2, 1]), lambda: drain(ls_w, sem_ls.at[2, 1])]

    for b in range(nb):
        got_back(b, dbr, sem_db)
        leg_up(b, pt, dbr, True)
        send_gather(b, dyr, sem_dy)
    if stop == 8:
        return end(*gw3, lambda: drain(gs_z, sem_gs.at[0, 1]), lambda: drain(st2, sem_st.at[1, 1]),
                   *[lambda b=b: drain(dyr.at[b], sem_dy.at[b, 1]) for b in range(nb)])

    for r in gw3:
        r()
    gw_ws[...] = jnp.sum(gw_w[...], axis=0)
    loss_out[...] = jnp.sum(ls_w[...], keepdims=True).reshape(1, 1) / total_points
    along("w", w_size, w, lambda o: (gw_ws, gw_w2.at[rows_at(w, n_w)]), sem_gw.at[3], gw_w2.at[pl.ds(0, (w_size - 1) * n_w)])
    drain(gs_z, sem_gs.at[0, 1])
    gs_sum[...] = jnp.sum(gs_z[...], axis=0)
    along("w", w_size, w, lambda o: (gs_sum, gs_w.at[w]), sem_gs.at[1], gs_w.at[pl.ds(0, w_size - 1)])
    drain(gw_w2, sem_gw.at[3, 1])
    along("h", h_size, h, lambda o: (gw_w2, gw_h2.at[rows_at(h, n_h)]), sem_gw.at[4], gw_h2.at[pl.ds(0, (h_size - 1) * n_h)])

    right, left = (dp + 1) % dp_size, (dp + dp_size - 1) % dp_size
    block_at = lambda d, o: gs_out.at[d % 2, l_own * o + d // 2]

    drain(st2, sem_st.at[1, 1])
    proj = jnp.sum(st2[...], axis=0) / (count * ndev)
    for b in range(nb):
        drain(dyr.at[b], sem_dy.at[b, 1])

        def finish(t, _, b=b):
            dn = dot(ft_tab[...], dyr[b, :, rows_at(t, 8), :].reshape(-1, nc))
            normed = (xr[b, t] - means[b]) * scales[b]
            dout[b, t] = dout[b, t] + scales[b] * (dn - normed * proj[b:b + 1])
            return 0

        lax.fori_loop(0, tq, finish, 0)
        along("w", w_size, w, lambda o, b=b: (dout.at[b, :, rows_at(o, npl)], dx_out.at[b, rows_at(w, tq)]), sem_o.at[b],
              dx_out.at[b, pl.ds(0, (w_size - 1) * tq)])
        if b == 0:
            drain(gw_h2, sem_gw.at[4, 1])
            along("dp", dp_size, dp, lambda o: (gw_h2, gw_f.at[rows_at(dp, n_z)]), sem_gw.at[5], gw_f.at[pl.ds(0, (dp_size - 1) * n_z)])
        if b == nb - 2:
            drain(gs_w, sem_gs.at[1, 1])
            for o in range(w_size):
                pltpu.make_async_copy(gs_w.at[o], block_at(dp, o), sem_gs.at[2, 0]).start()
                push(gs_w.at[o], block_at(dp, o), sem_gf.at[0, o], {"dp": right})
                push(gs_w.at[o], block_at(dp, o), sem_gf.at[1, o], {"dp": left})

    for o in range(w_size):
        way = 0 if o < w_size // 2 else 1
        source, target = (left, right) if way == 0 else (right, left)
        drain(gs_w.at[o], sem_gf.at[way, o, 1])
        push(block_at(source, o), block_at(source, o), sem_gf.at[2, o], {"dp": target})
    drain(gw_f, sem_gw.at[5, 1])
    fin = [(gw_f.at[:nc], gin_out.at[:, :nc]), (gw_f.at[nc:2 * nc], gin_out.at[:, nc:]), (gw_f.at[2 * nc:], gout_out)]
    fin = [pltpu.make_async_copy(s, d, sem_fin.at[i]) for i, (s, d) in enumerate(fin)]
    for c in fin:
        c.start()

    for b in range(nb):
        drain(dx_out.at[b], sem_o.at[b, 1])
    for o in range(w_size):
        drain(gs_w.at[o], sem_gf.at[1 if o < w_size // 2 else 0, o, 1])
        drain(gs_w.at[o], sem_gf.at[2, o, 1])
        for i in range(3):
            drain(gs_w.at[o], sem_gf.at[i, o, 0])
    drain(gs_w, sem_gs.at[2, 0])
    for c in fin:
        c.wait()
    settle()


def solution(mesh):
    dp_size, w_size, h_size = mesh.shape["dp"], mesh.shape["w"], mesh.shape["h"]

    def local_step(field, target, lat_weight, leg_fwd, leg_inv, spec_w, w_in, w_out):
        nb, nc, nt, npl = field.shape
        nlon = npl * w_size
        tq = nt // w_size
        nm = leg_fwd.shape[0] * w_size
        ng = nm // 4
        half = nc // 2
        ndev = h_size * w_size
        nlat = nt * h_size
        nl = leg_fwd.shape[1]
        lo = nl // ndev
        total_points = nb * dp_size * nc * nlat * nlon
        fwd_np, inv_np = dft_tables(nlon, nm)
        any_spec = pl.BlockSpec(memory_space=pl.ANY)
        vmem_spec = pl.BlockSpec(memory_space=pltpu.VMEM)
        sds = lambda *s: jax.ShapeDtypeStruct(s, F32)
        vm = lambda *s: pltpu.VMEM(s, F32)
        dma = lambda *s: pltpu.SemaphoreType.DMA(s)
        rows = 2 * nc + w_out.shape[0]
        n_z, n_h, n_w = rows // dp_size, rows // dp_size // h_size, rows // dp_size // h_size // w_size
        spread, owner, back, gather = vm(nb, 8 * nlat, half), vm(nb, ng, 8 * lo, nc), vm(nb, 8 * nl, half), vm(nb, ng, 8 * tq, nc)
        grid = vm(nb, tq, nlon, nc)
        args = (field.transpose(0, 2, 3, 1), target.transpose(0, 2, 3, 1), leg_fwd.transpose(0, 2, 1), leg_inv.transpose(0, 2, 1),
          spec_w, lat_weight, w_in, w_out, jnp.asarray(fwd_np), jnp.asarray(inv_np), jnp.asarray(fwd_np.T.copy()), jnp.asarray(inv_np.T.copy()))
        call = lambda stop: pl.pallas_call(
            functools.partial(block_kernel, (dp_size, h_size, w_size), total_points, stop),
            name="block" if stop is None else "stop%d" % stop,
            out_shape=[sds(nb, nt, npl, nc), sds(2, lo * w_size, nc, nc), sds(nc, 2 * nc), sds(2 * nc, nc), sds(1, 1)],
            in_specs=[any_spec] * 5 + [pl.BlockSpec(memory_space=pltpu.SMEM)] + [vmem_spec] * 6,
            out_specs=[any_spec] * 4 + [vmem_spec],
            scratch_shapes=[
                grid, grid, vm(ng, 2, nb, 8 * tq, half), spread, vm(nb, 8 * nl, half), owner, vm(nb, ng, 2, 8 * lo, half), back,
                vm(nb, 8 * nlat, half), gather, grid, spread, owner, back, gather,
                vm(8, nc), vm(ndev, 8, nc), vm(8, nc), vm(ndev, 8, nc), vm(4, nlat, nl), vm(4, nlat, nl), vm(4, nl, nlat), vm(4, nl, nlat),
                vm(2, lo, nc, nc),
                vm(rows, nc), vm(dp_size, n_z, nc), vm(n_z, nc), vm(h_size, n_h, nc), vm(n_h, nc), vm(w_size, n_w, nc), vm(n_w, nc),
                vm(n_h, nc), vm(n_z, nc), vm(rows, nc),
                vm(8, nc), vm(dp_size, 8, nc), vm(8, nc), vm(h_size, 8, nc), vm(8, nc), vm(w_size, 8, nc),
                vm(2 * lo, nc, nc), vm(dp_size, nc, nc), vm(nc, nc), vm(w_size, nc, nc),
            ] + [dma(nb, 2)] * 11 + [dma(2, 2), dma(2, 2), dma(1), dma(6, 2), dma(3, 2), dma(3, 2), dma(3, w_size, 2), dma(3)],
            compiler_params=pltpu.CompilerParams(collective_id=0 if stop is None else stop, has_side_effects=True, vmem_limit_bytes=62 * 1024 * 1024),
        )(*args)
        d_x, g_spec, g_in, g_out, loss = call(None)
        return loss.reshape(()), d_x.transpose(0, 3, 1, 2), g_spec, g_in, g_out

    grid_spec = P("dp", None, "h", "w")
    table_spec = P("w", None, "h")
    kernel_spec = P(None, "h", None, None)
    return jax.shard_map(local_step, mesh=mesh, in_specs=(grid_spec, grid_spec, P("h"), table_spec, table_spec, P(), P(), P()), out_specs=(P(), grid_spec, kernel_spec, P(), P()), check_vma=False)
```

```python
import functools
import jax
import jax.numpy as jnp
import numpy as np
from jax import lax
from jax.experimental import pallas as pl
from jax.experimental.pallas import tpu as pltpu
from jax.sharding import PartitionSpec as P

NORM_EPS = 1e-5
PRECISE = lax.Precision.HIGHEST
MESH = pl.DeviceIdType.MESH
F32 = jnp.float32
BF16 = jnp.bfloat16
GELU_C = float(np.sqrt(2.0 / np.pi))
GELU_A = 0.044715
NN = (((1,), (0,)), ((), ()))
NT = (((1,), (1,)), ((), ()))
TN = (((0,), (0,)), ((), ()))


def dot(a, b, dims=NN):
    return lax.dot_general(a, b, dims, precision=PRECISE, preferred_element_type=F32)


def bdot(a, b, dims=NN):
    return lax.dot_general(a, b, dims, preferred_element_type=F32)


def dft_tables(lon_count, num_modes):
    modes, lons = np.arange(num_modes), np.arange(lon_count)
    angle = 2.0 * np.pi * ((modes[:, None] * lons[None, :]) % lon_count) / lon_count
    fwd = np.stack([np.cos(angle), -np.sin(angle)], 0) * lon_count ** -0.5
    inv = fwd * np.where(modes == 0, 1.0, 2.0)[None, :, None]

    def rows(table):
        table = table.reshape(2, num_modes // 4, 4, lon_count).transpose(1, 0, 2, 3)
        return table.reshape(2 * num_modes, lon_count).astype(np.float32)

    return rows(fwd), rows(inv)


def drain(ref, sem):
    pltpu.make_async_copy(ref, ref, sem).wait()


def rows_at(i, n):
    return pl.ds(pl.multiple_of(i * n, n), n)


def lanes_at(half):
    return pl.ds(pl.multiple_of(half * 128, 128), 128)


def push(src, dst, sems, device):
    pltpu.make_async_remote_copy(src_ref=src, dst_ref=dst, send_sem=sems.at[0], recv_sem=sems.at[1],
                                 device_id=device, device_id_type=MESH).start()


def keep(src, dst, sems):
    pltpu.make_async_copy(src, dst, sems.at[1]).start()


def swap_parts(v):
    return jnp.concatenate([v[:, 4:], v[:, :4]], axis=1)


def block_kernel(sizes, total_points, stop,
                 x, tgt, leg_p, leg_q, spec_w, lat, w1, w2, f_tab, g_tab, ft_tab, gt_tab,
                 dx_out, gs_out, gin_out, gout_out, loss_out,
                 xr, tr, xs, sr, als, ar, bs, br, ys, yr, dout, dsr, dar, dbr, dyr,
                 st_s, st, st2_s, st2, tab_s, tab, pt, qt, ptt, qtt, ker,
                 gw, gw_z, gw_zs, gw_h, gw_hs, gw_w, gw_ws, gw_w2, gw_h2, gw_f,
                 ls, ls_z, ls_zs, ls_h, ls_hs, ls_w, gsp, gs_z, gs_sum, gs_w,
                 sem_x, sem_t, sem_s, sem_a, sem_b, sem_y, sem_ds, sem_da, sem_db, sem_dy, sem_o,
                 sem_st, sem_tab, sem_k, sem_gw, sem_ls, sem_gs, sem_gf, sem_fin):
    dp_size, h_size, w_size = sizes
    dp, h, w = lax.axis_index("dp"), lax.axis_index("h"), lax.axis_index("w")
    ndev = h_size * w_size
    me = h * w_size + w
    group_of = lambda h, w: (h // 2) * w_size + w
    group, half = group_of(h, w), h % 2
    nb, nt, npl, nc = x.shape
    tq = nt // w_size
    nlon = npl * w_size
    nlat = nt * h_size
    l_own = als.shape[1] // 8 // ndev
    first = group == 0
    rest = ndev - 1
    unsent = {}

    def peer(k):
        return (h + k // w_size) % h_size, (w + k % w_size) % w_size

    barrier = pltpu.get_barrier_semaphore()

    def meet(k, _):
        h2, w2_ = peer(k)
        pl.semaphore_signal(barrier, inc=1, device_id={"h": h2, "w": w2_}, device_id_type=MESH)
        return 0

    def meet_dp(k, _):
        pl.semaphore_signal(barrier, inc=1, device_id={"dp": (dp + k) % dp_size}, device_id_type=MESH)
        return 0

    lax.fori_loop(1, ndev, meet, 0)
    lax.fori_loop(1, dp_size, meet_dp, 0)
    load_k = pltpu.make_async_copy(spec_w.at[:, pl.ds(me * l_own, l_own)], ker, sem_k.at[0])
    load_k.start()
    tab_s[:, :, :leg_p.shape[2]] = leg_p[...]
    tab_s[:, :, leg_p.shape[2]:] = leg_q[...]
    for ref in (ar, br, dar, dbr, st_s, st2_s, gw, ls):
        ref[...] = jnp.zeros_like(ref)
    pl.semaphore_wait(barrier, ndev - 1 + dp_size - 1)

    def plane(refs, sems, size, key=None):
        src, dst = refs(me, group, half)
        keep(src, dst, sems)

        def body(k, _):
            h2, w2_ = peer(k)
            src, dst = refs(h2 * w_size + w2_, group_of(h2, w2_), h2 % 2)
            push(src, dst, sems, {"h": h2, "w": w2_})
            return 0

        lax.fori_loop(1, ndev, body, 0)
        unsent.setdefault(key, []).append(lambda: drain(size, sems.at[0]))

    def along(axis, size, index, refs, sems, sent=None):
        src, dst = refs(index)
        keep(src, dst, sems)

        def body(k, _):
            other = (index + k) % size
            src, dst = refs(other)
            push(src, dst, sems, {axis: other})
            return 0

        lax.fori_loop(1, size, body, 0)
        if sent is not None:
            unsent.setdefault(None, []).append(lambda: drain(sent, sems.at[0]))

    def holds(lin, g):
        return (lin + 1) * l_own > 4 * g

    def some(refs, sems, used, count, counts, key):
        src, dst = refs(me, group, half)

        @pl.when(used(me, group))
        def _():
            keep(src, dst, sems)

        def body(k, _):
            h2, w2_ = peer(k)
            lin, g = h2 * w_size + w2_, group_of(h2, w2_)

            @pl.when(used(lin, g))
            def _():
                src, dst = refs(lin, g, h2 % 2)
                push(src, dst, sems, {"h": h2, "w": w2_})
            return 0

        lax.fori_loop(1, ndev, body, 0)
        sent = count - jnp.where(used(me, group), 1, 0)
        unsent.setdefault(key, []).append(lambda: take(piece, sems.at[0], sent, sorted({n - i for n in counts for i in (0, 1)} - {0})))

    def take(one, sem, count, counts):
        for n in counts:
            @pl.when(count == n)
            def _():
                drain(als.at[0, pl.ds(0, n * one)], sem)

    n_groups = ((me + 1) * l_own + 3) // 4
    n_owners = ndev - (4 * group) // l_own
    piece = 8 * l_own
    all_groups = [2 * n for n in range(1, (ndev * l_own + 3) // 4 + 1)]
    all_owners = [ndev - (4 * g) // l_own for g in range(h_size // 2 * w_size)]

    def send_rows(src, dst, b, sem):
        along("w", w_size, w, lambda o: (src.at[b, rows_at(o, tq)], dst.at[b, :, rows_at(w, npl)]), sem.at[b],
              x.at[b, pl.ds(0, (w_size - 1) * tq)])

    def send_table(src, dst, sems):
        for c in range(2):
            for w2_ in range(w_size):
                h2 = 2 * w + c
                a, z = src.at[w2_ * 4:(w2_ + 1) * 4], dst.at[:, rows_at(h, nt)]
                mine = jnp.logical_and(h2 == h, w == w2_)

                @pl.when(mine)
                def _():
                    keep(a, z, sems)

                @pl.when(jnp.logical_not(mine))
                def _():
                    push(a, z, sems, {"h": h2, "w": w2_})

        def sent():
            @pl.when(h // 2 == w)
            def _():
                drain(dst.at[:, pl.ds(0, nlat - nt)], sems.at[0])

            @pl.when(h // 2 != w)
            def _():
                drain(dst, sems.at[0])

        unsent.setdefault(None, []).append(sent)

    def send_spread(b, dst, sem):
        plane(lambda lin, g, hf: (xs.at[g, hf, b], dst.at[b, rows_at(me, 8 * tq)]), sem.at[b], dst.at[b, pl.ds(0, rest * 8 * tq)], ("xs", b))

    def send_owner(b, dst, sem):
        some(lambda lin, g, hf: (als.at[b, rows_at(lin, 8 * l_own)], dst.at[b, group, :, lanes_at(half)]), sem.at[b],
             lambda lin, g: holds(lin, group), n_owners, all_owners, ("als", b))

    def got_owner(b, dst, sem):
        take(piece, sem.at[b, 1], 2 * n_groups, all_groups)

    def send_back(b, dst, sem):
        some(lambda lin, g, hf: (bs.at[b, g, hf], dst.at[b, rows_at(me, 8 * l_own)]), sem.at[b],
             lambda lin, g: holds(me, g), 2 * n_groups, all_groups, ("bs", b))

    def got_back(b, dst, sem):
        take(piece, sem.at[b, 1], n_owners, all_owners)

    def send_gather(b, dst, sem):
        plane(lambda lin, g, hf: (ys.at[b, rows_at(lin, 8 * tq)], dst.at[b, group, :, lanes_at(half)]), sem.at[b],
              ys.at[b, pl.ds(0, rest * 8 * tq)], ("ys", b))

    def settle(*keys):
        for key in keys or list(unsent):
            for wait in unsent.pop(key, []):
                wait()

    def put_spec(b, t, out):
        out = out.reshape(-1, 8, nc)
        for hf in range(2):
            xs[:, hf, b, rows_at(t, 8), :] = out[:, :, hf * 128:(hf + 1) * 128]

    def leg_down(b, tab, src, fix):
        settle(("als", b))
        for mi in range(4):
            parts = []
            for ri in range(2):
                part = src[b, pl.ds(ri * 4 + mi, nlat, stride=8), :]
                if fix and mi == 0 and ri == 0:
                    part = part - jnp.where(first, jnp.mean(part, axis=0, keepdims=True), 0.0)
                parts.append(part)
            out = dot(tab[mi], jnp.concatenate(parts, axis=1))
            for ri in range(2):
                als[b, pl.ds(ri * 4 + mi, out.shape[0], stride=8), :] = out[:, ri * 128:(ri + 1) * 128]

    def leg_up(b, tab, src, fix):
        settle(("ys", b))
        for mi in range(4):
            parts = [src[b, pl.ds(ri * 4 + mi, src.shape[1] // 8, stride=8), :] for ri in range(2)]
            out = dot(tab[mi], jnp.concatenate(parts, axis=1))
            for ri in range(2):
                part = out[:, ri * 128:(ri + 1) * 128]
                if fix and mi == 0 and ri == 0:
                    part = part - jnp.where(first, jnp.mean(part, axis=0, keepdims=True), 0.0)
                ys[b, pl.ds(ri * 4 + mi, nlat, stride=8), :] = part

    def put_back(b, l, out):
        for hf in range(2):
            bs[b, :, hf, l * 8:(l + 1) * 8, :] = out[:, :, hf * 128:(hf + 1) * 128]

    def end(*recvs):
        for r in recvs:
            r()
        settle()

    for b in range(nb):
        send_rows(x, xr, b, sem_x)
    send_table(tab_s, tab, sem_tab.at[0])

    for b in range(nb):
        drain(xr.at[b], sem_x.at[b, 1])

        def spec(t, total, b=b):
            rows = xr[b, t]
            put_spec(b, t, dot(f_tab[...], rows))
            return total + jnp.sum(rows, axis=0, keepdims=True)

        total = lax.fori_loop(0, tq, spec, jnp.zeros((1, nc), F32))
        send_spread(b, sr, sem_s)
        mean = total / (tq * nlon)

        def spread2(t, total, b=b, mean=mean):
            d = xr[b, t] - mean
            return total + jnp.sum(d * d, axis=0, keepdims=True)

        st_s[2 * b:2 * b + 1, :] = mean
        st_s[2 * b + 1:2 * b + 2, :] = lax.fori_loop(0, tq, spread2, jnp.zeros((1, nc), F32))
    plane(lambda lin, g, hf: (st_s, st.at[me]), sem_st.at[0], st.at[pl.ds(0, rest)])

    drain(tab, sem_tab.at[0, 1])
    for mi in range(4):
        both = tab[mi]
        pt[mi] = both[:, :pt.shape[2]]
        qt[mi] = both[:, pt.shape[2]:]
        ptt[mi] = both[:, :pt.shape[2]].T
        qtt[mi] = both[:, pt.shape[2]:].T
    if stop == 1:
        return end(load_k.wait, lambda: drain(st, sem_st.at[0, 1]), *[lambda b=b: drain(sr.at[b], sem_s.at[b, 1]) for b in range(nb)])

    for b in range(nb):
        drain(sr.at[b], sem_s.at[b, 1])
        leg_down(b, ptt, sr, True)
        send_owner(b, ar, sem_a)
    if stop == 2:
        return end(load_k.wait, lambda: drain(st, sem_st.at[0, 1]), *[lambda b=b: got_owner(b, ar, sem_a) for b in range(nb)])
    send_rows(tgt, tr, 0, sem_t)

    load_k.wait()
    drain(st, sem_st.at[0, 1])
    stats = st[...]
    mu = jnp.mean(stats, axis=0)
    dev = stats - mu[None]
    dev2 = jnp.sum(dev * dev, axis=0)
    m2 = jnp.sum(stats, axis=0)
    count = tq * nlon
    row_sign = jnp.where(lax.broadcasted_iota(jnp.int32, (1, 8, 1), 1) < 4, -1.0, 1.0)
    scales, means = [], []
    for b in range(nb):
        var = (m2[2 * b + 1:2 * b + 2] + count * dev2[2 * b:2 * b + 1]) / (count * ndev)
        scales.append(lax.rsqrt(var + NORM_EPS))
        means.append(mu[2 * b:2 * b + 1])
    for b in range(nb):
        got_owner(b, ar, sem_a)
        for l in range(l_own):
            a = ar[b, :, l * 8:(l + 1) * 8, :] * scales[b][None]
            ar[b, :, l * 8:(l + 1) * 8, :] = a
            a = a.reshape(-1, nc)
            own = dot(a, ker[0, l]).reshape(-1, 8, nc)
            other = dot(a, ker[1, l]).reshape(-1, 8, nc)
            put_back(b, l, own + row_sign * swap_parts(other))
        send_back(b, br, sem_b)
    if stop == 3:
        return end(lambda: drain(tr.at[0], sem_t.at[0, 1]), *[lambda b=b: got_back(b, br, sem_b) for b in range(nb)])
    send_rows(tgt, tr, 1, sem_t)

    for b in range(nb):
        got_back(b, br, sem_b)
        leg_up(b, qt, br, False)
        send_gather(b, yr, sem_y)
    for b in range(2, nb):
        send_rows(tgt, tr, b, sem_t)
    if stop == 4:
        return end(*[lambda b=b: drain(tr.at[b], sem_t.at[b, 1]) for b in range(nb)], *[lambda b=b: drain(yr.at[b], sem_y.at[b, 1]) for b in range(nb)])

    for b in range(nb):
        drain(yr.at[b], sem_y.at[b, 1])
        drain(tr.at[b], sem_t.at[b, 1])
        settle(("xs", b))

        def point(t, _, b=b):
            y = dot(gt_tab[...], yr[b, :, rows_at(t, 8), :].reshape(-1, nc))
            yb = y.astype(BF16)
            hid = bdot(yb, w1[...])
            th = jnp.tanh(GELU_C * (hid + GELU_A * (hid * hid * hid)))
            act = (hid * (0.5 * (1.0 + th))).astype(BF16)
            resid = xr[b, t] + y + bdot(act, w2[...]) - tr[b, t]
            d = lat[w * tq + t] * resid
            ls[...] += jnp.sum((d * resid).reshape(-1, 8, nc), axis=0)
            dout[b, t] = d
            db = d.astype(BF16)
            gw[2 * nc:, :] += bdot(act, db, TN)
            slope = 0.5 * (1.0 + th) + (0.5 * GELU_C) * hid * (1.0 - th * th) * (1.0 + (3.0 * GELU_A) * (hid * hid))
            dh = (bdot(db, w2[...], NT) * slope).astype(BF16)
            gin = bdot(yb, dh, TN)
            gw[:nc, :] += gin[:, :nc]
            gw[nc:2 * nc, :] += gin[:, nc:]
            dy = d + bdot(dh, w1[...], NT)
            put_spec(b, t, dot(g_tab[...], dy))
            return 0

        lax.fori_loop(0, tq, point, 0)
        send_spread(b, dsr, sem_ds)

    n_z, n_h, n_w = gw_zs.shape[0], gw_hs.shape[0], gw_ws.shape[0]
    along("dp", dp_size, dp, lambda o: (gw.at[rows_at(o, n_z)], gw_z.at[dp]), sem_gw.at[0], gw_z.at[pl.ds(0, dp_size - 1)])
    along("dp", dp_size, dp, lambda o: (ls, ls_z.at[dp]), sem_ls.at[0], ls_z.at[pl.ds(0, dp_size - 1)])
    gw1 = [lambda: drain(gw_z, sem_gw.at[0, 1]), lambda: drain(ls_z, sem_ls.at[0, 1])]
    if stop == 5:
        return end(*gw1, *[lambda b=b: drain(dsr.at[b], sem_ds.at[b, 1]) for b in range(nb)])

    for b in range(nb):
        drain(dsr.at[b], sem_ds.at[b, 1])
        leg_down(b, qtt, dsr, False)
        send_owner(b, dar, sem_da)
    if stop == 6:
        return end(*gw1, *[lambda b=b: got_owner(b, dar, sem_da) for b in range(nb)])

    for r in gw1:
        r()
    gw_zs[...] = jnp.sum(gw_z[...], axis=0)
    ls_zs[...] = jnp.sum(ls_z[...], axis=0)
    along("h", h_size, h, lambda o: (gw_zs.at[rows_at(o, n_h)], gw_h.at[h]), sem_gw.at[1], gw_h.at[pl.ds(0, h_size - 1)])
    along("h", h_size, h, lambda o: (ls_zs, ls_h.at[h]), sem_ls.at[1], ls_h.at[pl.ds(0, h_size - 1)])
    gw2 = [lambda: drain(gw_h, sem_gw.at[1, 1]), lambda: drain(ls_h, sem_ls.at[1, 1])]

    for b in range(nb):
        got_owner(b, dar, sem_da)
        settle(("bs", b))
        s2 = jnp.zeros((1, nc), F32)
        for l in range(l_own):
            d = dar[b, :, l * 8:(l + 1) * 8, :].reshape(-1, nc)
            own = dot(d, ker[0, l], NT).reshape(-1, 8, nc)
            other = dot(d, ker[1, l], NT).reshape(-1, 8, nc)
            da = own - row_sign * swap_parts(other)
            put_back(b, l, da)
            s2 = s2 + jnp.sum((da * ar[b, :, l * 8:(l + 1) * 8, :]).reshape(-1, nc), axis=0, keepdims=True)
        send_back(b, dbr, sem_db)
        st2_s[b:b + 1, :] = s2
    plane(lambda lin, g, hf: (st2_s, st2.at[me]), sem_st.at[1], st2.at[pl.ds(0, rest)])
    if stop == 7:
        return end(*gw2, lambda: drain(st2, sem_st.at[1, 1]), *[lambda b=b: got_back(b, dbr, sem_db) for b in range(nb)])

    for l in range(l_own):
        a = ar[:, :, l * 8:(l + 1) * 8, :].reshape(-1, nc)
        d3 = dar[:, :, l * 8:(l + 1) * 8, :].reshape(-1, 8, nc)
        gsp[2 * l] = dot(a, d3.reshape(-1, nc), TN)
        gsp[2 * l + 1] = dot(a, (-row_sign * swap_parts(d3)).reshape(-1, nc), TN)
    along("dp", dp_size, dp, lambda o: (gsp.at[o], gs_z.at[dp]), sem_gs.at[0], gs_z.at[pl.ds(0, dp_size - 1)])

    for r in gw2:
        r()
    gw_hs[...] = jnp.sum(gw_h[...], axis=0)
    ls_hs[...] = jnp.sum(ls_h[...], axis=0)
    along("w", w_size, w, lambda o: (gw_hs.at[rows_at(o, n_w)], gw_w.at[w]), sem_gw.at[2], gw_w.at[pl.ds(0, w_size - 1)])
    along("w", w_size, w, lambda o: (ls_hs, ls_w.at[w]), sem_ls.at[2], ls_w.at[pl.ds(0, w_size - 1)])
    gw3 = [lambda: drain(gw_w, sem_gw.at[2, 1]), lambda: drain(ls_w, sem_ls.at[2, 1])]

    for b in range(nb):
        got_back(b, dbr, sem_db)
        leg_up(b, pt, dbr, True)
        send_gather(b, dyr, sem_dy)
    if stop == 8:
        return end(*gw3, lambda: drain(gs_z, sem_gs.at[0, 1]), lambda: drain(st2, sem_st.at[1, 1]),
                   *[lambda b=b: drain(dyr.at[b], sem_dy.at[b, 1]) for b in range(nb)])

    for r in gw3:
        r()
    gw_ws[...] = jnp.sum(gw_w[...], axis=0)
    loss_out[...] = jnp.sum(ls_w[...], keepdims=True).reshape(1, 1) / total_points
    along("w", w_size, w, lambda o: (gw_ws, gw_w2.at[rows_at(w, n_w)]), sem_gw.at[3], gw_w2.at[pl.ds(0, (w_size - 1) * n_w)])
    drain(gs_z, sem_gs.at[0, 1])
    gs_sum[...] = jnp.sum(gs_z[...], axis=0)
    along("w", w_size, w, lambda o: (gs_sum, gs_w.at[w]), sem_gs.at[1], gs_w.at[pl.ds(0, w_size - 1)])
    drain(gw_w2, sem_gw.at[3, 1])
    along("h", h_size, h, lambda o: (gw_w2, gw_h2.at[rows_at(h, n_h)]), sem_gw.at[4], gw_h2.at[pl.ds(0, (h_size - 1) * n_h)])

    right, left = (dp + 1) % dp_size, (dp + dp_size - 1) % dp_size
    block_at = lambda d, o: gs_out.at[d % 2, l_own * o + d // 2]

    drain(st2, sem_st.at[1, 1])
    proj = jnp.sum(st2[...], axis=0) / (count * ndev)
    for b in range(nb):
        drain(dyr.at[b], sem_dy.at[b, 1])

        def finish(t, _, b=b):
            dn = dot(ft_tab[...], dyr[b, :, rows_at(t, 8), :].reshape(-1, nc))
            normed = (xr[b, t] - means[b]) * scales[b]
            dout[b, t] = dout[b, t] + scales[b] * (dn - normed * proj[b:b + 1])
            return 0

        lax.fori_loop(0, tq, finish, 0)
        along("w", w_size, w, lambda o, b=b: (dout.at[b, :, rows_at(o, npl)], dx_out.at[b, rows_at(w, tq)]), sem_o.at[b],
              dx_out.at[b, pl.ds(0, (w_size - 1) * tq)])
        if b == 0:
            drain(gw_h2, sem_gw.at[4, 1])
            along("dp", dp_size, dp, lambda o: (gw_h2, gw_f.at[rows_at(dp, n_z)]), sem_gw.at[5], gw_f.at[pl.ds(0, (dp_size - 1) * n_z)])
        if b == nb - 2:
            drain(gs_w, sem_gs.at[1, 1])
            for o in range(w_size):
                pltpu.make_async_copy(gs_w.at[o], block_at(dp, o), sem_gs.at[2, 0]).start()
                push(gs_w.at[o], block_at(dp, o), sem_gf.at[0, o], {"dp": right})
                push(gs_w.at[o], block_at(dp, o), sem_gf.at[1, o], {"dp": left})

    for o in range(w_size):
        way = 0 if o < w_size // 2 else 1
        source, target = (left, right) if way == 0 else (right, left)
        drain(gs_w.at[o], sem_gf.at[way, o, 1])
        push(block_at(source, o), block_at(source, o), sem_gf.at[2, o], {"dp": target})
    drain(gw_f, sem_gw.at[5, 1])
    fin = [(gw_f.at[:nc], gin_out.at[:, :nc]), (gw_f.at[nc:2 * nc], gin_out.at[:, nc:]), (gw_f.at[2 * nc:], gout_out)]
    fin = [pltpu.make_async_copy(s, d, sem_fin.at[i]) for i, (s, d) in enumerate(fin)]
    for c in fin:
        c.start()

    for b in range(nb):
        drain(dx_out.at[b], sem_o.at[b, 1])
    for o in range(w_size):
        drain(gs_w.at[o], sem_gf.at[1 if o < w_size // 2 else 0, o, 1])
        drain(gs_w.at[o], sem_gf.at[2, o, 1])
        for i in range(3):
            drain(gs_w.at[o], sem_gf.at[i, o, 0])
    drain(gs_w, sem_gs.at[2, 0])
    for c in fin:
        c.wait()
    settle()


def solution(mesh):
    dp_size, w_size, h_size = mesh.shape["dp"], mesh.shape["w"], mesh.shape["h"]

    def local_step(field, target, lat_weight, leg_fwd, leg_inv, spec_w, w_in, w_out):
        nb, nc, nt, npl = field.shape
        nlon = npl * w_size
        tq = nt // w_size
        nm = leg_fwd.shape[0] * w_size
        ng = nm // 4
        half = nc // 2
        ndev = h_size * w_size
        nlat = nt * h_size
        nl = leg_fwd.shape[1]
        lo = nl // ndev
        total_points = nb * dp_size * nc * nlat * nlon
        fwd_np, inv_np = dft_tables(nlon, nm)
        any_spec = pl.BlockSpec(memory_space=pl.ANY)
        vmem_spec = pl.BlockSpec(memory_space=pltpu.VMEM)
        sds = lambda *s: jax.ShapeDtypeStruct(s, F32)
        vm = lambda *s: pltpu.VMEM(s, F32)
        dma = lambda *s: pltpu.SemaphoreType.DMA(s)
        rows = 2 * nc + w_out.shape[0]
        n_z, n_h, n_w = rows // dp_size, rows // dp_size // h_size, rows // dp_size // h_size // w_size
        spread, owner, back, gather = vm(nb, 8 * nlat, half), vm(nb, ng, 8 * lo, nc), vm(nb, 8 * nl, half), vm(nb, ng, 8 * tq, nc)
        grid = vm(nb, tq, nlon, nc)
        args = (field.transpose(0, 2, 3, 1), target.transpose(0, 2, 3, 1), leg_fwd.transpose(0, 2, 1), leg_inv.transpose(0, 2, 1),
          spec_w, lat_weight, w_in, w_out, jnp.asarray(fwd_np), jnp.asarray(inv_np), jnp.asarray(fwd_np.T.copy()), jnp.asarray(inv_np.T.copy()))
        call = lambda stop: pl.pallas_call(
            functools.partial(block_kernel, (dp_size, h_size, w_size), total_points, stop),
            name="block" if stop is None else "stop%d" % stop,
            out_shape=[sds(nb, nt, npl, nc), sds(2, lo * w_size, nc, nc), sds(nc, 2 * nc), sds(2 * nc, nc), sds(1, 1)],
            in_specs=[any_spec] * 2 + [vmem_spec] * 2 + [any_spec] + [pl.BlockSpec(memory_space=pltpu.SMEM)] + [vmem_spec] * 6,
            out_specs=[any_spec] * 4 + [vmem_spec],
            scratch_shapes=[
                grid, grid, vm(ng, 2, nb, 8 * tq, half), spread, vm(nb, 8 * nl, half), owner, vm(nb, ng, 2, 8 * lo, half), back,
                vm(nb, 8 * nlat, half), gather, grid, spread, owner, back, gather,
                vm(8, nc), vm(ndev, 8, nc), vm(8, nc), vm(ndev, 8, nc), vm(leg_fwd.shape[0], nt, 2 * nl), vm(4, nlat, 2 * nl), vm(4, nlat, nl), vm(4, nlat, nl), vm(4, nl, nlat), vm(4, nl, nlat),
                vm(2, lo, nc, nc),
                vm(rows, nc), vm(dp_size, n_z, nc), vm(n_z, nc), vm(h_size, n_h, nc), vm(n_h, nc), vm(w_size, n_w, nc), vm(n_w, nc),
                vm(n_h, nc), vm(n_z, nc), vm(rows, nc),
                vm(8, nc), vm(dp_size, 8, nc), vm(8, nc), vm(h_size, 8, nc), vm(8, nc), vm(w_size, 8, nc),
                vm(2 * lo, nc, nc), vm(dp_size, nc, nc), vm(nc, nc), vm(w_size, nc, nc),
            ] + [dma(nb, 2)] * 11 + [dma(2, 2), dma(2, 2), dma(1), dma(6, 2), dma(3, 2), dma(3, 2), dma(3, w_size, 2), dma(3)],
            compiler_params=pltpu.CompilerParams(collective_id=0 if stop is None else stop, has_side_effects=True, vmem_limit_bytes=62 * 1024 * 1024),
        )(*args)
        d_x, g_spec, g_in, g_out, loss = call(None)
        return loss.reshape(()), d_x.transpose(0, 3, 1, 2), g_spec, g_in, g_out

    grid_spec = P("dp", None, "h", "w")
    table_spec = P("w", None, "h")
    kernel_spec = P(None, "h", None, None)
    return jax.shard_map(local_step, mesh=mesh, in_specs=(grid_spec, grid_spec, P("h"), table_spec, table_spec, P(), P(), P()), out_specs=(P(), grid_spec, kernel_spec, P(), P()), check_vma=False)
```

```python
import functools
import jax
import jax.numpy as jnp
import numpy as np
from jax import lax
from jax.experimental import pallas as pl
from jax.experimental.pallas import tpu as pltpu
from jax.sharding import PartitionSpec as P

NORM_EPS = 1e-5
PRECISE = lax.Precision.HIGHEST
MESH = pl.DeviceIdType.MESH
F32 = jnp.float32
BF16 = jnp.bfloat16
GELU_C = float(np.sqrt(2.0 / np.pi))
GELU_A = 0.044715
LANES = 128
NN = (((1,), (0,)), ((), ()))
NT = (((1,), (1,)), ((), ()))
TN = (((0,), (0,)), ((), ()))


def dot(a, b, dims=NN):
    return lax.dot_general(a, b, dims, precision=PRECISE, preferred_element_type=F32)


def bdot(a, b, dims=NN):
    return lax.dot_general(a, b, dims, preferred_element_type=F32)


def dft_tables(lon_count, num_modes, h_size):
    modes, lons = np.arange(num_modes), np.arange(lon_count)
    angle = 2.0 * np.pi * ((modes[:, None] * lons[None, :]) % lon_count) / lon_count
    fwd = np.stack([np.cos(angle), -np.sin(angle)], 0) * lon_count ** -0.5
    inv = fwd * np.where(modes == 0, 1.0, 2.0)[None, :, None]

    def rows(table):
        table = table.reshape(2, h_size, num_modes // h_size, lon_count).transpose(1, 0, 2, 3)
        return table.reshape(2 * num_modes, lon_count).astype(np.float32)

    return rows(fwd), rows(inv)


def drain(ref, sem):
    pltpu.make_async_copy(ref, ref, sem).wait()


def rows_at(i, n):
    return pl.ds(pl.multiple_of(i * n, n), n)


def lanes_at(i):
    return pl.ds(pl.multiple_of(i * LANES, LANES), LANES)


def push(src, dst, sems, device):
    pltpu.make_async_remote_copy(src_ref=src, dst_ref=dst, send_sem=sems.at[0], recv_sem=sems.at[1],
                                 device_id=device, device_id_type=MESH).start()


def keep(src, dst, sems):
    pltpu.make_async_copy(src, dst, sems.at[1]).start()


def flip(v):
    return pltpu.roll(v, LANES // 2, 1)


def low(v):
    return lax.broadcasted_iota(jnp.int32, v.shape, 1) < LANES // 2


def weave(a, b):
    return jnp.where(low(a), a, flip(b)), jnp.where(low(a), flip(a), b)


def weave_wide(tiles):
    pairs = [weave(tiles[j], tiles[j + 1]) for j in range(0, len(tiles), 2)]
    return jnp.concatenate([p[0] for p in pairs], axis=1), jnp.concatenate([p[1] for p in pairs], axis=1)


def weave_tiles(a, b):
    out = []
    for j in range(0, a.shape[1], LANES):
        out.extend(weave(a[:, j:j + LANES], b[:, j:j + LANES]))
    return out


def block_kernel(sizes, total_points, stop,
                 x, tgt, leg_p, leg_q, spec_w, lat, w1, w2, f_tab, g_tab, ft_tab, gt_tab,
                 dx_out, gs_out, gin_out, gout_out, loss_out,
                 xh, th, dout, pk, rows, yrow, hy,
                 xs, sr, dsr, ys, yr, dyr, als, ar, dar, bs, br, dbr, asave, dsave,
                 st_s, st_h, st_m, st_w, tab_s, tab, down_p, down_q, up_p, up_q, ker,
                 gw, gw_z, gw_zs, gw_h, gw_hs, gw_w, gw_ws, gw_w2, gw_h2, gw_f,
                 ls, ls_z, ls_zs, ls_h, ls_hs, ls_w, gsp, gs_z, gs_sum, gs_w,
                 sem_in, sem_x, sem_y, sem_d, sem_n, sem_s, sem_ds, sem_u, sem_du, sem_a, sem_da, sem_b, sem_db, sem_o,
                 sem_st, sem_tab, sem_k, sem_gw, sem_ls, sem_gz, sem_gs, sem_gf, sem_fin):
    dp_size, h_size, w_size = sizes
    dp, h, w = lax.axis_index("dp"), lax.axis_index("h"), lax.axis_index("w")
    ndev = h_size * w_size
    me = h * w_size + w
    nb, nt, npl, nc = x.shape
    ntp = nt // 2
    nlon = npl * w_size
    nlat = nt * h_size
    nl = als.shape[1] // 8
    l_own = nl // ndev
    piece = 8 * l_own
    unsent = {}

    def peer(k):
        return (h + k // w_size) % h_size, (w + k % w_size) % w_size

    barrier = pltpu.get_barrier_semaphore()

    def meet(k, _):
        h2, w2_ = peer(k)
        pl.semaphore_signal(barrier, inc=1, device_id={"h": h2, "w": w2_}, device_id_type=MESH)
        return 0

    def meet_dp(k, _):
        pl.semaphore_signal(barrier, inc=1, device_id={"dp": (dp + k) % dp_size}, device_id_type=MESH)
        return 0

    lax.fori_loop(1, ndev, meet, 0)
    lax.fori_loop(1, dp_size, meet_dp, 0)
    loads = [pltpu.make_async_copy(x.at[b], xh.at[b], sem_in.at[b, 0]) for b in range(nb)]
    load_t = [pltpu.make_async_copy(tgt.at[b], th.at[b], sem_in.at[b, 1]) for b in range(nb)]
    load_k = pltpu.make_async_copy(spec_w.at[:, pl.ds(me * l_own, l_own)], ker, sem_k.at[0])
    for c in loads + [load_k] + load_t:
        c.start()
    tab_s[:, :, :nl] = leg_p[...]
    tab_s[:, :, nl:] = leg_q[...]
    for ref in (ar, br, dar, dbr, st_s, gw, ls):
        ref[...] = jnp.zeros_like(ref)

    def settle(*keys):
        for key in keys or list(unsent):
            for wait in unsent.pop(key, []):
                wait()

    def along(axis, size, index, refs, sems, sent, key=None):
        src, dst = refs(index)
        keep(src, dst, sems)

        def body(k, _):
            other = (index + k) % size
            src, dst = refs(other)
            push(src, dst, sems, {axis: other})
            return 0

        lax.fori_loop(1, size, body, 0)
        unsent.setdefault(key, []).append(lambda: drain(sent, sems.at[0]))

    def holds(lin, h2):
        return (lin + 1) * l_own > 8 * h2

    def some(refs, sems, used, count, counts, key):
        src, dst = refs(h, w)
        keep(src, dst, sems)

        def body(k, _):
            h2, w2_ = peer(k)

            @pl.when(used(h2 * w_size + w2_, h2))
            def _():
                src, dst = refs(h2, w2_)
                push(src, dst, sems, {"h": h2, "w": w2_})
            return 0

        lax.fori_loop(1, ndev, body, 0)
        unsent.setdefault(key, []).append(lambda: take(sems.at[0], count - 1, [n - 1 for n in counts if n > 1]))

    def take(sem, count, counts):
        for n in counts:
            @pl.when(count == n)
            def _():
                drain(als.at[0, pl.ds(0, n * piece)], sem)

    n_orders = (((me + 1) * l_own + 7) // 8) * w_size
    n_owners = ndev - (8 * h) // l_own
    all_orders = [w_size * n for n in range(1, h_size + 1)]
    all_owners = [ndev - (8 * g) // l_own for g in range(h_size)]

    def send_home_rows(b, sem):
        along("w", w_size, w, lambda o: (pk.at[b, o], rows.at[b, :, rows_at(w, npl)]), sem.at[b], pk.at[b, pl.ds(0, w_size - 1)], ("pk", b))

    def send_rows_home(b, sem):
        along("w", w_size, w, lambda o: (yrow.at[b, o], hy.at[b, w]), sem.at[b], yrow.at[b, pl.ds(0, w_size - 1)], ("yrow", b))

    def send_orders(b, dst, sem):
        along("h", h_size, h, lambda o: (xs.at[b, o], dst.at[b, rows_at(h, 16 * ntp)]), sem.at[b], xs.at[b, pl.ds(0, h_size - 1)], ("xs", b))

    def send_lats(b, dst, sem):
        along("h", h_size, h, lambda o: (ys.at[b, rows_at(o, 16 * ntp)], dst.at[b, h]), sem.at[b], xs.at[b, pl.ds(0, h_size - 1)], ("ys", b))

    def send_owner(b, dst, sem):
        some(lambda h2, w2_: (als.at[b, rows_at(h2 * w_size + w2_, piece)], dst.at[b, h, :, lanes_at(w)]), sem.at[b],
             lambda lin, h2: holds(lin, h), n_owners, all_owners, ("als", b))

    def got_owner(b, sem):
        take(sem.at[b, 1], n_orders, all_orders)

    def send_back(b, dst, sem):
        some(lambda h2, w2_: (bs.at[b, h2, w2_], dst.at[b, rows_at(me, piece)]), sem.at[b],
             lambda lin, h2: holds(me, h2), n_orders, all_orders, ("bs", b))

    def got_back(b, sem):
        take(sem.at[b, 1], n_owners, all_owners)

    def dft(b, table):
        settle(("xs", b))

        def body(k, _):
            i = 2 * k
            both = jnp.concatenate([rows[b, i], rows[b, i + 1]], axis=1)
            out = dot(table[...], both).reshape(h_size, 16, 2 * LANES)
            xs[b, :, rows_at(i, 16), :] = out[:, :, :LANES]
            xs[b, :, rows_at(i + 1, 16), :] = out[:, :, LANES:]
            return 0

        lax.fori_loop(0, ntp // 2, body, 0)

    def idft(b, table, src):
        settle(("yrow", b))

        def body(k, _):
            i = 2 * k
            both = jnp.concatenate([src[b, :, rows_at(i + j, 16), :].reshape(-1, LANES) for j in range(2)], axis=1)
            out = dot(table[...], both)
            for j in range(2):
                yrow[b, :, i + j] = out[:, j * LANES:(j + 1) * LANES].reshape(w_size, npl, LANES)
            return 0

        lax.fori_loop(0, ntp // 2, body, 0)

    def level(v):
        mean = jnp.mean(v, axis=0, keepdims=True)
        mean = 0.5 * (mean + flip(mean))
        return v - jnp.where(h == 0, mean, 0.0)

    def leg_down(b, table, src, fix):
        settle(("als", b))
        for m in range(8):
            parts = [src[b, pl.ds(ri * 8 + m, ntp * h_size, stride=16), :] for ri in range(2)]
            if fix and m == 0:
                parts[0] = level(parts[0])
            out = dot(table[m], jnp.concatenate(parts, axis=1))
            re0, re1 = out[:nl, :LANES], out[nl:, :LANES]
            im0, im1 = out[:nl, LANES:], out[nl:, LANES:]
            als[b, pl.ds(m, nl, stride=8), :] = jnp.where(low(re0), re0, im1) + flip(jnp.where(low(re0), im0, re1))

    def leg_up(b, table, src, fix):
        settle(("ys", b))
        for m in range(8):
            out = dot(table[m], src[b, pl.ds(m, nl, stride=8), :])
            re, im = weave(out[:nlat // 2], out[nlat // 2:])
            if fix and m == 0:
                re = level(re)
            ys[b, pl.ds(m, ntp * h_size, stride=16), :] = re
            ys[b, pl.ds(8 + m, ntp * h_size, stride=16), :] = im

    def owned(b, l, src):
        tiles = [src[b, :, l * 8:(l + 1) * 8, j * LANES:(j + 1) * LANES].reshape(-1, LANES) for j in range(w_size)]
        return weave_wide(tiles)

    def put_back(b, l, re, im):
        for j, tile in enumerate(weave_tiles(re, im)):
            bs[b, :, j, l * 8:(l + 1) * 8, :] = tile.reshape(h_size, 8, LANES)

    def put_rows(b, i, v0, v1):
        for j, tile in enumerate(weave_tiles(v0, v1)):
            pk[b, j, i] = tile

    def get_rows(b, i):
        return weave_wide([hy[b, j, i] for j in range(w_size)])

    count = nt * npl
    sums = []
    for b in range(nb):
        loads[b].wait()

        def pack(i, total, b=b):
            v0, v1 = xh[b, i], xh[b, i + ntp]
            put_rows(b, i, v0, v1)
            return total + jnp.sum(v0 + v1, axis=0, keepdims=True)

        sums.append(lax.fori_loop(0, ntp, pack, jnp.zeros((1, nc), F32)))
        if b == 0:
            pl.semaphore_wait(barrier, ndev - 1 + dp_size - 1)
        send_home_rows(b, sem_x)
        if b == 0:
            for c in range(2):
                for w2_ in range(w_size):
                    h2 = 2 * w + c
                    src, dst = tab_s.at[8 * c:8 * (c + 1)], tab.at[:, rows_at(h, nt)]
                    mine = jnp.logical_and(h2 == h, w == w2_)

                    @pl.when(mine)
                    def _():
                        keep(src, dst, sem_tab.at[0])

                    @pl.when(jnp.logical_not(mine))
                    def _():
                        push(src, dst, sem_tab.at[0], {"h": h2, "w": w2_})

    def tables_sent():
        @pl.when(h // 2 == w)
        def _():
            drain(tab.at[:, pl.ds(0, nlat - nt)], sem_tab.at[0, 0])

        @pl.when(h // 2 != w)
        def _():
            drain(tab, sem_tab.at[0, 0])

    unsent.setdefault(None, []).append(tables_sent)

    for b in range(nb):
        mean = sums[b] / count

        def spread(t, total, b=b, mean=mean):
            d = xh[b, t] - mean
            return total + jnp.sum(d * d, axis=0, keepdims=True)

        st_s[2 * b:2 * b + 1, :] = mean
        st_s[2 * b + 1:2 * b + 2, :] = lax.fori_loop(0, nt, spread, jnp.zeros((1, nc), F32))
    along("h", h_size, h, lambda o: (st_s, st_h.at[h]), sem_st.at[0], st_h.at[pl.ds(0, h_size - 1)])

    def combine(stats, n):
        mean = jnp.mean(stats, axis=0)
        dev = stats - mean[None]
        dev2 = jnp.sum(dev * dev, axis=0)
        m2 = jnp.sum(stats, axis=0)
        return [(mean[2 * b:2 * b + 1], m2[2 * b + 1:2 * b + 2] + n * dev2[2 * b:2 * b + 1]) for b in range(nb)]

    def stats_w():
        drain(st_h, sem_st.at[0, 1])
        st_m[...] = jnp.zeros_like(st_m)
        for b, (mean, m2) in enumerate(combine(st_h[...], count)):
            st_m[2 * b:2 * b + 1, :] = mean
            st_m[2 * b + 1:2 * b + 2, :] = m2
        along("w", w_size, w, lambda o: (st_m, st_w.at[w]), sem_st.at[1], st_w.at[pl.ds(0, w_size - 1)])

    means, scales = [], []

    def stats_done():
        drain(st_w, sem_st.at[1, 1])
        for mean, m2 in combine(st_w[...], count * h_size):
            means.append(mean)
            scales.append(lax.rsqrt(m2 / (count * ndev) + NORM_EPS))

    def tables_done():
        drain(tab, sem_tab.at[0, 1])
        for m in range(8):
            both = tab[m].reshape(h_size, 2, ntp, 2 * nl)
            t0, t1 = both[:, 0].reshape(-1, 2 * nl), both[:, 1].reshape(-1, 2 * nl)
            for k, (down, up) in enumerate(((down_p, up_p), (down_q, up_q))):
                a, z = t0[:, k * nl:(k + 1) * nl], t1[:, k * nl:(k + 1) * nl]
                up[m, :nlat // 2, :] = a
                up[m, nlat // 2:, :] = z
                down[m, :nl, :] = a.T
                down[m, nl:, :] = z.T

    def fwd_d(b):
        drain(rows.at[b], sem_x.at[b, 1])
        dft(b, f_tab)
        send_orders(b, sr, sem_s)

    def fwd_l(b):
        drain(sr.at[b], sem_s.at[b, 1])
        leg_down(b, down_p, sr, True)
        send_owner(b, ar, sem_a)

    def fwd_o(b):
        got_owner(b, sem_a)
        settle(("bs", b))
        for l in range(l_own):
            re, im = owned(b, l, ar)
            a = jnp.concatenate([re, im], axis=0) * scales[b]
            asave[b, l] = a
            n = a.shape[0] // 2
            own, other = dot(a, ker[0, l]), dot(a, ker[1, l])
            put_back(b, l, own[:n] - other[n:], own[n:] + other[:n])
        send_back(b, br, sem_b)

    def fwd_u(b):
        got_back(b, sem_b)
        leg_up(b, up_q, br, False)
        send_lats(b, yr, sem_u)

    def fwd_i(b):
        drain(yr.at[b], sem_u.at[b, 1])
        idft(b, gt_tab, yr)
        send_rows_home(b, sem_y)

    def pointwise(b):
        drain(hy.at[b], sem_y.at[b, 1])
        load_t[b].wait()
        settle(("pk", b))

        def body(k, _):
            lats = [2 * k, 2 * k + ntp, 2 * k + 1, 2 * k + 1 + ntp]
            y = jnp.concatenate([v for j in range(2) for v in get_rows(b, 2 * k + j)], axis=0)
            yb = y.astype(BF16)
            hid = bdot(yb, w1[...])
            th_ = jnp.tanh(GELU_C * (hid + GELU_A * (hid * hid * hid)))
            act = (hid * (0.5 * (1.0 + th_))).astype(BF16)
            resid = y + bdot(act, w2[...])
            parts = []
            for j, t in enumerate(lats):
                r = resid[j * npl:(j + 1) * npl] + xh[b, t] - th[b, t]
                d = lat[t] * r
                ls[...] += jnp.sum((d * r).reshape(-1, 8, nc), axis=0)
                dout[b, t] = d
                parts.append(d)
            d = jnp.concatenate(parts, axis=0)
            db = d.astype(BF16)
            gw[2 * nc:, :] += bdot(act, db, TN)
            slope = 0.5 * (1.0 + th_) + (0.5 * GELU_C) * hid * (1.0 - th_ * th_) * (1.0 + (3.0 * GELU_A) * (hid * hid))
            dh = (bdot(db, w2[...], NT) * slope).astype(BF16)
            gin = bdot(yb, dh, TN)
            gw[:nc, :] += gin[:, :nc]
            gw[nc:2 * nc, :] += gin[:, nc:]
            dy = d + bdot(dh, w1[...], NT)
            for j in range(2):
                put_rows(b, 2 * k + j, dy[2 * j * npl:(2 * j + 1) * npl], dy[(2 * j + 1) * npl:(2 * j + 2) * npl])
            return 0

        lax.fori_loop(0, ntp // 2, body, 0)
        send_home_rows(b, sem_d)

    def bwd_d(b):
        drain(rows.at[b], sem_d.at[b, 1])
        dft(b, g_tab)
        send_orders(b, dsr, sem_ds)

    def bwd_l(b):
        drain(dsr.at[b], sem_ds.at[b, 1])
        leg_down(b, down_q, dsr, False)
        send_owner(b, dar, sem_da)

    def bwd_o(b):
        got_owner(b, sem_da)
        settle(("bs", b))
        s2 = jnp.zeros((1, nc), F32)
        for l in range(l_own):
            re, im = owned(b, l, dar)
            d = jnp.concatenate([re, im], axis=0)
            dsave[b, l] = d
            n = d.shape[0] // 2
            own, other = dot(d, ker[0, l], NT), dot(d, ker[1, l], NT)
            re, im = own[:n] + other[n:], own[n:] - other[:n]
            put_back(b, l, re, im)
            s2 = s2 + jnp.sum(re * asave[b, l, :n] + im * asave[b, l, n:], axis=0, keepdims=True)
        send_back(b, dbr, sem_db)
        st_s[b:b + 1, :] = s2

    def bwd_u(b):
        got_back(b, sem_db)
        leg_up(b, up_p, dbr, True)
        send_lats(b, dyr, sem_du)

    def bwd_i(b):
        drain(dyr.at[b], sem_du.at[b, 1])
        idft(b, ft_tab, dyr)
        send_rows_home(b, sem_n)

    n_z, n_h, n_w = gw_zs.shape[0], gw_hs.shape[0], gw_ws.shape[0]

    def gw_1():
        along("dp", dp_size, dp, lambda o: (gw.at[rows_at(o, n_z)], gw_z.at[dp]), sem_gw.at[0], gw_z.at[pl.ds(0, dp_size - 1)])
        along("dp", dp_size, dp, lambda o: (ls, ls_z.at[dp]), sem_ls.at[0], ls_z.at[pl.ds(0, dp_size - 1)])

    def gw_2():
        drain(gw_z, sem_gw.at[0, 1])
        drain(ls_z, sem_ls.at[0, 1])
        gw_zs[...] = jnp.sum(gw_z[...], axis=0)
        ls_zs[...] = jnp.sum(ls_z[...], axis=0)
        along("h", h_size, h, lambda o: (gw_zs.at[rows_at(o, n_h)], gw_h.at[h]), sem_gw.at[1], gw_h.at[pl.ds(0, h_size - 1)])
        along("h", h_size, h, lambda o: (ls_zs, ls_h.at[h]), sem_ls.at[1], ls_h.at[pl.ds(0, h_size - 1)])

    def gw_3():
        drain(gw_h, sem_gw.at[1, 1])
        drain(ls_h, sem_ls.at[1, 1])
        gw_hs[...] = jnp.sum(gw_h[...], axis=0)
        ls_hs[...] = jnp.sum(ls_h[...], axis=0)
        along("w", w_size, w, lambda o: (gw_hs.at[rows_at(o, n_w)], gw_w.at[w]), sem_gw.at[2], gw_w.at[pl.ds(0, w_size - 1)])
        along("w", w_size, w, lambda o: (ls_hs, ls_w.at[w]), sem_ls.at[2], ls_w.at[pl.ds(0, w_size - 1)])

    def gw_4():
        drain(gw_w, sem_gw.at[2, 1])
        drain(ls_w, sem_ls.at[2, 1])
        gw_ws[...] = jnp.sum(gw_w[...], axis=0)
        loss_out[...] = jnp.sum(ls_w[...], keepdims=True).reshape(1, 1) / total_points
        along("w", w_size, w, lambda o: (gw_ws, gw_w2.at[rows_at(w, n_w)]), sem_gw.at[3], gw_w2.at[pl.ds(0, (w_size - 1) * n_w)])

    def gw_5():
        drain(gw_w2, sem_gw.at[3, 1])
        along("h", h_size, h, lambda o: (gw_w2, gw_h2.at[rows_at(h, n_h)]), sem_gw.at[4], gw_h2.at[pl.ds(0, (h_size - 1) * n_h)])

    def gw_6():
        drain(gw_h2, sem_gw.at[4, 1])
        along("dp", dp_size, dp, lambda o: (gw_h2, gw_f.at[rows_at(dp, n_z)]), sem_gw.at[5], gw_f.at[pl.ds(0, (dp_size - 1) * n_z)])

    cuts, _, _, n_g, _ = gs_z.shape

    def gs_1():
        for l in range(l_own):
            a = asave[:, l].reshape(-1, nc)
            d = dsave[:, l].reshape(nb, 2, -1, nc)
            gsp[2 * l] = dot(a, d.reshape(-1, nc), TN)
            turned = jnp.concatenate([d[:, 1:], -d[:, :1]], axis=1).reshape(-1, nc)
            gsp[2 * l + 1] = dot(a, turned, TN)
        for q in range(cuts):
            along("dp", dp_size, dp, lambda o, q=q: (gsp.at[o, rows_at(q, n_g)], gs_z.at[q, dp, 0]), sem_gz.at[q],
                  gs_z.at[q, pl.ds(0, dp_size - 1)])

    def gs_2(q):
        drain(gs_z.at[q], sem_gz.at[q, 1])
        gs_sum[q] = jnp.sum(gs_z[q, :, 0], axis=0)
        along("w", w_size, w, lambda o: (gs_sum.at[q], gs_w.at[q, w]), sem_gs.at[q], gs_w.at[q, pl.ds(0, w_size - 1)])

    right, left = (dp + 1) % dp_size, (dp + dp_size - 1) % dp_size
    block_at = lambda d, o, q: gs_out.at[d % 2, l_own * o + d // 2, rows_at(q, n_g)]

    def gs_3(q):
        drain(gs_w.at[q], sem_gs.at[q, 1])
        for o in range(w_size):
            pltpu.make_async_copy(gs_w.at[q, o], block_at(dp, o, q), sem_gf.at[q, 3, o, 0]).start()
            push(gs_w.at[q, o], block_at(dp, o, q), sem_gf.at[q, 0, o], {"dp": right})
            push(gs_w.at[q, o], block_at(dp, o, q), sem_gf.at[q, 1, o], {"dp": left})

    def gs_4(q):
        for o in range(w_size):
            way = 0 if o < w_size // 2 else 1
            source, target = (left, right) if way == 0 else (right, left)
            drain(gs_w.at[q, o], sem_gf.at[q, way, o, 1])
            push(block_at(source, o, q), block_at(source, o, q), sem_gf.at[q, 2, o], {"dp": target})

    def gs_5(q):
        for o in range(w_size):
            drain(gs_w.at[q, o], sem_gf.at[q, 1 if o < w_size // 2 else 0, o, 1])
            drain(gs_w.at[q, o], sem_gf.at[q, 2, o, 1])
            for i in range(4):
                drain(gs_w.at[q, o], sem_gf.at[q, i, o, 0])

    def proj_h():
        st_s[nb:, :] = jnp.zeros_like(st_s[nb:, :])
        along("h", h_size, h, lambda o: (st_s, st_h.at[h]), sem_st.at[2], st_h.at[pl.ds(0, h_size - 1)])

    def proj_w():
        drain(st_h, sem_st.at[2, 1])
        st_m[...] = jnp.sum(st_h[...], axis=0)
        along("w", w_size, w, lambda o: (st_m, st_w.at[w]), sem_st.at[3], st_w.at[pl.ds(0, w_size - 1)])

    proj = []

    def proj_done():
        drain(st_w, sem_st.at[3, 1])
        proj.append(jnp.sum(st_w[...], axis=0) / (count * ndev))

    def finish(b):
        drain(hy.at[b], sem_n.at[b, 1])

        def body(i, _):
            for t, dn in zip((i, i + ntp), get_rows(b, i)):
                normed = (xh[b, t] - means[b]) * scales[b]
                dout[b, t] = dout[b, t] + scales[b] * (dn - normed * proj[0][b:b + 1])
            return 0

        lax.fori_loop(0, ntp, body, 0)
        pltpu.make_async_copy(dout.at[b], dx_out.at[b], sem_o.at[b]).start()

    assert nb == 3
    fwd_d(0)
    stats_w()
    tables_done()
    fwd_d(1)
    fwd_l(0)
    load_k.wait()
    stats_done()
    fwd_d(2)
    fwd_l(1)
    fwd_o(0)
    fwd_l(2)
    fwd_o(1)
    fwd_u(0)
    fwd_o(2)
    fwd_u(1)
    fwd_i(0)
    fwd_u(2)
    fwd_i(1)
    fwd_i(2)
    settle(None)
    pointwise(0)
    pointwise(1)
    pointwise(2)
    gw_1()
    bwd_d(0)
    bwd_d(1)
    bwd_l(0)
    gw_2()
    bwd_d(2)
    bwd_l(1)
    bwd_o(0)
    gw_3()
    bwd_l(2)
    bwd_o(1)
    gw_4()
    bwd_u(0)
    bwd_o(2)
    gs_1()
    proj_h()
    gw_5()
    bwd_u(1)
    bwd_i(0)
    gs_2(0)
    bwd_u(2)
    bwd_i(1)
    gs_2(1)
    gw_6()
    proj_w()
    bwd_i(2)
    gs_3(0)
    gs_3(1)
    proj_done()
    finish(0)
    gs_4(0)
    finish(1)
    gs_4(1)
    drain(gw_f, sem_gw.at[5, 1])
    fin = [(gw_f.at[:nc], gin_out.at[:, :nc]), (gw_f.at[nc:2 * nc], gin_out.at[:, nc:]), (gw_f.at[2 * nc:], gout_out)]
    fin = [pltpu.make_async_copy(s, d, sem_fin.at[i]) for i, (s, d) in enumerate(fin)]
    for c in fin:
        c.start()
    finish(2)
    for q in range(cuts):
        gs_5(q)
    for b in range(nb):
        drain(dx_out.at[b], sem_o.at[b])
    for c in fin:
        c.wait()
    settle()


def solution(mesh):
    dp_size, w_size, h_size = mesh.shape["dp"], mesh.shape["w"], mesh.shape["h"]

    def local_step(field, target, lat_weight, leg_fwd, leg_inv, spec_w, w_in, w_out):
        nb, nc, nt, npl = field.shape
        nlon = npl * w_size
        ntp = nt // 2
        nm = leg_fwd.shape[0] * w_size
        ndev = h_size * w_size
        nlat = nt * h_size
        nl = leg_fwd.shape[1]
        lo = nl // ndev
        assert nm == 8 * h_size and nc == w_size * LANES // 2 and h_size == 2 * w_size and 2 * lo == dp_size and 2 * nl == LANES
        total_points = nb * dp_size * nc * nlat * nlon
        fwd_np, inv_np = dft_tables(nlon, nm, h_size)
        any_spec = pl.BlockSpec(memory_space=pl.ANY)
        vmem_spec = pl.BlockSpec(memory_space=pltpu.VMEM)
        sds = lambda *s: jax.ShapeDtypeStruct(s, F32)
        vm = lambda *s: pltpu.VMEM(s, F32)
        dma = lambda *s: pltpu.SemaphoreType.DMA(s)
        n_rows = 2 * nc + w_out.shape[0]
        n_z, n_h, n_w = n_rows // dp_size, n_rows // dp_size // h_size, n_rows // dp_size // h_size // w_size
        home = vm(nb, nt, npl, nc)
        woven = vm(nb, w_size, ntp, npl, LANES)
        order = vm(nb, 16 * nlat // 2, LANES)
        degree = vm(nb, 8 * nl, LANES)
        owner = vm(nb, h_size, 8 * lo, w_size * LANES)
        saved = vm(nb, lo, 2 * nm, nc)
        cuts = 2
        args = (field.transpose(0, 2, 3, 1), target.transpose(0, 2, 3, 1), leg_fwd.transpose(0, 2, 1), leg_inv.transpose(0, 2, 1),
                spec_w, lat_weight, w_in, w_out, jnp.asarray(fwd_np), jnp.asarray(inv_np), jnp.asarray(fwd_np.T.copy()), jnp.asarray(inv_np.T.copy()))
        call = lambda stop: pl.pallas_call(
            functools.partial(block_kernel, (dp_size, h_size, w_size), total_points, stop),
            name="block" if stop is None else "stop%d" % stop,
            out_shape=[sds(nb, nt, npl, nc), sds(2, lo * w_size, nc, nc), sds(nc, 2 * nc), sds(2 * nc, nc), sds(1, 1)],
            in_specs=[any_spec] * 2 + [vmem_spec] * 2 + [any_spec] + [pl.BlockSpec(memory_space=pltpu.SMEM)] + [vmem_spec] * 6,
            out_specs=[any_spec] * 4 + [vmem_spec],
            scratch_shapes=[
                home, home, home, woven, vm(nb, ntp, nlon, LANES), woven, woven,
                vm(nb, h_size, 16 * ntp, LANES), order, order, order, vm(nb, h_size, 16 * ntp, LANES), vm(nb, h_size, 16 * ntp, LANES),
                degree, owner, owner, vm(nb, h_size, w_size, 8 * lo, LANES), degree, degree, saved, saved,
                vm(8, nc), vm(h_size, 8, nc), vm(8, nc), vm(w_size, 8, nc),
                vm(leg_fwd.shape[0], nt, 2 * nl), vm(8, nlat, 2 * nl),
                vm(8, 2 * nl, nlat // 2), vm(8, 2 * nl, nlat // 2), vm(8, nlat, nl), vm(8, nlat, nl),
                vm(2, lo, nc, nc),
                vm(n_rows, nc), vm(dp_size, n_z, nc), vm(n_z, nc), vm(h_size, n_h, nc), vm(n_h, nc), vm(w_size, n_w, nc), vm(n_w, nc),
                vm(n_h, nc), vm(n_z, nc), vm(n_rows, nc),
                vm(8, nc), vm(dp_size, 8, nc), vm(8, nc), vm(h_size, 8, nc), vm(8, nc), vm(w_size, 8, nc),
                vm(2 * lo, nc, nc), vm(cuts, dp_size, 1, nc // cuts, nc), vm(cuts, nc // cuts, nc), vm(cuts, w_size, nc // cuts, nc),
            ] + [dma(nb, 2)] * 13 + [dma(nb), dma(4, 2), dma(1, 2), dma(1), dma(6, 2), dma(3, 2), dma(cuts, 2), dma(cuts, 2), dma(cuts, 4, w_size, 2), dma(3)],
            compiler_params=pltpu.CompilerParams(collective_id=0 if stop is None else stop, has_side_effects=True, vmem_limit_bytes=62 * 1024 * 1024),
        )(*args)
        d_x, g_spec, g_in, g_out, loss = call(None)
        return loss.reshape(()), d_x.transpose(0, 3, 1, 2), g_spec, g_in, g_out

    grid_spec = P("dp", None, "h", "w")
    table_spec = P("w", None, "h")
    kernel_spec = P(None, "h", None, None)
    return jax.shard_map(local_step, mesh=mesh, in_specs=(grid_spec, grid_spec, P("h"), table_spec, table_spec, P(), P(), P()), out_specs=(P(), grid_spec, kernel_spec, P(), P()), check_vma=False)
```

```python
import functools
import jax
import jax.numpy as jnp
import numpy as np
from jax import lax
from jax.experimental import pallas as pl
from jax.experimental.pallas import tpu as pltpu
from jax.sharding import PartitionSpec as P

NORM_EPS = 1e-5
PRECISE = lax.Precision.HIGHEST
MESH = pl.DeviceIdType.MESH
F32 = jnp.float32
BF16 = jnp.bfloat16
GELU_C = float(np.sqrt(2.0 / np.pi))
GELU_A = 0.044715
LANES = 128
NN = (((1,), (0,)), ((), ()))
NT = (((1,), (1,)), ((), ()))
TN = (((0,), (0,)), ((), ()))


def dot(a, b, dims=NN):
    return lax.dot_general(a, b, dims, precision=PRECISE, preferred_element_type=F32)


def bdot(a, b, dims=NN):
    return lax.dot_general(a, b, dims, preferred_element_type=F32)


def dft_tables(lon_count, num_modes, h_size):
    modes, lons = np.arange(num_modes), np.arange(lon_count)
    angle = 2.0 * np.pi * ((modes[:, None] * lons[None, :]) % lon_count) / lon_count
    fwd = np.stack([np.cos(angle), -np.sin(angle)], 0) * lon_count ** -0.5
    inv = fwd * np.where(modes == 0, 1.0, 2.0)[None, :, None]

    def rows(table):
        table = table.reshape(2, h_size, num_modes // h_size, lon_count).transpose(1, 0, 2, 3)
        return table.reshape(2 * num_modes, lon_count).astype(np.float32)

    return rows(fwd), rows(inv)


def drain(ref, sem):
    pltpu.make_async_copy(ref, ref, sem).wait()


def rows_at(i, n):
    return pl.ds(pl.multiple_of(i * n, n), n)


def lanes_at(i):
    return pl.ds(pl.multiple_of(i * LANES, LANES), LANES)


def push(src, dst, sems, device):
    pltpu.make_async_remote_copy(src_ref=src, dst_ref=dst, send_sem=sems.at[0], recv_sem=sems.at[1],
                                 device_id=device, device_id_type=MESH).start()


def keep(src, dst, sems):
    pltpu.make_async_copy(src, dst, sems.at[1]).start()


def flip(v):
    return pltpu.roll(v, LANES // 2, 1)


def low(v):
    return lax.broadcasted_iota(jnp.int32, v.shape, 1) < LANES // 2


def weave(a, b):
    return jnp.where(low(a), a, flip(b)), jnp.where(low(a), flip(a), b)


def weave_wide(tiles):
    pairs = [weave(tiles[j], tiles[j + 1]) for j in range(0, len(tiles), 2)]
    return jnp.concatenate([p[0] for p in pairs], axis=1), jnp.concatenate([p[1] for p in pairs], axis=1)


def weave_tiles(a, b):
    out = []
    for j in range(0, a.shape[1], LANES):
        out.extend(weave(a[:, j:j + LANES], b[:, j:j + LANES]))
    return out


PARTS = 2
ORDER = " ".join((
    'go', 'sX21', 'tb2', 'st2', 'sX20', 'sX00', 'fd21', 'tb3', 'sX01', 'fd20',
    'fd00', 'fl2', 'sX11', 'fd01', 'fo2', 'fl0', 'sX10', 'fu2', 'fo0', 'fi20',
    'sY20', 'fd11', 'fi21', 'sY21', 'fd10', 'pw20', 'fu0', 'sD20', 'fl1', 'fi00',
    'sY00', 'fo1', 'fi01', 'sY01', 'fu1', 'pw21', 'sD21', 'fi10', 'sY10', 'pw01',
    'fi11', 'pw00', 'sY11', 'sD00', 'sD01', 'bd21', 'pw10', 'pw11', 'gw1', 'sD11',
    'sD10', 'bd20', 'bd00', 'bl2', 'bd01', 'gw2', 'bd11', 'bl0', 'bd10', 'gw3',
    'bo2', 'gw4', 'bl1', 'gw5', 'bu2', 'bo0', 'bo1', 'bi20', 'sN20', 'gw6',
    'gs1', 'gs20', 'bi21', 'bu1', 'pj1', 'gs21', 'gs30', 'bi11', 'sN11', 'pj2',
    'end', 'sN21', 'bu0', 'bi10', 'bi00', 'gs31', 'bi01', 'sN00', 'sN01', 'fn20',
    'gs40', 'fn21', 'sN10', 'gs41', 'fn11', 'fn01', 'fn00', 'fn10', 'gs50', 'gs51',
))


def block_kernel(sizes, total_points,
                 x, tgt, leg_p, leg_q, spec_w, lat, w1, w2, f_tab, g_tab, ft_tab, gt_tab,
                 dx_out, gs_out, gin_out, gout_out, loss_out,
                 xh, th, dout, pk, rows, yrow, hy,
                 xs, sr, dsr, ys, yr, dyr, als, ar, dar, bs, br, dbr, asave, dsave, aall, dall,
                 st_s, st_h, st_m, st_w, tab_s, tab_w, tab, down_p, down_q, up_p, up_q, ker,
                 gw, gw_z, gw_zs, gw_h, gw_hs, gw_w, gw_ws, gw_w2, gw_h2, gw_f,
                 ls, ls_z, ls_zs, ls_h, ls_hs, ls_w, gs_sum, gs_w,
                 sem_x, sem_y, sem_d, sem_n, sem_s, sem_ds, sem_u, sem_du, sem_a, sem_da, sem_b, sem_db, sem_az, sem_dz,
                 sem_in, sem_o, sem_st, sem_tab, sem_k, sem_gw, sem_ls, sem_gs, sem_gf, sem_fin):
    dp_size, h_size, w_size = sizes
    dp, h, w = lax.axis_index("dp"), lax.axis_index("h"), lax.axis_index("w")
    ndev = h_size * w_size
    me = h * w_size + w
    nb, nt, npl, nc = x.shape
    ntp = nt // 2
    part = ntp // PARTS
    nlon = npl * w_size
    nlat = nt * h_size
    nl = als.shape[1] // 8
    l_own = nl // ndev
    piece = 8 * l_own
    unsent, coming = {}, {}

    def got(key):
        coming.pop(key)()

    def peer(k):
        return (h + k // w_size) % h_size, (w + k % w_size) % w_size

    barrier = pltpu.get_barrier_semaphore()

    def meet(k, _):
        h2, w2_ = peer(k)
        pl.semaphore_signal(barrier, inc=1, device_id={"h": h2, "w": w2_}, device_id_type=MESH)
        return 0

    def meet_dp(k, _):
        pl.semaphore_signal(barrier, inc=1, device_id={"dp": (dp + k) % dp_size}, device_id_type=MESH)
        return 0

    lax.fori_loop(1, ndev, meet, 0)
    lax.fori_loop(1, dp_size, meet_dp, 0)
    loads = [pltpu.make_async_copy(x.at[b], xh.at[b], sem_in.at[b, 0]) for b in range(nb)]
    load_t = [pltpu.make_async_copy(tgt.at[b], th.at[b], sem_in.at[b, 1]) for b in range(nb)]
    load_k = pltpu.make_async_copy(spec_w.at[:, pl.ds(me * l_own, l_own)], ker, sem_k.at[0])
    for c in loads + [load_k] + load_t:
        c.start()
    coming["k"] = load_k.wait
    coming.update({("t", b): load_t[b].wait for b in range(nb)})
    tab_s[:, :, :nl] = leg_p[...]
    tab_s[:, :, nl:] = leg_q[...]
    for ref in (ar, br, dar, dbr, st_s, gw, ls):
        ref[...] = jnp.zeros_like(ref)

    def settle(*keys):
        for key in keys or list(unsent):
            for wait in unsent.pop(key, []):
                wait()

    def along(axis, refs, sems, sent, key=None):
        size, index = {"dp": (dp_size, dp), "h": (h_size, h), "w": (w_size, w)}[axis]
        src, dst = refs(index)
        keep(src, dst, sems)

        def body(k, _):
            other = (index + k) % size
            src, dst = refs(other)
            push(src, dst, sems, {axis: other})
            return 0

        lax.fori_loop(1, size, body, 0)
        unsent.setdefault(key, []).append(lambda: drain(sent, sems.at[0]))

    def holds(lin, h2):
        return (lin + 1) * l_own > 8 * h2

    def some(refs, sems, used, count, counts, key):
        src, dst = refs(h, w)
        keep(src, dst, sems)

        def body(k, _):
            h2, w2_ = peer(k)

            @pl.when(used(h2 * w_size + w2_, h2))
            def _():
                src, dst = refs(h2, w2_)
                push(src, dst, sems, {"h": h2, "w": w2_})
            return 0

        lax.fori_loop(1, ndev, body, 0)
        unsent.setdefault(key, []).append(lambda: take(sems.at[0], count - 1, [n - 1 for n in counts if n > 1]))

    def take(sem, count, counts):
        for n in counts:
            @pl.when(count == n)
            def _():
                drain(als.at[0, pl.ds(0, n * piece)], sem)

    n_orders = (((me + 1) * l_own + 7) // 8) * w_size
    n_owners = ndev - (8 * h) // l_own
    all_orders = [w_size * n for n in range(1, h_size + 1)]
    all_owners = [ndev - (8 * g) // l_own for g in range(h_size)]
    pairs = lambda k: pl.ds(k * part, part)

    def at_rows(i, k):
        return pl.ds(pl.multiple_of(i * 16 * ntp + k * 16 * part, 16 * part), 16 * part)

    def send_home_rows(b, k, sem, name):
        along("w", lambda o: (pk.at[b, o, pairs(k)], rows.at[b, pairs(k), rows_at(w, npl)]), sem.at[b, k],
              pk.at[b, pl.ds(0, w_size - 1), pairs(k)], ("pk", b, k))
        coming[name, b, k] = lambda: drain(rows.at[b, pairs(k)], sem.at[b, k, 1])

    def send_rows_home(b, k, sem, name):
        along("w", lambda o: (yrow.at[b, o, pairs(k)], hy.at[b, w, pairs(k)]), sem.at[b, k],
              yrow.at[b, pl.ds(0, w_size - 1), pairs(k)], ("yrow", b, k))
        coming[name, b, k] = lambda: drain(hy.at[b, :, pairs(k)], sem.at[b, k, 1])

    def send_orders(b, k, dst, sem, name):
        along("h", lambda o: (xs.at[b, o, at_rows(0, k)], dst.at[b, at_rows(h, k)]), sem.at[b, k],
              xs.at[b, pl.ds(0, h_size - 1), at_rows(0, k)], ("xs", b, k))
        coming[name, b, k] = lambda: drain(xs.at[b, :, at_rows(0, k)], sem.at[b, k, 1])

    def send_lats(b, dst, sem, name):
        for k in range(PARTS):
            along("h", lambda o: (ys.at[b, at_rows(o, k)], dst.at[b, h, at_rows(0, k)]), sem.at[b, k],
                  xs.at[b, pl.ds(0, h_size - 1), at_rows(0, k)], ("ys", b))
            coming[name, b, k] = lambda k=k: drain(dst.at[b, :, at_rows(0, k)], sem.at[b, k, 1])

    def send_owner(b, dst, sem, name):
        some(lambda h2, w2_: (als.at[b, rows_at(h2 * w_size + w2_, piece)], dst.at[b, h, :, lanes_at(w)]), sem.at[b],
             lambda lin, h2: holds(lin, h), n_owners, all_owners, ("als", b))
        coming[name, b] = lambda: take(sem.at[b, 1], n_orders, all_orders)

    def send_back(b, dst, sem, name):
        some(lambda h2, w2_: (bs.at[b, h2, w2_], dst.at[b, rows_at(me, piece)]), sem.at[b],
             lambda lin, h2: holds(me, h2), n_orders, all_orders, ("bs", b))
        coming[name, b] = lambda: take(sem.at[b, 1], n_owners, all_owners)

    def dft(b, k, table):
        settle(("xs", b, k))

        def body(n, _):
            i = 2 * n
            both = jnp.concatenate([rows[b, i], rows[b, i + 1]], axis=1)
            out = dot(table[...], both).reshape(h_size, 16, 2 * LANES)
            xs[b, :, rows_at(i, 16), :] = out[:, :, :LANES]
            xs[b, :, rows_at(i + 1, 16), :] = out[:, :, LANES:]
            return 0

        lax.fori_loop(k * part // 2, (k + 1) * part // 2, body, 0)

    def idft(b, k, table, src):
        settle(("yrow", b, k))

        def body(n, _):
            i = 2 * n
            both = jnp.concatenate([src[b, :, rows_at(i + j, 16), :].reshape(-1, LANES) for j in range(2)], axis=1)
            out = dot(table[...], both)
            for j in range(2):
                yrow[b, :, i + j] = out[:, j * LANES:(j + 1) * LANES].reshape(w_size, npl, LANES)
            return 0

        lax.fori_loop(k * part // 2, (k + 1) * part // 2, body, 0)

    def level(v):
        mean = jnp.mean(v, axis=0, keepdims=True)
        mean = 0.5 * (mean + flip(mean))
        return v - jnp.where(h == 0, mean, 0.0)

    def leg_down(b, table, src, fix):
        settle(("als", b))
        for m in range(8):
            parts = [src[b, pl.ds(ri * 8 + m, ntp * h_size, stride=16), :] for ri in range(2)]
            if fix and m == 0:
                parts[0] = level(parts[0])
            out = dot(table[m], jnp.concatenate(parts, axis=1))
            re0, re1 = out[:nl, :LANES], out[nl:, :LANES]
            im0, im1 = out[:nl, LANES:], out[nl:, LANES:]
            als[b, pl.ds(m, nl, stride=8), :] = jnp.where(low(re0), re0, im1) + flip(jnp.where(low(re0), im0, re1))

    def leg_up(b, table, src, fix):
        settle(("ys", b))
        for m in range(8):
            out = dot(table[m], src[b, pl.ds(m, nl, stride=8), :])
            re, im = weave(out[:nlat // 2], out[nlat // 2:])
            if fix and m == 0:
                re = level(re)
            ys[b, pl.ds(m, ntp * h_size, stride=16), :] = re
            ys[b, pl.ds(8 + m, ntp * h_size, stride=16), :] = im

    def owned(b, l, src):
        tiles = [src[b, :, l * 8:(l + 1) * 8, j * LANES:(j + 1) * LANES].reshape(-1, LANES) for j in range(w_size)]
        return weave_wide(tiles)

    def put_back(b, l, re, im):
        for j, tile in enumerate(weave_tiles(re, im)):
            bs[b, :, j, l * 8:(l + 1) * 8, :] = tile.reshape(h_size, 8, LANES)

    def put_rows(b, i, v0, v1):
        for j, tile in enumerate(weave_tiles(v0, v1)):
            pk[b, j, i] = tile

    def get_rows(b, i):
        return weave_wide([hy[b, j, i] for j in range(w_size)])

    count = nt * npl

    def combine(stats, n):
        mean = jnp.mean(stats, axis=0)
        dev = stats - mean[None]
        dev2 = jnp.sum(dev * dev, axis=0)
        m2 = jnp.sum(stats, axis=0)
        return [(mean[2 * b:2 * b + 1], m2[2 * b + 1:2 * b + 2] + n * dev2[2 * b:2 * b + 1]) for b in range(nb)]

    def go():
        for b in range(nb):
            loads[b].wait()

            def pack(i, total, b=b):
                v0, v1 = xh[b, i], xh[b, i + ntp]
                put_rows(b, i, v0, v1)
                return total + jnp.sum(v0 + v1, axis=0, keepdims=True)

            mean = lax.fori_loop(0, ntp, pack, jnp.zeros((1, nc), F32)) / count

            def spread(t, total, b=b, mean=mean):
                d = xh[b, t] - mean
                return total + jnp.sum(d * d, axis=0, keepdims=True)

            st_s[2 * b:2 * b + 1, :] = mean
            st_s[2 * b + 1:2 * b + 2, :] = lax.fori_loop(0, nt, spread, jnp.zeros((1, nc), F32))
        pl.semaphore_wait(barrier, ndev - 1 + dp_size - 1)
        along("w", lambda o: (st_s, st_w.at[w]), sem_st.at[0], st_w.at[pl.ds(0, w_size - 1)], "st")
        coming["st"] = lambda: drain(st_w, sem_st.at[0, 1])
        along("w", lambda o: (tab_s, tab_w.at[w]), sem_tab.at[0], tab_w.at[pl.ds(0, w_size - 1)])
        coming["tab"] = lambda: drain(tab_w, sem_tab.at[0, 1])

    def st2():
        got("st")
        st_m[...] = jnp.zeros_like(st_m)
        for b, (mean, m2) in enumerate(combine(st_w[...], count)):
            st_m[2 * b:2 * b + 1, :] = mean
            st_m[2 * b + 1:2 * b + 2, :] = m2
        along("h", lambda o: (st_m, st_h.at[h]), sem_st.at[1], st_h.at[pl.ds(0, h_size - 1)], "st")
        coming["st2"] = lambda: drain(st_h, sem_st.at[1, 1])

    means, scales = [], []

    def st3():
        got("st2")
        for mean, m2 in combine(st_h[...], count * w_size):
            means.append(mean)
            scales.append(lax.rsqrt(m2 / (count * ndev) + NORM_EPS))

    def tb2():
        got("tab")
        along("h", lambda o: (tab_w.at[o // 2, rows_at(o % 2, 8)], tab.at[:, rows_at(h, nt)]), sem_tab.at[1], tab.at[:, pl.ds(0, nlat - nt)])
        coming["tab2"] = lambda: drain(tab, sem_tab.at[1, 1])

    def tb3():
        got("tab2")
        for m in range(8):
            both = tab[m].reshape(h_size, 2, ntp, 2 * nl)
            t0, t1 = both[:, 0].reshape(-1, 2 * nl), both[:, 1].reshape(-1, 2 * nl)
            for k, (down, up) in enumerate(((down_p, up_p), (down_q, up_q))):
                a, z = t0[:, k * nl:(k + 1) * nl], t1[:, k * nl:(k + 1) * nl]
                up[m, :nlat // 2, :] = a
                up[m, nlat // 2:, :] = z
                down[m, :nl, :] = a.T
                down[m, nl:, :] = z.T

    def sX(b, k):
        send_home_rows(b, k, sem_x, "x")

    def fd(b, k):
        got(("x", b, k))
        dft(b, k, f_tab)
        send_orders(b, k, sr, sem_s, "s")

    def fl(b):
        for k in range(PARTS):
            got(("s", b, k))
        leg_down(b, down_p, sr, True)
        send_owner(b, ar, sem_a, "a")

    def fo(b):
        if not scales:
            got("k")
            st3()
        got(("a", b))
        settle(("bs", b))
        for l in range(l_own):
            re, im = owned(b, l, ar)
            a = jnp.concatenate([re, im], axis=0) * scales[b]
            asave[b, l] = a
            n = a.shape[0] // 2
            own, other = dot(a, ker[0, l]), dot(a, ker[1, l])
            put_back(b, l, own[:n] - other[n:], own[n:] + other[:n])
        send_back(b, br, sem_b, "b")
        along("dp", lambda o: (asave.at[b, o // 2], aall.at[dp, b]), sem_az.at[b], aall.at[pl.ds(0, dp_size - 1), b])
        coming["az", b] = lambda: drain(aall.at[:, b], sem_az.at[b, 1])

    def fu(b):
        got(("b", b))
        leg_up(b, up_q, br, False)
        send_lats(b, yr, sem_u, "u")

    def fi(b, k):
        got(("u", b, k))
        idft(b, k, gt_tab, yr)

    def sY(b, k):
        send_rows_home(b, k, sem_y, "y")

    def pw(b, k):
        got(("y", b, k))
        if ("t", b) in coming:
            got(("t", b))
        settle(("pk", b, k))

        def body(n, _):
            lats = [2 * n, 2 * n + ntp, 2 * n + 1, 2 * n + 1 + ntp]
            y = jnp.concatenate([v for j in range(2) for v in get_rows(b, 2 * n + j)], axis=0)
            yb = y.astype(BF16)
            hid = bdot(yb, w1[...])
            th_ = jnp.tanh(GELU_C * (hid + GELU_A * (hid * hid * hid)))
            act = (hid * (0.5 * (1.0 + th_))).astype(BF16)
            resid = y + bdot(act, w2[...])
            parts = []
            for j, t in enumerate(lats):
                r = resid[j * npl:(j + 1) * npl] + xh[b, t] - th[b, t]
                d = lat[t] * r
                ls[...] += jnp.sum((d * r).reshape(-1, 8, nc), axis=0)
                dout[b, t] = d
                parts.append(d)
            d = jnp.concatenate(parts, axis=0)
            db = d.astype(BF16)
            gw[2 * nc:, :] += bdot(act, db, TN)
            slope = 0.5 * (1.0 + th_) + (0.5 * GELU_C) * hid * (1.0 - th_ * th_) * (1.0 + (3.0 * GELU_A) * (hid * hid))
            dh = (bdot(db, w2[...], NT) * slope).astype(BF16)
            gin = bdot(yb, dh, TN)
            gw[:nc, :] += gin[:, :nc]
            gw[nc:2 * nc, :] += gin[:, nc:]
            dy = d + bdot(dh, w1[...], NT)
            for j in range(2):
                put_rows(b, 2 * n + j, dy[2 * j * npl:(2 * j + 1) * npl], dy[(2 * j + 1) * npl:(2 * j + 2) * npl])
            return 0

        lax.fori_loop(k * part // 2, (k + 1) * part // 2, body, 0)

    def sD(b, k):
        send_home_rows(b, k, sem_d, "d")

    def bd(b, k):
        got(("d", b, k))
        dft(b, k, g_tab)
        send_orders(b, k, dsr, sem_ds, "ds")

    def bl(b):
        for k in range(PARTS):
            got(("ds", b, k))
        leg_down(b, down_q, dsr, False)
        send_owner(b, dar, sem_da, "da")

    def bo(b):
        got(("da", b))
        settle(("bs", b), "st")
        s2 = jnp.zeros((1, nc), F32)
        for l in range(l_own):
            re, im = owned(b, l, dar)
            d = jnp.concatenate([re, im], axis=0)
            dsave[b, l] = d
            n = d.shape[0] // 2
            own, other = dot(d, ker[0, l], NT), dot(d, ker[1, l], NT)
            re, im = own[:n] + other[n:], own[n:] - other[:n]
            put_back(b, l, re, im)
            s2 = s2 + jnp.sum(re * asave[b, l, :n] + im * asave[b, l, n:], axis=0, keepdims=True)
        send_back(b, dbr, sem_db, "db")
        along("dp", lambda o: (dsave.at[b, o // 2, :, lanes_at(o % 2)], dall.at[dp, b]), sem_dz.at[b], dall.at[pl.ds(0, dp_size - 1), b])
        coming["dz", b] = lambda: drain(dall.at[:, b], sem_dz.at[b, 1])
        st_s[b:b + 1, :] = s2

    def bu(b):
        got(("db", b))
        leg_up(b, up_p, dbr, True)
        send_lats(b, dyr, sem_du, "du")

    def bi(b, k):
        got(("du", b, k))
        idft(b, k, ft_tab, dyr)

    def sN(b, k):
        send_rows_home(b, k, sem_n, "n")

    def pj1():
        st_s[nb:, :] = jnp.zeros_like(st_s[nb:, :])
        along("w", lambda o: (st_s, st_w.at[w]), sem_st.at[2], st_w.at[pl.ds(0, w_size - 1)])
        coming["pj"] = lambda: drain(st_w, sem_st.at[2, 1])

    def pj2():
        got("pj")
        st_m[...] = jnp.sum(st_w[...], axis=0)
        along("h", lambda o: (st_m, st_h.at[h]), sem_st.at[3], st_h.at[pl.ds(0, h_size - 1)])
        coming["pj2"] = lambda: drain(st_h, sem_st.at[3, 1])

    proj = []

    def fn(b, k):
        if not proj:
            got("pj2")
            proj.append(jnp.sum(st_h[...], axis=0) / (count * ndev))
        got(("n", b, k))

        def body(i, _):
            for t, dn in zip((i, i + ntp), get_rows(b, i)):
                normed = (xh[b, t] - means[b]) * scales[b]
                dout[b, t] = dout[b, t] + scales[b] * (dn - normed * proj[0][b:b + 1])
            return 0

        lax.fori_loop(k * part, (k + 1) * part, body, 0)
        for j in range(2):
            lats = pl.ds(j * ntp + k * part, part)
            pltpu.make_async_copy(dout.at[b, lats], dx_out.at[b, lats], sem_o.at[b, k, j]).start()
            unsent.setdefault(None, []).append(lambda lats=lats, j=j: drain(dx_out.at[b, lats], sem_o.at[b, k, j]))

    n_z, n_h, n_w = gw_zs.shape[0], gw_hs.shape[0], gw_ws.shape[0]

    def gw1():
        along("dp", lambda o: (gw.at[rows_at(o, n_z)], gw_z.at[dp]), sem_gw.at[0], gw_z.at[pl.ds(0, dp_size - 1)])
        along("dp", lambda o: (ls, ls_z.at[dp]), sem_ls.at[0], ls_z.at[pl.ds(0, dp_size - 1)])
        coming["gw1"] = lambda: (drain(gw_z, sem_gw.at[0, 1]), drain(ls_z, sem_ls.at[0, 1]))

    def gw2():
        got("gw1")
        gw_zs[...] = jnp.sum(gw_z[...], axis=0)
        ls_zs[...] = jnp.sum(ls_z[...], axis=0)
        along("h", lambda o: (gw_zs.at[rows_at(o, n_h)], gw_h.at[h]), sem_gw.at[1], gw_h.at[pl.ds(0, h_size - 1)])
        along("h", lambda o: (ls_zs, ls_h.at[h]), sem_ls.at[1], ls_h.at[pl.ds(0, h_size - 1)])
        coming["gw2"] = lambda: (drain(gw_h, sem_gw.at[1, 1]), drain(ls_h, sem_ls.at[1, 1]))

    def gw3():
        got("gw2")
        gw_hs[...] = jnp.sum(gw_h[...], axis=0)
        ls_hs[...] = jnp.sum(ls_h[...], axis=0)
        along("w", lambda o: (gw_hs.at[rows_at(o, n_w)], gw_w.at[w]), sem_gw.at[2], gw_w.at[pl.ds(0, w_size - 1)])
        along("w", lambda o: (ls_hs, ls_w.at[w]), sem_ls.at[2], ls_w.at[pl.ds(0, w_size - 1)])
        coming["gw3"] = lambda: (drain(gw_w, sem_gw.at[2, 1]), drain(ls_w, sem_ls.at[2, 1]))

    def gw4():
        got("gw3")
        gw_ws[...] = jnp.sum(gw_w[...], axis=0)
        loss_out[...] = jnp.sum(ls_w[...], keepdims=True).reshape(1, 1) / total_points
        along("w", lambda o: (gw_ws, gw_w2.at[rows_at(w, n_w)]), sem_gw.at[3], gw_w2.at[pl.ds(0, (w_size - 1) * n_w)])
        coming["gw4"] = lambda: drain(gw_w2, sem_gw.at[3, 1])

    def gw5():
        got("gw4")
        along("h", lambda o: (gw_w2, gw_h2.at[rows_at(h, n_h)]), sem_gw.at[4], gw_h2.at[pl.ds(0, (h_size - 1) * n_h)])
        coming["gw5"] = lambda: drain(gw_h2, sem_gw.at[4, 1])

    def gw6():
        got("gw5")
        along("dp", lambda o: (gw_h2, gw_f.at[rows_at(dp, n_z)]), sem_gw.at[5], gw_f.at[pl.ds(0, (dp_size - 1) * n_z)])
        coming["gw6"] = lambda: drain(gw_f, sem_gw.at[5, 1])

    def end():
        got("gw6")
        outs = [(gw_f.at[:nc], gin_out.at[:, :nc]), (gw_f.at[nc:2 * nc], gin_out.at[:, nc:]), (gw_f.at[2 * nc:], gout_out)]
        for i, (src, dst) in enumerate(outs):
            pltpu.make_async_copy(src, dst, sem_fin.at[i]).start()
            unsent.setdefault(None, []).append(lambda dst=dst, i=i: drain(dst, sem_fin.at[i]))

    cuts, _, n_g, _ = gs_sum.shape

    def gs1():
        for b in range(nb):
            got(("az", b))
            got(("dz", b))
        d = dall[...].reshape(dp_size * nb, 2, -1, LANES)
        turned = jnp.concatenate([d[:, 1:], -d[:, :1]], axis=1)
        both = jnp.concatenate([d.reshape(-1, LANES), turned.reshape(-1, LANES)], axis=1)
        out = dot(aall[...].reshape(-1, nc), both, TN)
        for q in range(cuts):
            for p in range(2):
                gs_sum[q, p] = out[q * n_g:(q + 1) * n_g, p * LANES:(p + 1) * LANES]

    def gs2(q):
        along("w", lambda o: (gs_sum.at[q], gs_w.at[q, w]), sem_gs.at[q], gs_w.at[q, pl.ds(0, w_size - 1)])
        coming["gs", q] = lambda: drain(gs_w.at[q], sem_gs.at[q, 1])

    right, left = (dp + 1) % dp_size, (dp + dp_size - 1) % dp_size
    block_at = lambda d, o, q: gs_out.at[:, l_own * o + d // 2, rows_at(q, n_g), lanes_at(d % 2)]

    def gs3(q):
        got(("gs", q))
        for o in range(w_size):
            pltpu.make_async_copy(gs_w.at[q, o], block_at(dp, o, q), sem_gf.at[q, 3, o, 0]).start()
            push(gs_w.at[q, o], block_at(dp, o, q), sem_gf.at[q, 0, o], {"dp": right})
            push(gs_w.at[q, o], block_at(dp, o, q), sem_gf.at[q, 1, o], {"dp": left})

    def gs4(q):
        for o in range(w_size):
            way = 0 if o < w_size // 2 else 1
            source, target = (left, right) if way == 0 else (right, left)
            drain(gs_w.at[q, o], sem_gf.at[q, way, o, 1])
            push(block_at(source, o, q), block_at(source, o, q), sem_gf.at[q, 2, o], {"dp": target})

    def gs5(q):
        for o in range(w_size):
            drain(gs_w.at[q, o], sem_gf.at[q, 1 if o < w_size // 2 else 0, o, 1])
            drain(gs_w.at[q, o], sem_gf.at[q, 2, o, 1])
            for i in range(4):
                drain(gs_w.at[q, o], sem_gf.at[q, i, o, 0])

    scope = dict(locals())
    for name in ORDER.split():
        call = name.rstrip("0123456789") or name
        if name in scope:
            scope[name]()
        elif name[:2] == "gs" and len(name) == 4:
            scope[name[:3]](int(name[3]))
        else:
            scope[call](*map(int, name[len(call):]))
    assert not coming
    settle()


def solution(mesh):
    dp_size, w_size, h_size = mesh.shape["dp"], mesh.shape["w"], mesh.shape["h"]

    def local_step(field, target, lat_weight, leg_fwd, leg_inv, spec_w, w_in, w_out):
        nb, nc, nt, npl = field.shape
        nlon = npl * w_size
        ntp = nt // 2
        nm = leg_fwd.shape[0] * w_size
        ndev = h_size * w_size
        nlat = nt * h_size
        nl = leg_fwd.shape[1]
        lo = nl // ndev
        assert nm == 8 * h_size and nc == w_size * LANES // 2 and h_size == 2 * w_size and 2 * lo == dp_size and 2 * nl == LANES
        total_points = nb * dp_size * nc * nlat * nlon
        fwd_np, inv_np = dft_tables(nlon, nm, h_size)
        any_spec = pl.BlockSpec(memory_space=pl.ANY)
        vmem_spec = pl.BlockSpec(memory_space=pltpu.VMEM)
        sds = lambda *s: jax.ShapeDtypeStruct(s, F32)
        vm = lambda *s: pltpu.VMEM(s, F32)
        dma = lambda *s: pltpu.SemaphoreType.DMA(s)
        n_rows = 2 * nc + w_out.shape[0]
        n_z, n_h, n_w = n_rows // dp_size, n_rows // dp_size // h_size, n_rows // dp_size // h_size // w_size
        home = vm(nb, nt, npl, nc)
        woven = vm(nb, w_size, ntp, npl, LANES)
        order = vm(nb, 16 * nlat // 2, LANES)
        degree = vm(nb, 8 * nl, LANES)
        owner = vm(nb, h_size, 8 * lo, w_size * LANES)
        saved = vm(nb, lo, 2 * nm, nc)
        cuts = 2
        d_x, g_spec, g_in, g_out, loss = pl.pallas_call(
            functools.partial(block_kernel, (dp_size, h_size, w_size), total_points),
            name="block",
            out_shape=[sds(nb, nt, npl, nc), sds(2, lo * w_size, nc, nc), sds(nc, 2 * nc), sds(2 * nc, nc), sds(1, 1)],
            in_specs=[any_spec] * 2 + [vmem_spec] * 2 + [any_spec] + [pl.BlockSpec(memory_space=pltpu.SMEM)] + [vmem_spec] * 6,
            out_specs=[any_spec] * 4 + [vmem_spec],
            scratch_shapes=[
                home, home, home, woven, vm(nb, ntp, nlon, LANES), woven, woven,
                vm(nb, h_size, 16 * ntp, LANES), order, order, order, vm(nb, h_size, 16 * ntp, LANES), vm(nb, h_size, 16 * ntp, LANES),
                degree, owner, owner, vm(nb, h_size, w_size, 8 * lo, LANES), degree, degree, saved, saved,
                vm(dp_size, nb, 2 * nm, nc), vm(dp_size, nb, 2 * nm, LANES),
                vm(8, nc), vm(h_size, 8, nc), vm(8, nc), vm(w_size, 8, nc),
                vm(leg_fwd.shape[0], nt, 2 * nl), vm(w_size, leg_fwd.shape[0], nt, 2 * nl), vm(8, nlat, 2 * nl),
                vm(8, 2 * nl, nlat // 2), vm(8, 2 * nl, nlat // 2), vm(8, nlat, nl), vm(8, nlat, nl),
                vm(2, lo, nc, nc),
                vm(n_rows, nc), vm(dp_size, n_z, nc), vm(n_z, nc), vm(h_size, n_h, nc), vm(n_h, nc), vm(w_size, n_w, nc), vm(n_w, nc),
                vm(n_h, nc), vm(n_z, nc), vm(n_rows, nc),
                vm(8, nc), vm(dp_size, 8, nc), vm(8, nc), vm(h_size, 8, nc), vm(8, nc), vm(w_size, 8, nc),
                vm(cuts, 2, nc // cuts, LANES), vm(cuts, w_size, 2, nc // cuts, LANES),
            ] + [dma(nb, PARTS, 2)] * 8 + [dma(nb, 2)] * 6 + [dma(nb, 2), dma(nb, PARTS, 2), dma(4, 2), dma(2, 2), dma(1), dma(6, 2), dma(3, 2),
                 dma(cuts, 2), dma(cuts, 4, w_size, 2), dma(3)],
            compiler_params=pltpu.CompilerParams(collective_id=0, has_side_effects=True, vmem_limit_bytes=62 * 1024 * 1024),
        )(field.transpose(0, 2, 3, 1), target.transpose(0, 2, 3, 1), leg_fwd.transpose(0, 2, 1), leg_inv.transpose(0, 2, 1),
          spec_w, lat_weight, w_in, w_out, jnp.asarray(fwd_np), jnp.asarray(inv_np), jnp.asarray(fwd_np.T.copy()), jnp.asarray(inv_np.T.copy()))
        return loss.reshape(()), d_x.transpose(0, 3, 1, 2), g_spec, g_in, g_out

    grid_spec = P("dp", None, "h", "w")
    table_spec = P("w", None, "h")
    kernel_spec = P(None, "h", None, None)
    return jax.shard_map(local_step, mesh=mesh, in_specs=(grid_spec, grid_spec, P("h"), table_spec, table_spec, P(), P(), P()), out_specs=(P(), grid_spec, kernel_spec, P(), P()), check_vma=False)
```

```python
import functools
import jax
import jax.numpy as jnp
import numpy as np
from jax import lax
from jax.experimental import pallas as pl
from jax.experimental.pallas import tpu as pltpu
from jax.sharding import PartitionSpec as P

NORM_EPS = 1e-5
PRECISE = lax.Precision.HIGHEST
MESH = pl.DeviceIdType.MESH
F32 = jnp.float32
BF16 = jnp.bfloat16
GELU_C = float(np.sqrt(2.0 / np.pi))
GELU_A = 0.044715
LANES = 128
NN = (((1,), (0,)), ((), ()))
NT = (((1,), (1,)), ((), ()))
TN = (((0,), (0,)), ((), ()))


def dot(a, b, dims=NN):
    return lax.dot_general(a, b, dims, precision=PRECISE, preferred_element_type=F32)


def bdot(a, b, dims=NN):
    return lax.dot_general(a, b, dims, preferred_element_type=F32)


def dft_tables(lon_count, num_modes, h_size):
    modes, lons = np.arange(num_modes), np.arange(lon_count)
    angle = 2.0 * np.pi * ((modes[:, None] * lons[None, :]) % lon_count) / lon_count
    fwd = np.stack([np.cos(angle), -np.sin(angle)], 0) * lon_count ** -0.5
    inv = fwd * np.where(modes == 0, 1.0, 2.0)[None, :, None]

    def rows(table):
        table = table.reshape(2, h_size, num_modes // h_size, lon_count).transpose(1, 0, 2, 3)
        return table.reshape(2 * num_modes, lon_count).astype(np.float32)

    return rows(fwd), rows(inv)


def drain(ref, sem):
    pltpu.make_async_copy(ref, ref, sem).wait()


def rows_at(i, n):
    return pl.ds(pl.multiple_of(i * n, n), n)


def lanes_at(i):
    return pl.ds(pl.multiple_of(i * LANES, LANES), LANES)


def push(src, dst, sems, device):
    pltpu.make_async_remote_copy(src_ref=src, dst_ref=dst, send_sem=sems.at[0], recv_sem=sems.at[1],
                                 device_id=device, device_id_type=MESH).start()


def keep(src, dst, sems):
    pltpu.make_async_copy(src, dst, sems.at[1]).start()


def flip(v):
    return pltpu.roll(v, LANES // 2, 1)


def low(v):
    return lax.broadcasted_iota(jnp.int32, v.shape, 1) < LANES // 2


def weave(a, b):
    return jnp.where(low(a), a, flip(b)), jnp.where(low(a), flip(a), b)


def weave_wide(tiles):
    pairs = [weave(tiles[j], tiles[j + 1]) for j in range(0, len(tiles), 2)]
    return jnp.concatenate([p[0] for p in pairs], axis=1), jnp.concatenate([p[1] for p in pairs], axis=1)


def weave_tiles(a, b):
    out = []
    for j in range(0, a.shape[1], LANES):
        out.extend(weave(a[:, j:j + LANES], b[:, j:j + LANES]))
    return out


PARTS = 2
ORDER = " ".join((
    'go', 'sX20', 'sX21', 'sX00', 'tb1', 'fd20', 'tb2', 'fd21', 'sX01', 'sX11',
    'fd00', 'tb3', 'fl2', 'fd01', 'st2', 'sX10', 'fd11', 'fo2', 'fl0', 'fd10',
    'fu2', 'fo0', 'fl1', 'fi20', 'sY20', 'fi21', 'sY21', 'fu0', 'fo1', 'fi00',
    'sY00', 'fi01', 'sY01', 'fu1', 'pw00', 'sD00', 'fi10', 'sY10', 'fi11', 'pw21',
    'pw20', 'bd00', 'pw01', 'sY11', 'sD01', 'pw10', 'sD10', 'pw11', 'gw1', 'sD11',
    'sD21', 'bd01', 'sD20', 'bd10', 'bl0', 'bd11', 'gw2', 'bd21', 'bl1', 'gw3',
    'bd20', 'bo0', 'gw4', 'bl2', 'gw5', 'bu0', 'bo1', 'bo2', 'gw6', 'pj1',
    'bi00', 'sN00', 'gs1', 'gs20', 'bi01', 'pj2', 'bu2', 'gs300', 'sN01', 'bu1',
    'gs303', 'gs302', 'bi21', 'fn00', 'end', 'sN21', 'gs301', 'bi11', 'sN11', 'gs403',
    'bi10', 'fn21', 'gs400', 'bi20', 'sN10', 'fn01', 'fn11', 'sN20', 'gs401', 'gs402',
    'fn10', 'gs501', 'gs502', 'gs500', 'gs503', 'fn20',
))


def block_kernel(sizes, total_points,
                 x, tgt, leg_p_in, leg_q_in, spec_w, lat_in, w1_in, w2_in, f_in, g_in,
                 dx_out, gs_out, gin_out, gout_out, loss_out,
                 leg_p, leg_q, lat, w1, w2, f_tab, g_tab, ft_tab, gt_tab,
                 xh, th, dout, pk, rows, yrow, hy,
                 xs, sr, dsr, ys, yr, dyr, als, ar, dar, bs, br, dbr, asave, dsave, aall, dall,
                 st_s, st_h, st_m, st_w, tab_s, tab_w, tab, down_p, down_q, up_p, up_q, ker,
                 gw, gw_z, gw_zs, gw_h, gw_hs, gw_w, gw_ws, gw_w2, gw_h2, gw_f,
                 ls, ls_z, ls_zs, ls_h, ls_hs, ls_w, gs_sum, gs_w,
                 sem_x, sem_y, sem_d, sem_n, sem_s, sem_ds, sem_u, sem_du, sem_a, sem_da, sem_b, sem_db, sem_az, sem_dz,
                 sem_in, sem_o, sem_st, sem_tab, sem_k, sem_gw, sem_ls, sem_gs, sem_gf, sem_fin, sem_small):
    dp_size, h_size, w_size = sizes
    dp, h, w = lax.axis_index("dp"), lax.axis_index("h"), lax.axis_index("w")
    ndev = h_size * w_size
    me = h * w_size + w
    nb, nt, npl, nc = x.shape
    ntp = nt // 2
    part = ntp // PARTS
    nlon = npl * w_size
    nlat = nt * h_size
    nl = als.shape[1] // 8
    l_own = nl // ndev
    piece = 8 * l_own
    unsent, coming = {}, {}

    def got(key):
        coming.pop(key)()

    def peer(k):
        return (h + k // w_size) % h_size, (w + k % w_size) % w_size

    barrier = pltpu.get_barrier_semaphore()

    def meet(k, _):
        h2, w2_ = peer(k)
        pl.semaphore_signal(barrier, inc=1, device_id={"h": h2, "w": w2_}, device_id_type=MESH)
        return 0

    def meet_dp(k, _):
        pl.semaphore_signal(barrier, inc=1, device_id={"dp": (dp + k) % dp_size}, device_id_type=MESH)
        return 0

    lax.fori_loop(1, ndev, meet, 0)
    lax.fori_loop(1, dp_size, meet_dp, 0)
    loads = [pltpu.make_async_copy(x.at[b], xh.at[b], sem_in.at[b, 0]) for b in range(nb)]
    load_t = [pltpu.make_async_copy(tgt.at[b], th.at[b], sem_in.at[b, 1]) for b in range(nb)]
    load_k = pltpu.make_async_copy(spec_w.at[:, pl.ds(me * l_own, l_own)], ker, sem_k.at[0])
    small = [pltpu.make_async_copy(src, dst, sem_small.at[i]) for i, (src, dst) in enumerate((
        (leg_p_in, leg_p), (leg_q_in, leg_q), (f_in, f_tab), (g_in, g_tab), (lat_in, lat), (w1_in, w1), (w2_in, w2)))]
    for c in loads + small[:4] + [load_k] + load_t + small[4:]:
        c.start()
    coming["k"] = load_k.wait
    coming["small"] = lambda: [c.wait() for c in small[4:]]
    coming.update({("t", b): load_t[b].wait for b in range(nb)})
    for ref in (ar, br, dar, dbr, st_s, gw, ls):
        ref[...] = jnp.zeros_like(ref)

    def settle(*keys):
        for key in keys or list(unsent):
            for wait in unsent.pop(key, []):
                wait()

    def along(axis, refs, sems, sent, key=None):
        size, index = {"dp": (dp_size, dp), "h": (h_size, h), "w": (w_size, w)}[axis]
        src, dst = refs(index)
        keep(src, dst, sems)

        def body(k, _):
            other = (index + k) % size
            src, dst = refs(other)
            push(src, dst, sems, {axis: other})
            return 0

        lax.fori_loop(1, size, body, 0)
        unsent.setdefault(key, []).append(lambda: drain(sent, sems.at[0]))

    def some(refs, sems, low_h, high_h, count, counts, key):
        src, dst = refs(h, w)
        keep(src, dst, sems)

        def one(h2, k):
            w2_ = (w + k) % w_size
            src, dst = refs(h2, w2_)
            push(src, dst, sems, {"h": h2, "w": w2_})

        for k in range(1, w_size):
            one(h, k)

        def body(h2, _):
            for k in range(w_size):
                one(h2, k)
            return 0

        lax.fori_loop(low_h, high_h, body, 0)
        unsent.setdefault(key, []).append(lambda: take(sems.at[0], count - 1, [n - 1 for n in counts]))

    def take(sem, count, counts):
        for n in counts:
            @pl.when(count == n)
            def _():
                drain(als.at[0, pl.ds(0, n * piece)], sem)

    n_orders, n_owners = (h + 1) * w_size, (h_size - h) * w_size
    counts = [w_size * n for n in range(1, h_size + 1)]
    pairs = lambda k: pl.ds(k * part, part)

    def at_rows(i, k):
        return pl.ds(pl.multiple_of(i * 16 * ntp + k * 16 * part, 16 * part), 16 * part)

    def send_home_rows(b, k, sem, name):
        along("w", lambda o: (pk.at[b, o, pairs(k)], rows.at[b, pairs(k), rows_at(w, npl)]), sem.at[b, k],
              pk.at[b, pl.ds(0, w_size - 1), pairs(k)], ("pk", b, k))
        coming[name, b, k] = lambda: drain(rows.at[b, pairs(k)], sem.at[b, k, 1])

    def send_rows_home(b, k, sem, name):
        along("w", lambda o: (yrow.at[b, o, pairs(k)], hy.at[b, w, pairs(k)]), sem.at[b, k],
              yrow.at[b, pl.ds(0, w_size - 1), pairs(k)], ("yrow", b, k))
        coming[name, b, k] = lambda: drain(hy.at[b, :, pairs(k)], sem.at[b, k, 1])

    def send_orders(b, k, dst, sem, name):
        along("h", lambda o: (xs.at[b, o, at_rows(0, k)], dst.at[b, at_rows(h, k)]), sem.at[b, k],
              xs.at[b, pl.ds(0, h_size - 1), at_rows(0, k)], ("xs", b, k))
        coming[name, b, k] = lambda: drain(xs.at[b, :, at_rows(0, k)], sem.at[b, k, 1])

    def send_lats(b, dst, sem, name):
        for k in range(PARTS):
            along("h", lambda o: (ys.at[b, at_rows(o, k)], dst.at[b, h, at_rows(0, k)]), sem.at[b, k],
                  xs.at[b, pl.ds(0, h_size - 1), at_rows(0, k)], ("ys", b))
            coming[name, b, k] = lambda k=k: drain(dst.at[b, :, at_rows(0, k)], sem.at[b, k, 1])

    def send_owner(b, dst, sem, name):
        some(lambda h2, w2_: (als.at[b, rows_at(h2 * w_size + w2_, piece)], dst.at[b, h, :, lanes_at(w)]), sem.at[b],
             h + 1, h_size, n_owners, counts, ("als", b))
        coming[name, b] = lambda: take(sem.at[b, 1], n_orders, counts)

    def send_back(b, dst, sem, name):
        some(lambda h2, w2_: (bs.at[b, h2, w2_], dst.at[b, rows_at(me, piece)]), sem.at[b],
             0, h, n_orders, counts, ("bs", b))
        coming[name, b] = lambda: take(sem.at[b, 1], n_owners, counts)

    def dft(b, k, table):
        settle(("xs", b, k))

        def body(n, _):
            i = 2 * n
            both = jnp.concatenate([rows[b, i], rows[b, i + 1]], axis=1)
            out = dot(table[...], both).reshape(h_size, 16, 2 * LANES)
            xs[b, :, rows_at(i, 16), :] = out[:, :, :LANES]
            xs[b, :, rows_at(i + 1, 16), :] = out[:, :, LANES:]
            return 0

        lax.fori_loop(k * part // 2, (k + 1) * part // 2, body, 0)

    def idft(b, k, table, src):
        settle(("yrow", b, k))

        def body(n, _):
            i = 2 * n
            both = jnp.concatenate([src[b, :, rows_at(i + j, 16), :].reshape(-1, LANES) for j in range(2)], axis=1)
            out = dot(table[...], both)
            for j in range(2):
                yrow[b, :, i + j] = out[:, j * LANES:(j + 1) * LANES].reshape(w_size, npl, LANES)
            return 0

        lax.fori_loop(k * part // 2, (k + 1) * part // 2, body, 0)

    def level(v):
        mean = jnp.mean(v, axis=0, keepdims=True)
        mean = 0.5 * (mean + flip(mean))
        return v - jnp.where(h == 0, mean, 0.0)

    def leg_down(b, table, src, fix):
        settle(("als", b))
        for m in range(8):
            parts = [src[b, pl.ds(ri * 8 + m, ntp * h_size, stride=16), :] for ri in range(2)]
            if fix and m == 0:
                parts[0] = level(parts[0])
            out = dot(table[m], jnp.concatenate(parts, axis=1))
            re0, re1 = out[:nl, :LANES], out[nl:, :LANES]
            im0, im1 = out[:nl, LANES:], out[nl:, LANES:]
            als[b, pl.ds(m, nl, stride=8), :] = jnp.where(low(re0), re0, im1) + flip(jnp.where(low(re0), im0, re1))

    def leg_up(b, table, src, fix):
        settle(("ys", b))
        for m in range(8):
            out = dot(table[m], src[b, pl.ds(m, nl, stride=8), :])
            re, im = weave(out[:nlat // 2], out[nlat // 2:])
            if fix and m == 0:
                re = level(re)
            ys[b, pl.ds(m, ntp * h_size, stride=16), :] = re
            ys[b, pl.ds(8 + m, ntp * h_size, stride=16), :] = im

    def owned(b, l, src):
        tiles = [src[b, :, l * 8:(l + 1) * 8, j * LANES:(j + 1) * LANES].reshape(-1, LANES) for j in range(w_size)]
        return weave_wide(tiles)

    def put_back(b, l, re, im):
        for j, tile in enumerate(weave_tiles(re, im)):
            bs[b, :, j, l * 8:(l + 1) * 8, :] = tile.reshape(h_size, 8, LANES)

    def put_rows(b, i, v0, v1):
        for j, tile in enumerate(weave_tiles(v0, v1)):
            pk[b, j, i] = tile

    def get_rows(b, i):
        return weave_wide([hy[b, j, i] for j in range(w_size)])

    count = nt * npl
    n_tab = tab_s.shape[0] // dp_size

    def combine(stats, n):
        mean = jnp.mean(stats, axis=0)
        dev = stats - mean[None]
        dev2 = jnp.sum(dev * dev, axis=0)
        m2 = jnp.sum(stats, axis=0)
        return [(mean[2 * b:2 * b + 1], m2[2 * b + 1:2 * b + 2] + n * dev2[2 * b:2 * b + 1]) for b in range(nb)]

    def go():
        for b in range(nb):
            loads[b].wait()

            def pack(i, total, b=b):
                v0, v1 = xh[b, i], xh[b, i + ntp]
                put_rows(b, i, v0, v1)
                return total + jnp.sum(v0 + v1, axis=0, keepdims=True)

            mean = lax.fori_loop(0, ntp, pack, jnp.zeros((1, nc), F32)) / count

            def spread(t, total, b=b, mean=mean):
                d = xh[b, t] - mean
                return total + jnp.sum(d * d, axis=0, keepdims=True)

            st_s[2 * b:2 * b + 1, :] = mean
            st_s[2 * b + 1:2 * b + 2, :] = lax.fori_loop(0, nt, spread, jnp.zeros((1, nc), F32))
        for c in small[:4]:
            c.wait()
        tab_s[:, :, :nl] = leg_p[...]
        tab_s[:, :, nl:] = leg_q[...]
        ft_tab[...] = f_tab[...].T
        gt_tab[...] = g_tab[...].T
        pl.semaphore_wait(barrier, ndev - 1 + dp_size - 1)
        along("w", lambda o: (st_s, st_w.at[w]), sem_st.at[0], st_w.at[pl.ds(0, w_size - 1)], "st")
        coming["st"] = lambda: drain(st_w, sem_st.at[0, 1])
        along("w", lambda o: (tab_s.at[rows_at(dp, n_tab)], tab_w.at[w, rows_at(dp, n_tab)]), sem_tab.at[0], tab_w.at[pl.ds(0, w_size - 1), pl.ds(0, n_tab)])
        coming["tab"] = lambda: drain(tab_w.at[:, pl.ds(0, n_tab)], sem_tab.at[0, 1])

    def st2():
        got("st")
        st_m[...] = jnp.zeros_like(st_m)
        for b, (mean, m2) in enumerate(combine(st_w[...], count)):
            st_m[2 * b:2 * b + 1, :] = mean
            st_m[2 * b + 1:2 * b + 2, :] = m2
        along("h", lambda o: (st_m, st_h.at[h]), sem_st.at[1], st_h.at[pl.ds(0, h_size - 1)], "st")
        coming["st2"] = lambda: drain(st_h, sem_st.at[1, 1])

    means, scales = [], []

    def st3():
        got("st2")
        for mean, m2 in combine(st_h[...], count * w_size):
            means.append(mean)
            scales.append(lax.rsqrt(m2 / (count * ndev) + NORM_EPS))

    def tb1():
        got("tab")
        share = tab_w.at[:, rows_at(dp, n_tab)]
        for k in range(1, dp_size):
            push(share, share, sem_tab.at[2], {"dp": (dp + k) % dp_size})
        others = tab_w.at[:, pl.ds(0, (dp_size - 1) * n_tab)]
        unsent.setdefault(None, []).append(lambda: drain(others, sem_tab.at[2, 0]))
        coming["tab1"] = lambda: drain(others, sem_tab.at[2, 1])

    def tb2():
        got("tab1")
        along("h", lambda o: (tab_w.at[o // 2, rows_at(o % 2, 8)], tab.at[:, rows_at(h, nt)]), sem_tab.at[1], tab.at[:, pl.ds(0, nlat - nt)])
        coming["tab2"] = lambda: drain(tab, sem_tab.at[1, 1])

    def tb3():
        got("tab2")
        for m in range(8):
            both = tab[m].reshape(h_size, 2, ntp, 2 * nl)
            t0, t1 = both[:, 0].reshape(-1, 2 * nl), both[:, 1].reshape(-1, 2 * nl)
            for k, (down, up) in enumerate(((down_p, up_p), (down_q, up_q))):
                a, z = t0[:, k * nl:(k + 1) * nl], t1[:, k * nl:(k + 1) * nl]
                up[m, :nlat // 2, :] = a
                up[m, nlat // 2:, :] = z
                down[m, :nl, :] = a.T
                down[m, nl:, :] = z.T

    def sX(b, k):
        send_home_rows(b, k, sem_x, "x")

    def fd(b, k):
        got(("x", b, k))
        dft(b, k, f_tab)
        send_orders(b, k, sr, sem_s, "s")

    def fl(b):
        for k in range(PARTS):
            got(("s", b, k))
        leg_down(b, down_p, sr, True)
        send_owner(b, ar, sem_a, "a")

    def fo(b):
        if not scales:
            got("k")
            st3()
        got(("a", b))
        settle(("bs", b))
        for l in range(l_own):
            re, im = owned(b, l, ar)
            a = jnp.concatenate([re, im], axis=0) * scales[b]
            asave[b, l] = a
            n = a.shape[0] // 2
            own, other = dot(a, ker[0, l]), dot(a, ker[1, l])
            put_back(b, l, own[:n] - other[n:], own[n:] + other[:n])
        send_back(b, br, sem_b, "b")
        along("dp", lambda o: (asave.at[b, o // 2], aall.at[dp, b]), sem_az.at[b], aall.at[pl.ds(0, dp_size - 1), b])
        coming["az", b] = lambda: drain(aall.at[:, b], sem_az.at[b, 1])

    def fu(b):
        got(("b", b))
        leg_up(b, up_q, br, False)
        send_lats(b, yr, sem_u, "u")

    def fi(b, k):
        got(("u", b, k))
        idft(b, k, gt_tab, yr)

    def sY(b, k):
        send_rows_home(b, k, sem_y, "y")

    def pw(b, k):
        got(("y", b, k))
        if ("t", b) in coming:
            got(("t", b))
        if "small" in coming:
            got("small")
        settle(("pk", b, k))

        def body(n, _):
            lats = [2 * n, 2 * n + ntp, 2 * n + 1, 2 * n + 1 + ntp]
            y = jnp.concatenate([v for j in range(2) for v in get_rows(b, 2 * n + j)], axis=0)
            yb = y.astype(BF16)
            hid = bdot(yb, w1[...])
            th_ = jnp.tanh(GELU_C * (hid + GELU_A * (hid * hid * hid)))
            act = (hid * (0.5 * (1.0 + th_))).astype(BF16)
            resid = y + bdot(act, w2[...])
            parts = []
            for j, t in enumerate(lats):
                r = resid[j * npl:(j + 1) * npl] + xh[b, t] - th[b, t]
                d = lat[t] * r
                ls[...] += jnp.sum((d * r).reshape(-1, 8, nc), axis=0)
                dout[b, t] = d
                parts.append(d)
            d = jnp.concatenate(parts, axis=0)
            db = d.astype(BF16)
            gw[2 * nc:, :] += bdot(act, db, TN)
            slope = 0.5 * (1.0 + th_) + (0.5 * GELU_C) * hid * (1.0 - th_ * th_) * (1.0 + (3.0 * GELU_A) * (hid * hid))
            dh = (bdot(db, w2[...], NT) * slope).astype(BF16)
            gin = bdot(yb, dh, TN)
            gw[:nc, :] += gin[:, :nc]
            gw[nc:2 * nc, :] += gin[:, nc:]
            dy = d + bdot(dh, w1[...], NT)
            for j in range(2):
                put_rows(b, 2 * n + j, dy[2 * j * npl:(2 * j + 1) * npl], dy[(2 * j + 1) * npl:(2 * j + 2) * npl])
            return 0

        lax.fori_loop(k * part // 2, (k + 1) * part // 2, body, 0)

    def sD(b, k):
        send_home_rows(b, k, sem_d, "d")

    def bd(b, k):
        got(("d", b, k))
        dft(b, k, g_tab)
        send_orders(b, k, dsr, sem_ds, "ds")

    def bl(b):
        for k in range(PARTS):
            got(("ds", b, k))
        leg_down(b, down_q, dsr, False)
        send_owner(b, dar, sem_da, "da")

    def bo(b):
        got(("da", b))
        settle(("bs", b), "st")
        s2 = jnp.zeros((1, nc), F32)
        for l in range(l_own):
            re, im = owned(b, l, dar)
            d = jnp.concatenate([re, im], axis=0)
            dsave[b, l] = d
            n = d.shape[0] // 2
            own, other = dot(d, ker[0, l], NT), dot(d, ker[1, l], NT)
            re, im = own[:n] + other[n:], own[n:] - other[:n]
            put_back(b, l, re, im)
            s2 = s2 + jnp.sum(re * asave[b, l, :n] + im * asave[b, l, n:], axis=0, keepdims=True)
        send_back(b, dbr, sem_db, "db")
        along("dp", lambda o: (dsave.at[b, o // 2, :, lanes_at(o % 2)], dall.at[dp, b]), sem_dz.at[b], dall.at[pl.ds(0, dp_size - 1), b])
        coming["dz", b] = lambda: drain(dall.at[:, b], sem_dz.at[b, 1])
        st_s[b:b + 1, :] = s2

    def bu(b):
        got(("db", b))
        leg_up(b, up_p, dbr, True)
        send_lats(b, dyr, sem_du, "du")

    def bi(b, k):
        got(("du", b, k))
        idft(b, k, ft_tab, dyr)

    def sN(b, k):
        send_rows_home(b, k, sem_n, "n")

    def pj1():
        st_s[nb:, :] = jnp.zeros_like(st_s[nb:, :])
        along("w", lambda o: (st_s, st_w.at[w]), sem_st.at[2], st_w.at[pl.ds(0, w_size - 1)])
        coming["pj"] = lambda: drain(st_w, sem_st.at[2, 1])

    def pj2():
        got("pj")
        st_m[...] = jnp.sum(st_w[...], axis=0)
        along("h", lambda o: (st_m, st_h.at[h]), sem_st.at[3], st_h.at[pl.ds(0, h_size - 1)])
        coming["pj2"] = lambda: drain(st_h, sem_st.at[3, 1])

    proj = []

    def fn(b, k):
        if not proj:
            got("pj2")
            proj.append(jnp.sum(st_h[...], axis=0) / (count * ndev))
        got(("n", b, k))

        def body(i, _):
            for t, dn in zip((i, i + ntp), get_rows(b, i)):
                normed = (xh[b, t] - means[b]) * scales[b]
                dout[b, t] = dout[b, t] + scales[b] * (dn - normed * proj[0][b:b + 1])
            return 0

        lax.fori_loop(k * part, (k + 1) * part, body, 0)
        for j in range(2):
            lats = pl.ds(j * ntp + k * part, part)
            pltpu.make_async_copy(dout.at[b, lats], dx_out.at[b, lats], sem_o.at[b, k, j]).start()
            unsent.setdefault(None, []).append(lambda lats=lats, j=j: drain(dx_out.at[b, lats], sem_o.at[b, k, j]))

    n_z, n_h, n_w = gw_zs.shape[0], gw_hs.shape[0], gw_ws.shape[0]

    def gw1():
        along("dp", lambda o: (gw.at[rows_at(o, n_z)], gw_z.at[dp]), sem_gw.at[0], gw_z.at[pl.ds(0, dp_size - 1)])
        along("dp", lambda o: (ls, ls_z.at[dp]), sem_ls.at[0], ls_z.at[pl.ds(0, dp_size - 1)])
        coming["gw1"] = lambda: (drain(gw_z, sem_gw.at[0, 1]), drain(ls_z, sem_ls.at[0, 1]))

    def gw2():
        got("gw1")
        gw_zs[...] = jnp.sum(gw_z[...], axis=0)
        ls_zs[...] = jnp.sum(ls_z[...], axis=0)
        along("h", lambda o: (gw_zs.at[rows_at(o, n_h)], gw_h.at[h]), sem_gw.at[1], gw_h.at[pl.ds(0, h_size - 1)])
        along("h", lambda o: (ls_zs, ls_h.at[h]), sem_ls.at[1], ls_h.at[pl.ds(0, h_size - 1)])
        coming["gw2"] = lambda: (drain(gw_h, sem_gw.at[1, 1]), drain(ls_h, sem_ls.at[1, 1]))

    def gw3():
        got("gw2")
        gw_hs[...] = jnp.sum(gw_h[...], axis=0)
        ls_hs[...] = jnp.sum(ls_h[...], axis=0)
        along("w", lambda o: (gw_hs.at[rows_at(o, n_w)], gw_w.at[w]), sem_gw.at[2], gw_w.at[pl.ds(0, w_size - 1)])
        along("w", lambda o: (ls_hs, ls_w.at[w]), sem_ls.at[2], ls_w.at[pl.ds(0, w_size - 1)])
        coming["gw3"] = lambda: (drain(gw_w, sem_gw.at[2, 1]), drain(ls_w, sem_ls.at[2, 1]))

    def gw4():
        got("gw3")
        gw_ws[...] = jnp.sum(gw_w[...], axis=0)
        loss_out[...] = jnp.sum(ls_w[...], keepdims=True).reshape(1, 1) / total_points
        along("w", lambda o: (gw_ws, gw_w2.at[rows_at(w, n_w)]), sem_gw.at[3], gw_w2.at[pl.ds(0, (w_size - 1) * n_w)])
        coming["gw4"] = lambda: drain(gw_w2, sem_gw.at[3, 1])

    def gw5():
        got("gw4")
        along("h", lambda o: (gw_w2, gw_h2.at[rows_at(h, n_h)]), sem_gw.at[4], gw_h2.at[pl.ds(0, (h_size - 1) * n_h)])
        coming["gw5"] = lambda: drain(gw_h2, sem_gw.at[4, 1])

    def gw6():
        got("gw5")
        along("dp", lambda o: (gw_h2, gw_f.at[rows_at(dp, n_z)]), sem_gw.at[5], gw_f.at[pl.ds(0, (dp_size - 1) * n_z)])
        coming["gw6"] = lambda: drain(gw_f, sem_gw.at[5, 1])

    def end():
        got("gw6")
        outs = [(gw_f.at[:nc], gin_out.at[:, :nc]), (gw_f.at[nc:2 * nc], gin_out.at[:, nc:]), (gw_f.at[2 * nc:], gout_out)]
        for i, (src, dst) in enumerate(outs):
            pltpu.make_async_copy(src, dst, sem_fin.at[i]).start()
            unsent.setdefault(None, []).append(lambda dst=dst, i=i: drain(dst, sem_fin.at[i]))

    cuts, _, n_g, _ = gs_sum.shape

    def gs1():
        for b in range(nb):
            got(("az", b))
            got(("dz", b))
        d = dall[...].reshape(dp_size * nb, 2, -1, LANES)
        turned = jnp.concatenate([d[:, 1:], -d[:, :1]], axis=1)
        both = jnp.concatenate([d.reshape(-1, LANES), turned.reshape(-1, LANES)], axis=1)
        out = dot(aall[...].reshape(-1, nc), both, TN)
        for q in range(cuts):
            for p in range(2):
                gs_sum[q, p] = out[q * n_g:(q + 1) * n_g, p * LANES:(p + 1) * LANES]

    def gs2(q):
        keep(gs_sum.at[q], gs_w.at[q, 0], sem_gs.at[q, 0])
        for k in (1, 3, 2):
            push(gs_sum.at[q], gs_w.at[q, k], sem_gs.at[q, k], {"w": (w + k) % w_size})
            unsent.setdefault(None, []).append(lambda k=k: drain(gs_w.at[q, k], sem_gs.at[q, k, 0]))
        coming.update({("gs", q, k): lambda k=k: drain(gs_w.at[q, k], sem_gs.at[q, k, 1]) for k in range(w_size)})

    right, left = (dp + 1) % dp_size, (dp + dp_size - 1) % dp_size
    block_at = lambda d, k, q: gs_out.at[:, l_own * ((w + w_size - k) % w_size) + d // 2, rows_at(q, n_g), lanes_at(d % 2)]

    def gs3(q, k):
        got(("gs", q, k))
        pltpu.make_async_copy(gs_w.at[q, k], block_at(dp, k, q), sem_gf.at[q, 3, k, 0]).start()
        push(gs_w.at[q, k], block_at(dp, k, q), sem_gf.at[q, 0, k], {"dp": right})
        push(gs_w.at[q, k], block_at(dp, k, q), sem_gf.at[q, 1, k], {"dp": left})

    def gs4(q, k):
        way = 0 if k < w_size // 2 else 1
        source, target = (left, right) if way == 0 else (right, left)
        drain(gs_w.at[q, k], sem_gf.at[q, way, k, 1])
        push(block_at(source, k, q), block_at(source, k, q), sem_gf.at[q, 2, k], {"dp": target})

    def gs5(q, k):
        drain(gs_w.at[q, k], sem_gf.at[q, 1 if k < w_size // 2 else 0, k, 1])
        drain(gs_w.at[q, k], sem_gf.at[q, 2, k, 1])
        for i in range(4):
            drain(gs_w.at[q, k], sem_gf.at[q, i, k, 0])

    scope = dict(locals())
    for name in ORDER.split():
        call = name.rstrip("0123456789") or name
        if name in scope:
            scope[name]()
        elif name[:3] in scope:
            scope[name[:3]](*map(int, name[3:]))
        else:
            scope[call](*map(int, name[len(call):]))
    assert not coming
    settle()


def hand_on_kernel(*refs):
    n = len(refs) // 3
    srcs, dsts, bufs, sem = refs[:n], refs[n:2 * n], refs[2 * n:3 * n], refs[3 * n]
    cuts = [(i, k) for i in range(n) for k in range(srcs[i].shape[0])]
    reads = [pltpu.make_async_copy(srcs[i].at[k], bufs[i].at[k], sem.at[0, j]) for j, (i, k) in enumerate(cuts)]
    writes = [pltpu.make_async_copy(bufs[i].at[k], dsts[i].at[k], sem.at[1, j]) for j, (i, k) in enumerate(cuts)]
    for c in reads:
        c.start()
    for c, d in zip(reads, writes):
        c.wait()
        d.start()
    for d in writes:
        d.wait()


def hand_on(arrays):
    views = [a.reshape(v) for a, v in zip(arrays, ((6, -1, LANES * 2), (8, -1, LANES * 2), (1, *arrays[2].shape), (1, *arrays[3].shape)))]
    any_spec = pl.BlockSpec(memory_space=pl.ANY)
    out = pl.pallas_call(
        hand_on_kernel, name="hand_on",
        out_shape=[jax.ShapeDtypeStruct(v.shape, F32) for v in views],
        in_specs=[any_spec] * len(views), out_specs=[any_spec] * len(views),
        scratch_shapes=[pltpu.VMEM(v.shape, F32) for v in views] + [pltpu.SemaphoreType.DMA((2, sum(v.shape[0] for v in views)))],
        compiler_params=pltpu.CompilerParams(vmem_limit_bytes=62 * 1024 * 1024),
    )(*views)
    return [o.reshape(a.shape) for o, a in zip(out, arrays)]


def solution(mesh):
    dp_size, w_size, h_size = mesh.shape["dp"], mesh.shape["w"], mesh.shape["h"]

    def local_step(field, target, lat_weight, leg_fwd, leg_inv, spec_w, w_in, w_out):
        nb, nc, nt, npl = field.shape
        nlon = npl * w_size
        ntp = nt // 2
        nm = leg_fwd.shape[0] * w_size
        ndev = h_size * w_size
        nlat = nt * h_size
        nl = leg_fwd.shape[1]
        lo = nl // ndev
        assert nm == 8 * h_size and nc == w_size * LANES // 2 and h_size == 2 * w_size and 2 * lo == dp_size and 2 * nl == LANES
        total_points = nb * dp_size * nc * nlat * nlon
        fwd_np, inv_np = dft_tables(nlon, nm, h_size)
        any_spec = pl.BlockSpec(memory_space=pl.ANY)
        vmem_spec = pl.BlockSpec(memory_space=pltpu.VMEM)
        sds = lambda *s: jax.ShapeDtypeStruct(s, F32)
        vm = lambda *s: pltpu.VMEM(s, F32)
        dma = lambda *s: pltpu.SemaphoreType.DMA(s)
        n_rows = 2 * nc + w_out.shape[0]
        n_z, n_h, n_w = n_rows // dp_size, n_rows // dp_size // h_size, n_rows // dp_size // h_size // w_size
        home = vm(nb, nt, npl, nc)
        woven = vm(nb, w_size, ntp, npl, LANES)
        order = vm(nb, 16 * nlat // 2, LANES)
        degree = vm(nb, 8 * nl, LANES)
        owner = vm(nb, h_size, 8 * lo, w_size * LANES)
        saved = vm(nb, lo, 2 * nm, nc)
        cuts = 1
        results = pl.pallas_call(
            functools.partial(block_kernel, (dp_size, h_size, w_size), total_points),
            name="block",
            out_shape=[sds(nb, nt, npl, nc), sds(2, lo * w_size, nc, nc), sds(nc, 2 * nc), sds(2 * nc, nc), sds(1, 1)],
            in_specs=[any_spec] * 10,
            out_specs=[any_spec] * 4 + [vmem_spec],
            scratch_shapes=[
                vm(*leg_fwd.shape[:1], nt, nl), vm(*leg_fwd.shape[:1], nt, nl), pltpu.SMEM((nt,), F32), pltpu.VMEM(w_in.shape, BF16),
                pltpu.VMEM(w_out.shape, BF16), vm(2 * nm, nlon), vm(2 * nm, nlon), vm(nlon, 2 * nm), vm(nlon, 2 * nm),
                home, home, home, woven, vm(nb, ntp, nlon, LANES), woven, woven,
                vm(nb, h_size, 16 * ntp, LANES), order, order, order, vm(nb, h_size, 16 * ntp, LANES), vm(nb, h_size, 16 * ntp, LANES),
                degree, owner, owner, vm(nb, h_size, w_size, 8 * lo, LANES), degree, degree, saved, saved,
                vm(dp_size, nb, 2 * nm, nc), vm(dp_size, nb, 2 * nm, LANES),
                vm(8, nc), vm(h_size, 8, nc), vm(8, nc), vm(w_size, 8, nc),
                vm(leg_fwd.shape[0], nt, 2 * nl), vm(w_size, leg_fwd.shape[0], nt, 2 * nl), vm(8, nlat, 2 * nl),
                vm(8, 2 * nl, nlat // 2), vm(8, 2 * nl, nlat // 2), vm(8, nlat, nl), vm(8, nlat, nl),
                vm(2, lo, nc, nc),
                vm(n_rows, nc), vm(dp_size, n_z, nc), vm(n_z, nc), vm(h_size, n_h, nc), vm(n_h, nc), vm(w_size, n_w, nc), vm(n_w, nc),
                vm(n_h, nc), vm(n_z, nc), vm(n_rows, nc),
                vm(8, nc), vm(dp_size, 8, nc), vm(8, nc), vm(h_size, 8, nc), vm(8, nc), vm(w_size, 8, nc),
                vm(cuts, 2, nc // cuts, LANES), vm(cuts, w_size, 2, nc // cuts, LANES),
            ] + [dma(nb, PARTS, 2)] * 8 + [dma(nb, 2)] * 6 + [dma(nb, 2), dma(nb, PARTS, 2), dma(4, 2), dma(3, 2), dma(1), dma(6, 2), dma(3, 2),
                 dma(cuts, w_size, 2), dma(cuts, 4, w_size, 2), dma(3), dma(7)],
            compiler_params=pltpu.CompilerParams(collective_id=0, has_side_effects=True, vmem_limit_bytes=62 * 1024 * 1024),
        )(field.transpose(0, 2, 3, 1), target.transpose(0, 2, 3, 1), leg_fwd.transpose(0, 2, 1), leg_inv.transpose(0, 2, 1),
          spec_w, lat_weight, w_in, w_out, jnp.asarray(fwd_np), jnp.asarray(inv_np))
        d_x, g_spec, g_in, g_out = hand_on(results[:4])
        loss = results[4]
        return loss.reshape(()), d_x.transpose(0, 3, 1, 2), g_spec, g_in, g_out

    grid_spec = P("dp", None, "h", "w")
    table_spec = P("w", None, "h")
    kernel_spec = P(None, "h", None, None)
    return jax.shard_map(local_step, mesh=mesh, in_specs=(grid_spec, grid_spec, P("h"), table_spec, table_spec, P(), P(), P()), out_specs=(P(), grid_spec, kernel_spec, P(), P()), check_vma=False)
```

```python
import functools
import jax
import jax.numpy as jnp
import numpy as np
from jax import lax
from jax.experimental import pallas as pl
from jax.experimental.pallas import tpu as pltpu
from jax.sharding import PartitionSpec as P

NORM_EPS = 1e-5
PRECISE = lax.Precision.HIGHEST
MESH = pl.DeviceIdType.MESH
F32 = jnp.float32
BF16 = jnp.bfloat16
GELU_C = float(np.sqrt(2.0 / np.pi))
GELU_A = 0.044715
LANES = 128
NN = (((1,), (0,)), ((), ()))
NT = (((1,), (1,)), ((), ()))
TN = (((0,), (0,)), ((), ()))


def dot(a, b, dims=NN):
    return lax.dot_general(a, b, dims, precision=PRECISE, preferred_element_type=F32)


def bdot(a, b, dims=NN):
    return lax.dot_general(a, b, dims, preferred_element_type=F32)


def dft_tables(lon_count, num_modes, h_size):
    modes, lons = np.arange(num_modes), np.arange(lon_count)
    angle = 2.0 * np.pi * ((modes[:, None] * lons[None, :]) % lon_count) / lon_count
    fwd = np.stack([np.cos(angle), -np.sin(angle)], 0) * lon_count ** -0.5
    inv = fwd * np.where(modes == 0, 1.0, 2.0)[None, :, None]

    def rows(table):
        table = table.reshape(2, h_size, num_modes // h_size, lon_count).transpose(1, 0, 2, 3)
        return table.reshape(2 * num_modes, lon_count).astype(np.float32)

    return rows(fwd), rows(inv)


def drain(ref, sem):
    pltpu.make_async_copy(ref, ref, sem).wait()


def rows_at(i, n):
    return pl.ds(pl.multiple_of(i * n, n), n)


def lanes_at(i):
    return pl.ds(pl.multiple_of(i * LANES, LANES), LANES)


def push(src, dst, sems, device):
    pltpu.make_async_remote_copy(src_ref=src, dst_ref=dst, send_sem=sems.at[0], recv_sem=sems.at[1],
                                 device_id=device, device_id_type=MESH).start()


def keep(src, dst, sems):
    pltpu.make_async_copy(src, dst, sems.at[1]).start()


def flip(v):
    return pltpu.roll(v, LANES // 2, 1)


def low(v):
    return lax.broadcasted_iota(jnp.int32, v.shape, 1) < LANES // 2


def weave(a, b):
    return jnp.where(low(a), a, flip(b)), jnp.where(low(a), flip(a), b)


def weave_wide(tiles):
    pairs = [weave(tiles[j], tiles[j + 1]) for j in range(0, len(tiles), 2)]
    return jnp.concatenate([p[0] for p in pairs], axis=1), jnp.concatenate([p[1] for p in pairs], axis=1)


def weave_tiles(a, b):
    out = []
    for j in range(0, a.shape[1], LANES):
        out.extend(weave(a[:, j:j + LANES], b[:, j:j + LANES]))
    return out


PARTS = 2
ORDER = " ".join((
    'go', 'sX20', 'sX21', 'sX00', 'tb1', 'fd20', 'tb2', 'fd21', 'sX01', 'sX11',
    'fd00', 'tb3', 'fl2', 'fd01', 'st2', 'sX10', 'fd11', 'fo2', 'fl0', 'fd10',
    'fu2', 'fo0', 'fl1', 'fi20', 'sY20', 'fi21', 'sY21', 'fu0', 'fo1', 'fi00',
    'sY00', 'fi01', 'sY01', 'fu1', 'pw00', 'sD00', 'fi10', 'sY10', 'fi11', 'pw21',
    'pw20', 'bd00', 'pw01', 'sY11', 'sD01', 'pw10', 'sD10', 'pw11', 'gw1', 'sD11',
    'sD21', 'bd01', 'sD20', 'bd10', 'bl0', 'bd11', 'gw2', 'bd21', 'bl1', 'gw3',
    'bd20', 'bo0', 'gw4', 'bl2', 'gw5', 'bu0', 'bo1', 'bo2', 'gw6', 'pj1',
    'bi00', 'sN00', 'gs1', 'gs20', 'bi01', 'pj2', 'bu2', 'gs300', 'sN01', 'bu1',
    'gs303', 'gs302', 'bi21', 'fn00', 'end', 'sN21', 'gs301', 'bi11', 'sN11', 'gs403',
    'bi10', 'fn21', 'gs400', 'bi20', 'sN10', 'fn01', 'fn11', 'sN20', 'gs401', 'gs402',
    'fn10', 'gs501', 'gs502', 'gs500', 'gs503', 'fn20',
))


def block_kernel(sizes, total_points,
                 x, tgt, leg_p_in, leg_q_in, spec_w, lat_in, w1_in, w2_in, f_in, g_in,
                 dout, gs_out, gin_out, gout_out, loss_out,
                 leg_p, leg_q, lat, w1, w2, f_tab, g_tab, ft_tab, gt_tab,
                 xh, th, pk, rows, yrow, hy,
                 xs, sr, dsr, ys, yr, dyr, als, ar, dar, bs, br, dbr, asave, dsave, aall, dall,
                 st_s, st_h, st_m, st_w, tab_s, tab_w, tab, down_p, down_q, up_p, up_q, ker,
                 gw, gw_z, gw_zs, gw_h, gw_hs, gw_w, gw_ws, gw_w2, gw_h2, gw_f,
                 ls, ls_z, ls_zs, ls_h, ls_hs, ls_w, gs_sum, gs_w,
                 sem_x, sem_y, sem_d, sem_n, sem_s, sem_ds, sem_u, sem_du, sem_a, sem_da, sem_b, sem_db, sem_az, sem_dz,
                 sem_in, sem_st, sem_tab, sem_k, sem_gw, sem_ls, sem_gs, sem_gf, sem_fin, sem_small):
    dp_size, h_size, w_size = sizes
    dp, h, w = lax.axis_index("dp"), lax.axis_index("h"), lax.axis_index("w")
    ndev = h_size * w_size
    me = h * w_size + w
    nb, nt, npl, nc = x.shape
    ntp = nt // 2
    part = ntp // PARTS
    nlon = npl * w_size
    nlat = nt * h_size
    nl = als.shape[1] // 8
    l_own = nl // ndev
    piece = 8 * l_own
    unsent, coming = {}, {}

    def got(key):
        coming.pop(key)()

    def peer(k):
        return (h + k // w_size) % h_size, (w + k % w_size) % w_size

    barrier = pltpu.get_barrier_semaphore()

    def meet(k, _):
        h2, w2_ = peer(k)
        pl.semaphore_signal(barrier, inc=1, device_id={"h": h2, "w": w2_}, device_id_type=MESH)
        return 0

    def meet_dp(k, _):
        pl.semaphore_signal(barrier, inc=1, device_id={"dp": (dp + k) % dp_size}, device_id_type=MESH)
        return 0

    lax.fori_loop(1, ndev, meet, 0)
    lax.fori_loop(1, dp_size, meet_dp, 0)
    loads = [pltpu.make_async_copy(x.at[b], xh.at[b], sem_in.at[b, 0]) for b in range(nb)]
    load_t = [pltpu.make_async_copy(tgt.at[b], th.at[b], sem_in.at[b, 1]) for b in range(nb)]
    load_k = pltpu.make_async_copy(spec_w.at[:, pl.ds(me * l_own, l_own)], ker, sem_k.at[0])
    small = [pltpu.make_async_copy(src, dst, sem_small.at[i]) for i, (src, dst) in enumerate((
        (leg_p_in, leg_p), (leg_q_in, leg_q), (f_in, f_tab), (g_in, g_tab), (lat_in, lat), (w1_in, w1), (w2_in, w2)))]
    for c in loads + small[:4] + [load_k] + load_t + small[4:]:
        c.start()
    coming["k"] = load_k.wait
    coming["small"] = lambda: [c.wait() for c in small[4:]]
    coming.update({("t", b): load_t[b].wait for b in range(nb)})
    for ref in (ar, br, dar, dbr, st_s, gw, ls):
        ref[...] = jnp.zeros_like(ref)

    def settle(*keys):
        for key in keys or list(unsent):
            for wait in unsent.pop(key, []):
                wait()

    def along(axis, refs, sems, sent, key=None):
        size, index = {"dp": (dp_size, dp), "h": (h_size, h), "w": (w_size, w)}[axis]
        src, dst = refs(index)
        keep(src, dst, sems)

        def body(k, _):
            other = (index + k) % size
            src, dst = refs(other)
            push(src, dst, sems, {axis: other})
            return 0

        lax.fori_loop(1, size, body, 0)
        unsent.setdefault(key, []).append(lambda: drain(sent, sems.at[0]))

    def some(refs, sems, low_h, high_h, count, counts, key):
        src, dst = refs(h, w)
        keep(src, dst, sems)

        def one(h2, k):
            w2_ = (w + k) % w_size
            src, dst = refs(h2, w2_)
            push(src, dst, sems, {"h": h2, "w": w2_})

        for k in range(1, w_size):
            one(h, k)

        def body(h2, _):
            for k in range(w_size):
                one(h2, k)
            return 0

        lax.fori_loop(low_h, high_h, body, 0)
        unsent.setdefault(key, []).append(lambda: take(sems.at[0], count - 1, [n - 1 for n in counts]))

    def take(sem, count, counts):
        for n in counts:
            @pl.when(count == n)
            def _():
                drain(als.at[0, pl.ds(0, n * piece)], sem)

    n_orders, n_owners = (h + 1) * w_size, (h_size - h) * w_size
    counts = [w_size * n for n in range(1, h_size + 1)]
    pairs = lambda k: pl.ds(k * part, part)

    def at_rows(i, k):
        return pl.ds(pl.multiple_of(i * 16 * ntp + k * 16 * part, 16 * part), 16 * part)

    def send_home_rows(b, k, sem, name):
        along("w", lambda o: (pk.at[b, o, pairs(k)], rows.at[b, pairs(k), rows_at(w, npl)]), sem.at[b, k],
              pk.at[b, pl.ds(0, w_size - 1), pairs(k)], ("pk", b, k))
        coming[name, b, k] = lambda: drain(rows.at[b, pairs(k)], sem.at[b, k, 1])

    def send_rows_home(b, k, sem, name):
        along("w", lambda o: (yrow.at[b, o, pairs(k)], hy.at[b, w, pairs(k)]), sem.at[b, k],
              yrow.at[b, pl.ds(0, w_size - 1), pairs(k)], ("yrow", b, k))
        coming[name, b, k] = lambda: drain(hy.at[b, :, pairs(k)], sem.at[b, k, 1])

    def send_orders(b, k, dst, sem, name):
        along("h", lambda o: (xs.at[b, o, at_rows(0, k)], dst.at[b, at_rows(h, k)]), sem.at[b, k],
              xs.at[b, pl.ds(0, h_size - 1), at_rows(0, k)], ("xs", b, k))
        coming[name, b, k] = lambda: drain(xs.at[b, :, at_rows(0, k)], sem.at[b, k, 1])

    def send_lats(b, dst, sem, name):
        for k in range(PARTS):
            along("h", lambda o: (ys.at[b, at_rows(o, k)], dst.at[b, h, at_rows(0, k)]), sem.at[b, k],
                  xs.at[b, pl.ds(0, h_size - 1), at_rows(0, k)], ("ys", b))
            coming[name, b, k] = lambda k=k: drain(dst.at[b, :, at_rows(0, k)], sem.at[b, k, 1])

    def send_owner(b, dst, sem, name):
        some(lambda h2, w2_: (als.at[b, rows_at(h2 * w_size + w2_, piece)], dst.at[b, h, :, lanes_at(w)]), sem.at[b],
             h + 1, h_size, n_owners, counts, ("als", b))
        coming[name, b] = lambda: take(sem.at[b, 1], n_orders, counts)

    def send_back(b, dst, sem, name):
        some(lambda h2, w2_: (bs.at[b, h2, w2_], dst.at[b, rows_at(me, piece)]), sem.at[b],
             0, h, n_orders, counts, ("bs", b))
        coming[name, b] = lambda: take(sem.at[b, 1], n_owners, counts)

    def dft(b, k, table):
        settle(("xs", b, k))

        def body(n, _):
            i = 2 * n
            both = jnp.concatenate([rows[b, i], rows[b, i + 1]], axis=1)
            out = dot(table[...], both).reshape(h_size, 16, 2 * LANES)
            xs[b, :, rows_at(i, 16), :] = out[:, :, :LANES]
            xs[b, :, rows_at(i + 1, 16), :] = out[:, :, LANES:]
            return 0

        lax.fori_loop(k * part // 2, (k + 1) * part // 2, body, 0)

    def idft(b, k, table, src):
        settle(("yrow", b, k))

        def body(n, _):
            i = 2 * n
            both = jnp.concatenate([src[b, :, rows_at(i + j, 16), :].reshape(-1, LANES) for j in range(2)], axis=1)
            out = dot(table[...], both)
            for j in range(2):
                yrow[b, :, i + j] = out[:, j * LANES:(j + 1) * LANES].reshape(w_size, npl, LANES)
            return 0

        lax.fori_loop(k * part // 2, (k + 1) * part // 2, body, 0)

    def level(v):
        mean = jnp.mean(v, axis=0, keepdims=True)
        mean = 0.5 * (mean + flip(mean))
        return v - jnp.where(h == 0, mean, 0.0)

    def leg_down(b, table, src, fix):
        settle(("als", b))
        for m in range(8):
            parts = [src[b, pl.ds(ri * 8 + m, ntp * h_size, stride=16), :] for ri in range(2)]
            if fix and m == 0:
                parts[0] = level(parts[0])
            out = dot(table[m], jnp.concatenate(parts, axis=1))
            re0, re1 = out[:nl, :LANES], out[nl:, :LANES]
            im0, im1 = out[:nl, LANES:], out[nl:, LANES:]
            als[b, pl.ds(m, nl, stride=8), :] = jnp.where(low(re0), re0, im1) + flip(jnp.where(low(re0), im0, re1))

    def leg_up(b, table, src, fix):
        settle(("ys", b))
        for m in range(8):
            out = dot(table[m], src[b, pl.ds(m, nl, stride=8), :])
            re, im = weave(out[:nlat // 2], out[nlat // 2:])
            if fix and m == 0:
                re = level(re)
            ys[b, pl.ds(m, ntp * h_size, stride=16), :] = re
            ys[b, pl.ds(8 + m, ntp * h_size, stride=16), :] = im

    def owned(b, l, src):
        tiles = [src[b, :, l * 8:(l + 1) * 8, j * LANES:(j + 1) * LANES].reshape(-1, LANES) for j in range(w_size)]
        return weave_wide(tiles)

    def put_back(b, l, re, im):
        for j, tile in enumerate(weave_tiles(re, im)):
            bs[b, :, j, l * 8:(l + 1) * 8, :] = tile.reshape(h_size, 8, LANES)

    def put_rows(b, i, v0, v1):
        for j, tile in enumerate(weave_tiles(v0, v1)):
            pk[b, j, i] = tile

    def get_rows(b, i):
        return weave_wide([hy[b, j, i] for j in range(w_size)])

    count = nt * npl
    n_tab = tab_s.shape[0] // dp_size

    def combine(stats, n):
        mean = jnp.mean(stats, axis=0)
        dev = stats - mean[None]
        dev2 = jnp.sum(dev * dev, axis=0)
        m2 = jnp.sum(stats, axis=0)
        return [(mean[2 * b:2 * b + 1], m2[2 * b + 1:2 * b + 2] + n * dev2[2 * b:2 * b + 1]) for b in range(nb)]

    def go():
        for b in range(nb):
            loads[b].wait()

            def pack(i, total, b=b):
                v0, v1 = xh[b, i], xh[b, i + ntp]
                put_rows(b, i, v0, v1)
                return total + jnp.sum(v0 + v1, axis=0, keepdims=True)

            mean = lax.fori_loop(0, ntp, pack, jnp.zeros((1, nc), F32)) / count

            def spread(t, total, b=b, mean=mean):
                d = xh[b, t] - mean
                return total + jnp.sum(d * d, axis=0, keepdims=True)

            st_s[2 * b:2 * b + 1, :] = mean
            st_s[2 * b + 1:2 * b + 2, :] = lax.fori_loop(0, nt, spread, jnp.zeros((1, nc), F32))
        for c in small[:4]:
            c.wait()
        tab_s[:, :, :nl] = leg_p[...]
        tab_s[:, :, nl:] = leg_q[...]
        ft_tab[...] = f_tab[...].T
        gt_tab[...] = g_tab[...].T
        pl.semaphore_wait(barrier, ndev - 1 + dp_size - 1)
        along("w", lambda o: (st_s, st_w.at[w]), sem_st.at[0], st_w.at[pl.ds(0, w_size - 1)], "st")
        coming["st"] = lambda: drain(st_w, sem_st.at[0, 1])
        along("w", lambda o: (tab_s.at[rows_at(dp, n_tab)], tab_w.at[w, rows_at(dp, n_tab)]), sem_tab.at[0], tab_w.at[pl.ds(0, w_size - 1), pl.ds(0, n_tab)])
        coming["tab"] = lambda: drain(tab_w.at[:, pl.ds(0, n_tab)], sem_tab.at[0, 1])

    def st2():
        got("st")
        st_m[...] = jnp.zeros_like(st_m)
        for b, (mean, m2) in enumerate(combine(st_w[...], count)):
            st_m[2 * b:2 * b + 1, :] = mean
            st_m[2 * b + 1:2 * b + 2, :] = m2
        along("h", lambda o: (st_m, st_h.at[h]), sem_st.at[1], st_h.at[pl.ds(0, h_size - 1)], "st")
        coming["st2"] = lambda: drain(st_h, sem_st.at[1, 1])

    means, scales = [], []

    def st3():
        got("st2")
        for mean, m2 in combine(st_h[...], count * w_size):
            means.append(mean)
            scales.append(lax.rsqrt(m2 / (count * ndev) + NORM_EPS))

    def tb1():
        got("tab")
        share = tab_w.at[:, rows_at(dp, n_tab)]
        for k in range(1, dp_size):
            push(share, share, sem_tab.at[2], {"dp": (dp + k) % dp_size})
        others = tab_w.at[:, pl.ds(0, (dp_size - 1) * n_tab)]
        unsent.setdefault(None, []).append(lambda: drain(others, sem_tab.at[2, 0]))
        coming["tab1"] = lambda: drain(others, sem_tab.at[2, 1])

    def tb2():
        got("tab1")
        along("h", lambda o: (tab_w.at[o // 2, rows_at(o % 2, 8)], tab.at[:, rows_at(h, nt)]), sem_tab.at[1], tab.at[:, pl.ds(0, nlat - nt)])
        coming["tab2"] = lambda: drain(tab, sem_tab.at[1, 1])

    def tb3():
        got("tab2")
        for m in range(8):
            both = tab[m].reshape(h_size, 2, ntp, 2 * nl)
            t0, t1 = both[:, 0].reshape(-1, 2 * nl), both[:, 1].reshape(-1, 2 * nl)
            for k, (down, up) in enumerate(((down_p, up_p), (down_q, up_q))):
                a, z = t0[:, k * nl:(k + 1) * nl], t1[:, k * nl:(k + 1) * nl]
                up[m, :nlat // 2, :] = a
                up[m, nlat // 2:, :] = z
                down[m, :nl, :] = a.T
                down[m, nl:, :] = z.T

    def sX(b, k):
        send_home_rows(b, k, sem_x, "x")

    def fd(b, k):
        got(("x", b, k))
        dft(b, k, f_tab)
        send_orders(b, k, sr, sem_s, "s")

    def fl(b):
        for k in range(PARTS):
            got(("s", b, k))
        leg_down(b, down_p, sr, True)
        send_owner(b, ar, sem_a, "a")

    def fo(b):
        if not scales:
            got("k")
            st3()
        got(("a", b))
        settle(("bs", b))
        for l in range(l_own):
            re, im = owned(b, l, ar)
            a = jnp.concatenate([re, im], axis=0) * scales[b]
            asave[b, l] = a
            n = a.shape[0] // 2
            own, other = dot(a, ker[0, l]), dot(a, ker[1, l])
            put_back(b, l, own[:n] - other[n:], own[n:] + other[:n])
        send_back(b, br, sem_b, "b")
        along("dp", lambda o: (asave.at[b, o // 2], aall.at[dp, b]), sem_az.at[b], aall.at[pl.ds(0, dp_size - 1), b])
        coming["az", b] = lambda: drain(aall.at[:, b], sem_az.at[b, 1])

    def fu(b):
        got(("b", b))
        leg_up(b, up_q, br, False)
        send_lats(b, yr, sem_u, "u")

    def fi(b, k):
        got(("u", b, k))
        idft(b, k, gt_tab, yr)

    def sY(b, k):
        send_rows_home(b, k, sem_y, "y")

    def pw(b, k):
        got(("y", b, k))
        if ("t", b) in coming:
            got(("t", b))
        if "small" in coming:
            got("small")
        settle(("pk", b, k))

        def body(n, _):
            lats = [2 * n, 2 * n + ntp, 2 * n + 1, 2 * n + 1 + ntp]
            y = jnp.concatenate([v for j in range(2) for v in get_rows(b, 2 * n + j)], axis=0)
            yb = y.astype(BF16)
            hid = bdot(yb, w1[...])
            th_ = jnp.tanh(GELU_C * (hid + GELU_A * (hid * hid * hid)))
            act = (hid * (0.5 * (1.0 + th_))).astype(BF16)
            resid = y + bdot(act, w2[...])
            parts = []
            for j, t in enumerate(lats):
                r = resid[j * npl:(j + 1) * npl] + xh[b, t] - th[b, t]
                d = lat[t] * r
                ls[...] += jnp.sum((d * r).reshape(-1, 8, nc), axis=0)
                dout[b, t] = d
                parts.append(d)
            d = jnp.concatenate(parts, axis=0)
            db = d.astype(BF16)
            gw[2 * nc:, :] += bdot(act, db, TN)
            slope = 0.5 * (1.0 + th_) + (0.5 * GELU_C) * hid * (1.0 - th_ * th_) * (1.0 + (3.0 * GELU_A) * (hid * hid))
            dh = (bdot(db, w2[...], NT) * slope).astype(BF16)
            gin = bdot(yb, dh, TN)
            gw[:nc, :] += gin[:, :nc]
            gw[nc:2 * nc, :] += gin[:, nc:]
            dy = d + bdot(dh, w1[...], NT)
            for j in range(2):
                put_rows(b, 2 * n + j, dy[2 * j * npl:(2 * j + 1) * npl], dy[(2 * j + 1) * npl:(2 * j + 2) * npl])
            return 0

        lax.fori_loop(k * part // 2, (k + 1) * part // 2, body, 0)

    def sD(b, k):
        send_home_rows(b, k, sem_d, "d")

    def bd(b, k):
        got(("d", b, k))
        dft(b, k, g_tab)
        send_orders(b, k, dsr, sem_ds, "ds")

    def bl(b):
        for k in range(PARTS):
            got(("ds", b, k))
        leg_down(b, down_q, dsr, False)
        send_owner(b, dar, sem_da, "da")

    def bo(b):
        got(("da", b))
        settle(("bs", b), "st")
        s2 = jnp.zeros((1, nc), F32)
        for l in range(l_own):
            re, im = owned(b, l, dar)
            d = jnp.concatenate([re, im], axis=0)
            dsave[b, l] = d
            n = d.shape[0] // 2
            own, other = dot(d, ker[0, l], NT), dot(d, ker[1, l], NT)
            re, im = own[:n] + other[n:], own[n:] - other[:n]
            put_back(b, l, re, im)
            s2 = s2 + jnp.sum(re * asave[b, l, :n] + im * asave[b, l, n:], axis=0, keepdims=True)
        send_back(b, dbr, sem_db, "db")
        along("dp", lambda o: (dsave.at[b, o // 2, :, lanes_at(o % 2)], dall.at[dp, b]), sem_dz.at[b], dall.at[pl.ds(0, dp_size - 1), b])
        coming["dz", b] = lambda: drain(dall.at[:, b], sem_dz.at[b, 1])
        st_s[b:b + 1, :] = s2

    def bu(b):
        got(("db", b))
        leg_up(b, up_p, dbr, True)
        send_lats(b, dyr, sem_du, "du")

    def bi(b, k):
        got(("du", b, k))
        idft(b, k, ft_tab, dyr)

    def sN(b, k):
        send_rows_home(b, k, sem_n, "n")

    def pj1():
        st_s[nb:, :] = jnp.zeros_like(st_s[nb:, :])
        along("w", lambda o: (st_s, st_w.at[w]), sem_st.at[2], st_w.at[pl.ds(0, w_size - 1)])
        coming["pj"] = lambda: drain(st_w, sem_st.at[2, 1])

    def pj2():
        got("pj")
        st_m[...] = jnp.sum(st_w[...], axis=0)
        along("h", lambda o: (st_m, st_h.at[h]), sem_st.at[3], st_h.at[pl.ds(0, h_size - 1)])
        coming["pj2"] = lambda: drain(st_h, sem_st.at[3, 1])

    proj = []

    def fn(b, k):
        if not proj:
            got("pj2")
            proj.append(jnp.sum(st_h[...], axis=0) / (count * ndev))
        got(("n", b, k))

        def body(i, _):
            for t, dn in zip((i, i + ntp), get_rows(b, i)):
                normed = (xh[b, t] - means[b]) * scales[b]
                dout[b, t] = dout[b, t] + scales[b] * (dn - normed * proj[0][b:b + 1])
            return 0

        lax.fori_loop(k * part, (k + 1) * part, body, 0)

    n_z, n_h, n_w = gw_zs.shape[0], gw_hs.shape[0], gw_ws.shape[0]

    def gw1():
        along("dp", lambda o: (gw.at[rows_at(o, n_z)], gw_z.at[dp]), sem_gw.at[0], gw_z.at[pl.ds(0, dp_size - 1)])
        along("dp", lambda o: (ls, ls_z.at[dp]), sem_ls.at[0], ls_z.at[pl.ds(0, dp_size - 1)])
        coming["gw1"] = lambda: (drain(gw_z, sem_gw.at[0, 1]), drain(ls_z, sem_ls.at[0, 1]))

    def gw2():
        got("gw1")
        gw_zs[...] = jnp.sum(gw_z[...], axis=0)
        ls_zs[...] = jnp.sum(ls_z[...], axis=0)
        along("h", lambda o: (gw_zs.at[rows_at(o, n_h)], gw_h.at[h]), sem_gw.at[1], gw_h.at[pl.ds(0, h_size - 1)])
        along("h", lambda o: (ls_zs, ls_h.at[h]), sem_ls.at[1], ls_h.at[pl.ds(0, h_size - 1)])
        coming["gw2"] = lambda: (drain(gw_h, sem_gw.at[1, 1]), drain(ls_h, sem_ls.at[1, 1]))

    def gw3():
        got("gw2")
        gw_hs[...] = jnp.sum(gw_h[...], axis=0)
        ls_hs[...] = jnp.sum(ls_h[...], axis=0)
        along("w", lambda o: (gw_hs.at[rows_at(o, n_w)], gw_w.at[w]), sem_gw.at[2], gw_w.at[pl.ds(0, w_size - 1)])
        along("w", lambda o: (ls_hs, ls_w.at[w]), sem_ls.at[2], ls_w.at[pl.ds(0, w_size - 1)])
        coming["gw3"] = lambda: (drain(gw_w, sem_gw.at[2, 1]), drain(ls_w, sem_ls.at[2, 1]))

    def gw4():
        got("gw3")
        gw_ws[...] = jnp.sum(gw_w[...], axis=0)
        loss_out[...] = jnp.sum(ls_w[...], keepdims=True).reshape(1, 1) / total_points
        along("w", lambda o: (gw_ws, gw_w2.at[rows_at(w, n_w)]), sem_gw.at[3], gw_w2.at[pl.ds(0, (w_size - 1) * n_w)])
        coming["gw4"] = lambda: drain(gw_w2, sem_gw.at[3, 1])

    def gw5():
        got("gw4")
        along("h", lambda o: (gw_w2, gw_h2.at[rows_at(h, n_h)]), sem_gw.at[4], gw_h2.at[pl.ds(0, (h_size - 1) * n_h)])
        coming["gw5"] = lambda: drain(gw_h2, sem_gw.at[4, 1])

    def gw6():
        got("gw5")
        along("dp", lambda o: (gw_h2, gw_f.at[rows_at(dp, n_z)]), sem_gw.at[5], gw_f.at[pl.ds(0, (dp_size - 1) * n_z)])
        coming["gw6"] = lambda: drain(gw_f, sem_gw.at[5, 1])

    def end():
        got("gw6")
        outs = [(gw_f.at[:nc], gin_out.at[:, :nc]), (gw_f.at[nc:2 * nc], gin_out.at[:, nc:]), (gw_f.at[2 * nc:], gout_out)]
        for i, (src, dst) in enumerate(outs):
            pltpu.make_async_copy(src, dst, sem_fin.at[i]).start()
            unsent.setdefault(None, []).append(lambda dst=dst, i=i: drain(dst, sem_fin.at[i]))

    cuts, _, n_g, _ = gs_sum.shape

    def gs1():
        for b in range(nb):
            got(("az", b))
            got(("dz", b))
        d = dall[...].reshape(dp_size * nb, 2, -1, LANES)
        turned = jnp.concatenate([d[:, 1:], -d[:, :1]], axis=1)
        both = jnp.concatenate([d.reshape(-1, LANES), turned.reshape(-1, LANES)], axis=1)
        out = dot(aall[...].reshape(-1, nc), both, TN)
        for q in range(cuts):
            for p in range(2):
                gs_sum[q, p] = out[q * n_g:(q + 1) * n_g, p * LANES:(p + 1) * LANES]

    def gs2(q):
        keep(gs_sum.at[q], gs_w.at[q, 0], sem_gs.at[q, 0])
        for k in (1, 3, 2):
            push(gs_sum.at[q], gs_w.at[q, k], sem_gs.at[q, k], {"w": (w + k) % w_size})
            unsent.setdefault(None, []).append(lambda k=k: drain(gs_w.at[q, k], sem_gs.at[q, k, 0]))
        coming.update({("gs", q, k): lambda k=k: drain(gs_w.at[q, k], sem_gs.at[q, k, 1]) for k in range(w_size)})

    right, left = (dp + 1) % dp_size, (dp + dp_size - 1) % dp_size
    block_at = lambda d, k, q: gs_out.at[:, l_own * ((w + w_size - k) % w_size) + d // 2, rows_at(q, n_g), lanes_at(d % 2)]

    def gs3(q, k):
        got(("gs", q, k))
        pltpu.make_async_copy(gs_w.at[q, k], block_at(dp, k, q), sem_gf.at[q, 3, k, 0]).start()
        push(gs_w.at[q, k], block_at(dp, k, q), sem_gf.at[q, 0, k], {"dp": right})
        push(gs_w.at[q, k], block_at(dp, k, q), sem_gf.at[q, 1, k], {"dp": left})

    def gs4(q, k):
        way = 0 if k < w_size // 2 else 1
        source, target = (left, right) if way == 0 else (right, left)
        drain(gs_w.at[q, k], sem_gf.at[q, way, k, 1])
        push(block_at(source, k, q), block_at(source, k, q), sem_gf.at[q, 2, k], {"dp": target})

    def gs5(q, k):
        drain(gs_w.at[q, k], sem_gf.at[q, 1 if k < w_size // 2 else 0, k, 1])
        drain(gs_w.at[q, k], sem_gf.at[q, 2, k, 1])
        for i in range(4):
            drain(gs_w.at[q, k], sem_gf.at[q, i, k, 0])

    scope = dict(locals())
    for name in ORDER.split():
        call = name.rstrip("0123456789") or name
        if name in scope:
            scope[name]()
        elif name[:3] in scope:
            scope[name[:3]](*map(int, name[3:]))
        else:
            scope[call](*map(int, name[len(call):]))
    assert not coming
    settle()


def hand_on_kernel(*refs):
    n = len(refs) // 2
    copies = [pltpu.make_async_copy(refs[i], refs[n + i], refs[2 * n].at[i]) for i in range(n)]
    for c in copies:
        c.start()
    for c in copies:
        c.wait()


def hand_on(arrays):
    return pl.pallas_call(
        hand_on_kernel, name="hand_on",
        out_shape=[jax.ShapeDtypeStruct(a.shape, F32) for a in arrays],
        in_specs=[pl.BlockSpec(memory_space=pltpu.VMEM)] * len(arrays), out_specs=[pl.BlockSpec(memory_space=pl.ANY)] * len(arrays),
        scratch_shapes=[pltpu.SemaphoreType.DMA((len(arrays),))],
        compiler_params=pltpu.CompilerParams(vmem_limit_bytes=12 * 1024 * 1024),
    )(*[pltpu.with_memory_space_constraint(a, pltpu.VMEM) for a in arrays])


def solution(mesh):
    dp_size, w_size, h_size = mesh.shape["dp"], mesh.shape["w"], mesh.shape["h"]

    def local_step(field, target, lat_weight, leg_fwd, leg_inv, spec_w, w_in, w_out):
        nb, nc, nt, npl = field.shape
        nlon = npl * w_size
        ntp = nt // 2
        nm = leg_fwd.shape[0] * w_size
        ndev = h_size * w_size
        nlat = nt * h_size
        nl = leg_fwd.shape[1]
        lo = nl // ndev
        assert nm == 8 * h_size and nc == w_size * LANES // 2 and h_size == 2 * w_size and 2 * lo == dp_size and 2 * nl == LANES
        total_points = nb * dp_size * nc * nlat * nlon
        fwd_np, inv_np = dft_tables(nlon, nm, h_size)
        any_spec = pl.BlockSpec(memory_space=pl.ANY)
        vmem_spec = pl.BlockSpec(memory_space=pltpu.VMEM)
        sds = lambda *s: jax.ShapeDtypeStruct(s, F32)
        vm = lambda *s: pltpu.VMEM(s, F32)
        dma = lambda *s: pltpu.SemaphoreType.DMA(s)
        n_rows = 2 * nc + w_out.shape[0]
        n_z, n_h, n_w = n_rows // dp_size, n_rows // dp_size // h_size, n_rows // dp_size // h_size // w_size
        home = vm(nb, nt, npl, nc)
        woven = vm(nb, w_size, ntp, npl, LANES)
        order = vm(nb, 16 * nlat // 2, LANES)
        degree = vm(nb, 8 * nl, LANES)
        owner = vm(nb, h_size, 8 * lo, w_size * LANES)
        saved = vm(nb, lo, 2 * nm, nc)
        cuts = 1
        results = pl.pallas_call(
            functools.partial(block_kernel, (dp_size, h_size, w_size), total_points),
            name="block",
            out_shape=[vm(nb, nt, npl, nc), vm(2, lo * w_size, nc, nc), vm(nc, 2 * nc), vm(2 * nc, nc), sds(1, 1)],
            in_specs=[any_spec] * 10,
            out_specs=[vmem_spec] * 5,
            scratch_shapes=[
                vm(*leg_fwd.shape[:1], nt, nl), vm(*leg_fwd.shape[:1], nt, nl), pltpu.SMEM((nt,), F32), pltpu.VMEM(w_in.shape, BF16),
                pltpu.VMEM(w_out.shape, BF16), vm(2 * nm, nlon), vm(2 * nm, nlon), vm(nlon, 2 * nm), vm(nlon, 2 * nm),
                home, home, woven, vm(nb, ntp, nlon, LANES), woven, woven,
                vm(nb, h_size, 16 * ntp, LANES), order, order, order, vm(nb, h_size, 16 * ntp, LANES), vm(nb, h_size, 16 * ntp, LANES),
                degree, owner, owner, vm(nb, h_size, w_size, 8 * lo, LANES), degree, degree, saved, saved,
                vm(dp_size, nb, 2 * nm, nc), vm(dp_size, nb, 2 * nm, LANES),
                vm(8, nc), vm(h_size, 8, nc), vm(8, nc), vm(w_size, 8, nc),
                vm(leg_fwd.shape[0], nt, 2 * nl), vm(w_size, leg_fwd.shape[0], nt, 2 * nl), vm(8, nlat, 2 * nl),
                vm(8, 2 * nl, nlat // 2), vm(8, 2 * nl, nlat // 2), vm(8, nlat, nl), vm(8, nlat, nl),
                vm(2, lo, nc, nc),
                vm(n_rows, nc), vm(dp_size, n_z, nc), vm(n_z, nc), vm(h_size, n_h, nc), vm(n_h, nc), vm(w_size, n_w, nc), vm(n_w, nc),
                vm(n_h, nc), vm(n_z, nc), vm(n_rows, nc),
                vm(8, nc), vm(dp_size, 8, nc), vm(8, nc), vm(h_size, 8, nc), vm(8, nc), vm(w_size, 8, nc),
                vm(cuts, 2, nc // cuts, LANES), vm(cuts, w_size, 2, nc // cuts, LANES),
            ] + [dma(nb, PARTS, 2)] * 8 + [dma(nb, 2)] * 6 + [dma(nb, 2), dma(4, 2), dma(3, 2), dma(1), dma(6, 2), dma(3, 2),
                 dma(cuts, w_size, 2), dma(cuts, 4, w_size, 2), dma(3), dma(7)],
            compiler_params=pltpu.CompilerParams(collective_id=0, has_side_effects=True, vmem_limit_bytes=54 * 1024 * 1024),
        )(field.transpose(0, 2, 3, 1), target.transpose(0, 2, 3, 1), leg_fwd.transpose(0, 2, 1), leg_inv.transpose(0, 2, 1),
          spec_w, lat_weight, w_in, w_out, jnp.asarray(fwd_np), jnp.asarray(inv_np))
        d_x, g_spec, g_in, g_out = hand_on(results[:4])
        loss = results[4]
        return loss.reshape(()), d_x.transpose(0, 3, 1, 2), g_spec, g_in, g_out

    grid_spec = P("dp", None, "h", "w")
    table_spec = P("w", None, "h")
    kernel_spec = P(None, "h", None, None)
    return jax.shard_map(local_step, mesh=mesh, in_specs=(grid_spec, grid_spec, P("h"), table_spec, table_spec, P(), P(), P()), out_specs=(P(), grid_spec, kernel_spec, P(), P()), check_vma=False)
```

```python
import functools
import jax
import jax.numpy as jnp
import numpy as np
from jax import lax
from jax.experimental import pallas as pl
from jax.experimental.pallas import tpu as pltpu
from jax.sharding import PartitionSpec as P

NORM_EPS = 1e-5
PRECISE = lax.Precision.HIGHEST
MESH = pl.DeviceIdType.MESH
F32 = jnp.float32
BF16 = jnp.bfloat16
GELU_C = float(np.sqrt(2.0 / np.pi))
GELU_A = 0.044715
LANES = 128
NN = (((1,), (0,)), ((), ()))
NT = (((1,), (1,)), ((), ()))
TN = (((0,), (0,)), ((), ()))


def dot(a, b, dims=NN):
    return lax.dot_general(a, b, dims, precision=PRECISE, preferred_element_type=F32)


def bdot(a, b, dims=NN):
    return lax.dot_general(a, b, dims, preferred_element_type=F32)


def dft_tables(lon_count, num_modes, h_size):
    modes, lons = np.arange(num_modes), np.arange(lon_count)
    angle = 2.0 * np.pi * ((modes[:, None] * lons[None, :]) % lon_count) / lon_count
    fwd = np.stack([np.cos(angle), -np.sin(angle)], 0) * lon_count ** -0.5
    inv = fwd * np.where(modes == 0, 1.0, 2.0)[None, :, None]

    def rows(table):
        table = table.reshape(2, h_size, num_modes // h_size, lon_count).transpose(1, 0, 2, 3)
        return table.reshape(2 * num_modes, lon_count).astype(np.float32)

    return rows(fwd), rows(inv)


def drain(ref, sem):
    pltpu.make_async_copy(ref, ref, sem).wait()


def rows_at(i, n):
    return pl.ds(pl.multiple_of(i * n, n), n)


def lanes_at(i):
    return pl.ds(pl.multiple_of(i * LANES, LANES), LANES)


def push(src, dst, sems, device):
    pltpu.make_async_remote_copy(src_ref=src, dst_ref=dst, send_sem=sems.at[0], recv_sem=sems.at[1],
                                 device_id=device, device_id_type=MESH).start()


def keep(src, dst, sems):
    pltpu.make_async_copy(src, dst, sems.at[1]).start()


def flip(v):
    return pltpu.roll(v, LANES // 2, 1)


def low(v):
    return lax.broadcasted_iota(jnp.int32, v.shape, 1) < LANES // 2


def weave(a, b):
    return jnp.where(low(a), a, flip(b)), jnp.where(low(a), flip(a), b)


def weave_wide(tiles):
    pairs = [weave(tiles[j], tiles[j + 1]) for j in range(0, len(tiles), 2)]
    return jnp.concatenate([p[0] for p in pairs], axis=1), jnp.concatenate([p[1] for p in pairs], axis=1)


def weave_tiles(a, b):
    out = []
    for j in range(0, a.shape[1], LANES):
        out.extend(weave(a[:, j:j + LANES], b[:, j:j + LANES]))
    return out


PARTS = 2
GS_ROWS = 176
GS_FIRST = (0, 1, 2)
ORDER = " ".join((
    'go', 'sX01', 'sX00', 'sX10', 'sX11', 'tb1', 'fd01', 'tb2', 'fd00', 'tb3',
    'tb4', 'st2', 'fl0', 'fd10', 'sX21', 'fd11', 'fo0', 'fl1', 'tb5', 'sX20',
    'fu0', 'fo1', 'fd21', 'fi00', 'sY00', 'fi01', 'sY01', 'fd20', 'pw00', 'sD00',
    'fu1', 'fl2', 'pw01', 'fi10', 'sY10', 'bd00', 'fi11', 'sD01', 'fo2', 'pw10',
    'sY11', 'bd01', 'sD10', 'fu2', 'pw11', 'sD11', 'bl0', 'fi21', 'sY21', 'fi20',
    'bd10', 'bo0', 'sY20', 'bd11', 'pw21', 'sD21', 'bu0', 'pw20', 'sD20', 'bl1',
    'bd21', 'gw1', 'gsa', 'bi00', 'bi01', 'gw2', 'sN01', 'bd20', 'bo1', 'gw3',
    'bl2', 'sN00', 'bu1', 'bo2', 'pj1', 'gw4', 'bi10', 'sN10', 'gsb', 'gw5',
    'gs1', 'gs20', 'gs21', 'gs310', 'gs300', 'bi11', 'gw6', 'gs61', 'sN11', 'gs303',
    'gw7', 'gs311', 'gs301', 'bu2', 'gs313', 'gs60', 'gs411', 'gs400', 'gs312', 'bi20',
    'gw8', 'pj2', 'gs403', 'bi21', 'sN21', 'fn00', 'gs413', 'gs302', 'gs500', 'gs410',
    'sN20', 'gs401', 'gs511', 'fn10', 'end', 'gs510', 'gs412', 'gs402', 'gs502', 'fn11',
    'gs501', 'gs513', 'fn01', 'fn20', 'fn21', 'gs503', 'gs512',
))


def block_kernel(sizes, total_points,
                 x, tgt, leg_p_in, leg_q_in, spec_w, lat_in, w1_in, w2_in, f_in, g_in,
                 dout, gs_out, gin_out, gout_out, loss_out,
                 leg_p, leg_q, lat, w1, w2, f_tab, g_tab, ft_tab, gt_tab,
                 xh, th, pk, rows, yrow, hy,
                 xs, sr, dsr, ys, yr, dyr, als, ar, dar, bs, br, dbr, asave, dsave, aall, dall,
                 st_s, st_h, st_m, st_w, tab_s, tab_w, tab, down_p, down_q, up_p, up_q, ker,
                 gw, gw_p, gw_a, gw_z, gw_zs, gw_h, gw_hs, gw_w, gw_ws, gw_w2, gw_h2, gw_f, gw_o,
                 ls, ls_p, ls_a, ls_z, ls_zs, ls_h, ls_hs, ls_w, gs_acc, gs_sum0, gs_sum1, gs_b0, gs_b1,
                 sem_x, sem_y, sem_d, sem_n, sem_s, sem_ds, sem_u, sem_du, sem_a, sem_da, sem_b, sem_db, sem_az, sem_dz,
                 sem_in, sem_st, sem_tab, sem_k, sem_gw, sem_ls, sem_gs, sem_gf, sem_fin, sem_small):
    dp_size, h_size, w_size = sizes
    dp, h, w = lax.axis_index("dp"), lax.axis_index("h"), lax.axis_index("w")
    ndev = h_size * w_size
    me = h * w_size + w
    nb, nt, npl, nc = x.shape
    ntp = nt // 2
    part = ntp // PARTS
    nlon = npl * w_size
    nlat = nt * h_size
    nl = als.shape[1] // 8
    l_own = nl // ndev
    piece = 8 * l_own
    unsent, coming = {}, {}

    def got(key):
        coming.pop(key)()

    def peer(k):
        return (h + k // w_size) % h_size, (w + k % w_size) % w_size

    barrier = pltpu.get_barrier_semaphore()

    def meet(k, _):
        h2, w2_ = peer(k)
        pl.semaphore_signal(barrier, inc=1, device_id={"h": h2, "w": w2_}, device_id_type=MESH)
        return 0

    def meet_dp(k, _):
        pl.semaphore_signal(barrier, inc=1, device_id={"dp": (dp + k) % dp_size}, device_id_type=MESH)
        return 0

    lax.fori_loop(1, ndev, meet, 0)
    lax.fori_loop(1, dp_size, meet_dp, 0)
    loads = [pltpu.make_async_copy(x.at[b], xh.at[b], sem_in.at[b, 0]) for b in range(nb)]
    load_t = [pltpu.make_async_copy(tgt.at[b], th.at[b], sem_in.at[b, 1]) for b in range(nb)]
    load_k = pltpu.make_async_copy(spec_w.at[:, pl.ds(me * l_own, l_own)], ker, sem_k.at[0])
    small = [pltpu.make_async_copy(src, dst, sem_small.at[i]) for i, (src, dst) in enumerate((
        (leg_p_in, leg_p), (leg_q_in, leg_q), (f_in, f_tab), (g_in, g_tab), (lat_in, lat), (w1_in, w1), (w2_in, w2)))]
    for c in loads + small[:4] + [load_k] + load_t + small[4:]:
        c.start()
    coming["k"] = load_k.wait
    coming["small"] = lambda: [c.wait() for c in small[4:]]
    coming.update({("t", b): load_t[b].wait for b in range(nb)})
    for ref in (ar, br, dar, dbr, st_s, gw, ls):
        ref[...] = jnp.zeros_like(ref)

    def settle(*keys):
        for key in keys or list(unsent):
            for wait in unsent.pop(key, []):
                wait()

    def along(axis, refs, sems, sent, key=None):
        size, index = {"dp": (dp_size, dp), "h": (h_size, h), "w": (w_size, w)}[axis]
        src, dst = refs(index)
        keep(src, dst, sems)

        def body(k, _):
            other = (index + k) % size
            src, dst = refs(other)
            push(src, dst, sems, {axis: other})
            return 0

        lax.fori_loop(1, size, body, 0)
        unsent.setdefault(key, []).append(lambda: drain(sent, sems.at[0]))

    def some(refs, sems, low_h, high_h, count, counts, key):
        src, dst = refs(h, w)
        keep(src, dst, sems)

        def one(h2, k):
            w2_ = (w + k) % w_size
            src, dst = refs(h2, w2_)
            push(src, dst, sems, {"h": h2, "w": w2_})

        for k in range(1, w_size):
            one(h, k)

        def body(h2, _):
            for k in range(w_size):
                one(h2, k)
            return 0

        lax.fori_loop(low_h, high_h, body, 0)
        unsent.setdefault(key, []).append(lambda: take(sems.at[0], count - 1, [n - 1 for n in counts]))

    def take(sem, count, counts):
        for n in counts:
            @pl.when(count == n)
            def _():
                drain(als.at[0, pl.ds(0, n * piece)], sem)

    n_orders, n_owners = (h + 1) * w_size, (h_size - h) * w_size
    counts = [w_size * n for n in range(1, h_size + 1)]
    pairs = lambda k: pl.ds(k * part, part)

    def at_rows(i, k):
        return pl.ds(pl.multiple_of(i * 16 * ntp + k * 16 * part, 16 * part), 16 * part)

    def send_home_rows(b, k, sem, name):
        along("w", lambda o: (pk.at[b, o, pairs(k)], rows.at[b, pairs(k), rows_at(w, npl)]), sem.at[b, k],
              pk.at[b, pl.ds(0, w_size - 1), pairs(k)], ("pk", b, k))
        coming[name, b, k] = lambda: drain(rows.at[b, pairs(k)], sem.at[b, k, 1])

    def send_rows_home(b, k, sem, name):
        along("w", lambda o: (yrow.at[b, o, pairs(k)], hy.at[b, w, pairs(k)]), sem.at[b, k],
              yrow.at[b, pl.ds(0, w_size - 1), pairs(k)], ("yrow", b, k))
        coming[name, b, k] = lambda: drain(hy.at[b, :, pairs(k)], sem.at[b, k, 1])

    def send_orders(b, k, dst, sem, name):
        along("h", lambda o: (xs.at[b, o, at_rows(0, k)], dst.at[b, at_rows(h, k)]), sem.at[b, k],
              xs.at[b, pl.ds(0, h_size - 1), at_rows(0, k)], ("xs", b, k))
        coming[name, b, k] = lambda: drain(xs.at[b, :, at_rows(0, k)], sem.at[b, k, 1])

    def send_lats(b, dst, sem, name):
        for k in range(PARTS):
            along("h", lambda o: (ys.at[b, at_rows(o, k)], dst.at[b, h, at_rows(0, k)]), sem.at[b, k],
                  xs.at[b, pl.ds(0, h_size - 1), at_rows(0, k)], ("ys", b))
            coming[name, b, k] = lambda k=k: drain(dst.at[b, :, at_rows(0, k)], sem.at[b, k, 1])

    def send_owner(b, dst, sem, name):
        some(lambda h2, w2_: (als.at[b, rows_at(h2 * w_size + w2_, piece)], dst.at[b, h, :, lanes_at(w)]), sem.at[b],
             h + 1, h_size, n_owners, counts, ("als", b))
        coming[name, b] = lambda: take(sem.at[b, 1], n_orders, counts)

    def send_back(b, dst, sem, name):
        some(lambda h2, w2_: (bs.at[b, h2, w2_], dst.at[b, rows_at(me, piece)]), sem.at[b],
             0, h, n_orders, counts, ("bs", b))
        coming[name, b] = lambda: take(sem.at[b, 1], n_owners, counts)

    def dft(b, k, table):
        settle(("xs", b, k))

        def body(n, _):
            i = 2 * n
            both = jnp.concatenate([rows[b, i], rows[b, i + 1]], axis=1)
            out = dot(table[...], both).reshape(h_size, 16, 2 * LANES)
            xs[b, :, rows_at(i, 16), :] = out[:, :, :LANES]
            xs[b, :, rows_at(i + 1, 16), :] = out[:, :, LANES:]
            return 0

        lax.fori_loop(k * part // 2, (k + 1) * part // 2, body, 0)

    def idft(b, k, table, src):
        settle(("yrow", b, k))

        def body(n, _):
            i = 2 * n
            both = jnp.concatenate([src[b, :, rows_at(i + j, 16), :].reshape(-1, LANES) for j in range(2)], axis=1)
            out = dot(table[...], both)
            for j in range(2):
                yrow[b, :, i + j] = out[:, j * LANES:(j + 1) * LANES].reshape(w_size, npl, LANES)
            return 0

        lax.fori_loop(k * part // 2, (k + 1) * part // 2, body, 0)

    def level(v):
        mean = jnp.mean(v, axis=0, keepdims=True)
        mean = 0.5 * (mean + flip(mean))
        return v - jnp.where(h == 0, mean, 0.0)

    def leg_down(b, table, src, fix):
        settle(("als", b))
        for m in range(8):
            parts = [src[b, pl.ds(ri * 8 + m, ntp * h_size, stride=16), :] for ri in range(2)]
            if fix and m == 0:
                parts[0] = level(parts[0])
            out = dot(table[m], jnp.concatenate(parts, axis=1))
            re0, re1 = out[:nl, :LANES], out[nl:, :LANES]
            im0, im1 = out[:nl, LANES:], out[nl:, LANES:]
            als[b, pl.ds(m, nl, stride=8), :] = jnp.where(low(re0), re0, im1) + flip(jnp.where(low(re0), im0, re1))

    def leg_up(b, table, src, fix):
        settle(("ys", b))
        for m in range(8):
            out = dot(table[m], src[b, pl.ds(m, nl, stride=8), :])
            re, im = weave(out[:nlat // 2], out[nlat // 2:])
            if fix and m == 0:
                re = level(re)
            ys[b, pl.ds(m, ntp * h_size, stride=16), :] = re
            ys[b, pl.ds(8 + m, ntp * h_size, stride=16), :] = im

    def owned(b, l, src):
        tiles = [src[b, :, l * 8:(l + 1) * 8, j * LANES:(j + 1) * LANES].reshape(-1, LANES) for j in range(w_size)]
        return weave_wide(tiles)

    def put_back(b, l, re, im):
        for j, tile in enumerate(weave_tiles(re, im)):
            bs[b, :, j, l * 8:(l + 1) * 8, :] = tile.reshape(h_size, 8, LANES)

    def put_rows(b, i, v0, v1):
        for j, tile in enumerate(weave_tiles(v0, v1)):
            pk[b, j, i] = tile

    def get_rows(b, i):
        return weave_wide([hy[b, j, i] for j in range(w_size)])

    count = nt * npl
    n_tab = tab_s.shape[1] // dp_size

    def combine(stats, n):
        mean = jnp.mean(stats, axis=0)
        dev = stats - mean[None]
        dev2 = jnp.sum(dev * dev, axis=0)
        m2 = jnp.sum(stats, axis=0)
        return [(mean[2 * b:2 * b + 1], m2[2 * b + 1:2 * b + 2] + n * dev2[2 * b:2 * b + 1]) for b in range(nb)]

    def go():
        for b in range(nb):
            loads[b].wait()

            def pack(i, total, b=b):
                v0, v1 = xh[b, i], xh[b, i + ntp]
                put_rows(b, i, v0, v1)
                return total + jnp.sum(v0 + v1, axis=0, keepdims=True)

            mean = lax.fori_loop(0, ntp, pack, jnp.zeros((1, nc), F32)) / count

            def spread(t, total, b=b, mean=mean):
                d = xh[b, t] - mean
                return total + jnp.sum(d * d, axis=0, keepdims=True)

            st_s[2 * b:2 * b + 1, :] = mean
            st_s[2 * b + 1:2 * b + 2, :] = lax.fori_loop(0, nt, spread, jnp.zeros((1, nc), F32))
        for c in small[:4]:
            c.wait()
        for a, leg in enumerate((leg_p, leg_q)):
            for m in range(leg.shape[0]):
                tab_s[a, m // 2, :, m % 2 * nl:(m % 2 + 1) * nl] = leg[m]
        ft_tab[...] = f_tab[...].T
        gt_tab[...] = g_tab[...].T
        pl.semaphore_wait(barrier, ndev - 1 + dp_size - 1)
        along("w", lambda o: (st_s, st_w.at[w]), sem_st.at[0], st_w.at[pl.ds(0, w_size - 1)], "st")
        coming["st"] = lambda: drain(st_w, sem_st.at[0, 1])
        along("w", lambda o: (tab_s.at[:, rows_at(dp, n_tab)], tab_w.at[:, w, rows_at(dp, n_tab)]), sem_tab.at[0],
              tab_w.at[:, pl.ds(0, w_size - 1), pl.ds(0, n_tab)])
        coming["tab"] = lambda: drain(tab_w.at[:, :, pl.ds(0, n_tab)], sem_tab.at[0, 1])

    def st2():
        got("st")
        st_m[...] = jnp.zeros_like(st_m)
        for b, (mean, m2) in enumerate(combine(st_w[...], count)):
            st_m[2 * b:2 * b + 1, :] = mean
            st_m[2 * b + 1:2 * b + 2, :] = m2
        along("h", lambda o: (st_m, st_h.at[h]), sem_st.at[1], st_h.at[pl.ds(0, h_size - 1)], "st")
        coming["st2"] = lambda: drain(st_h, sem_st.at[1, 1])

    means, scales = [], []

    def st3():
        got("st2")
        for mean, m2 in combine(st_h[...], count * w_size):
            means.append(mean)
            scales.append(lax.rsqrt(m2 / (count * ndev) + NORM_EPS))

    def tb1():
        got("tab")
        for a in range(2):
            share = tab_w.at[a, :, rows_at(dp, n_tab)]
            for k in range(1, dp_size):
                push(share, share, sem_tab.at[1 + a], {"dp": (dp + k) % dp_size})
            others = tab_w.at[a, :, pl.ds(0, (dp_size - 1) * n_tab)]
            unsent.setdefault(None, []).append(lambda a=a, others=others: drain(others, sem_tab.at[1 + a, 0]))
            coming["tab1", a] = lambda a=a, others=others: drain(others, sem_tab.at[1 + a, 1])

    def table_out(a):
        got(("tab1", a))
        along("h", lambda o: (tab_w.at[a, o // 2, rows_at(o % 2, 4)], tab.at[a, :, rows_at(h, nt)]), sem_tab.at[3 + a],
              tab.at[a, :, pl.ds(0, nlat - nt)])
        coming["tab2", a] = lambda: drain(tab.at[a], sem_tab.at[3 + a, 1])

    def table_in(a, down, up):
        got(("tab2", a))
        for m in range(8):
            both = tab[a, m // 2].reshape(h_size, 2, ntp, 2 * nl)
            for j in range(2):
                t = both[:, j].reshape(-1, 2 * nl)[:, m % 2 * nl:(m % 2 + 1) * nl]
                up[m, j * (nlat // 2):(j + 1) * (nlat // 2), :] = t
                down[m, j * nl:(j + 1) * nl, :] = t.T

    def tb2():
        table_out(0)

    def tb3():
        table_in(0, down_p, up_p)

    def tb4():
        table_out(1)

    def tb5():
        table_in(1, down_q, up_q)

    def sX(b, k):
        send_home_rows(b, k, sem_x, "x")

    def fd(b, k):
        got(("x", b, k))
        dft(b, k, f_tab)
        send_orders(b, k, sr, sem_s, "s")

    def fl(b):
        for k in range(PARTS):
            got(("s", b, k))
        leg_down(b, down_p, sr, True)
        send_owner(b, ar, sem_a, "a")

    def fo(b):
        if not scales:
            got("k")
            st3()
        got(("a", b))
        settle(("bs", b))
        for l in range(l_own):
            re, im = owned(b, l, ar)
            a = jnp.concatenate([re, im], axis=0) * scales[b]
            asave[b, l] = a
            n = a.shape[0] // 2
            own, other = dot(a, ker[0, l]), dot(a, ker[1, l])
            put_back(b, l, own[:n] - other[n:], own[n:] + other[:n])
        send_back(b, br, sem_b, "b")
        along("dp", lambda o: (asave.at[b, o // 2], aall.at[dp, b]), sem_az.at[b], aall.at[pl.ds(0, dp_size - 1), b])
        coming["az", b] = lambda: drain(aall.at[:, b], sem_az.at[b, 1])

    def fu(b):
        got(("b", b))
        leg_up(b, up_q, br, False)
        send_lats(b, yr, sem_u, "u")

    def fi(b, k):
        got(("u", b, k))
        idft(b, k, gt_tab, yr)

    def sY(b, k):
        send_rows_home(b, k, sem_y, "y")

    def pw(b, k):
        got(("y", b, k))
        if ("t", b) in coming:
            got(("t", b))
        if "small" in coming:
            got("small")
        settle(("pk", b, k))

        def body(n, _):
            lats = [2 * n, 2 * n + ntp, 2 * n + 1, 2 * n + 1 + ntp]
            y = jnp.concatenate([v for j in range(2) for v in get_rows(b, 2 * n + j)], axis=0)
            yb = y.astype(BF16)
            hid = bdot(yb, w1[...])
            th_ = jnp.tanh(GELU_C * (hid + GELU_A * (hid * hid * hid)))
            act = (hid * (0.5 * (1.0 + th_))).astype(BF16)
            resid = y + bdot(act, w2[...])
            parts = []
            for j, t in enumerate(lats):
                r = resid[j * npl:(j + 1) * npl] + xh[b, t] - th[b, t]
                d = lat[t] * r
                ls[...] += jnp.sum((d * r).reshape(-1, 8, nc), axis=0)
                dout[b, t] = d
                parts.append(d)
            d = jnp.concatenate(parts, axis=0)
            db = d.astype(BF16)
            gw[2 * nc:, :] += bdot(act, db, TN)
            slope = 0.5 * (1.0 + th_) + (0.5 * GELU_C) * hid * (1.0 - th_ * th_) * (1.0 + (3.0 * GELU_A) * (hid * hid))
            dh = (bdot(db, w2[...], NT) * slope).astype(BF16)
            gin = bdot(yb, dh, TN)
            gw[:nc, :] += gin[:, :nc]
            gw[nc:2 * nc, :] += gin[:, nc:]
            dy = d + bdot(dh, w1[...], NT)
            for j in range(2):
                put_rows(b, 2 * n + j, dy[2 * j * npl:(2 * j + 1) * npl], dy[(2 * j + 1) * npl:(2 * j + 2) * npl])
            return 0

        lax.fori_loop(k * part // 2, (k + 1) * part // 2, body, 0)

    def sD(b, k):
        send_home_rows(b, k, sem_d, "d")

    def bd(b, k):
        got(("d", b, k))
        dft(b, k, g_tab)
        send_orders(b, k, dsr, sem_ds, "ds")

    def bl(b):
        for k in range(PARTS):
            got(("ds", b, k))
        leg_down(b, down_q, dsr, False)
        send_owner(b, dar, sem_da, "da")

    def bo(b):
        got(("da", b))
        settle(("bs", b), "st")
        s2 = jnp.zeros((1, nc), F32)
        for l in range(l_own):
            re, im = owned(b, l, dar)
            d = jnp.concatenate([re, im], axis=0)
            dsave[b, l] = d
            n = d.shape[0] // 2
            own, other = dot(d, ker[0, l], NT), dot(d, ker[1, l], NT)
            re, im = own[:n] + other[n:], own[n:] - other[:n]
            put_back(b, l, re, im)
            s2 = s2 + jnp.sum(re * asave[b, l, :n] + im * asave[b, l, n:], axis=0, keepdims=True)
        send_back(b, dbr, sem_db, "db")
        along("dp", lambda o: (dsave.at[b, o // 2, :, lanes_at(o % 2)], dall.at[dp, b]), sem_dz.at[b], dall.at[pl.ds(0, dp_size - 1), b])
        coming["dz", b] = lambda: drain(dall.at[:, b], sem_dz.at[b, 1])
        st_s[b:b + 1, :] = s2

    def bu(b):
        got(("db", b))
        leg_up(b, up_p, dbr, True)
        send_lats(b, dyr, sem_du, "du")

    def bi(b, k):
        got(("du", b, k))
        idft(b, k, ft_tab, dyr)

    def sN(b, k):
        send_rows_home(b, k, sem_n, "n")

    def pj1():
        st_s[nb:, :] = jnp.zeros_like(st_s[nb:, :])
        along("w", lambda o: (st_s, st_w.at[w]), sem_st.at[2], st_w.at[pl.ds(0, w_size - 1)])
        coming["pj"] = lambda: drain(st_w, sem_st.at[2, 1])

    def pj2():
        got("pj")
        st_m[...] = jnp.sum(st_w[...], axis=0)
        along("h", lambda o: (st_m, st_h.at[h]), sem_st.at[3], st_h.at[pl.ds(0, h_size - 1)])
        coming["pj2"] = lambda: drain(st_h, sem_st.at[3, 1])

    proj = []

    def fn(b, k):
        if not proj:
            got("pj2")
            proj.append(jnp.sum(st_h[...], axis=0) / (count * ndev))
        got(("n", b, k))

        def body(i, _):
            for t, dn in zip((i, i + ntp), get_rows(b, i)):
                normed = (xh[b, t] - means[b]) * scales[b]
                dout[b, t] = dout[b, t] + scales[b] * (dn - normed * proj[0][b:b + 1])
            return 0

        lax.fori_loop(k * part, (k + 1) * part, body, 0)

    n_c, n_z, n_h, n_w = gw_a.shape[0], gw_zs.shape[0], gw_hs.shape[0], gw_ws.shape[0]
    chip, core = h // 2, h % 2
    chips = h_size // 2

    def over_chips(refs, sems, sent):
        src, dst = refs(chip)
        keep(src, dst, sems)
        for k in range(1, chips):
            o = (chip + k) % chips
            src, dst = refs(o)
            push(src, dst, sems, {"h": 2 * o + core})
        unsent.setdefault(None, []).append(lambda: drain(sent, sems.at[0]))

    def twin(src, dst, sems):
        push(src, dst, sems, {"h": h + 1 - 2 * core})
        unsent.setdefault(None, []).append(lambda: drain(dst, sems.at[0]))

    def gw1():
        twin(gw.at[rows_at(1 - core, n_c)], gw_p, sem_gw.at[0])
        twin(ls, ls_p, sem_ls.at[0])
        coming["gw1"] = lambda: (drain(gw_p, sem_gw.at[0, 1]), drain(ls_p, sem_ls.at[0, 1]))

    def gw2():
        got("gw1")
        gw_a[...] = gw[rows_at(core, n_c), :] + gw_p[...]
        ls_a[...] = ls[...] + ls_p[...]
        along("dp", lambda o: (gw_a.at[rows_at(o, n_z)], gw_z.at[dp]), sem_gw.at[1], gw_z.at[pl.ds(0, dp_size - 1)])
        along("dp", lambda o: (ls_a, ls_z.at[dp]), sem_ls.at[1], ls_z.at[pl.ds(0, dp_size - 1)])
        coming["gw2"] = lambda: (drain(gw_z, sem_gw.at[1, 1]), drain(ls_z, sem_ls.at[1, 1]))

    def gw3():
        got("gw2")
        gw_zs[...] = jnp.sum(gw_z[...], axis=0)
        ls_zs[...] = jnp.sum(ls_z[...], axis=0)
        over_chips(lambda o: (gw_zs.at[rows_at(o, n_h)], gw_h.at[chip]), sem_gw.at[2], gw_h.at[pl.ds(0, chips - 1)])
        over_chips(lambda o: (ls_zs, ls_h.at[chip]), sem_ls.at[2], ls_h.at[pl.ds(0, chips - 1)])
        coming["gw3"] = lambda: (drain(gw_h, sem_gw.at[2, 1]), drain(ls_h, sem_ls.at[2, 1]))

    def gw4():
        got("gw3")
        gw_hs[...] = jnp.sum(gw_h[...], axis=0)
        ls_hs[...] = jnp.sum(ls_h[...], axis=0)
        along("w", lambda o: (gw_hs.at[rows_at(o, n_w)], gw_w.at[w]), sem_gw.at[3], gw_w.at[pl.ds(0, w_size - 1)])
        along("w", lambda o: (ls_hs, ls_w.at[w]), sem_ls.at[3], ls_w.at[pl.ds(0, w_size - 1)])
        coming["gw4"] = lambda: (drain(gw_w, sem_gw.at[3, 1]), drain(ls_w, sem_ls.at[3, 1]))

    def gw5():
        got("gw4")
        gw_ws[...] = jnp.sum(gw_w[...], axis=0)
        loss_out[...] = jnp.sum(ls_w[...], keepdims=True).reshape(1, 1) / total_points
        along("w", lambda o: (gw_ws, gw_w2.at[rows_at(w, n_w)]), sem_gw.at[4], gw_w2.at[pl.ds(0, (w_size - 1) * n_w)])
        coming["gw5"] = lambda: drain(gw_w2, sem_gw.at[4, 1])

    def gw6():
        got("gw5")
        over_chips(lambda o: (gw_w2, gw_h2.at[rows_at(chip, n_h)]), sem_gw.at[5], gw_h2.at[pl.ds(0, (chips - 1) * n_h)])
        coming["gw6"] = lambda: drain(gw_h2, sem_gw.at[5, 1])

    def gw7():
        got("gw6")
        along("dp", lambda o: (gw_h2, gw_f.at[rows_at(dp, n_z)]), sem_gw.at[6], gw_f.at[pl.ds(0, (dp_size - 1) * n_z)])
        coming["gw7"] = lambda: drain(gw_f, sem_gw.at[6, 1])

    def gw8():
        got("gw7")
        twin(gw_f, gw_o, sem_gw.at[7])
        coming["gw8"] = lambda: drain(gw_o, sem_gw.at[7, 1])

    def end():
        got("gw8")
        for c, halves in enumerate(((gw_f, gw_o), (gw_o, gw_f))):
            @pl.when(core == c)
            def _():
                first, second = halves
                for i, (src, dst) in enumerate(((first.at[:nc], gin_out.at[:, :nc]), (first.at[nc:], gin_out.at[:, nc:]), (second, gout_out))):
                    pltpu.make_async_copy(src, dst, sem_fin.at[i]).start()
        for i, dst in enumerate((gin_out.at[:, :nc], gin_out.at[:, nc:], gout_out)):
            unsent.setdefault(None, []).append(lambda dst=dst, i=i: drain(dst, sem_fin.at[i]))

    gs_sum, gs_b = (gs_sum0, gs_sum1), (gs_b0, gs_b1)
    first_rows = (0, gs_sum0.shape[1])
    axes = (("w", "dp"), ("dp", "w"))
    place = {"w": (w, w_size), "dp": (dp, dp_size)}

    def next_to(axis, k):
        index, size = place[axis]
        return (index + k + size) % size

    def sample_grad(b):
        got(("az", b))
        got(("dz", b))
        d = dall[:, b].reshape(dp_size, 2, -1, LANES)
        turned = jnp.concatenate([d[:, 1:], -d[:, :1]], axis=1)
        both = jnp.concatenate([d.reshape(-1, LANES), turned.reshape(-1, LANES)], axis=1)
        return dot(aall[:, b].reshape(-1, nc), both, TN)

    def gsa():
        gs_acc[...] = sample_grad(GS_FIRST[0])

    def gsb():
        gs_acc[...] += sample_grad(GS_FIRST[1])

    def gs1():
        out = gs_acc[...] + sample_grad(GS_FIRST[2])
        for q in range(2):
            for p in range(2):
                gs_sum[q][p] = out[first_rows[q]:first_rows[q] + gs_sum[q].shape[1], p * LANES:(p + 1) * LANES]

    def once(key):
        if key in coming:
            got(key)

    def sent_later(ref, sem):
        unsent.setdefault(None, []).append(lambda: drain(ref, sem))

    def gs2(q):
        keep(gs_sum[q], gs_b[q].at[0], sem_gs.at[q, 0])
        for slot, k in ((1, 1), (3, -1)):
            push(gs_sum[q], gs_b[q].at[slot], sem_gs.at[q, slot], {axes[q][0]: next_to(axes[q][0], k)})
            sent_later(gs_sum[q], sem_gs.at[q, slot, 0])
        coming.update({("gs", q, k): lambda k=k: drain(gs_b[q].at[k], sem_gs.at[q, k, 1]) for k in (0, 1, 3)})

    def gs6(q):
        for slot, p, k, i in ((1, 0, 1, 2), (3, 1, -1, 4)):
            once(("gs", q, slot))
            push(gs_b[q].at[slot, p], gs_b[q].at[2, p], sem_gs.at[q, i], {axes[q][0]: next_to(axes[q][0], k)})
            sent_later(gs_b[q].at[2, p], sem_gs.at[q, i, 0])
        coming["gs", q, 2] = lambda: (drain(gs_b[q].at[2, 0], sem_gs.at[q, 2, 1]), drain(gs_b[q].at[2, 1], sem_gs.at[q, 4, 1]))

    def block_at(q, k, shift):
        at = {axes[q][0]: next_to(axes[q][0], -k), axes[q][1]: next_to(axes[q][1], shift)}
        return gs_out.at[:, l_own * at["w"] + at["dp"] // 2, pl.ds(first_rows[q], gs_sum[q].shape[1]), lanes_at(at["dp"] % 2)]

    def gs3(q, k):
        once(("gs", q, k))
        mine = block_at(q, k, 0)
        pltpu.make_async_copy(gs_b[q].at[k], mine, sem_gf.at[q, 3, k, 0]).start()
        for way, shift in ((0, 1), (1, -1)):
            push(gs_b[q].at[k], mine, sem_gf.at[q, way, k], {axes[q][1]: next_to(axes[q][1], shift)})

    def gs4(q, k):
        way, shift = (0, 1) if k < 2 else (1, -1)
        drain(gs_b[q].at[k], sem_gf.at[q, way, k, 1])
        block = block_at(q, k, -shift)
        push(block, block, sem_gf.at[q, 2, k], {axes[q][1]: next_to(axes[q][1], shift)})

    def gs5(q, k):
        drain(gs_b[q].at[k], sem_gf.at[q, 1 if k < 2 else 0, k, 1])
        drain(gs_b[q].at[k], sem_gf.at[q, 2, k, 1])
        for i in range(4):
            drain(gs_b[q].at[k], sem_gf.at[q, i, k, 0])

    scope = dict(locals())
    for name in ORDER.split():
        call = name.rstrip("0123456789") or name
        if name in scope:
            scope[name]()
        elif name[:3] in scope:
            scope[name[:3]](*map(int, name[3:]))
        else:
            scope[call](*map(int, name[len(call):]))
    assert not coming
    settle()


def hand_on_kernel(*refs):
    n = len(refs) // 2
    copies = [pltpu.make_async_copy(refs[i], refs[n + i], refs[2 * n].at[i]) for i in range(n)]
    for c in copies:
        c.start()
    for c in copies:
        c.wait()


def hand_on(arrays):
    return pl.pallas_call(
        hand_on_kernel, name="hand_on",
        out_shape=[jax.ShapeDtypeStruct(a.shape, F32) for a in arrays],
        in_specs=[pl.BlockSpec(memory_space=pltpu.VMEM)] * len(arrays), out_specs=[pl.BlockSpec(memory_space=pl.ANY)] * len(arrays),
        scratch_shapes=[pltpu.SemaphoreType.DMA((len(arrays),))],
        compiler_params=pltpu.CompilerParams(vmem_limit_bytes=12 * 1024 * 1024),
    )(*[pltpu.with_memory_space_constraint(a, pltpu.VMEM) for a in arrays])


def solution(mesh):
    dp_size, w_size, h_size = mesh.shape["dp"], mesh.shape["w"], mesh.shape["h"]

    def local_step(field, target, lat_weight, leg_fwd, leg_inv, spec_w, w_in, w_out):
        nb, nc, nt, npl = field.shape
        nlon = npl * w_size
        ntp = nt // 2
        nm = leg_fwd.shape[0] * w_size
        ndev = h_size * w_size
        nlat = nt * h_size
        nl = leg_fwd.shape[1]
        lo = nl // ndev
        assert nm == 8 * h_size and nc == w_size * LANES // 2 and h_size == 2 * w_size and 2 * lo == dp_size and 2 * nl == LANES
        total_points = nb * dp_size * nc * nlat * nlon
        fwd_np, inv_np = dft_tables(nlon, nm, h_size)
        any_spec = pl.BlockSpec(memory_space=pl.ANY)
        vmem_spec = pl.BlockSpec(memory_space=pltpu.VMEM)
        sds = lambda *s: jax.ShapeDtypeStruct(s, F32)
        vm = lambda *s: pltpu.VMEM(s, F32)
        dma = lambda *s: pltpu.SemaphoreType.DMA(s)
        n_rows = 2 * nc + w_out.shape[0]
        n_z, n_h, n_w = n_rows // dp_size, n_rows // dp_size // h_size, n_rows // dp_size // h_size // w_size
        home = vm(nb, nt, npl, nc)
        woven = vm(nb, w_size, ntp, npl, LANES)
        order = vm(nb, 16 * nlat // 2, LANES)
        degree = vm(nb, 8 * nl, LANES)
        owner = vm(nb, h_size, 8 * lo, w_size * LANES)
        saved = vm(nb, lo, 2 * nm, nc)
        cut = GS_ROWS
        n_pairs = leg_fwd.shape[0] // 2
        n_c = n_rows // 2
        n_z, n_h, n_w = n_c // dp_size, n_c // dp_size // w_size, n_c // dp_size // w_size // w_size
        results = pl.pallas_call(
            functools.partial(block_kernel, (dp_size, h_size, w_size), total_points),
            name="block",
            out_shape=[vm(nb, nt, npl, nc), vm(2, lo * w_size, nc, nc), vm(nc, 2 * nc), vm(2 * nc, nc), sds(1, 1)],
            in_specs=[any_spec] * 10,
            out_specs=[vmem_spec] * 5,
            scratch_shapes=[
                vm(*leg_fwd.shape[:1], nt, nl), vm(*leg_fwd.shape[:1], nt, nl), pltpu.SMEM((nt,), F32), pltpu.VMEM(w_in.shape, BF16),
                pltpu.VMEM(w_out.shape, BF16), vm(2 * nm, nlon), vm(2 * nm, nlon), vm(nlon, 2 * nm), vm(nlon, 2 * nm),
                home, home, woven, vm(nb, ntp, nlon, LANES), woven, woven,
                vm(nb, h_size, 16 * ntp, LANES), order, order, order, vm(nb, h_size, 16 * ntp, LANES), vm(nb, h_size, 16 * ntp, LANES),
                degree, owner, owner, vm(nb, h_size, w_size, 8 * lo, LANES), degree, degree, saved, saved,
                vm(dp_size, nb, 2 * nm, nc), vm(dp_size, nb, 2 * nm, LANES),
                vm(8, nc), vm(h_size, 8, nc), vm(8, nc), vm(w_size, 8, nc),
                vm(2, n_pairs, nt, 2 * nl), vm(2, w_size, n_pairs, nt, 2 * nl), vm(2, 4, nlat, 2 * nl),
                vm(8, 2 * nl, nlat // 2), vm(8, 2 * nl, nlat // 2), vm(8, nlat, nl), vm(8, nlat, nl),
                vm(2, lo, nc, nc),
                vm(n_rows, nc), vm(n_c, nc), vm(n_c, nc), vm(dp_size, n_z, nc), vm(n_z, nc), vm(w_size, n_h, nc), vm(n_h, nc),
                vm(w_size, n_w, nc), vm(n_w, nc), vm(n_h, nc), vm(n_z, nc), vm(n_c, nc), vm(n_c, nc),
                vm(8, nc), vm(8, nc), vm(8, nc), vm(dp_size, 8, nc), vm(8, nc), vm(w_size, 8, nc), vm(8, nc), vm(w_size, 8, nc),
                vm(nc, nc), vm(2, cut, LANES), vm(2, nc - cut, LANES), vm(4, 2, cut, LANES), vm(4, 2, nc - cut, LANES),
            ] + [dma(nb, PARTS, 2)] * 8 + [dma(nb, 2)] * 6 + [dma(nb, 2), dma(4, 2), dma(5, 2), dma(1), dma(8, 2), dma(4, 2),
                 dma(2, 5, 2), dma(2, 4, 4, 2), dma(3), dma(7)],
            compiler_params=pltpu.CompilerParams(collective_id=0, has_side_effects=True, vmem_limit_bytes=54 * 1024 * 1024),
        )(field.transpose(0, 2, 3, 1), target.transpose(0, 2, 3, 1), leg_fwd.transpose(0, 2, 1), leg_inv.transpose(0, 2, 1),
          spec_w, lat_weight, w_in, w_out, jnp.asarray(fwd_np), jnp.asarray(inv_np))
        d_x, g_spec, g_in, g_out = hand_on(results[:4])
        loss = results[4]
        return loss.reshape(()), d_x.transpose(0, 3, 1, 2), g_spec, g_in, g_out

    grid_spec = P("dp", None, "h", "w")
    table_spec = P("w", None, "h")
    kernel_spec = P(None, "h", None, None)
    return jax.shard_map(local_step, mesh=mesh, in_specs=(grid_spec, grid_spec, P("h"), table_spec, table_spec, P(), P(), P()), out_specs=(P(), grid_spec, kernel_spec, P(), P()), check_vma=False)
```

```python
import functools
import jax
import jax.numpy as jnp
import numpy as np
from jax import lax
from jax.experimental import pallas as pl
from jax.experimental.pallas import tpu as pltpu
from jax.sharding import PartitionSpec as P

NORM_EPS = 1e-5
PRECISE = lax.Precision.HIGHEST
MESH = pl.DeviceIdType.MESH
F32 = jnp.float32
BF16 = jnp.bfloat16
GELU_C = float(np.sqrt(2.0 / np.pi))
GELU_A = 0.044715
LANES = 128
NN = (((1,), (0,)), ((), ()))
NT = (((1,), (1,)), ((), ()))
TN = (((0,), (0,)), ((), ()))


def dot(a, b, dims=NN):
    return lax.dot_general(a, b, dims, precision=PRECISE, preferred_element_type=F32)


def bdot(a, b, dims=NN):
    return lax.dot_general(a, b, dims, preferred_element_type=F32)


def dft_table(lon_count, num_modes, h_size):
    modes, lons = np.arange(num_modes), np.arange(lon_count)
    angle = 2.0 * np.pi * ((modes[:, None] * lons[None, :]) % lon_count) / lon_count
    table = np.stack([np.cos(angle), -np.sin(angle)], 0) * lon_count ** -0.5
    table = table.reshape(2, h_size, num_modes // h_size, lon_count).transpose(1, 0, 2, 3)
    return table.reshape(2 * num_modes, lon_count).astype(np.float32)


def drain(ref, sem):
    pltpu.make_async_copy(ref, ref, sem).wait()


def rows_at(i, n):
    return pl.ds(pl.multiple_of(i * n, n), n)


def lanes_at(i):
    return pl.ds(pl.multiple_of(i * LANES, LANES), LANES)


def push(src, dst, sems, device):
    pltpu.make_async_remote_copy(src_ref=src, dst_ref=dst, send_sem=sems.at[0], recv_sem=sems.at[1],
                                 device_id=device, device_id_type=MESH).start()


def keep(src, dst, sems):
    pltpu.make_async_copy(src, dst, sems.at[1]).start()


def flip(v):
    return pltpu.roll(v, LANES // 2, 1)


def low(v):
    return lax.broadcasted_iota(jnp.int32, v.shape, 1) < LANES // 2


def weave(a, b):
    return jnp.where(low(a), a, flip(b)), jnp.where(low(a), flip(a), b)


def weave_wide(tiles):
    pairs = [weave(tiles[j], tiles[j + 1]) for j in range(0, len(tiles), 2)]
    return jnp.concatenate([p[0] for p in pairs], axis=1), jnp.concatenate([p[1] for p in pairs], axis=1)


def weave_tiles(a, b):
    out = []
    for j in range(0, a.shape[1], LANES):
        out.extend(weave(a[:, j:j + LANES], b[:, j:j + LANES]))
    return out


PARTS = 4
GS_ROWS = 176
GS_FIRST = (0, 1, 2)
ORDER = " ".join((
    'go', 'sX03', 'sX00', 'tb1', 'sX02', 'sX01', 'st2', 'fd03', 'tb2', 'sX10',
    'fd00', 'sX13', 'fd02', 'fd01', 'tb4', 'sX12', 'sX11', 'tb3', 'fd13', 'fl0',
    'fd10', 'sX20', 'sX22', 'fd11', 'tb5', 'fd12', 'fo0', 'fl1', 'sX23', 'fd20',
    'fu0', 'sX21', 'fo1', 'fi00', 'sY00', 'fd23', 'fi02', 'sY02', 'fi03', 'sY03',
    'fi01', 'pw00', 'sD00', 'fu1', 'sY01', 'pw02', 'pw03', 'fd21', 'sD02', 'bd00',
    'fd22', 'fi10', 'fi11', 'sD03', 'fi12', 'pw01', 'sD01', 'sY10', 'fl2', 'sY11',
    'bd01', 'fi13', 'bd02', 'pw10', 'sY12', 'bd03', 'fo2', 'sY13', 'pw11', 'sD11',
    'bl0', 'pw12', 'sD10', 'fu2', 'sD12', 'fi21', 'sY21', 'bo0', 'fi23', 'bd12',
    'bd10', 'sY23', 'bd11', 'fi22', 'pw21', 'sY22', 'fi20', 'sY20', 'bu0', 'pw23',
    'pw13', 'sD13', 'pw22', 'sD22', 'sD23', 'bi01', 'bd13', 'sD21', 'pw20', 'bi03',
    'gw1', 'bd22', 'sD20', 'bl1', 'bi00', 'bd23', 'bi02', 'bd21', 'sN00', 'gw2',
    'sN03', 'bd20', 'bo1', 'bl2', 'sN01', 'sN02', 'gw3', 'bu1', 'gsa', 'bo2',
    'gsb', 'pj1', 'gw4', 'bi10', 'sN10', 'bi11', 'sN11', 'gs1', 'pj2', 'gs20',
    'gw5', 'bi13', 'gs21', 'gs310', 'bu2', 'gs300', 'gs311', 'gs61', 'fn11', 'bi12',
    'sN13', 'gs301', 'gw6', 'sN12', 'gs303', 'gs313', 'gs60', 'bi22', 'gs410', 'gw7',
    'fn03', 'bi23', 'bi20', 'sN20', 'bi21', 'gs312', 'gs302', 'sN22', 'fn00', 'fn13',
    'gs401', 'fn12', 'gw8', 'sN23', 'gs411', 'sN21', 'gs413', 'gs403', 'gs510', 'gs412',
    'fn02', 'fn20', 'fn01', 'gs400', 'fn22', 'gs402', 'end', 'gs500', 'fn10', 'gs503',
    'gs511', 'gs502', 'fn21', 'gs513', 'fn23', 'gs501', 'gs512',
))


def block_kernel(sizes, total_points,
                 x, tgt, leg_p_in, leg_q_in, spec_w, lat_in, w1_in, w2_in, f_in,
                 dout, gs_out, gin_out, gout_out, loss_out,
                 leg_p, leg_q, lat, w1, w2, f_tab, g_tab, ft_tab, gt_tab,
                 xh, th, pk, rows, yrow, hy,
                 xs, sr, dsr, ys, yr, dyr, als, ar, dar, bs, br, dbr, asave, dsave, aall, dall,
                 st_s, st_h, st_m, st_w, tab_s, tab_w, tab, down_p, down_q, up_p, up_q, ker,
                 gw, gw_p, gw_a, gw_z, gw_zs, gw_h, gw_hs, gw_w, gw_ws, gw_w2, gw_h2, gw_f, gw_o,
                 ls, ls_p, ls_a, ls_z, ls_zs, ls_h, ls_hs, ls_w, gs_acc, gs_sum0, gs_sum1, gs_b0, gs_b1,
                 sem_x, sem_y, sem_d, sem_n, sem_s, sem_ds, sem_u, sem_du, sem_a, sem_da, sem_b, sem_db, sem_az, sem_dz,
                 sem_in, sem_st, sem_tab, sem_k, sem_gw, sem_ls, sem_gs, sem_gf, sem_fin, sem_small):
    dp_size, h_size, w_size = sizes
    dp, h, w = lax.axis_index("dp"), lax.axis_index("h"), lax.axis_index("w")
    ndev = h_size * w_size
    me = h * w_size + w
    nb, nt, npl, nc = x.shape
    ntp = nt // 2
    part = ntp // PARTS
    nlon = npl * w_size
    nlat = nt * h_size
    nl = als.shape[1] // 8
    l_own = nl // ndev
    piece = 8 * l_own
    unsent, coming = {}, {}

    def got(key):
        coming.pop(key)()

    def peer(k):
        return (h + k // w_size) % h_size, (w + k % w_size) % w_size

    barrier = pltpu.get_barrier_semaphore()

    def meet(k, _):
        h2, w2_ = peer(k)
        pl.semaphore_signal(barrier, inc=1, device_id={"h": h2, "w": w2_}, device_id_type=MESH)
        return 0

    def meet_dp(k, _):
        pl.semaphore_signal(barrier, inc=1, device_id={"dp": (dp + k) % dp_size}, device_id_type=MESH)
        return 0

    lax.fori_loop(1, ndev, meet, 0)
    lax.fori_loop(1, dp_size, meet_dp, 0)
    loads = [pltpu.make_async_copy(x.at[b], xh.at[b], sem_in.at[b, 0]) for b in range(nb)]
    load_t = [pltpu.make_async_copy(tgt.at[b], th.at[b], sem_in.at[b, 1]) for b in range(nb)]
    load_k = pltpu.make_async_copy(spec_w.at[:, pl.ds(me * l_own, l_own)], ker, sem_k.at[0])
    small = [pltpu.make_async_copy(src, dst, sem_small.at[i]) for i, (src, dst) in enumerate((
        (leg_p_in, leg_p), (leg_q_in, leg_q), (f_in, f_tab), (lat_in, lat), (w1_in, w1), (w2_in, w2)))]
    for c in loads + small[:3] + [load_k] + load_t + small[3:]:
        c.start()
    coming["k"] = load_k.wait
    coming["small"] = lambda: [c.wait() for c in small[3:]]
    coming.update({("t", b): load_t[b].wait for b in range(nb)})
    for ref in (ar, br, dar, dbr, st_s, gw, ls):
        ref[...] = jnp.zeros_like(ref)

    def settle(*keys):
        for key in keys or list(unsent):
            for wait in unsent.pop(key, []):
                wait()

    def along(axis, refs, sems, sent, key=None):
        size, index = {"dp": (dp_size, dp), "h": (h_size, h), "w": (w_size, w)}[axis]
        src, dst = refs(index)
        keep(src, dst, sems)

        def body(k, _):
            other = (index + k) % size
            src, dst = refs(other)
            push(src, dst, sems, {axis: other})
            return 0

        lax.fori_loop(1, size, body, 0)
        unsent.setdefault(key, []).append(lambda: drain(sent, sems.at[0]))

    def some(refs, sems, low_h, high_h, count, counts, key):
        src, dst = refs(h, w)
        keep(src, dst, sems)

        def one(h2, k):
            w2_ = (w + k) % w_size
            src, dst = refs(h2, w2_)
            push(src, dst, sems, {"h": h2, "w": w2_})

        for k in range(1, w_size):
            one(h, k)

        def body(h2, _):
            for k in range(w_size):
                one(h2, k)
            return 0

        lax.fori_loop(low_h, high_h, body, 0)
        unsent.setdefault(key, []).append(lambda: take(sems.at[0], count - 1, [n - 1 for n in counts]))

    def take(sem, count, counts):
        for n in counts:
            @pl.when(count == n)
            def _():
                drain(als.at[0, pl.ds(0, n * piece)], sem)

    n_orders, n_owners = (h + 1) * w_size, (h_size - h) * w_size
    counts = [w_size * n for n in range(1, h_size + 1)]
    pairs = lambda k: pl.ds(k * part, part)

    def at_rows(i, k):
        return pl.ds(pl.multiple_of(i * 16 * ntp + k * 16 * part, 16 * part), 16 * part)

    def send_home_rows(b, k, sem, name):
        along("w", lambda o: (pk.at[b, o, pairs(k)], rows.at[b, pairs(k), rows_at(w, npl)]), sem.at[b, k],
              pk.at[b, pl.ds(0, w_size - 1), pairs(k)], ("pk", b, k))
        coming[name, b, k] = lambda: drain(rows.at[b, pairs(k)], sem.at[b, k, 1])

    def send_rows_home(b, k, sem, name):
        along("w", lambda o: (yrow.at[b, o, pairs(k)], hy.at[b, w, pairs(k)]), sem.at[b, k],
              yrow.at[b, pl.ds(0, w_size - 1), pairs(k)], ("yrow", b, k))
        coming[name, b, k] = lambda: drain(hy.at[b, :, pairs(k)], sem.at[b, k, 1])

    def send_orders(b, k, dst, sem, name):
        along("h", lambda o: (xs.at[b, o, at_rows(0, k)], dst.at[b, at_rows(h, k)]), sem.at[b, k],
              xs.at[b, pl.ds(0, h_size - 1), at_rows(0, k)], ("xs", b, k))
        coming[name, b, k] = lambda: drain(xs.at[b, :, at_rows(0, k)], sem.at[b, k, 1])

    def send_lats(b, dst, sem, name):
        def one(k, _):
            keep(ys.at[b, at_rows(h, k)], dst.at[b, h, at_rows(0, k)], sem.at[b, k])

            def body(j, _):
                o = (h + j) % h_size
                push(ys.at[b, at_rows(o, k)], dst.at[b, h, at_rows(0, k)], sem.at[b, k], {"h": o})
                return 0

            return lax.fori_loop(1, h_size, body, 0)

        lax.fori_loop(0, PARTS, one, 0)
        for k in range(PARTS):
            unsent.setdefault(("ys", b), []).append(lambda k=k: drain(xs.at[b, pl.ds(0, h_size - 1), at_rows(0, k)], sem.at[b, k, 0]))
            coming[name, b, k] = lambda k=k: drain(dst.at[b, :, at_rows(0, k)], sem.at[b, k, 1])

    def send_owner(b, dst, sem, name):
        some(lambda h2, w2_: (als.at[b, rows_at(h2 * w_size + w2_, piece)], dst.at[b, h, :, lanes_at(w)]), sem.at[b],
             h + 1, h_size, n_owners, counts, ("als", b))
        coming[name, b] = lambda: take(sem.at[b, 1], n_orders, counts)

    def send_back(b, dst, sem, name):
        some(lambda h2, w2_: (bs.at[b, h2, w2_], dst.at[b, rows_at(me, piece)]), sem.at[b],
             0, h, n_orders, counts, ("bs", b))
        coming[name, b] = lambda: take(sem.at[b, 1], n_owners, counts)

    def dft(b, k, table):
        settle(("xs", b, k))

        def body(n, _):
            i = 2 * n
            both = jnp.concatenate([rows[b, i], rows[b, i + 1]], axis=1)
            out = dot(table[...], both).reshape(h_size, 16, 2 * LANES)
            xs[b, :, rows_at(i, 16), :] = out[:, :, :LANES]
            xs[b, :, rows_at(i + 1, 16), :] = out[:, :, LANES:]
            return 0

        lax.fori_loop(k * part // 2, (k + 1) * part // 2, body, 0)

    def idft(b, k, table, src):
        settle(("yrow", b, k))

        def body(n, _):
            i = 2 * n
            both = jnp.concatenate([src[b, :, rows_at(i + j, 16), :].reshape(-1, LANES) for j in range(2)], axis=1)
            out = dot(table[...], both)
            for j in range(2):
                yrow[b, :, i + j] = out[:, j * LANES:(j + 1) * LANES].reshape(w_size, npl, LANES)
            return 0

        lax.fori_loop(k * part // 2, (k + 1) * part // 2, body, 0)

    def level(v, here):
        mean = jnp.mean(v, axis=0, keepdims=True)
        mean = 0.5 * (mean + flip(mean))
        return v - jnp.where(jnp.logical_and(h == 0, here), mean, 0.0)

    def orders(body):
        def four(n, _):
            for i in range(4):
                body(4 * n + i, n == 0 if i == 0 else None)
            return 0

        lax.fori_loop(0, 2, four, 0)

    def leg_down(b, table, src, fix):
        settle(("als", b))

        def one(m, here):
            re, im = (src[b, pl.ds(ri * 8 + m, ntp * h_size, stride=16), :] for ri in range(2))
            if fix and here is not None:
                re = level(re, here)
            als[b, pl.ds(m, nl, stride=8), :] = dot(table[m], jnp.concatenate(weave(re, im), axis=0))

        orders(one)

    def leg_up(b, table, src, fix):
        settle(("ys", b))

        def one(m, here):
            out = dot(table[m], src[b, pl.ds(m, nl, stride=8), :])
            re, im = weave(out[:nlat // 2], out[nlat // 2:])
            if fix and here is not None:
                re = level(re, here)
            ys[b, pl.ds(m, ntp * h_size, stride=16), :] = re
            ys[b, pl.ds(8 + m, ntp * h_size, stride=16), :] = im

        orders(one)

    def owned(b, l, src):
        tiles = [src[b, :, rows_at(l, 8), j * LANES:(j + 1) * LANES].reshape(-1, LANES) for j in range(w_size)]
        return weave_wide(tiles)

    def put_back(b, l, re, im):
        for j, tile in enumerate(weave_tiles(re, im)):
            bs[b, :, j, rows_at(l, 8), :] = tile.reshape(h_size, 8, LANES)

    def put_rows(b, i, v0, v1):
        for j, tile in enumerate(weave_tiles(v0, v1)):
            pk[b, j, i] = tile

    def get_rows(b, i):
        return weave_wide([hy[b, j, i] for j in range(w_size)])

    count = nt * npl
    n_tab = tab_s.shape[1] // dp_size

    def combine(stats, n):
        mean = jnp.mean(stats, axis=0)
        dev = stats - mean[None]
        dev2 = jnp.sum(dev * dev, axis=0)
        m2 = jnp.sum(stats, axis=0)
        return [(mean[2 * b:2 * b + 1], m2[2 * b + 1:2 * b + 2] + n * dev2[2 * b:2 * b + 1]) for b in range(nb)]

    def go():
        for b in range(nb):
            loads[b].wait()

            def pack(i, total, b=b):
                v0, v1 = xh[b, i], xh[b, i + ntp]
                put_rows(b, i, v0, v1)
                return total + jnp.sum(v0 + v1, axis=0, keepdims=True)

            mean = lax.fori_loop(0, ntp, pack, jnp.zeros((1, nc), F32)) / count

            def spread(t, total, b=b, mean=mean):
                d = xh[b, t] - mean
                return total + jnp.sum(d * d, axis=0, keepdims=True)

            st_s[2 * b:2 * b + 1, :] = mean
            st_s[2 * b + 1:2 * b + 2, :] = lax.fori_loop(0, nt, spread, jnp.zeros((1, nc), F32))
        for c in small[:3]:
            c.wait()
        for a, leg in enumerate((leg_p, leg_q)):
            for m in range(leg.shape[0]):
                tab_s[a, m // 2, :, m % 2 * nl:(m % 2 + 1) * nl] = leg[m]
        g_tab[...] = jnp.where(lax.broadcasted_iota(jnp.int32, f_tab.shape, 0) == 0, 1.0, 2.0) * f_tab[...]
        ft_tab[...] = f_tab[...].T
        gt_tab[...] = g_tab[...].T
        pl.semaphore_wait(barrier, ndev - 1 + dp_size - 1)
        along("w", lambda o: (st_s, st_w.at[w]), sem_st.at[0], st_w.at[pl.ds(0, w_size - 1)], "st")
        coming["st"] = lambda: drain(st_w, sem_st.at[0, 1])
        along("w", lambda o: (tab_s.at[:, rows_at(dp, n_tab)], tab_w.at[:, w, rows_at(dp, n_tab)]), sem_tab.at[0],
              tab_w.at[:, pl.ds(0, w_size - 1), pl.ds(0, n_tab)])
        coming["tab"] = lambda: drain(tab_w.at[:, :, pl.ds(0, n_tab)], sem_tab.at[0, 1])

    def st2():
        got("st")
        st_m[...] = jnp.zeros_like(st_m)
        for b, (mean, m2) in enumerate(combine(st_w[...], count)):
            st_m[2 * b:2 * b + 1, :] = mean
            st_m[2 * b + 1:2 * b + 2, :] = m2
        along("h", lambda o: (st_m, st_h.at[h]), sem_st.at[1], st_h.at[pl.ds(0, h_size - 1)], "st")
        coming["st2"] = lambda: drain(st_h, sem_st.at[1, 1])

    means, scales = [], []

    def st3():
        got("st2")
        for mean, m2 in combine(st_h[...], count * w_size):
            means.append(mean)
            scales.append(lax.rsqrt(m2 / (count * ndev) + NORM_EPS))

    def tb1():
        got("tab")
        for a in range(2):
            share = tab_w.at[a, :, rows_at(dp, n_tab)]
            for k in range(1, dp_size):
                push(share, share, sem_tab.at[1 + a], {"dp": (dp + k) % dp_size})
            others = tab_w.at[a, :, pl.ds(0, (dp_size - 1) * n_tab)]
            unsent.setdefault(None, []).append(lambda a=a, others=others: drain(others, sem_tab.at[1 + a, 0]))
            coming["tab1", a] = lambda a=a, others=others: drain(others, sem_tab.at[1 + a, 1])

    def table_out(a):
        got(("tab1", a))
        along("h", lambda o: (tab_w.at[a, o // 2, rows_at(o % 2, 4)], tab.at[a, :, rows_at(h, nt)]), sem_tab.at[3 + a],
              tab.at[a, :, pl.ds(0, nlat - nt)])
        coming["tab2", a] = lambda: drain(tab.at[a], sem_tab.at[3 + a, 1])

    def table_in(a, down, up):
        got(("tab2", a))

        def body(n, _):
            both = tab[a, n].reshape(h_size, 2, ntp, 2 * nl)
            both = jnp.concatenate([both[:, j].reshape(-1, 2 * nl) for j in range(2)], axis=0)
            for j in range(2):
                t = both[:, j * nl:(j + 1) * nl]
                up[2 * n + j] = t
                down[2 * n + j] = t.T
            return 0

        lax.fori_loop(0, tab.shape[1], body, 0)

    def tb2():
        table_out(0)

    def tb3():
        table_in(0, down_p, up_p)

    def tb4():
        table_out(1)

    def tb5():
        table_in(1, down_q, up_q)

    def sX(b, k):
        send_home_rows(b, k, sem_x, "x")

    def fd(b, k):
        got(("x", b, k))
        dft(b, k, f_tab)
        send_orders(b, k, sr, sem_s, "s")

    def fl(b):
        for k in range(PARTS):
            got(("s", b, k))
        leg_down(b, down_p, sr, True)
        send_owner(b, ar, sem_a, "a")

    def fo(b):
        if not scales:
            got("k")
            st3()
        got(("a", b))
        settle(("bs", b))

        def one(l, _):
            re, im = owned(b, l, ar)
            a = jnp.concatenate([re, im], axis=0) * scales[b]
            asave[b, l] = a
            n = a.shape[0] // 2
            own, other = dot(a, ker[0, l]), dot(a, ker[1, l])
            put_back(b, l, own[:n] - other[n:], own[n:] + other[:n])
            return 0

        lax.fori_loop(0, l_own, one, 0)
        send_back(b, br, sem_b, "b")
        along("dp", lambda o: (asave.at[b, o // 2], aall.at[dp, b]), sem_az.at[b], aall.at[pl.ds(0, dp_size - 1), b])
        coming["az", b] = lambda: drain(aall.at[:, b], sem_az.at[b, 1])

    def fu(b):
        got(("b", b))
        leg_up(b, up_q, br, False)
        send_lats(b, yr, sem_u, "u")

    def fi(b, k):
        got(("u", b, k))
        idft(b, k, gt_tab, yr)

    def sY(b, k):
        send_rows_home(b, k, sem_y, "y")

    def pw(b, k):
        got(("y", b, k))
        if ("t", b) in coming:
            got(("t", b))
        if "small" in coming:
            got("small")
        settle(("pk", b, k))

        def body(n, _):
            lats = [n, n + ntp]
            y = jnp.concatenate(get_rows(b, n), axis=0)
            yb = y.astype(BF16)
            hid = bdot(yb, w1[...])
            th_ = jnp.tanh(GELU_C * (hid + GELU_A * (hid * hid * hid)))
            act = (hid * (0.5 * (1.0 + th_))).astype(BF16)
            resid = y + bdot(act, w2[...])
            parts = []
            for j, t in enumerate(lats):
                r = resid[j * npl:(j + 1) * npl] + xh[b, t] - th[b, t]
                d = lat[t] * r
                ls[...] += jnp.sum((d * r).reshape(-1, 8, nc), axis=0)
                dout[b, t] = d
                parts.append(d)
            d = jnp.concatenate(parts, axis=0)
            db = d.astype(BF16)
            gw[2 * nc:, :] += bdot(act, db, TN)
            slope = 0.5 * (1.0 + th_) + (0.5 * GELU_C) * hid * (1.0 - th_ * th_) * (1.0 + (3.0 * GELU_A) * (hid * hid))
            dh = (bdot(db, w2[...], NT) * slope).astype(BF16)
            gin = bdot(yb, dh, TN)
            gw[:nc, :] += gin[:, :nc]
            gw[nc:2 * nc, :] += gin[:, nc:]
            dy = d + bdot(dh, w1[...], NT)
            put_rows(b, n, dy[:npl], dy[npl:])
            return 0

        lax.fori_loop(k * part, (k + 1) * part, body, 0)

    def sD(b, k):
        send_home_rows(b, k, sem_d, "d")

    def bd(b, k):
        got(("d", b, k))
        dft(b, k, g_tab)
        send_orders(b, k, dsr, sem_ds, "ds")

    def bl(b):
        for k in range(PARTS):
            got(("ds", b, k))
        leg_down(b, down_q, dsr, False)
        send_owner(b, dar, sem_da, "da")

    def bo(b):
        got(("da", b))
        settle(("bs", b), "st")

        def one(l, s2):
            re, im = owned(b, l, dar)
            d = jnp.concatenate([re, im], axis=0)
            dsave[b, l] = d
            n = d.shape[0] // 2
            own, other = dot(d, ker[0, l], NT), dot(d, ker[1, l], NT)
            re, im = own[:n] + other[n:], own[n:] - other[:n]
            put_back(b, l, re, im)
            return s2 + jnp.sum(re * asave[b, l, :n] + im * asave[b, l, n:], axis=0, keepdims=True)

        s2 = lax.fori_loop(0, l_own, one, jnp.zeros((1, nc), F32))
        send_back(b, dbr, sem_db, "db")
        along("dp", lambda o: (dsave.at[b, o // 2, :, lanes_at(o % 2)], dall.at[dp, b]), sem_dz.at[b], dall.at[pl.ds(0, dp_size - 1), b])
        coming["dz", b] = lambda: drain(dall.at[:, b], sem_dz.at[b, 1])
        st_s[b:b + 1, :] = s2

    def bu(b):
        got(("db", b))
        leg_up(b, up_p, dbr, True)
        send_lats(b, dyr, sem_du, "du")

    def bi(b, k):
        got(("du", b, k))
        idft(b, k, ft_tab, dyr)

    def sN(b, k):
        send_rows_home(b, k, sem_n, "n")

    def pj1():
        st_s[nb:, :] = jnp.zeros_like(st_s[nb:, :])
        along("w", lambda o: (st_s, st_w.at[w]), sem_st.at[2], st_w.at[pl.ds(0, w_size - 1)])
        coming["pj"] = lambda: drain(st_w, sem_st.at[2, 1])

    def pj2():
        got("pj")
        st_m[...] = jnp.sum(st_w[...], axis=0)
        along("h", lambda o: (st_m, st_h.at[h]), sem_st.at[3], st_h.at[pl.ds(0, h_size - 1)])
        coming["pj2"] = lambda: drain(st_h, sem_st.at[3, 1])

    proj = []

    def fn(b, k):
        if not proj:
            got("pj2")
            proj.append(jnp.sum(st_h[...], axis=0) / (count * ndev))
        got(("n", b, k))

        def body(i, _):
            for t, dn in zip((i, i + ntp), get_rows(b, i)):
                normed = (xh[b, t] - means[b]) * scales[b]
                dout[b, t] = dout[b, t] + scales[b] * (dn - normed * proj[0][b:b + 1])
            return 0

        lax.fori_loop(k * part, (k + 1) * part, body, 0)

    n_c, n_z, n_h, n_w = gw_a.shape[0], gw_zs.shape[0], gw_hs.shape[0], gw_ws.shape[0]
    chip, core = h // 2, h % 2
    chips = h_size // 2

    def over_chips(refs, sems, sent):
        src, dst = refs(chip)
        keep(src, dst, sems)
        for k in range(1, chips):
            o = (chip + k) % chips
            src, dst = refs(o)
            push(src, dst, sems, {"h": 2 * o + core})
        unsent.setdefault(None, []).append(lambda: drain(sent, sems.at[0]))

    def twin(src, dst, sems):
        push(src, dst, sems, {"h": h + 1 - 2 * core})
        unsent.setdefault(None, []).append(lambda: drain(dst, sems.at[0]))

    def gw1():
        twin(gw.at[rows_at(1 - core, n_c)], gw_p, sem_gw.at[0])
        twin(ls, ls_p, sem_ls.at[0])
        coming["gw1"] = lambda: (drain(gw_p, sem_gw.at[0, 1]), drain(ls_p, sem_ls.at[0, 1]))

    def gw2():
        got("gw1")
        gw_a[...] = gw[rows_at(core, n_c), :] + gw_p[...]
        ls_a[...] = ls[...] + ls_p[...]
        along("dp", lambda o: (gw_a.at[rows_at(o, n_z)], gw_z.at[dp]), sem_gw.at[1], gw_z.at[pl.ds(0, dp_size - 1)])
        along("dp", lambda o: (ls_a, ls_z.at[dp]), sem_ls.at[1], ls_z.at[pl.ds(0, dp_size - 1)])
        coming["gw2"] = lambda: (drain(gw_z, sem_gw.at[1, 1]), drain(ls_z, sem_ls.at[1, 1]))

    def gw3():
        got("gw2")
        gw_zs[...] = jnp.sum(gw_z[...], axis=0)
        ls_zs[...] = jnp.sum(ls_z[...], axis=0)
        over_chips(lambda o: (gw_zs.at[rows_at(o, n_h)], gw_h.at[chip]), sem_gw.at[2], gw_h.at[pl.ds(0, chips - 1)])
        over_chips(lambda o: (ls_zs, ls_h.at[chip]), sem_ls.at[2], ls_h.at[pl.ds(0, chips - 1)])
        coming["gw3"] = lambda: (drain(gw_h, sem_gw.at[2, 1]), drain(ls_h, sem_ls.at[2, 1]))

    def gw4():
        got("gw3")
        gw_hs[...] = jnp.sum(gw_h[...], axis=0)
        ls_hs[...] = jnp.sum(ls_h[...], axis=0)
        along("w", lambda o: (gw_hs.at[rows_at(o, n_w)], gw_w.at[w]), sem_gw.at[3], gw_w.at[pl.ds(0, w_size - 1)])
        along("w", lambda o: (ls_hs, ls_w.at[w]), sem_ls.at[3], ls_w.at[pl.ds(0, w_size - 1)])
        coming["gw4"] = lambda: (drain(gw_w, sem_gw.at[3, 1]), drain(ls_w, sem_ls.at[3, 1]))

    def gw5():
        got("gw4")
        gw_ws[...] = jnp.sum(gw_w[...], axis=0)
        loss_out[...] = jnp.sum(ls_w[...], keepdims=True).reshape(1, 1) / total_points
        along("w", lambda o: (gw_ws, gw_w2.at[rows_at(w, n_w)]), sem_gw.at[4], gw_w2.at[pl.ds(0, (w_size - 1) * n_w)])
        coming["gw5"] = lambda: drain(gw_w2, sem_gw.at[4, 1])

    def gw6():
        got("gw5")
        over_chips(lambda o: (gw_w2, gw_h2.at[rows_at(chip, n_h)]), sem_gw.at[5], gw_h2.at[pl.ds(0, (chips - 1) * n_h)])
        coming["gw6"] = lambda: drain(gw_h2, sem_gw.at[5, 1])

    def gw7():
        got("gw6")
        along("dp", lambda o: (gw_h2, gw_f.at[rows_at(dp, n_z)]), sem_gw.at[6], gw_f.at[pl.ds(0, (dp_size - 1) * n_z)])
        coming["gw7"] = lambda: drain(gw_f, sem_gw.at[6, 1])

    def gw8():
        got("gw7")
        twin(gw_f, gw_o, sem_gw.at[7])
        coming["gw8"] = lambda: drain(gw_o, sem_gw.at[7, 1])

    def end():
        got("gw8")
        for c, halves in enumerate(((gw_f, gw_o), (gw_o, gw_f))):
            @pl.when(core == c)
            def _():
                first, second = halves
                for i, (src, dst) in enumerate(((first.at[:nc], gin_out.at[:, :nc]), (first.at[nc:], gin_out.at[:, nc:]), (second, gout_out))):
                    pltpu.make_async_copy(src, dst, sem_fin.at[i]).start()
        for i, dst in enumerate((gin_out.at[:, :nc], gin_out.at[:, nc:], gout_out)):
            unsent.setdefault(None, []).append(lambda dst=dst, i=i: drain(dst, sem_fin.at[i]))

    gs_sum, gs_b = (gs_sum0, gs_sum1), (gs_b0, gs_b1)
    first_rows = (0, gs_sum0.shape[1])
    axes = (("w", "dp"), ("dp", "w"))
    place = {"w": (w, w_size), "dp": (dp, dp_size)}

    def next_to(axis, k):
        index, size = place[axis]
        return (index + k + size) % size

    def add_sample(b):
        got(("az", b))
        got(("dz", b))

        def body(n, _):
            d = dall[n, b]
            half = d.shape[0] // 2
            both = jnp.concatenate([d, jnp.concatenate([d[half:], -d[:half]], axis=0)], axis=1)
            gs_acc[...] += dot(aall[n, b], both, TN)
            return 0

        lax.fori_loop(0, dp_size, body, 0)

    def gsa():
        gs_acc[...] = jnp.zeros_like(gs_acc)
        add_sample(GS_FIRST[0])

    def gsb():
        add_sample(GS_FIRST[1])

    def gs1():
        add_sample(GS_FIRST[2])
        for q in range(2):
            rows_q = pl.ds(first_rows[q], gs_sum[q].shape[1])
            for p in range(2):
                gs_sum[q][p] = gs_acc[rows_q, p * LANES:(p + 1) * LANES]

    def once(key):
        if key in coming:
            got(key)

    def sent_later(ref, sem):
        unsent.setdefault(None, []).append(lambda: drain(ref, sem))

    def gs2(q):
        keep(gs_sum[q], gs_b[q].at[0], sem_gs.at[q, 0])
        for slot, k in ((1, 1), (3, -1)):
            push(gs_sum[q], gs_b[q].at[slot], sem_gs.at[q, slot], {axes[q][0]: next_to(axes[q][0], k)})
            sent_later(gs_sum[q], sem_gs.at[q, slot, 0])
        coming.update({("gs", q, k): lambda k=k: drain(gs_b[q].at[k], sem_gs.at[q, k, 1]) for k in (0, 1, 3)})

    def gs6(q):
        for slot, p, k, i in ((1, 0, 1, 2), (3, 1, -1, 4)):
            once(("gs", q, slot))
            push(gs_b[q].at[slot, p], gs_b[q].at[2, p], sem_gs.at[q, i], {axes[q][0]: next_to(axes[q][0], k)})
            sent_later(gs_b[q].at[2, p], sem_gs.at[q, i, 0])
        coming["gs", q, 2] = lambda: (drain(gs_b[q].at[2, 0], sem_gs.at[q, 2, 1]), drain(gs_b[q].at[2, 1], sem_gs.at[q, 4, 1]))

    def block_at(q, k, shift):
        at = {axes[q][0]: next_to(axes[q][0], -k), axes[q][1]: next_to(axes[q][1], shift)}
        return gs_out.at[:, l_own * at["w"] + at["dp"] // 2, pl.ds(first_rows[q], gs_sum[q].shape[1]), lanes_at(at["dp"] % 2)]

    def gs3(q, k):
        once(("gs", q, k))
        mine = block_at(q, k, 0)
        pltpu.make_async_copy(gs_b[q].at[k], mine, sem_gf.at[q, 3, k, 0]).start()
        for way, shift in ((0, 1), (1, -1)):
            push(gs_b[q].at[k], mine, sem_gf.at[q, way, k], {axes[q][1]: next_to(axes[q][1], shift)})

    def gs4(q, k):
        way, shift = (0, 1) if k < 2 else (1, -1)
        drain(gs_b[q].at[k], sem_gf.at[q, way, k, 1])
        block = block_at(q, k, -shift)
        push(block, block, sem_gf.at[q, 2, k], {axes[q][1]: next_to(axes[q][1], shift)})

    def gs5(q, k):
        drain(gs_b[q].at[k], sem_gf.at[q, 1 if k < 2 else 0, k, 1])
        drain(gs_b[q].at[k], sem_gf.at[q, 2, k, 1])
        for i in range(4):
            drain(gs_b[q].at[k], sem_gf.at[q, i, k, 0])

    scope = dict(locals())
    for name in ORDER.split():
        call = name.rstrip("0123456789") or name
        if name in scope:
            scope[name]()
        elif name[:3] in scope:
            scope[name[:3]](*map(int, name[3:]))
        else:
            scope[call](*map(int, name[len(call):]))
    assert not coming
    settle()


def hand_on_kernel(*refs):
    n = len(refs) // 2
    pairs = []
    for src, dst in zip(refs[:n], refs[n:2 * n]):
        lead = [()] if len(src.shape) == 2 else [(i,) for i in range(src.shape[0])]
        pairs += [(src.at[i], dst.at[i]) if i else (src, dst) for i in lead]
    copies = [pltpu.make_async_copy(src, dst, refs[2 * n].at[i]) for i, (src, dst) in enumerate(pairs)]
    for c in copies:
        c.start()
    for c in copies:
        c.wait()


def hand_on(arrays):
    return pl.pallas_call(
        hand_on_kernel, name="hand_on",
        out_shape=[jax.ShapeDtypeStruct(a.shape, F32) for a in arrays],
        in_specs=[pl.BlockSpec(memory_space=pltpu.VMEM)] * len(arrays), out_specs=[pl.BlockSpec(memory_space=pl.ANY)] * len(arrays),
        scratch_shapes=[pltpu.SemaphoreType.DMA((32,))],
        compiler_params=pltpu.CompilerParams(vmem_limit_bytes=12 * 1024 * 1024),
    )(*[pltpu.with_memory_space_constraint(a, pltpu.VMEM) for a in arrays])


def solution(mesh):
    dp_size, w_size, h_size = mesh.shape["dp"], mesh.shape["w"], mesh.shape["h"]

    def local_step(field, target, lat_weight, leg_fwd, leg_inv, spec_w, w_in, w_out):
        nb, nc, nt, npl = field.shape
        nlon = npl * w_size
        ntp = nt // 2
        nm = leg_fwd.shape[0] * w_size
        ndev = h_size * w_size
        nlat = nt * h_size
        nl = leg_fwd.shape[1]
        lo = nl // ndev
        assert nm == 8 * h_size and nc == w_size * LANES // 2 and h_size == 2 * w_size and 2 * lo == dp_size and 2 * nl == LANES
        total_points = nb * dp_size * nc * nlat * nlon
        any_spec = pl.BlockSpec(memory_space=pl.ANY)
        vmem_spec = pl.BlockSpec(memory_space=pltpu.VMEM)
        sds = lambda *s: jax.ShapeDtypeStruct(s, F32)
        vm = lambda *s: pltpu.VMEM(s, F32)
        dma = lambda *s: pltpu.SemaphoreType.DMA(s)
        n_rows = 2 * nc + w_out.shape[0]
        n_z, n_h, n_w = n_rows // dp_size, n_rows // dp_size // h_size, n_rows // dp_size // h_size // w_size
        home = vm(nb, nt, npl, nc)
        woven = vm(nb, w_size, ntp, npl, LANES)
        order = vm(nb, 16 * nlat // 2, LANES)
        degree = vm(nb, 8 * nl, LANES)
        owner = vm(nb, h_size, 8 * lo, w_size * LANES)
        saved = vm(nb, lo, 2 * nm, nc)
        cut = GS_ROWS
        n_pairs = leg_fwd.shape[0] // 2
        n_c = n_rows // 2
        n_z, n_h, n_w = n_c // dp_size, n_c // dp_size // w_size, n_c // dp_size // w_size // w_size
        results = pl.pallas_call(
            functools.partial(block_kernel, (dp_size, h_size, w_size), total_points),
            name="block",
            out_shape=[vm(nb, nt, npl, nc), vm(2, lo * w_size, nc, nc), vm(nc, 2 * nc), vm(2 * nc, nc), sds(1, 1)],
            in_specs=[any_spec] * 9,
            out_specs=[vmem_spec] * 5,
            scratch_shapes=[
                vm(*leg_fwd.shape[:1], nt, nl), vm(*leg_fwd.shape[:1], nt, nl), pltpu.SMEM((nt,), F32), pltpu.VMEM(w_in.shape, BF16),
                pltpu.VMEM(w_out.shape, BF16), vm(2 * nm, nlon), vm(2 * nm, nlon), vm(nlon, 2 * nm), vm(nlon, 2 * nm),
                home, home, woven, vm(nb, ntp, nlon, LANES), woven, woven,
                vm(nb, h_size, 16 * ntp, LANES), order, order, order, vm(nb, h_size, 16 * ntp, LANES), vm(nb, h_size, 16 * ntp, LANES),
                degree, owner, owner, vm(nb, h_size, w_size, 8 * lo, LANES), degree, degree, saved, saved,
                vm(dp_size, nb, 2 * nm, nc), vm(dp_size, nb, 2 * nm, LANES),
                vm(8, nc), vm(h_size, 8, nc), vm(8, nc), vm(w_size, 8, nc),
                vm(2, n_pairs, nt, 2 * nl), vm(2, w_size, n_pairs, nt, 2 * nl), vm(2, 4, nlat, 2 * nl),
                vm(8, nl, nlat), vm(8, nl, nlat), vm(8, nlat, nl), vm(8, nlat, nl),
                vm(2, lo, nc, nc),
                vm(n_rows, nc), vm(n_c, nc), vm(n_c, nc), vm(dp_size, n_z, nc), vm(n_z, nc), vm(w_size, n_h, nc), vm(n_h, nc),
                vm(w_size, n_w, nc), vm(n_w, nc), vm(n_h, nc), vm(n_z, nc), vm(n_c, nc), vm(n_c, nc),
                vm(8, nc), vm(8, nc), vm(8, nc), vm(dp_size, 8, nc), vm(8, nc), vm(w_size, 8, nc), vm(8, nc), vm(w_size, 8, nc),
                vm(nc, nc), vm(2, cut, LANES), vm(2, nc - cut, LANES), vm(4, 2, cut, LANES), vm(4, 2, nc - cut, LANES),
            ] + [dma(nb, PARTS, 2)] * 8 + [dma(nb, 2)] * 6 + [dma(nb, 2), dma(4, 2), dma(5, 2), dma(1), dma(8, 2), dma(4, 2),
                 dma(2, 5, 2), dma(2, 4, 4, 2), dma(3), dma(6)],
            compiler_params=pltpu.CompilerParams(collective_id=0, has_side_effects=True, vmem_limit_bytes=54 * 1024 * 1024),
        )(field.transpose(0, 2, 3, 1), target.transpose(0, 2, 3, 1), leg_fwd.transpose(0, 2, 1), leg_inv.transpose(0, 2, 1),
          spec_w, lat_weight, w_in, w_out, jnp.asarray(dft_table(nlon, nm, h_size)))
        d_x, g_spec, g_in, g_out = hand_on(results[:4])
        loss = results[4]
        return loss.reshape(()), d_x.transpose(0, 3, 1, 2), g_spec, g_in, g_out

    grid_spec = P("dp", None, "h", "w")
    table_spec = P("w", None, "h")
    kernel_spec = P(None, "h", None, None)
    return jax.shard_map(local_step, mesh=mesh, in_specs=(grid_spec, grid_spec, P("h"), table_spec, table_spec, P(), P(), P()), out_specs=(P(), grid_spec, kernel_spec, P(), P()), check_vma=False)
```

```python
import functools
import jax
import jax.numpy as jnp
import numpy as np
from jax import lax
from jax.experimental import pallas as pl
from jax.experimental.pallas import tpu as pltpu
from jax.sharding import PartitionSpec as P

NORM_EPS = 1e-5
PRECISE = lax.Precision.HIGHEST
MESH = pl.DeviceIdType.MESH
F32 = jnp.float32
BF16 = jnp.bfloat16
GELU_C = float(np.sqrt(2.0 / np.pi))
GELU_A = 0.044715
LANES = 128
NN = (((1,), (0,)), ((), ()))
NT = (((1,), (1,)), ((), ()))
TN = (((0,), (0,)), ((), ()))


def dot(a, b, dims=NN):
    return lax.dot_general(a, b, dims, precision=PRECISE, preferred_element_type=F32)


def bdot(a, b, dims=NN):
    return lax.dot_general(a, b, dims, preferred_element_type=F32)


def dft_table(lon_count, num_modes, h_size):
    modes, lons = np.arange(num_modes), np.arange(lon_count)
    angle = 2.0 * np.pi * ((modes[:, None] * lons[None, :]) % lon_count) / lon_count
    table = np.stack([np.cos(angle), -np.sin(angle)], 0) * lon_count ** -0.5
    table = table.reshape(2, h_size, num_modes // h_size, lon_count).transpose(1, 0, 2, 3)
    return table.reshape(2 * num_modes, lon_count).astype(np.float32)


def drain(ref, sem):
    pltpu.make_async_copy(ref, ref, sem).wait()


def rows_at(i, n):
    return pl.ds(pl.multiple_of(i * n, n), n)


def lanes_at(i):
    return pl.ds(pl.multiple_of(i * LANES, LANES), LANES)


def push(src, dst, sems, device):
    pltpu.make_async_remote_copy(src_ref=src, dst_ref=dst, send_sem=sems.at[0], recv_sem=sems.at[1],
                                 device_id=device, device_id_type=MESH).start()


def keep(src, dst, sems):
    pltpu.make_async_copy(src, dst, sems.at[1]).start()


def flip(v):
    return pltpu.roll(v, LANES // 2, 1)


def low(v):
    return lax.broadcasted_iota(jnp.int32, v.shape, 1) < LANES // 2


def weave(a, b):
    return jnp.where(low(a), a, flip(b)), jnp.where(low(a), flip(a), b)


def weave_wide(tiles):
    pairs = [weave(tiles[j], tiles[j + 1]) for j in range(0, len(tiles), 2)]
    return jnp.concatenate([p[0] for p in pairs], axis=1), jnp.concatenate([p[1] for p in pairs], axis=1)


def weave_tiles(a, b):
    out = []
    for j in range(0, a.shape[1], LANES):
        out.extend(weave(a[:, j:j + LANES], b[:, j:j + LANES]))
    return out


PARTS = 4
GS_ROWS = 176
GS_FIRST = (0, 1, 2)
ORDER = " ".join((
    'pk0', 'pk1', 'go', 'sX03', 'sX01', 'pk2', 'tb1', 'sX00', 'sX02', 'sX11',
    'sX10', 'fd03', 'sX13', 'tb2', 'fd00', 'fd01', 'fd02', 'tb3', 'st1', 'tb4',
    'sX12', 'fd11', 'fl0', 'st2', 'fd13', 'fd10', 'sX20', 'fd12', 'sX22', 'tb5',
    'fo0', 'sX23', 'fl1', 'fu0', 'fd23', 'sX21', 'fd22', 'fd20', 'fo1', 'fi00',
    'sY00', 'fi02', 'sY02', 'fi01', 'fi03', 'fd21', 'sY03', 'pw00', 'sY01', 'pw02',
    'sD02', 'fl2', 'fu1', 'pw03', 'sD03', 'pw01', 'sD00', 'fo2', 'fi11', 'sD01',
    'sY11', 'fi12', 'sY12', 'fi13', 'fi10', 'sY10', 'bd00', 'bd02', 'bd03', 'bd01',
    'sY13', 'fu2', 'bl0', 'fi21', 'sY21', 'fi22', 'pw10', 'pw13', 'sY22', 'pw11',
    'pw12', 'sD10', 'bo0', 'fi20', 'sD12', 'pw21', 'fi23', 'sY23', 'pw22', 'bd10',
    'sD11', 'sY20', 'bu0', 'pw23', 'sD13', 'bi00', 'bd11', 'sD23', 'bd12', 'pw20',
    'sD22', 'gw1', 'sD20', 'bi01', 'bd13', 'gw2', 'sD21', 'bd23', 'bi03', 'bi02',
    'bl1', 'sN03', 'bd22', 'bd20', 'bd21', 'sN02', 'gw3', 'bo1', 'bl2', 'gw4',
    'sN01', 'sN00', 'bu1', 'gw5', 'bo2', 'pj1', 'bi10', 'sN10', 'bi11', 'gsa',
    'sN11', 'gsb', 'gs1', 'gs21', 'gs20', 'gw6', 'bi12', 'gs300', 'sN12', 'bu2',
    'gs311', 'gs61', 'gs313', 'gs301', 'gw7', 'bi13', 'bi21', 'gs303', 'gs60', 'gs312',
    'sN13', 'gs411', 'pj2', 'fn10', 'bi22', 'gs310', 'bi23', 'gs302', 'sN23', 'fn01',
    'gw8', 'gs401', 'fn02', 'sN21', 'gs410', 'fn00', 'sN22', 'fn03', 'bi20', 'gs403',
    'end', 'fn13', 'sN20', 'gs412', 'gs402', 'gs510', 'gs413', 'gs501', 'fn21', 'fn11',
    'gs511', 'gs400', 'fn12', 'gs503', 'fn20', 'fn22', 'gs512', 'fn23', 'gs500', 'gs502',
    'gs513',
))


def block_kernel(sizes, total_points,
                 x, tgt, leg_p_in, leg_q_in, spec_w, lat_in, w1_in, w2_in, f_in,
                 dout, gs_out, gin_out, gout_out, loss_out,
                 leg_p, leg_q, lat, w1, w2, f_tab, g_tab, ft_tab, gt_tab,
                 xh, th, pk, rows, yrow, hy,
                 xs, sr, dsr, ys, yr, dyr, als, ar, dar, bs, br, dbr, asave, dsave, aall, dall,
                 st_s, st_h, st_m, st_w, tab_s, tab_w, tab, down_p, down_q, up_p, up_q, ker,
                 gw, gw_p, gw_a, gw_z, gw_zs, gw_h, gw_hs, gw_w, gw_ws, gw_w2, gw_h2, gw_f, gw_o,
                 ls, ls_p, ls_a, ls_z, ls_zs, ls_h, ls_hs, ls_w, gs_acc, gs_sum0, gs_sum1, gs_b0, gs_b1,
                 sem_x, sem_y, sem_d, sem_n, sem_s, sem_ds, sem_u, sem_du, sem_a, sem_da, sem_b, sem_db, sem_az, sem_dz,
                 sem_in, sem_st, sem_tab, sem_k, sem_gw, sem_ls, sem_gs, sem_gf, sem_fin, sem_small):
    dp_size, h_size, w_size = sizes
    dp, h, w = lax.axis_index("dp"), lax.axis_index("h"), lax.axis_index("w")
    ndev = h_size * w_size
    me = h * w_size + w
    nb, nt, npl, nc = x.shape
    ntp = nt // 2
    part = ntp // PARTS
    nlon = npl * w_size
    nlat = nt * h_size
    nl = als.shape[1] // 8
    l_own = nl // ndev
    piece = 8 * l_own
    unsent, coming = {}, {}

    def got(key):
        coming.pop(key)()

    def peer(k):
        return (h + k // w_size) % h_size, (w + k % w_size) % w_size

    barrier = pltpu.get_barrier_semaphore()

    def meet(k, _):
        h2, w2_ = peer(k)
        pl.semaphore_signal(barrier, inc=1, device_id={"h": h2, "w": w2_}, device_id_type=MESH)
        return 0

    def meet_dp(k, _):
        pl.semaphore_signal(barrier, inc=1, device_id={"dp": (dp + k) % dp_size}, device_id_type=MESH)
        return 0

    lax.fori_loop(1, ndev, meet, 0)
    lax.fori_loop(1, dp_size, meet_dp, 0)
    loads = [pltpu.make_async_copy(x.at[b], xh.at[b], sem_in.at[b, 0]) for b in range(nb)]
    load_t = [pltpu.make_async_copy(tgt.at[b], th.at[b], sem_in.at[b, 1]) for b in range(nb)]
    load_k = pltpu.make_async_copy(spec_w.at[:, pl.ds(me * l_own, l_own)], ker, sem_k.at[0])
    small = [pltpu.make_async_copy(src, dst, sem_small.at[i]) for i, (src, dst) in enumerate((
        (leg_p_in, leg_p), (leg_q_in, leg_q), (f_in, f_tab), (lat_in, lat), (w1_in, w1), (w2_in, w2)))]
    for c in loads + small[:3] + [load_k] + load_t + small[3:]:
        c.start()
    coming["k"] = load_k.wait
    coming["small"] = lambda: [c.wait() for c in small[3:]]
    coming.update({("t", b): load_t[b].wait for b in range(nb)})
    for ref in (ar, br, dar, dbr, st_s, gw, ls):
        ref[...] = jnp.zeros_like(ref)

    def settle(*keys):
        for key in keys or list(unsent):
            for wait in unsent.pop(key, []):
                wait()

    def along(axis, refs, sems, sent, key=None):
        size, index = {"dp": (dp_size, dp), "h": (h_size, h), "w": (w_size, w)}[axis]
        src, dst = refs(index)
        keep(src, dst, sems)

        def body(k, _):
            other = (index + k) % size
            src, dst = refs(other)
            push(src, dst, sems, {axis: other})
            return 0

        lax.fori_loop(1, size, body, 0)
        unsent.setdefault(key, []).append(lambda: drain(sent, sems.at[0]))

    def some(refs, sems, low_h, high_h, count, counts, key):
        src, dst = refs(h, w)
        keep(src, dst, sems)

        def one(h2, k):
            w2_ = (w + k) % w_size
            src, dst = refs(h2, w2_)
            push(src, dst, sems, {"h": h2, "w": w2_})

        for k in range(1, w_size):
            one(h, k)

        def body(h2, _):
            for k in range(w_size):
                one(h2, k)
            return 0

        lax.fori_loop(low_h, high_h, body, 0)
        unsent.setdefault(key, []).append(lambda: take(sems.at[0], count - 1, [n - 1 for n in counts]))

    def take(sem, count, counts):
        for n in counts:
            @pl.when(count == n)
            def _():
                drain(als.at[0, pl.ds(0, n * piece)], sem)

    n_orders, n_owners = (h + 1) * w_size, (h_size - h) * w_size
    counts = [w_size * n for n in range(1, h_size + 1)]
    pairs = lambda k: pl.ds(k * part, part)

    def at_rows(i, k):
        return pl.ds(pl.multiple_of(i * 16 * ntp + k * 16 * part, 16 * part), 16 * part)

    def send_home_rows(b, k, sem, name):
        along("w", lambda o: (pk.at[b, o, pairs(k)], rows.at[b, pairs(k), rows_at(w, npl)]), sem.at[b, k],
              pk.at[b, pl.ds(0, w_size - 1), pairs(k)], ("pk", b, k))
        coming[name, b, k] = lambda: drain(rows.at[b, pairs(k)], sem.at[b, k, 1])

    def send_rows_home(b, k, sem, name):
        along("w", lambda o: (yrow.at[b, o, pairs(k)], hy.at[b, w, pairs(k)]), sem.at[b, k],
              yrow.at[b, pl.ds(0, w_size - 1), pairs(k)], ("yrow", b, k))
        coming[name, b, k] = lambda: drain(hy.at[b, :, pairs(k)], sem.at[b, k, 1])

    def send_orders(b, k, dst, sem, name):
        along("h", lambda o: (xs.at[b, o, at_rows(0, k)], dst.at[b, at_rows(h, k)]), sem.at[b, k],
              xs.at[b, pl.ds(0, h_size - 1), at_rows(0, k)], ("xs", b, k))
        coming[name, b, k] = lambda: drain(xs.at[b, :, at_rows(0, k)], sem.at[b, k, 1])

    def send_lats(b, dst, sem, name):
        def one(k, _):
            keep(ys.at[b, at_rows(h, k)], dst.at[b, h, at_rows(0, k)], sem.at[b, k])

            def body(j, _):
                o = (h + j) % h_size
                push(ys.at[b, at_rows(o, k)], dst.at[b, h, at_rows(0, k)], sem.at[b, k], {"h": o})
                return 0

            return lax.fori_loop(1, h_size, body, 0)

        lax.fori_loop(0, PARTS, one, 0)
        for k in range(PARTS):
            unsent.setdefault(("ys", b), []).append(lambda k=k: drain(xs.at[b, pl.ds(0, h_size - 1), at_rows(0, k)], sem.at[b, k, 0]))
            coming[name, b, k] = lambda k=k: drain(dst.at[b, :, at_rows(0, k)], sem.at[b, k, 1])

    def send_owner(b, dst, sem, name):
        some(lambda h2, w2_: (als.at[b, rows_at(h2 * w_size + w2_, piece)], dst.at[b, h, :, lanes_at(w)]), sem.at[b],
             h + 1, h_size, n_owners, counts, ("als", b))
        coming[name, b] = lambda: take(sem.at[b, 1], n_orders, counts)

    def send_back(b, dst, sem, name):
        some(lambda h2, w2_: (bs.at[b, h2, w2_], dst.at[b, rows_at(me, piece)]), sem.at[b],
             0, h, n_orders, counts, ("bs", b))
        coming[name, b] = lambda: take(sem.at[b, 1], n_owners, counts)

    def dft(b, k, table):
        settle(("xs", b, k))

        def body(n, _):
            i = 2 * n
            both = jnp.concatenate([rows[b, i], rows[b, i + 1]], axis=1)
            out = dot(table[...], both).reshape(h_size, 16, 2 * LANES)
            xs[b, :, rows_at(i, 16), :] = out[:, :, :LANES]
            xs[b, :, rows_at(i + 1, 16), :] = out[:, :, LANES:]
            return 0

        lax.fori_loop(k * part // 2, (k + 1) * part // 2, body, 0)

    def idft(b, k, table, src):
        settle(("yrow", b, k))

        def body(n, _):
            i = 2 * n
            both = jnp.concatenate([src[b, :, rows_at(i + j, 16), :].reshape(-1, LANES) for j in range(2)], axis=1)
            out = dot(table[...], both)
            for j in range(2):
                yrow[b, :, i + j] = out[:, j * LANES:(j + 1) * LANES].reshape(w_size, npl, LANES)
            return 0

        lax.fori_loop(k * part // 2, (k + 1) * part // 2, body, 0)

    def level(v, here):
        mean = jnp.mean(v, axis=0, keepdims=True)
        mean = 0.5 * (mean + flip(mean))
        return v - jnp.where(jnp.logical_and(h == 0, here), mean, 0.0)

    def orders(body):
        def four(n, _):
            for i in range(4):
                body(4 * n + i, n == 0 if i == 0 else None)
            return 0

        lax.fori_loop(0, 2, four, 0)

    def leg_down(b, table, src, fix):
        settle(("als", b))

        def one(m, here):
            re, im = (src[b, pl.ds(ri * 8 + m, ntp * h_size, stride=16), :] for ri in range(2))
            if fix and here is not None:
                re = level(re, here)
            als[b, pl.ds(m, nl, stride=8), :] = dot(table[m], jnp.concatenate(weave(re, im), axis=0))

        orders(one)

    def leg_up(b, table, src, fix):
        settle(("ys", b))

        def one(m, here):
            out = dot(table[m], src[b, pl.ds(m, nl, stride=8), :])
            re, im = weave(out[:nlat // 2], out[nlat // 2:])
            if fix and here is not None:
                re = level(re, here)
            ys[b, pl.ds(m, ntp * h_size, stride=16), :] = re
            ys[b, pl.ds(8 + m, ntp * h_size, stride=16), :] = im

        orders(one)

    def owned(b, l, src):
        tiles = [src[b, :, rows_at(l, 8), j * LANES:(j + 1) * LANES].reshape(-1, LANES) for j in range(w_size)]
        return weave_wide(tiles)

    def put_back(b, l, re, im):
        for j, tile in enumerate(weave_tiles(re, im)):
            bs[b, :, j, rows_at(l, 8), :] = tile.reshape(h_size, 8, LANES)

    def put_rows(b, i, v0, v1):
        for j, tile in enumerate(weave_tiles(v0, v1)):
            pk[b, j, i] = tile

    def get_rows(b, i):
        return weave_wide([hy[b, j, i] for j in range(w_size)])

    count = nt * npl
    n_tab = tab_s.shape[1] // dp_size

    def combine(stats, n):
        mean = jnp.mean(stats, axis=0)
        dev = stats - mean[None]
        dev2 = jnp.sum(dev * dev, axis=0)
        m2 = jnp.sum(stats, axis=0)
        return [(mean[2 * b:2 * b + 1], m2[2 * b + 1:2 * b + 2] + n * dev2[2 * b:2 * b + 1]) for b in range(nb)]

    sums = {}

    def pk_(b):
        loads[b].wait()

        def body(i, total):
            v0, v1 = xh[b, i], xh[b, i + ntp]
            put_rows(b, i, v0, v1)
            return total + jnp.sum(v0 + v1, axis=0, keepdims=True)

        sums[b] = lax.fori_loop(0, ntp, body, jnp.zeros((1, nc), F32))

    def go():
        for c in small[:3]:
            c.wait()
        for a, leg in enumerate((leg_p, leg_q)):
            for m in range(leg.shape[0]):
                tab_s[a, m // 2, :, m % 2 * nl:(m % 2 + 1) * nl] = leg[m]
        pl.semaphore_wait(barrier, ndev - 1 + dp_size - 1)
        along("w", lambda o: (tab_s.at[:, rows_at(dp, n_tab)], tab_w.at[:, w, rows_at(dp, n_tab)]), sem_tab.at[0],
              tab_w.at[:, pl.ds(0, w_size - 1), pl.ds(0, n_tab)])
        coming["tab"] = lambda: drain(tab_w.at[:, :, pl.ds(0, n_tab)], sem_tab.at[0, 1])

    def st1():
        for b in range(nb):
            mean = sums[b] / count

            def body(t, total, b=b, mean=mean):
                d = xh[b, t] - mean
                return total + jnp.sum(d * d, axis=0, keepdims=True)

            st_s[2 * b:2 * b + 1, :] = mean
            st_s[2 * b + 1:2 * b + 2, :] = lax.fori_loop(0, nt, body, jnp.zeros((1, nc), F32))
        along("w", lambda o: (st_s, st_w.at[w]), sem_st.at[0], st_w.at[pl.ds(0, w_size - 1)], "st")
        coming["st"] = lambda: drain(st_w, sem_st.at[0, 1])
        g_tab[...] = jnp.where(lax.broadcasted_iota(jnp.int32, f_tab.shape, 0) == 0, 1.0, 2.0) * f_tab[...]
        ft_tab[...] = f_tab[...].T
        gt_tab[...] = g_tab[...].T

    def st2():
        got("st")
        st_m[...] = jnp.zeros_like(st_m)
        for b, (mean, m2) in enumerate(combine(st_w[...], count)):
            st_m[2 * b:2 * b + 1, :] = mean
            st_m[2 * b + 1:2 * b + 2, :] = m2
        along("h", lambda o: (st_m, st_h.at[h]), sem_st.at[1], st_h.at[pl.ds(0, h_size - 1)], "st")
        coming["st2"] = lambda: drain(st_h, sem_st.at[1, 1])

    means, scales = [], []

    def st3():
        got("st2")
        for mean, m2 in combine(st_h[...], count * w_size):
            means.append(mean)
            scales.append(lax.rsqrt(m2 / (count * ndev) + NORM_EPS))

    def tb1():
        got("tab")
        for a in range(2):
            share = tab_w.at[a, :, rows_at(dp, n_tab)]
            for k in range(1, dp_size):
                push(share, share, sem_tab.at[1 + a], {"dp": (dp + k) % dp_size})
            others = tab_w.at[a, :, pl.ds(0, (dp_size - 1) * n_tab)]
            unsent.setdefault(None, []).append(lambda a=a, others=others: drain(others, sem_tab.at[1 + a, 0]))
            coming["tab1", a] = lambda a=a, others=others: drain(others, sem_tab.at[1 + a, 1])

    def table_out(a):
        got(("tab1", a))
        along("h", lambda o: (tab_w.at[a, o // 2, rows_at(o % 2, 4)], tab.at[a, :, rows_at(h, nt)]), sem_tab.at[3 + a],
              tab.at[a, :, pl.ds(0, nlat - nt)])
        coming["tab2", a] = lambda: drain(tab.at[a], sem_tab.at[3 + a, 1])

    def table_in(a, down, up):
        got(("tab2", a))

        def body(n, _):
            both = tab[a, n].reshape(h_size, 2, ntp, 2 * nl)
            both = jnp.concatenate([both[:, j].reshape(-1, 2 * nl) for j in range(2)], axis=0)
            for j in range(2):
                t = both[:, j * nl:(j + 1) * nl]
                up[2 * n + j] = t
                down[2 * n + j] = t.T
            return 0

        lax.fori_loop(0, tab.shape[1], body, 0)

    def tb2():
        table_out(0)

    def tb3():
        table_in(0, down_p, up_p)

    def tb4():
        table_out(1)

    def tb5():
        table_in(1, down_q, up_q)

    def sX(b, k):
        send_home_rows(b, k, sem_x, "x")

    def fd(b, k):
        got(("x", b, k))
        dft(b, k, f_tab)
        send_orders(b, k, sr, sem_s, "s")

    def fl(b):
        for k in range(PARTS):
            got(("s", b, k))
        leg_down(b, down_p, sr, True)
        send_owner(b, ar, sem_a, "a")

    def fo(b):
        if not scales:
            got("k")
            st3()
        got(("a", b))
        settle(("bs", b))

        def one(l, _):
            re, im = owned(b, l, ar)
            a = jnp.concatenate([re, im], axis=0) * scales[b]
            asave[b, l] = a
            n = a.shape[0] // 2
            own, other = dot(a, ker[0, l]), dot(a, ker[1, l])
            put_back(b, l, own[:n] - other[n:], own[n:] + other[:n])
            return 0

        lax.fori_loop(0, l_own, one, 0)
        send_back(b, br, sem_b, "b")
        along("dp", lambda o: (asave.at[b, o // 2], aall.at[dp, b]), sem_az.at[b], aall.at[pl.ds(0, dp_size - 1), b])
        coming["az", b] = lambda: drain(aall.at[:, b], sem_az.at[b, 1])

    def fu(b):
        got(("b", b))
        leg_up(b, up_q, br, False)
        send_lats(b, yr, sem_u, "u")

    def fi(b, k):
        got(("u", b, k))
        idft(b, k, gt_tab, yr)

    def sY(b, k):
        send_rows_home(b, k, sem_y, "y")

    def pw(b, k):
        got(("y", b, k))
        if ("t", b) in coming:
            got(("t", b))
        if "small" in coming:
            got("small")
        settle(("pk", b, k))

        def body(n, _):
            lats = [n, n + ntp]
            y = jnp.concatenate(get_rows(b, n), axis=0)
            yb = y.astype(BF16)
            hid = bdot(yb, w1[...])
            th_ = jnp.tanh(GELU_C * (hid + GELU_A * (hid * hid * hid)))
            act = (hid * (0.5 * (1.0 + th_))).astype(BF16)
            resid = y + bdot(act, w2[...])
            parts = []
            for j, t in enumerate(lats):
                r = resid[j * npl:(j + 1) * npl] + xh[b, t] - th[b, t]
                d = lat[t] * r
                ls[...] += jnp.sum((d * r).reshape(-1, 8, nc), axis=0)
                dout[b, t] = d
                parts.append(d)
            d = jnp.concatenate(parts, axis=0)
            db = d.astype(BF16)
            gw[2 * nc:, :] += bdot(act, db, TN)
            slope = 0.5 * (1.0 + th_) + (0.5 * GELU_C) * hid * (1.0 - th_ * th_) * (1.0 + (3.0 * GELU_A) * (hid * hid))
            dh = (bdot(db, w2[...], NT) * slope).astype(BF16)
            gin = bdot(yb, dh, TN)
            gw[:nc, :] += gin[:, :nc]
            gw[nc:2 * nc, :] += gin[:, nc:]
            dy = d + bdot(dh, w1[...], NT)
            put_rows(b, n, dy[:npl], dy[npl:])
            return 0

        lax.fori_loop(k * part, (k + 1) * part, body, 0)

    def sD(b, k):
        send_home_rows(b, k, sem_d, "d")

    def bd(b, k):
        got(("d", b, k))
        dft(b, k, g_tab)
        send_orders(b, k, dsr, sem_ds, "ds")

    def bl(b):
        for k in range(PARTS):
            got(("ds", b, k))
        leg_down(b, down_q, dsr, False)
        send_owner(b, dar, sem_da, "da")

    def bo(b):
        got(("da", b))
        settle(("bs", b), "st")

        def one(l, s2):
            re, im = owned(b, l, dar)
            d = jnp.concatenate([re, im], axis=0)
            dsave[b, l] = d
            n = d.shape[0] // 2
            own, other = dot(d, ker[0, l], NT), dot(d, ker[1, l], NT)
            re, im = own[:n] + other[n:], own[n:] - other[:n]
            put_back(b, l, re, im)
            return s2 + jnp.sum(re * asave[b, l, :n] + im * asave[b, l, n:], axis=0, keepdims=True)

        s2 = lax.fori_loop(0, l_own, one, jnp.zeros((1, nc), F32))
        send_back(b, dbr, sem_db, "db")
        along("dp", lambda o: (dsave.at[b, o // 2, :, lanes_at(o % 2)], dall.at[dp, b]), sem_dz.at[b], dall.at[pl.ds(0, dp_size - 1), b])
        coming["dz", b] = lambda: drain(dall.at[:, b], sem_dz.at[b, 1])
        st_s[b:b + 1, :] = s2

    def bu(b):
        got(("db", b))
        leg_up(b, up_p, dbr, True)
        send_lats(b, dyr, sem_du, "du")

    def bi(b, k):
        got(("du", b, k))
        idft(b, k, ft_tab, dyr)

    def sN(b, k):
        send_rows_home(b, k, sem_n, "n")

    def pj1():
        st_s[nb:, :] = jnp.zeros_like(st_s[nb:, :])
        along("w", lambda o: (st_s, st_w.at[w]), sem_st.at[2], st_w.at[pl.ds(0, w_size - 1)])
        coming["pj"] = lambda: drain(st_w, sem_st.at[2, 1])

    def pj2():
        got("pj")
        st_m[...] = jnp.sum(st_w[...], axis=0)
        along("h", lambda o: (st_m, st_h.at[h]), sem_st.at[3], st_h.at[pl.ds(0, h_size - 1)])
        coming["pj2"] = lambda: drain(st_h, sem_st.at[3, 1])

    proj = []

    def fn(b, k):
        if not proj:
            got("pj2")
            proj.append(jnp.sum(st_h[...], axis=0) / (count * ndev))
        got(("n", b, k))

        def body(i, _):
            for t, dn in zip((i, i + ntp), get_rows(b, i)):
                normed = (xh[b, t] - means[b]) * scales[b]
                dout[b, t] = dout[b, t] + scales[b] * (dn - normed * proj[0][b:b + 1])
            return 0

        lax.fori_loop(k * part, (k + 1) * part, body, 0)

    n_c, n_z, n_h, n_w = gw_a.shape[0], gw_zs.shape[0], gw_hs.shape[0], gw_ws.shape[0]
    chip, core = h // 2, h % 2
    chips = h_size // 2

    def over_chips(refs, sems, sent):
        src, dst = refs(chip)
        keep(src, dst, sems)
        for k in range(1, chips):
            o = (chip + k) % chips
            src, dst = refs(o)
            push(src, dst, sems, {"h": 2 * o + core})
        unsent.setdefault(None, []).append(lambda: drain(sent, sems.at[0]))

    def twin(src, dst, sems):
        push(src, dst, sems, {"h": h + 1 - 2 * core})
        unsent.setdefault(None, []).append(lambda: drain(dst, sems.at[0]))

    def gw1():
        twin(gw.at[rows_at(1 - core, n_c)], gw_p, sem_gw.at[0])
        twin(ls, ls_p, sem_ls.at[0])
        coming["gw1"] = lambda: (drain(gw_p, sem_gw.at[0, 1]), drain(ls_p, sem_ls.at[0, 1]))

    def gw2():
        got("gw1")
        gw_a[...] = gw[rows_at(core, n_c), :] + gw_p[...]
        ls_a[...] = ls[...] + ls_p[...]
        along("dp", lambda o: (gw_a.at[rows_at(o, n_z)], gw_z.at[dp]), sem_gw.at[1], gw_z.at[pl.ds(0, dp_size - 1)])
        along("dp", lambda o: (ls_a, ls_z.at[dp]), sem_ls.at[1], ls_z.at[pl.ds(0, dp_size - 1)])
        coming["gw2"] = lambda: (drain(gw_z, sem_gw.at[1, 1]), drain(ls_z, sem_ls.at[1, 1]))

    def gw3():
        got("gw2")
        gw_zs[...] = jnp.sum(gw_z[...], axis=0)
        ls_zs[...] = jnp.sum(ls_z[...], axis=0)
        over_chips(lambda o: (gw_zs.at[rows_at(o, n_h)], gw_h.at[chip]), sem_gw.at[2], gw_h.at[pl.ds(0, chips - 1)])
        over_chips(lambda o: (ls_zs, ls_h.at[chip]), sem_ls.at[2], ls_h.at[pl.ds(0, chips - 1)])
        coming["gw3"] = lambda: (drain(gw_h, sem_gw.at[2, 1]), drain(ls_h, sem_ls.at[2, 1]))

    def gw4():
        got("gw3")
        gw_hs[...] = jnp.sum(gw_h[...], axis=0)
        ls_hs[...] = jnp.sum(ls_h[...], axis=0)
        along("w", lambda o: (gw_hs.at[rows_at(o, n_w)], gw_w.at[w]), sem_gw.at[3], gw_w.at[pl.ds(0, w_size - 1)])
        along("w", lambda o: (ls_hs, ls_w.at[w]), sem_ls.at[3], ls_w.at[pl.ds(0, w_size - 1)])
        coming["gw4"] = lambda: (drain(gw_w, sem_gw.at[3, 1]), drain(ls_w, sem_ls.at[3, 1]))

    def gw5():
        got("gw4")
        gw_ws[...] = jnp.sum(gw_w[...], axis=0)
        loss_out[...] = jnp.sum(ls_w[...], keepdims=True).reshape(1, 1) / total_points
        along("w", lambda o: (gw_ws, gw_w2.at[rows_at(w, n_w)]), sem_gw.at[4], gw_w2.at[pl.ds(0, (w_size - 1) * n_w)])
        coming["gw5"] = lambda: drain(gw_w2, sem_gw.at[4, 1])

    def gw6():
        got("gw5")
        over_chips(lambda o: (gw_w2, gw_h2.at[rows_at(chip, n_h)]), sem_gw.at[5], gw_h2.at[pl.ds(0, (chips - 1) * n_h)])
        coming["gw6"] = lambda: drain(gw_h2, sem_gw.at[5, 1])

    def gw7():
        got("gw6")
        along("dp", lambda o: (gw_h2, gw_f.at[rows_at(dp, n_z)]), sem_gw.at[6], gw_f.at[pl.ds(0, (dp_size - 1) * n_z)])
        coming["gw7"] = lambda: drain(gw_f, sem_gw.at[6, 1])

    def gw8():
        got("gw7")
        twin(gw_f, gw_o, sem_gw.at[7])
        coming["gw8"] = lambda: drain(gw_o, sem_gw.at[7, 1])

    def end():
        got("gw8")
        for c, halves in enumerate(((gw_f, gw_o), (gw_o, gw_f))):
            @pl.when(core == c)
            def _():
                first, second = halves
                for i, (src, dst) in enumerate(((first.at[:nc], gin_out.at[:, :nc]), (first.at[nc:], gin_out.at[:, nc:]), (second, gout_out))):
                    pltpu.make_async_copy(src, dst, sem_fin.at[i]).start()
        for i, dst in enumerate((gin_out.at[:, :nc], gin_out.at[:, nc:], gout_out)):
            unsent.setdefault(None, []).append(lambda dst=dst, i=i: drain(dst, sem_fin.at[i]))

    gs_sum, gs_b = (gs_sum0, gs_sum1), (gs_b0, gs_b1)
    first_rows = (0, gs_sum0.shape[1])
    axes = (("w", "dp"), ("dp", "w"))
    place = {"w": (w, w_size), "dp": (dp, dp_size)}

    def next_to(axis, k):
        index, size = place[axis]
        return (index + k + size) % size

    def add_sample(b):
        got(("az", b))
        got(("dz", b))

        def body(n, _):
            d = dall[n, b]
            half = d.shape[0] // 2
            both = jnp.concatenate([d, jnp.concatenate([d[half:], -d[:half]], axis=0)], axis=1)
            gs_acc[...] += dot(aall[n, b], both, TN)
            return 0

        lax.fori_loop(0, dp_size, body, 0)

    def gsa():
        gs_acc[...] = jnp.zeros_like(gs_acc)
        add_sample(GS_FIRST[0])

    def gsb():
        add_sample(GS_FIRST[1])

    def gs1():
        add_sample(GS_FIRST[2])
        for q in range(2):
            rows_q = pl.ds(first_rows[q], gs_sum[q].shape[1])
            for p in range(2):
                gs_sum[q][p] = gs_acc[rows_q, p * LANES:(p + 1) * LANES]

    def once(key):
        if key in coming:
            got(key)

    def sent_later(ref, sem):
        unsent.setdefault(None, []).append(lambda: drain(ref, sem))

    def gs2(q):
        keep(gs_sum[q], gs_b[q].at[0], sem_gs.at[q, 0])
        for slot, k in ((1, 1), (3, -1)):
            push(gs_sum[q], gs_b[q].at[slot], sem_gs.at[q, slot], {axes[q][0]: next_to(axes[q][0], k)})
            sent_later(gs_sum[q], sem_gs.at[q, slot, 0])
        coming.update({("gs", q, k): lambda k=k: drain(gs_b[q].at[k], sem_gs.at[q, k, 1]) for k in (0, 1, 3)})

    def gs6(q):
        for slot, p, k, i in ((1, 0, 1, 2), (3, 1, -1, 4)):
            once(("gs", q, slot))
            push(gs_b[q].at[slot, p], gs_b[q].at[2, p], sem_gs.at[q, i], {axes[q][0]: next_to(axes[q][0], k)})
            sent_later(gs_b[q].at[2, p], sem_gs.at[q, i, 0])
        coming["gs", q, 2] = lambda: (drain(gs_b[q].at[2, 0], sem_gs.at[q, 2, 1]), drain(gs_b[q].at[2, 1], sem_gs.at[q, 4, 1]))

    def block_at(q, k, shift):
        at = {axes[q][0]: next_to(axes[q][0], -k), axes[q][1]: next_to(axes[q][1], shift)}
        return gs_out.at[:, l_own * at["w"] + at["dp"] // 2, pl.ds(first_rows[q], gs_sum[q].shape[1]), lanes_at(at["dp"] % 2)]

    def gs3(q, k):
        once(("gs", q, k))
        mine = block_at(q, k, 0)
        pltpu.make_async_copy(gs_b[q].at[k], mine, sem_gf.at[q, 3, k, 0]).start()
        for way, shift in ((0, 1), (1, -1)):
            push(gs_b[q].at[k], mine, sem_gf.at[q, way, k], {axes[q][1]: next_to(axes[q][1], shift)})

    def gs4(q, k):
        way, shift = (0, 1) if k < 2 else (1, -1)
        drain(gs_b[q].at[k], sem_gf.at[q, way, k, 1])
        block = block_at(q, k, -shift)
        push(block, block, sem_gf.at[q, 2, k], {axes[q][1]: next_to(axes[q][1], shift)})

    def gs5(q, k):
        drain(gs_b[q].at[k], sem_gf.at[q, 1 if k < 2 else 0, k, 1])
        drain(gs_b[q].at[k], sem_gf.at[q, 2, k, 1])
        for i in range(4):
            drain(gs_b[q].at[k], sem_gf.at[q, i, k, 0])

    scope = dict(locals())
    scope["pk"] = pk_
    for name in ORDER.split():
        call = name.rstrip("0123456789") or name
        if name in scope:
            scope[name]()
        elif name[:3] in scope:
            scope[name[:3]](*map(int, name[3:]))
        else:
            scope[call](*map(int, name[len(call):]))
    assert not coming
    settle()


def hand_on_kernel(*refs):
    n = len(refs) // 2
    pairs = []
    for src, dst in zip(refs[:n], refs[n:2 * n]):
        lead = [()] if len(src.shape) == 2 else [(i,) for i in range(src.shape[0])]
        pairs += [(src.at[i], dst.at[i]) if i else (src, dst) for i in lead]
    copies = [pltpu.make_async_copy(src, dst, refs[2 * n].at[i]) for i, (src, dst) in enumerate(pairs)]
    for c in copies:
        c.start()
    for c in copies:
        c.wait()


def hand_on(arrays):
    return pl.pallas_call(
        hand_on_kernel, name="hand_on",
        out_shape=[jax.ShapeDtypeStruct(a.shape, F32) for a in arrays],
        in_specs=[pl.BlockSpec(memory_space=pltpu.VMEM)] * len(arrays), out_specs=[pl.BlockSpec(memory_space=pl.ANY)] * len(arrays),
        scratch_shapes=[pltpu.SemaphoreType.DMA((32,))],
        compiler_params=pltpu.CompilerParams(vmem_limit_bytes=12 * 1024 * 1024),
    )(*[pltpu.with_memory_space_constraint(a, pltpu.VMEM) for a in arrays])


def solution(mesh):
    dp_size, w_size, h_size = mesh.shape["dp"], mesh.shape["w"], mesh.shape["h"]

    def local_step(field, target, lat_weight, leg_fwd, leg_inv, spec_w, w_in, w_out):
        nb, nc, nt, npl = field.shape
        nlon = npl * w_size
        ntp = nt // 2
        nm = leg_fwd.shape[0] * w_size
        ndev = h_size * w_size
        nlat = nt * h_size
        nl = leg_fwd.shape[1]
        lo = nl // ndev
        assert nm == 8 * h_size and nc == w_size * LANES // 2 and h_size == 2 * w_size and 2 * lo == dp_size and 2 * nl == LANES
        total_points = nb * dp_size * nc * nlat * nlon
        any_spec = pl.BlockSpec(memory_space=pl.ANY)
        vmem_spec = pl.BlockSpec(memory_space=pltpu.VMEM)
        sds = lambda *s: jax.ShapeDtypeStruct(s, F32)
        vm = lambda *s: pltpu.VMEM(s, F32)
        dma = lambda *s: pltpu.SemaphoreType.DMA(s)
        n_rows = 2 * nc + w_out.shape[0]
        n_z, n_h, n_w = n_rows // dp_size, n_rows // dp_size // h_size, n_rows // dp_size // h_size // w_size
        home = vm(nb, nt, npl, nc)
        woven = vm(nb, w_size, ntp, npl, LANES)
        order = vm(nb, 16 * nlat // 2, LANES)
        degree = vm(nb, 8 * nl, LANES)
        owner = vm(nb, h_size, 8 * lo, w_size * LANES)
        saved = vm(nb, lo, 2 * nm, nc)
        cut = GS_ROWS
        n_pairs = leg_fwd.shape[0] // 2
        n_c = n_rows // 2
        n_z, n_h, n_w = n_c // dp_size, n_c // dp_size // w_size, n_c // dp_size // w_size // w_size
        results = pl.pallas_call(
            functools.partial(block_kernel, (dp_size, h_size, w_size), total_points),
            name="block",
            out_shape=[vm(nb, nt, npl, nc), vm(2, lo * w_size, nc, nc), vm(nc, 2 * nc), vm(2 * nc, nc), sds(1, 1)],
            in_specs=[any_spec] * 9,
            out_specs=[vmem_spec] * 5,
            scratch_shapes=[
                vm(*leg_fwd.shape[:1], nt, nl), vm(*leg_fwd.shape[:1], nt, nl), pltpu.SMEM((nt,), F32), pltpu.VMEM(w_in.shape, BF16),
                pltpu.VMEM(w_out.shape, BF16), vm(2 * nm, nlon), vm(2 * nm, nlon), vm(nlon, 2 * nm), vm(nlon, 2 * nm),
                home, home, woven, vm(nb, ntp, nlon, LANES), woven, woven,
                vm(nb, h_size, 16 * ntp, LANES), order, order, order, vm(nb, h_size, 16 * ntp, LANES), vm(nb, h_size, 16 * ntp, LANES),
                degree, owner, owner, vm(nb, h_size, w_size, 8 * lo, LANES), degree, degree, saved, saved,
                vm(dp_size, nb, 2 * nm, nc), vm(dp_size, nb, 2 * nm, LANES),
                vm(8, nc), vm(h_size, 8, nc), vm(8, nc), vm(w_size, 8, nc),
                vm(2, n_pairs, nt, 2 * nl), vm(2, w_size, n_pairs, nt, 2 * nl), vm(2, 4, nlat, 2 * nl),
                vm(8, nl, nlat), vm(8, nl, nlat), vm(8, nlat, nl), vm(8, nlat, nl),
                vm(2, lo, nc, nc),
                vm(n_rows, nc), vm(n_c, nc), vm(n_c, nc), vm(dp_size, n_z, nc), vm(n_z, nc), vm(w_size, n_h, nc), vm(n_h, nc),
                vm(w_size, n_w, nc), vm(n_w, nc), vm(n_h, nc), vm(n_z, nc), vm(n_c, nc), vm(n_c, nc),
                vm(8, nc), vm(8, nc), vm(8, nc), vm(dp_size, 8, nc), vm(8, nc), vm(w_size, 8, nc), vm(8, nc), vm(w_size, 8, nc),
                vm(nc, nc), vm(2, cut, LANES), vm(2, nc - cut, LANES), vm(4, 2, cut, LANES), vm(4, 2, nc - cut, LANES),
            ] + [dma(nb, PARTS, 2)] * 8 + [dma(nb, 2)] * 6 + [dma(nb, 2), dma(4, 2), dma(5, 2), dma(1), dma(8, 2), dma(4, 2),
                 dma(2, 5, 2), dma(2, 4, 4, 2), dma(3), dma(6)],
            compiler_params=pltpu.CompilerParams(collective_id=0, has_side_effects=True, vmem_limit_bytes=54 * 1024 * 1024),
        )(field.transpose(0, 2, 3, 1), target.transpose(0, 2, 3, 1), leg_fwd.transpose(0, 2, 1), leg_inv.transpose(0, 2, 1),
          spec_w, lat_weight, w_in, w_out, jnp.asarray(dft_table(nlon, nm, h_size)))
        d_x, g_spec, g_in, g_out = hand_on(results[:4])
        loss = results[4]
        return loss.reshape(()), d_x.transpose(0, 3, 1, 2), g_spec, g_in, g_out

    grid_spec = P("dp", None, "h", "w")
    table_spec = P("w", None, "h")
    kernel_spec = P(None, "h", None, None)
    return jax.shard_map(local_step, mesh=mesh, in_specs=(grid_spec, grid_spec, P("h"), table_spec, table_spec, P(), P(), P()), out_specs=(P(), grid_spec, kernel_spec, P(), P()), check_vma=False)
```

```python
import functools
import jax
import jax.numpy as jnp
import numpy as np
from jax import lax
from jax.experimental import pallas as pl
from jax.experimental.pallas import tpu as pltpu
from jax.sharding import PartitionSpec as P

NORM_EPS = 1e-5
PRECISE = lax.Precision.HIGHEST
MESH = pl.DeviceIdType.MESH
F32 = jnp.float32
BF16 = jnp.bfloat16
GELU_C = float(np.sqrt(2.0 / np.pi))
GELU_A = 0.044715
LANES = 128
NN = (((1,), (0,)), ((), ()))
NT = (((1,), (1,)), ((), ()))
TN = (((0,), (0,)), ((), ()))


def dot(a, b, dims=NN):
    return lax.dot_general(a, b, dims, precision=PRECISE, preferred_element_type=F32)


def bdot(a, b, dims=NN):
    return lax.dot_general(a, b, dims, preferred_element_type=F32)


def dft_table(lon_count, num_modes, h_size):
    modes, lons = np.arange(num_modes), np.arange(lon_count)
    angle = 2.0 * np.pi * ((modes[:, None] * lons[None, :]) % lon_count) / lon_count
    table = np.stack([np.cos(angle), -np.sin(angle)], 0) * lon_count ** -0.5
    groups = table.reshape(2, 2 * h_size, num_modes // h_size // 2, lon_count)
    table = np.stack([groups[:, :h_size], groups[:, :h_size - 1:-1]], 2).transpose(1, 0, 2, 3, 4)
    return table.reshape(2 * num_modes, lon_count).astype(np.float32)


def drain(ref, sem):
    pltpu.make_async_copy(ref, ref, sem).wait()


def rows_at(i, n):
    return pl.ds(pl.multiple_of(i * n, n), n)


def lanes_at(i):
    return pl.ds(pl.multiple_of(i * LANES, LANES), LANES)


def push(src, dst, sems, device):
    pltpu.make_async_remote_copy(src_ref=src, dst_ref=dst, send_sem=sems.at[0], recv_sem=sems.at[1],
                                 device_id=device, device_id_type=MESH).start()


def keep(src, dst, sems):
    pltpu.make_async_copy(src, dst, sems.at[1]).start()


def flip(v):
    return pltpu.roll(v, LANES // 2, 1)


def low(v):
    return lax.broadcasted_iota(jnp.int32, v.shape, 1) < LANES // 2


def weave(a, b):
    return jnp.where(low(a), a, flip(b)), jnp.where(low(a), flip(a), b)


def weave_wide(tiles):
    pairs = [weave(tiles[j], tiles[j + 1]) for j in range(0, len(tiles), 2)]
    return jnp.concatenate([p[0] for p in pairs], axis=1), jnp.concatenate([p[1] for p in pairs], axis=1)


def weave_tiles(a, b):
    out = []
    for j in range(0, a.shape[1], LANES):
        out.extend(weave(a[:, j:j + LANES], b[:, j:j + LANES]))
    return out


PARTS = 4
N_PARTS = 2
GS_ROWS = 176
GS_FIRST = (0, 1, 2)
ORDER = " ".join((
    'go', 'pk0', 'sX03', 'pk2', 'sX00', 'pk1', 'sX02', 'tb1', 'sX01', 'st1',
    'sX11', 'fd03', 'fd00', 'sX10', 'tb2', 'fd01', 'fd02', 'tb4', 'sX12', 'tb3',
    'st2', 'sX13', 'fd10', 'fl0', 'sX21', 'fd12', 'fd13', 'fd11', 'tb5', 'sX23',
    'fo0', 'fl1', 'sX20', 'sX22', 'fu0', 'fo1', 'fi00', 'sY00', 'fd23', 'fi01',
    'fd21', 'sY01', 'fd22', 'fi02', 'sY02', 'fd20', 'pw00', 'fi03', 'sY03', 'fu1',
    'pw01', 'sD01', 'fl2', 'sD00', 'fi12', 'fi10', 'pw02', 'sY12', 'bd01', 'sY10',
    'fi11', 'fi13', 'fo2', 'sY11', 'pw03', 'sY13', 'pw12', 'sD03', 'sD02', 'fu2',
    'bd00', 'pw10', 'pw13', 'fi20', 'sD10', 'sD12', 'fi21', 'pw11', 'sD13', 'sD11',
    'bd02', 'bd03', 'sY20', 'fi22', 'bl0', 'bd11', 'bd12', 'bd13', 'bd10', 'sY21',
    'fi23', 'sY23', 'bo0', 'pw20', 'sY22', 'bl1', 'pw21', 'pw23', 'sD20', 'bu0',
    'sD23', 'pw22', 'sD21', 'sD22', 'gw1', 'bo1', 'bd20', 'gw2', 'bd23', 'bi00',
    'sN00', 'bd21', 'bd22', 'gsa', 'gw3', 'bi01', 'bl2', 'bu1', 'gw4', 'sN01',
    'gsb', 'gw5', 'bo2', 'bi10', 'sN10', 'gw6', 'pj1', 'gs1', 'gs20', 'gs21',
    'bi11', 'bu2', 'gs300', 'gw7', 'sN11', 'gs61', 'pj2', 'gs60', 'bi20', 'gs310',
    'gs400', 'gs313', 'bi21', 'fn10', 'fn11', 'sN21', 'gs303', 'gs311', 'gs312', 'gs302',
    'gs403', 'gs301', 'gs410', 'fn01', 'sN20', 'gs402', 'gs413', 'fn21', 'gs401', 'gw8',
    'gs412', 'gs503', 'fn00', 'gs411', 'end', 'gs501', 'fn20', 'gs513', 'gs510', 'gs500',
    'gs512', 'gs502', 'gs511',
))


def block_kernel(sizes, total_points,
                 x, tgt, leg_p_in, leg_q_in, spec_w, lat_in, w1_in, w2_in, f_in,
                 dout, gs_out, gin_out, gout_out, loss_out,
                 leg_p, leg_q, lat, w1, w2, f_tab, g_tab, ft_tab, gt_tab,
                 xh, th, pk, rows, yrow, hy,
                 xs, sr, dsr, ys, yr, dyr, als, ar, dar, bs, br, dbr, asave, dsave, aall, dall, mix,
                 st_s, st_h, st_m, st_w, tab_s, tab_w, tab, turned, down_p, down_q, up_p, up_q, ker,
                 gw, gw_p, gw_a, gw_z, gw_zs, gw_h, gw_hs, gw_w, gw_ws, gw_w2, gw_h2, gw_f, gw_o,
                 ls, ls_p, ls_a, ls_z, ls_zs, ls_h, ls_hs, ls_w, gs_acc, gs_sum0, gs_sum1, gs_b0, gs_b1,
                 sem_x, sem_y, sem_d, sem_n, sem_s, sem_ds, sem_u, sem_du, sem_a, sem_da, sem_b, sem_db, sem_az, sem_dz,
                 sem_in, sem_st, sem_tab, sem_k, sem_gw, sem_ls, sem_gs, sem_gf, sem_fin, sem_small):
    dp_size, h_size, w_size = sizes
    dp, h, w = lax.axis_index("dp"), lax.axis_index("h"), lax.axis_index("w")
    ndev = h_size * w_size
    me = h * w_size + w
    nb, nt, npl, nc = x.shape
    ntp = nt // 2
    nlon = npl * w_size
    nlat = nt * h_size
    nl = als.shape[1] // 8
    l_own = nl // ndev
    piece = 8 * l_own
    unsent, coming = {}, {}

    def got(key):
        coming.pop(key)()

    def peer(k):
        return (h + k // w_size) % h_size, (w + k % w_size) % w_size

    barrier = pltpu.get_barrier_semaphore()

    def meet(k, _):
        h2, w2_ = peer(k)
        pl.semaphore_signal(barrier, inc=1, device_id={"h": h2, "w": w2_}, device_id_type=MESH)
        return 0

    def meet_dp(k, _):
        pl.semaphore_signal(barrier, inc=1, device_id={"dp": (dp + k) % dp_size}, device_id_type=MESH)
        return 0

    lax.fori_loop(1, ndev, meet, 0)
    lax.fori_loop(1, dp_size, meet_dp, 0)
    loads = [pltpu.make_async_copy(x.at[b], xh.at[b], sem_in.at[b, 0]) for b in range(nb)]
    load_t = [pltpu.make_async_copy(tgt.at[b], th.at[b], sem_in.at[b, 1]) for b in range(nb)]
    load_k = pltpu.make_async_copy(spec_w.at[:, pl.ds(me * l_own, l_own)], ker, sem_k.at[0])
    small = [pltpu.make_async_copy(src, dst, sem_small.at[i]) for i, (src, dst) in enumerate((
        (leg_p_in, leg_p), (leg_q_in, leg_q), (f_in, f_tab), (lat_in, lat), (w1_in, w1), (w2_in, w2)))]
    for c in loads + small[:3] + [load_k] + load_t + small[3:]:
        c.start()
    coming["k"] = load_k.wait
    coming["small"] = lambda: [c.wait() for c in small[3:]]
    coming.update({("t", b): load_t[b].wait for b in range(nb)})
    for ref in (ar, br, dar, dbr, st_s, gw, ls):
        ref[...] = jnp.zeros_like(ref)

    def settle(*keys):
        for key in keys or list(unsent):
            for wait in unsent.pop(key, []):
                wait()

    def along(axis, refs, sems, sent, key=None):
        size, index = {"dp": (dp_size, dp), "h": (h_size, h), "w": (w_size, w)}[axis]
        src, dst = refs(index)
        keep(src, dst, sems)

        def body(k, _):
            other = (index + k) % size
            src, dst = refs(other)
            push(src, dst, sems, {axis: other})
            return 0

        lax.fori_loop(1, size, body, 0)
        unsent.setdefault(key, []).append(lambda: drain(sent, sems.at[0]))

    def take(sem, count, counts):
        for n in counts:
            @pl.when(count == n)
            def _():
                drain(als.at[0, pl.ds(0, n * 8)], sem)

    n_groups = 2 * h_size
    reach = ((me + 1) * l_own + 3) // 4
    last = n_groups - 1
    low_owner = (4 * h // l_own, 4 * (last - h) // l_own)
    both_mine = last - h < reach
    n_met = 2 * ndev - 4 * last // l_own
    reaches = [(n, ((n + 1) * l_own + 3) // 4) for n in range(ndev)]
    back_counts = sorted({r * w_size - 1 - int(last - n // w_size < r) for n, r in reaches})
    pairs = lambda k, parts: pl.ds(k * (ntp // parts), ntp // parts)

    def at_rows(i, k, parts):
        size = 16 * ntp // parts
        return pl.ds(pl.multiple_of(i * 16 * ntp + k * size, size), size)

    def send_home_rows(b, k, sem, name):
        along("w", lambda o: (pk.at[b, o, pairs(k, PARTS)], rows.at[b, pairs(k, PARTS), rows_at(w, npl)]), sem.at[b, k],
              pk.at[b, pl.ds(0, w_size - 1), pairs(k, PARTS)], ("pk", b, k))
        coming[name, b, k] = lambda: drain(rows.at[b, pairs(k, PARTS)], sem.at[b, k, 1])

    def send_rows_home(b, k, sem, name, parts):
        along("w", lambda o: (yrow.at[b, o, pairs(k, parts)], hy.at[b, w, pairs(k, parts)]), sem.at[b, k],
              yrow.at[b, pl.ds(0, w_size - 1), pairs(k, parts)], (name, "row", b, k))
        coming[name, b, k] = lambda: drain(hy.at[b, :, pairs(k, parts)], sem.at[b, k, 1])

    def send_orders(b, k, dst, sem, name):
        along("h", lambda o: (xs.at[b, o, at_rows(0, k, PARTS)], dst.at[b, at_rows(h, k, PARTS)]), sem.at[b, k],
              xs.at[b, pl.ds(0, h_size - 1), at_rows(0, k, PARTS)], ("xs", b, k))
        coming[name, b, k] = lambda: drain(xs.at[b, :, at_rows(0, k, PARTS)], sem.at[b, k, 1])

    def send_lats(b, dst, sem, name, parts):
        def one(k, _):
            keep(ys.at[b, at_rows(h, k, parts)], dst.at[b, h, at_rows(0, k, parts)], sem.at[b, k])

            def body(j, _):
                o = (h + j) % h_size
                push(ys.at[b, at_rows(o, k, parts)], dst.at[b, h, at_rows(0, k, parts)], sem.at[b, k], {"h": o})
                return 0

            return lax.fori_loop(1, h_size, body, 0)

        lax.fori_loop(0, parts, one, 0)
        for k in range(parts):
            unsent.setdefault(("ys", b), []).append(lambda k=k: drain(xs.at[b, pl.ds(0, h_size - 1), at_rows(0, k, parts)], sem.at[b, k, 0]))
            coming[name, b, k] = lambda k=k: drain(dst.at[b, :, at_rows(0, k, parts)], sem.at[b, k, 1])

    def send_owner(b, dst, sem, name):
        sems = sem.at[b]
        for g in range(2):
            tile = lambda lin, g=g: (als.at[b, rows_at(lin * 2 + g, 8)], dst.at[b, h, pl.ds(g * 8, 8), lanes_at(w)])

            def body(n, _, g=g, tile=tile):
                lin = low_owner[g] + (n + me) % (ndev - low_owner[g])

                @pl.when(lin != me)
                def _():
                    push(*tile(lin), sems, {"h": lin // w_size, "w": lin % w_size})
                return 0

            if g == 0:
                keep(*tile(me), sems)
            else:
                @pl.when(both_mine)
                def _():
                    keep(*tile(me), sems)
            lax.fori_loop(0, ndev - low_owner[g], body, 0)
        unsent.setdefault(("als", b), []).append(lambda: take(sems.at[0], n_met - 1 - jnp.where(both_mine, 1, 0), [n_met - 1, n_met - 2]))
        coming[name, b] = lambda: take(sems.at[1], reach * w_size, [n * w_size for n in range(1, n_groups + 1)])

    def send_back(b, dst, sem, name):
        sems = sem.at[b]
        tile = lambda h2, w2_, g: (bs.at[b, h2, w2_, rows_at(g, 8)], dst.at[b, rows_at(me * 2 + g, 8)])

        def body(n, _):
            g = n // h_size
            h2 = jnp.where(g == 0, n, last - n)
            for k in range(w_size):
                w2_ = (w + k) % w_size
                if k:
                    push(*tile(h2, w2_, g), sems, {"h": h2, "w": w2_})
                else:
                    @pl.when(h2 != h)
                    def _():
                        push(*tile(h2, w2_, g), sems, {"h": h2, "w": w2_})
            return 0

        keep(*tile(h, w, 0), sems)

        @pl.when(both_mine)
        def _():
            keep(*tile(h, w, 1), sems)

        lax.fori_loop(0, reach, body, 0)
        count = reach * w_size - 1 - jnp.where(both_mine, 1, 0)
        unsent.setdefault(("bs", b), []).append(
            lambda: take(sems.at[0], count, back_counts))
        coming[name, b] = lambda: drain(als.at[0, pl.ds(0, n_met * 8)], sems.at[1])

    def dft(b, k, table):
        settle(("xs", b, k))

        def body(n, _):
            i = 2 * n
            both = jnp.concatenate([rows[b, i], rows[b, i + 1]], axis=1)
            out = dot(table[...], both).reshape(h_size, 16, 2 * LANES)
            xs[b, :, rows_at(i, 16), :] = out[:, :, :LANES]
            xs[b, :, rows_at(i + 1, 16), :] = out[:, :, LANES:]
            return 0

        lax.fori_loop(k * ntp // PARTS // 2, (k + 1) * ntp // PARTS // 2, body, 0)

    def idft(b, k, table, src, parts):
        settle(*(("y", "row", b, j) for j in range(PARTS * k // parts, PARTS * (k + 1) // parts)))

        def body(n, _):
            i = 2 * n
            both = jnp.concatenate([src[b, :, rows_at(i + j, 16), :].reshape(-1, LANES) for j in range(2)], axis=1)
            out = dot(table[...], both)
            for j in range(2):
                yrow[b, :, i + j] = out[:, j * LANES:(j + 1) * LANES].reshape(w_size, npl, LANES)
            return 0

        lax.fori_loop(k * ntp // parts // 2, (k + 1) * ntp // parts // 2, body, 0)

    def level(v, here):
        mean = jnp.mean(v, axis=0, keepdims=True)
        mean = 0.5 * (mean + flip(mean))
        return v - jnp.where(jnp.logical_and(h == 0, here), mean, 0.0)

    def orders(body):
        def four(n, _):
            for i in range(4):
                body(4 * n + i, n == 0 if i == 0 else None, [pl.ds(8 * n + 4 * l + i, nl // 2, stride=16) for l in range(2)])
            return 0

        lax.fori_loop(0, 2, four, 0)

    def leg_down(b, table, src, fix):
        settle(("als", b))

        def one(m, here, at):
            re, im = (src[b, pl.ds(ri * 8 + m, ntp * h_size, stride=16), :] for ri in range(2))
            if fix and here is not None:
                re = level(re, here)
            out = dot(table[m], jnp.concatenate(weave(re, im), axis=0))
            for l in range(2):
                als[b, at[l], :] = out[l * (nl // 2):(l + 1) * (nl // 2)]

        orders(one)

    def leg_up(b, table, src, fix):
        settle(("ys", b))

        def one(m, here, at):
            out = dot(table[m], jnp.concatenate([src[b, at[l], :] for l in range(2)], axis=0))
            re, im = weave(out[:nlat // 2], out[nlat // 2:])
            if fix and here is not None:
                re = level(re, here)
            ys[b, pl.ds(m, ntp * h_size, stride=16), :] = re
            ys[b, pl.ds(8 + m, ntp * h_size, stride=16), :] = im

        orders(one)

    def halves(a, b):
        upper = lax.broadcasted_iota(jnp.int32, a.shape, 1) < 4
        turn = lambda v: jnp.concatenate([v[:, 4:], v[:, :4]], axis=1)
        return jnp.where(upper, a, turn(b)), jnp.where(upper, turn(a), b)

    def take_in(b, src):
        for j in range(w_size):
            lanes = slice(j * LANES, (j + 1) * LANES)
            for l, v in enumerate(halves(src[b, :, :8, lanes], src[b, :, 8:, lanes])):
                mix[l, j] = v.reshape(-1, LANES)

    def give_out(b):
        for j in range(w_size):
            for g, v in enumerate(halves(*(mix[l, j].reshape(h_size, 8, LANES) for l in range(2)))):
                bs[b, :, j, g * 8:(g + 1) * 8, :] = v

    def owned(l):
        return weave_wide([mix[l, j] for j in range(w_size)])

    def put_back(l, re, im):
        for j, tile in enumerate(weave_tiles(re, im)):
            mix[l, j] = tile

    def put_rows(b, i, v0, v1):
        for j, tile in enumerate(weave_tiles(v0, v1)):
            pk[b, j, i] = tile

    def get_rows(b, i):
        return weave_wide([hy[b, j, i] for j in range(w_size)])

    count = nt * npl
    n_tab = tab_s.shape[1] // dp_size

    def combine(stats, n):
        mean = jnp.mean(stats, axis=0)
        dev = stats - mean[None]
        dev2 = jnp.sum(dev * dev, axis=0)
        m2 = jnp.sum(stats, axis=0)
        return [(mean[2 * b:2 * b + 1], m2[2 * b + 1:2 * b + 2] + n * dev2[2 * b:2 * b + 1]) for b in range(nb)]

    sums = {}

    def pk_(b):
        loads[b].wait()

        def body(i, total):
            v0, v1 = xh[b, i], xh[b, i + ntp]
            put_rows(b, i, v0, v1)
            return total + jnp.sum(v0 + v1, axis=0, keepdims=True)

        sums[b] = lax.fori_loop(0, ntp, body, jnp.zeros((1, nc), F32))

    def go():
        for c in small[:3]:
            c.wait()
        for a, leg in enumerate((leg_p, leg_q)):
            for m in range(leg.shape[0]):
                tab_s[a, m // 2, :, m % 2 * nl:(m % 2 + 1) * nl] = leg[m]
        pl.semaphore_wait(barrier, ndev - 1 + dp_size - 1)
        along("w", lambda o: (tab_s.at[:, rows_at(dp, n_tab)], tab_w.at[:, w, rows_at(dp, n_tab)]), sem_tab.at[0],
              tab_w.at[:, pl.ds(0, w_size - 1), pl.ds(0, n_tab)])
        coming["tab"] = lambda: drain(tab_w.at[:, :, pl.ds(0, n_tab)], sem_tab.at[0, 1])

    def st1():
        for b in range(nb):
            mean = sums[b] / count

            def body(t, total, b=b, mean=mean):
                d = xh[b, t] - mean
                return total + jnp.sum(d * d, axis=0, keepdims=True)

            st_s[2 * b:2 * b + 1, :] = mean
            st_s[2 * b + 1:2 * b + 2, :] = lax.fori_loop(0, nt, body, jnp.zeros((1, nc), F32))
        along("w", lambda o: (st_s, st_w.at[w]), sem_st.at[0], st_w.at[pl.ds(0, w_size - 1)], "st")
        coming["st"] = lambda: drain(st_w, sem_st.at[0, 1])
        g_tab[...] = jnp.where(lax.broadcasted_iota(jnp.int32, f_tab.shape, 0) == 0, 1.0, 2.0) * f_tab[...]
        ft_tab[...] = f_tab[...].T
        gt_tab[...] = g_tab[...].T

    def st2():
        got("st")
        st_m[...] = jnp.zeros_like(st_m)
        for b, (mean, m2) in enumerate(combine(st_w[...], count)):
            st_m[2 * b:2 * b + 1, :] = mean
            st_m[2 * b + 1:2 * b + 2, :] = m2
        along("h", lambda o: (st_m, st_h.at[h]), sem_st.at[1], st_h.at[pl.ds(0, h_size - 1)], "st")
        coming["st2"] = lambda: drain(st_h, sem_st.at[1, 1])

    means, scales = [], []

    def st3():
        got("st2")
        for mean, m2 in combine(st_h[...], count * w_size):
            means.append(mean)
            scales.append(lax.rsqrt(m2 / (count * ndev) + NORM_EPS))

    def tb1():
        got("tab")
        for a in range(2):
            share = tab_w.at[a, :, rows_at(dp, n_tab)]
            for k in range(1, dp_size):
                push(share, share, sem_tab.at[1 + a], {"dp": (dp + k) % dp_size})
            others = tab_w.at[a, :, pl.ds(0, (dp_size - 1) * n_tab)]
            unsent.setdefault(None, []).append(lambda a=a, others=others: drain(others, sem_tab.at[1 + a, 0]))
            coming["tab1", a] = lambda a=a, others=others: drain(others, sem_tab.at[1 + a, 1])

    def table_out(a):
        got(("tab1", a))
        shards = w_size
        for g in range(2):
            def refs(o, g=g):
                group = o if g == 0 else last - o
                return tab_w.at[a, group // shards, rows_at(group % shards, 2)], tab.at[a, pl.ds(2 * g, 2), rows_at(h, nt)]

            along("h", refs, sem_tab.at[3 + a], tab.at[a, pl.ds(0, 2), pl.ds(0, nlat - nt)], ("table", a, g))
        for g in range(2):
            unsent.pop(("table", a, g))
        unsent.setdefault(None, []).append(lambda: drain(tab.at[a, :, pl.ds(0, nlat - nt)], sem_tab.at[3 + a, 0]))
        coming["tab2", a] = lambda: drain(tab.at[a], sem_tab.at[3 + a, 1])

    def table_in(a, down, up):
        got(("tab2", a))

        def body(n, _):
            both = tab[a, n].reshape(h_size, 2, ntp, 2 * nl)
            both = jnp.concatenate([both[:, j].reshape(-1, 2 * nl) for j in range(2)], axis=0)
            for j in range(2):
                turned[...] = both[:, j * nl:(j + 1) * nl].T
                t = jnp.concatenate([turned[pl.ds(l, nl // 2, stride=2), :] for l in range(2)], axis=0)
                down[2 * n + j] = t
                up[2 * n + j] = t.T
            return 0

        lax.fori_loop(0, tab.shape[1], body, 0)

    def tb2():
        table_out(0)

    def tb3():
        table_in(0, down_p, up_p)

    def tb4():
        table_out(1)

    def tb5():
        table_in(1, down_q, up_q)

    def sX(b, k):
        send_home_rows(b, k, sem_x, "x")

    def fd(b, k):
        got(("x", b, k))
        dft(b, k, f_tab)
        send_orders(b, k, sr, sem_s, "s")

    def fl(b):
        for k in range(PARTS):
            got(("s", b, k))
        leg_down(b, down_p, sr, True)
        send_owner(b, ar, sem_a, "a")

    def fo(b):
        if not scales:
            got("k")
            st3()
        got(("a", b))
        settle(("bs", b))

        def one(l, _):
            re, im = owned(l)
            a = jnp.concatenate([re, im], axis=0) * scales[b]
            asave[b, l] = a
            n = a.shape[0] // 2
            own, other = dot(a, ker[0, l]), dot(a, ker[1, l])
            put_back(l, own[:n] - other[n:], own[n:] + other[:n])
            return 0

        take_in(b, ar)
        lax.fori_loop(0, l_own, one, 0)
        give_out(b)
        send_back(b, br, sem_b, "b")
        along("dp", lambda o: (asave.at[b, o // 2], aall.at[dp, b]), sem_az.at[b], aall.at[pl.ds(0, dp_size - 1), b])
        coming["az", b] = lambda: drain(aall.at[:, b], sem_az.at[b, 1])

    def fu(b):
        got(("b", b))
        leg_up(b, up_q, br, False)
        send_lats(b, yr, sem_u, "u", PARTS)

    def fi(b, k):
        got(("u", b, k))
        idft(b, k, gt_tab, yr, PARTS)

    def sY(b, k):
        send_rows_home(b, k, sem_y, "y", PARTS)

    def pw(b, k):
        got(("y", b, k))
        if ("t", b) in coming:
            got(("t", b))
        if "small" in coming:
            got("small")
        settle(("pk", b, k))

        def body(n, _):
            lats = [n, n + ntp]
            y = jnp.concatenate(get_rows(b, n), axis=0)
            yb = y.astype(BF16)
            hid = bdot(yb, w1[...])
            th_ = jnp.tanh(GELU_C * (hid + GELU_A * (hid * hid * hid)))
            act = (hid * (0.5 * (1.0 + th_))).astype(BF16)
            resid = y + bdot(act, w2[...])
            parts = []
            for j, t in enumerate(lats):
                r = resid[j * npl:(j + 1) * npl] + xh[b, t] - th[b, t]
                d = lat[t] * r
                ls[...] += jnp.sum((d * r).reshape(-1, 8, nc), axis=0)
                dout[b, t] = d
                parts.append(d)
            d = jnp.concatenate(parts, axis=0)
            db = d.astype(BF16)
            gw[2 * nc:, :] += bdot(act, db, TN)
            slope = 0.5 * (1.0 + th_) + (0.5 * GELU_C) * hid * (1.0 - th_ * th_) * (1.0 + (3.0 * GELU_A) * (hid * hid))
            dh = (bdot(db, w2[...], NT) * slope).astype(BF16)
            gin = bdot(yb, dh, TN)
            gw[:nc, :] += gin[:, :nc]
            gw[nc:2 * nc, :] += gin[:, nc:]
            dy = d + bdot(dh, w1[...], NT)
            put_rows(b, n, dy[:npl], dy[npl:])
            return 0

        lax.fori_loop(k * ntp // PARTS, (k + 1) * ntp // PARTS, body, 0)

    def sD(b, k):
        send_home_rows(b, k, sem_d, "d")

    def bd(b, k):
        got(("d", b, k))
        dft(b, k, g_tab)
        send_orders(b, k, dsr, sem_ds, "ds")

    def bl(b):
        for k in range(PARTS):
            got(("ds", b, k))
        leg_down(b, down_q, dsr, False)
        send_owner(b, dar, sem_da, "da")

    def bo(b):
        got(("da", b))
        settle(("bs", b), "st")

        def one(l, s2):
            re, im = owned(l)
            d = jnp.concatenate([re, im], axis=0)
            dsave[b, l] = d
            n = d.shape[0] // 2
            own, other = dot(d, ker[0, l], NT), dot(d, ker[1, l], NT)
            re, im = own[:n] + other[n:], own[n:] - other[:n]
            put_back(l, re, im)
            return s2 + jnp.sum(re * asave[b, l, :n] + im * asave[b, l, n:], axis=0, keepdims=True)

        take_in(b, dar)
        s2 = lax.fori_loop(0, l_own, one, jnp.zeros((1, nc), F32))
        give_out(b)
        send_back(b, dbr, sem_db, "db")
        along("dp", lambda o: (dsave.at[b, o // 2, :, lanes_at(o % 2)], dall.at[dp, b]), sem_dz.at[b], dall.at[pl.ds(0, dp_size - 1), b])
        coming["dz", b] = lambda: drain(dall.at[:, b], sem_dz.at[b, 1])
        st_s[b:b + 1, :] = s2

    def bu(b):
        got(("db", b))
        leg_up(b, up_p, dbr, True)
        send_lats(b, dyr, sem_du, "du", N_PARTS)

    def bi(b, k):
        got(("du", b, k))
        idft(b, k, ft_tab, dyr, N_PARTS)

    def sN(b, k):
        send_rows_home(b, k, sem_n, "n", N_PARTS)

    def pj1():
        st_s[nb:, :] = jnp.zeros_like(st_s[nb:, :])
        along("w", lambda o: (st_s, st_w.at[w]), sem_st.at[2], st_w.at[pl.ds(0, w_size - 1)])
        coming["pj"] = lambda: drain(st_w, sem_st.at[2, 1])

    def pj2():
        got("pj")
        st_m[...] = jnp.sum(st_w[...], axis=0)
        along("h", lambda o: (st_m, st_h.at[h]), sem_st.at[3], st_h.at[pl.ds(0, h_size - 1)])
        coming["pj2"] = lambda: drain(st_h, sem_st.at[3, 1])

    proj = []

    def fn(b, k):
        if not proj:
            got("pj2")
            proj.append(jnp.sum(st_h[...], axis=0) / (count * ndev))
        got(("n", b, k))

        def body(i, _):
            for t, dn in zip((i, i + ntp), get_rows(b, i)):
                normed = (xh[b, t] - means[b]) * scales[b]
                dout[b, t] = dout[b, t] + scales[b] * (dn - normed * proj[0][b:b + 1])
            return 0

        lax.fori_loop(k * ntp // N_PARTS, (k + 1) * ntp // N_PARTS, body, 0)

    n_c, n_z, n_h, n_w = gw_a.shape[0], gw_zs.shape[0], gw_hs.shape[0], gw_ws.shape[0]
    chip, core = h // 2, h % 2
    chips = h_size // 2

    def over_chips(refs, sems, sent):
        src, dst = refs(chip)
        keep(src, dst, sems)
        for k in range(1, chips):
            o = (chip + k) % chips
            src, dst = refs(o)
            push(src, dst, sems, {"h": 2 * o + core})
        unsent.setdefault(None, []).append(lambda: drain(sent, sems.at[0]))

    def twin(src, dst, sems):
        push(src, dst, sems, {"h": h + 1 - 2 * core})
        unsent.setdefault(None, []).append(lambda: drain(dst, sems.at[0]))

    def gw1():
        twin(gw.at[rows_at(1 - core, n_c)], gw_p, sem_gw.at[0])
        twin(ls, ls_p, sem_ls.at[0])
        coming["gw1"] = lambda: (drain(gw_p, sem_gw.at[0, 1]), drain(ls_p, sem_ls.at[0, 1]))

    def gw2():
        got("gw1")
        gw_a[...] = gw[rows_at(core, n_c), :] + gw_p[...]
        ls_a[...] = ls[...] + ls_p[...]
        along("dp", lambda o: (gw_a.at[rows_at(o, n_z)], gw_z.at[dp]), sem_gw.at[1], gw_z.at[pl.ds(0, dp_size - 1)])
        along("dp", lambda o: (ls_a, ls_z.at[dp]), sem_ls.at[1], ls_z.at[pl.ds(0, dp_size - 1)])
        coming["gw2"] = lambda: (drain(gw_z, sem_gw.at[1, 1]), drain(ls_z, sem_ls.at[1, 1]))

    def gw3():
        got("gw2")
        gw_zs[...] = jnp.sum(gw_z[...], axis=0)
        ls_zs[...] = jnp.sum(ls_z[...], axis=0)
        over_chips(lambda o: (gw_zs.at[rows_at(o, n_h)], gw_h.at[chip]), sem_gw.at[2], gw_h.at[pl.ds(0, chips - 1)])
        over_chips(lambda o: (ls_zs, ls_h.at[chip]), sem_ls.at[2], ls_h.at[pl.ds(0, chips - 1)])
        coming["gw3"] = lambda: (drain(gw_h, sem_gw.at[2, 1]), drain(ls_h, sem_ls.at[2, 1]))

    def gw4():
        got("gw3")
        gw_hs[...] = jnp.sum(gw_h[...], axis=0)
        ls_hs[...] = jnp.sum(ls_h[...], axis=0)
        along("w", lambda o: (gw_hs.at[rows_at(o, n_w)], gw_w.at[w]), sem_gw.at[3], gw_w.at[pl.ds(0, w_size - 1)])
        along("w", lambda o: (ls_hs, ls_w.at[w]), sem_ls.at[3], ls_w.at[pl.ds(0, w_size - 1)])
        coming["gw4"] = lambda: (drain(gw_w, sem_gw.at[3, 1]), drain(ls_w, sem_ls.at[3, 1]))

    def gw5():
        got("gw4")
        gw_ws[...] = jnp.sum(gw_w[...], axis=0)
        loss_out[...] = jnp.sum(ls_w[...], keepdims=True).reshape(1, 1) / total_points
        along("w", lambda o: (gw_ws, gw_w2.at[rows_at(w, n_w)]), sem_gw.at[4], gw_w2.at[pl.ds(0, (w_size - 1) * n_w)])
        coming["gw5"] = lambda: drain(gw_w2, sem_gw.at[4, 1])

    def gw6():
        got("gw5")
        over_chips(lambda o: (gw_w2, gw_h2.at[rows_at(chip, n_h)]), sem_gw.at[5], gw_h2.at[pl.ds(0, (chips - 1) * n_h)])
        coming["gw6"] = lambda: drain(gw_h2, sem_gw.at[5, 1])

    def gw7():
        got("gw6")
        along("dp", lambda o: (gw_h2, gw_f.at[rows_at(dp, n_z)]), sem_gw.at[6], gw_f.at[pl.ds(0, (dp_size - 1) * n_z)])
        coming["gw7"] = lambda: drain(gw_f, sem_gw.at[6, 1])

    def gw8():
        got("gw7")
        twin(gw_f, gw_o, sem_gw.at[7])
        coming["gw8"] = lambda: drain(gw_o, sem_gw.at[7, 1])

    def end():
        got("gw8")
        for c, halves in enumerate(((gw_f, gw_o), (gw_o, gw_f))):
            @pl.when(core == c)
            def _():
                first, second = halves
                for i, (src, dst) in enumerate(((first.at[:nc], gin_out.at[:, :nc]), (first.at[nc:], gin_out.at[:, nc:]), (second, gout_out))):
                    pltpu.make_async_copy(src, dst, sem_fin.at[i]).start()
        for i, dst in enumerate((gin_out.at[:, :nc], gin_out.at[:, nc:], gout_out)):
            unsent.setdefault(None, []).append(lambda dst=dst, i=i: drain(dst, sem_fin.at[i]))

    gs_sum, gs_b = (gs_sum0, gs_sum1), (gs_b0, gs_b1)
    first_rows = (0, gs_sum0.shape[1])
    axes = (("w", "dp"), ("dp", "w"))
    place = {"w": (w, w_size), "dp": (dp, dp_size)}

    def next_to(axis, k):
        index, size = place[axis]
        return (index + k + size) % size

    def add_sample(b):
        got(("az", b))
        got(("dz", b))

        def body(n, _):
            d = dall[n, b]
            half = d.shape[0] // 2
            both = jnp.concatenate([d, jnp.concatenate([d[half:], -d[:half]], axis=0)], axis=1)
            gs_acc[...] += dot(aall[n, b], both, TN)
            return 0

        lax.fori_loop(0, dp_size, body, 0)

    def gsa():
        gs_acc[...] = jnp.zeros_like(gs_acc)
        add_sample(GS_FIRST[0])

    def gsb():
        add_sample(GS_FIRST[1])

    def gs1():
        add_sample(GS_FIRST[2])
        for q in range(2):
            rows_q = pl.ds(first_rows[q], gs_sum[q].shape[1])
            for p in range(2):
                gs_sum[q][p] = gs_acc[rows_q, p * LANES:(p + 1) * LANES]

    def once(key):
        if key in coming:
            got(key)

    def sent_later(ref, sem):
        unsent.setdefault(None, []).append(lambda: drain(ref, sem))

    def gs2(q):
        keep(gs_sum[q], gs_b[q].at[0], sem_gs.at[q, 0])
        for slot, k in ((1, 1), (3, -1)):
            push(gs_sum[q], gs_b[q].at[slot], sem_gs.at[q, slot], {axes[q][0]: next_to(axes[q][0], k)})
            sent_later(gs_sum[q], sem_gs.at[q, slot, 0])
        coming.update({("gs", q, k): lambda k=k: drain(gs_b[q].at[k], sem_gs.at[q, k, 1]) for k in (0, 1, 3)})

    def gs6(q):
        for slot, p, k, i in ((1, 0, 1, 2), (3, 1, -1, 4)):
            once(("gs", q, slot))
            push(gs_b[q].at[slot, p], gs_b[q].at[2, p], sem_gs.at[q, i], {axes[q][0]: next_to(axes[q][0], k)})
            sent_later(gs_b[q].at[2, p], sem_gs.at[q, i, 0])
        coming["gs", q, 2] = lambda: (drain(gs_b[q].at[2, 0], sem_gs.at[q, 2, 1]), drain(gs_b[q].at[2, 1], sem_gs.at[q, 4, 1]))

    def block_at(q, k, shift):
        at = {axes[q][0]: next_to(axes[q][0], -k), axes[q][1]: next_to(axes[q][1], shift)}
        return gs_out.at[:, l_own * at["w"] + at["dp"] // 2, pl.ds(first_rows[q], gs_sum[q].shape[1]), lanes_at(at["dp"] % 2)]

    def gs3(q, k):
        once(("gs", q, k))
        mine = block_at(q, k, 0)
        pltpu.make_async_copy(gs_b[q].at[k], mine, sem_gf.at[q, 3, k, 0]).start()
        for way, shift in ((0, 1), (1, -1)):
            push(gs_b[q].at[k], mine, sem_gf.at[q, way, k], {axes[q][1]: next_to(axes[q][1], shift)})

    def gs4(q, k):
        way, shift = (0, 1) if k < 2 else (1, -1)
        drain(gs_b[q].at[k], sem_gf.at[q, way, k, 1])
        block = block_at(q, k, -shift)
        push(block, block, sem_gf.at[q, 2, k], {axes[q][1]: next_to(axes[q][1], shift)})

    def gs5(q, k):
        drain(gs_b[q].at[k], sem_gf.at[q, 1 if k < 2 else 0, k, 1])
        drain(gs_b[q].at[k], sem_gf.at[q, 2, k, 1])
        for i in range(4):
            drain(gs_b[q].at[k], sem_gf.at[q, i, k, 0])

    scope = dict(locals())
    scope["pk"] = pk_
    for name in ORDER.split():
        call = name.rstrip("0123456789") or name
        if name in scope:
            scope[name]()
        elif name[:3] in scope:
            scope[name[:3]](*map(int, name[3:]))
        else:
            scope[call](*map(int, name[len(call):]))
    assert not coming
    settle()


def hand_on_kernel(*refs):
    n = len(refs) // 2
    pairs = []
    for src, dst in zip(refs[:n], refs[n:2 * n]):
        lead = [()] if len(src.shape) == 2 else [(i,) for i in range(src.shape[0])]
        pairs += [(src.at[i], dst.at[i]) if i else (src, dst) for i in lead]
    copies = [pltpu.make_async_copy(src, dst, refs[2 * n].at[i]) for i, (src, dst) in enumerate(pairs)]
    for c in copies:
        c.start()
    for c in copies:
        c.wait()


def hand_on(arrays):
    return pl.pallas_call(
        hand_on_kernel, name="hand_on",
        out_shape=[jax.ShapeDtypeStruct(a.shape, F32) for a in arrays],
        in_specs=[pl.BlockSpec(memory_space=pltpu.VMEM)] * len(arrays), out_specs=[pl.BlockSpec(memory_space=pl.ANY)] * len(arrays),
        scratch_shapes=[pltpu.SemaphoreType.DMA((32,))],
        compiler_params=pltpu.CompilerParams(vmem_limit_bytes=12 * 1024 * 1024),
    )(*[pltpu.with_memory_space_constraint(a, pltpu.VMEM) for a in arrays])


def solution(mesh):
    dp_size, w_size, h_size = mesh.shape["dp"], mesh.shape["w"], mesh.shape["h"]

    def local_step(field, target, lat_weight, leg_fwd, leg_inv, spec_w, w_in, w_out):
        nb, nc, nt, npl = field.shape
        nlon = npl * w_size
        ntp = nt // 2
        nm = leg_fwd.shape[0] * w_size
        ndev = h_size * w_size
        nlat = nt * h_size
        nl = leg_fwd.shape[1]
        lo = nl // ndev
        assert nm == 8 * h_size and nc == w_size * LANES // 2 and h_size == 2 * w_size and 2 * lo == dp_size and 2 * nl == LANES
        total_points = nb * dp_size * nc * nlat * nlon
        any_spec = pl.BlockSpec(memory_space=pl.ANY)
        vmem_spec = pl.BlockSpec(memory_space=pltpu.VMEM)
        sds = lambda *s: jax.ShapeDtypeStruct(s, F32)
        vm = lambda *s: pltpu.VMEM(s, F32)
        dma = lambda *s: pltpu.SemaphoreType.DMA(s)
        n_rows = 2 * nc + w_out.shape[0]
        n_z, n_h, n_w = n_rows // dp_size, n_rows // dp_size // h_size, n_rows // dp_size // h_size // w_size
        home = vm(nb, nt, npl, nc)
        woven = vm(nb, w_size, ntp, npl, LANES)
        order = vm(nb, 16 * nlat // 2, LANES)
        degree = vm(nb, 8 * nl, LANES)
        owner = vm(nb, h_size, 8 * lo, w_size * LANES)
        saved = vm(nb, lo, 2 * nm, nc)
        cut = GS_ROWS
        n_pairs = leg_fwd.shape[0] // 2
        n_c = n_rows // 2
        n_z, n_h, n_w = n_c // dp_size, n_c // dp_size // w_size, n_c // dp_size // w_size // w_size
        results = pl.pallas_call(
            functools.partial(block_kernel, (dp_size, h_size, w_size), total_points),
            name="block",
            out_shape=[vm(nb, nt, npl, nc), vm(2, lo * w_size, nc, nc), vm(nc, 2 * nc), vm(2 * nc, nc), sds(1, 1)],
            in_specs=[any_spec] * 9,
            out_specs=[vmem_spec] * 5,
            scratch_shapes=[
                vm(*leg_fwd.shape[:1], nt, nl), vm(*leg_fwd.shape[:1], nt, nl), pltpu.SMEM((nt,), F32), pltpu.VMEM(w_in.shape, BF16),
                pltpu.VMEM(w_out.shape, BF16), vm(2 * nm, nlon), vm(2 * nm, nlon), vm(nlon, 2 * nm), vm(nlon, 2 * nm),
                home, home, woven, vm(nb, ntp, nlon, LANES), woven, woven,
                vm(nb, h_size, 16 * ntp, LANES), order, order, order, vm(nb, h_size, 16 * ntp, LANES), vm(nb, h_size, 16 * ntp, LANES),
                degree, owner, owner, vm(nb, h_size, w_size, 8 * lo, LANES), degree, degree, saved, saved,
                vm(dp_size, nb, 2 * nm, nc), vm(dp_size, nb, 2 * nm, LANES), vm(lo, w_size, nm, LANES),
                vm(8, nc), vm(h_size, 8, nc), vm(8, nc), vm(w_size, 8, nc),
                vm(2, n_pairs, nt, 2 * nl), vm(2, w_size, n_pairs, nt, 2 * nl), vm(2, 4, nlat, 2 * nl), vm(nl, nlat),
                vm(8, nl, nlat), vm(8, nl, nlat), vm(8, nlat, nl), vm(8, nlat, nl),
                vm(2, lo, nc, nc),
                vm(n_rows, nc), vm(n_c, nc), vm(n_c, nc), vm(dp_size, n_z, nc), vm(n_z, nc), vm(w_size, n_h, nc), vm(n_h, nc),
                vm(w_size, n_w, nc), vm(n_w, nc), vm(n_h, nc), vm(n_z, nc), vm(n_c, nc), vm(n_c, nc),
                vm(8, nc), vm(8, nc), vm(8, nc), vm(dp_size, 8, nc), vm(8, nc), vm(w_size, 8, nc), vm(8, nc), vm(w_size, 8, nc),
                vm(nc, nc), vm(2, cut, LANES), vm(2, nc - cut, LANES), vm(4, 2, cut, LANES), vm(4, 2, nc - cut, LANES),
            ] + [dma(nb, PARTS, 2)] * 8 + [dma(nb, 2)] * 6 + [dma(nb, 2), dma(4, 2), dma(5, 2), dma(1), dma(8, 2), dma(4, 2),
                 dma(2, 5, 2), dma(2, 4, 4, 2), dma(3), dma(6)],
            compiler_params=pltpu.CompilerParams(collective_id=0, has_side_effects=True, vmem_limit_bytes=54 * 1024 * 1024),
        )(field.transpose(0, 2, 3, 1), target.transpose(0, 2, 3, 1), leg_fwd.transpose(0, 2, 1), leg_inv.transpose(0, 2, 1),
          spec_w, lat_weight, w_in, w_out, jnp.asarray(dft_table(nlon, nm, h_size)))
        d_x, g_spec, g_in, g_out = hand_on(results[:4])
        loss = results[4]
        return loss.reshape(()), d_x.transpose(0, 3, 1, 2), g_spec, g_in, g_out

    grid_spec = P("dp", None, "h", "w")
    table_spec = P("w", None, "h")
    kernel_spec = P(None, "h", None, None)
    return jax.shard_map(local_step, mesh=mesh, in_specs=(grid_spec, grid_spec, P("h"), table_spec, table_spec, P(), P(), P()), out_specs=(P(), grid_spec, kernel_spec, P(), P()), check_vma=False)
```

```python
import functools
import jax
import jax.numpy as jnp
import numpy as np
from jax import lax
from jax.experimental import pallas as pl
from jax.experimental.pallas import tpu as pltpu
from jax.sharding import PartitionSpec as P

NORM_EPS = 1e-5
PRECISE = lax.Precision.HIGHEST
MESH = pl.DeviceIdType.MESH
F32 = jnp.float32
BF16 = jnp.bfloat16
GELU_C = float(np.sqrt(2.0 / np.pi))
GELU_A = 0.044715
LANES = 128
NN = (((1,), (0,)), ((), ()))
NT = (((1,), (1,)), ((), ()))
TN = (((0,), (0,)), ((), ()))


def dot(a, b, dims=NN):
    return lax.dot_general(a, b, dims, precision=PRECISE, preferred_element_type=F32)


def bdot(a, b, dims=NN):
    return lax.dot_general(a, b, dims, preferred_element_type=F32)


def dft_table(lon_count, num_modes, h_size):
    modes, lons = np.arange(num_modes), np.arange(lon_count)
    angle = 2.0 * np.pi * ((modes[:, None] * lons[None, :]) % lon_count) / lon_count
    table = np.stack([np.cos(angle), -np.sin(angle)], 0) * lon_count ** -0.5
    groups = table.reshape(2, 2 * h_size, num_modes // h_size // 2, lon_count)
    table = np.stack([groups[:, :h_size], groups[:, :h_size - 1:-1]], 2).transpose(1, 0, 2, 3, 4)
    return table.reshape(2 * num_modes, lon_count).astype(np.float32)


def drain(ref, sem):
    pltpu.make_async_copy(ref, ref, sem).wait()


def rows_at(i, n):
    return pl.ds(pl.multiple_of(i * n, n), n)


def lanes_at(i):
    return pl.ds(pl.multiple_of(i * LANES, LANES), LANES)


def push(src, dst, sems, device):
    pltpu.make_async_remote_copy(src_ref=src, dst_ref=dst, send_sem=sems.at[0], recv_sem=sems.at[1],
                                 device_id=device, device_id_type=MESH).start()


def keep(src, dst, sems):
    pltpu.make_async_copy(src, dst, sems.at[1]).start()


def flip(v):
    return pltpu.roll(v, LANES // 2, 1)


def low(v):
    return lax.broadcasted_iota(jnp.int32, v.shape, 1) < LANES // 2


def weave(a, b):
    return jnp.where(low(a), a, flip(b)), jnp.where(low(a), flip(a), b)


def weave_wide(tiles):
    pairs = [weave(tiles[j], tiles[j + 1]) for j in range(0, len(tiles), 2)]
    return jnp.concatenate([p[0] for p in pairs], axis=1), jnp.concatenate([p[1] for p in pairs], axis=1)


def weave_tiles(a, b):
    out = []
    for j in range(0, a.shape[1], LANES):
        out.extend(weave(a[:, j:j + LANES], b[:, j:j + LANES]))
    return out


PARTS = 4
N_PARTS = 2
GS_ROWS = 176
GS_FIRST = (0, 1, 2)
ORDER = " ".join((
    'pk1', 'pk0', 'go', 'sX03', 'pk2', 'sX02', 'sX01', 'st1', 'tb1', 'fd03',
    'sX00', 'sX11', 'tb2', 'sX13', 'fd02', 'sX12', 'st2', 'fd01', 'fd00', 'tb3',
    'fd11', 'sX10', 'tb4', 'fl0', 'fd13', 'sX21', 'fd10', 'tb5', 'sX23', 'fd12',
    'fo0', 'fl1', 'sX22', 'fu0', 'sX20', 'fo1', 'fi00', 'sY00', 'fi01', 'fd20',
    'sY01', 'fi02', 'fi03', 'fd21', 'sY03', 'fd23', 'pw00', 'fd22', 'sY02', 'fu1',
    'sD00', 'fi10', 'sY10', 'fi11', 'fl2', 'fi12', 'pw03', 'sY11', 'pw01', 'fi13',
    'sY13', 'pw02', 'fo2', 'sD02', 'pw11', 'sY12', 'sD03', 'sD01', 'pw13', 'pw10',
    'fu2', 'sD13', 'sD11', 'bd00', 'bd03', 'pw12', 'fi22', 'sD12', 'fi20', 'bd02',
    'sY20', 'bd01', 'bl0', 'fi23', 'fi21', 'bd12', 'sD10', 'pw20', 'bd11', 'sY22',
    'bd13', 'sY21', 'bo0', 'sY23', 'sD20', 'bd10', 'pw22', 'pw21', 'bl1', 'bu0',
    'pw23', 'sD23', 'gw1', 'sD22', 'bd20', 'gsa', 'sD21', 'gw2', 'bo1', 'bi01',
    'bd23', 'bd22', 'sN01', 'bd21', 'gw3', 'gsb', 'bi00', 'bl2', 'gw4', 'bu1',
    'sN00', 'gw5', 'bo2', 'bi10', 'sN10', 'gs1', 'pj1', 'gs20', 'gs21', 'gs300',
    'gs310', 'bu2', 'gs311', 'bi11', 'gs303', 'gs61', 'gs60', 'bi20', 'gw6', 'sN20',
    'gs301', 'pj2', 'gs410', 'fn10', 'gw7', 'fn01', 'gs400', 'sN11', 'gs312', 'gs302',
    'gs403', 'gs411', 'bi21', 'gs401', 'gs313', 'sN21', 'fn20', 'gs511', 'gs413', 'fn11',
    'fn00', 'gs412', 'gs402', 'gw8', 'fn21', 'gs510', 'gs500', 'end', 'gs502', 'gs513',
    'gs501', 'gs503', 'gs512',
))


def block_kernel(sizes, total_points,
                 x, tgt, leg_p_in, leg_q_in, spec_w, lat_in, w1_in, w2_in, f_in,
                 dout, gs_out, gin_out, gout_out, loss_out,
                 leg_p, leg_q, lat, w1, w2, f_tab, g_tab, ft_tab, gt_tab,
                 xh, th, pk, rows, yrow, hy,
                 xs, sr, dsr, ys, yr, dyr, als, ar, dar, bs, br, dbr, asave, dsave, aall, dall, mix,
                 st_s, st_h, st_m, st_w, tab_s, tab_w, tab, turned, down_p, down_q, up_p, up_q, ker,
                 gw, gw_p, gw_a, gw_z, gw_zs, gw_h, gw_hs, gw_w, gw_ws, gw_w2, gw_h2, gw_f, gw_o,
                 ls, ls_p, ls_a, ls_z, ls_zs, ls_h, ls_hs, ls_w, gs_acc, gs_sum0, gs_sum1, gs_b0, gs_b1,
                 sem_x, sem_y, sem_d, sem_n, sem_s, sem_ds, sem_u, sem_du, sem_a, sem_da, sem_b, sem_db, sem_az, sem_dz,
                 sem_in, sem_st, sem_tab, sem_k, sem_gw, sem_ls, sem_gs, sem_gf, sem_fin, sem_small):
    dp_size, h_size, w_size = sizes
    dp, h, w = lax.axis_index("dp"), lax.axis_index("h"), lax.axis_index("w")
    ndev = h_size * w_size
    me = h * w_size + w
    nb, nt, npl, nc = x.shape
    ntp = nt // 2
    nlon = npl * w_size
    nlat = nt * h_size
    nl = als.shape[1] // 8
    l_own = nl // ndev
    piece = 8 * l_own
    unsent, coming = {}, {}

    def got(key):
        coming.pop(key)()

    def peer(k):
        return (h + k // w_size) % h_size, (w + k % w_size) % w_size

    barrier = pltpu.get_barrier_semaphore()

    def meet(k, _):
        h2, w2_ = peer(k)
        pl.semaphore_signal(barrier, inc=1, device_id={"h": h2, "w": w2_}, device_id_type=MESH)
        return 0

    def meet_dp(k, _):
        pl.semaphore_signal(barrier, inc=1, device_id={"dp": (dp + k) % dp_size}, device_id_type=MESH)
        return 0

    lax.fori_loop(1, ndev, meet, 0)
    lax.fori_loop(1, dp_size, meet_dp, 0)
    loads = [pltpu.make_async_copy(x.at[b], xh.at[b], sem_in.at[b, 0]) for b in range(nb)]
    load_t = [pltpu.make_async_copy(tgt.at[b], th.at[b], sem_in.at[b, 1]) for b in range(nb)]
    load_k = pltpu.make_async_copy(spec_w.at[:, pl.ds(me * l_own, l_own)], ker, sem_k.at[0])
    small = [pltpu.make_async_copy(src, dst, sem_small.at[i]) for i, (src, dst) in enumerate((
        (leg_p_in, leg_p), (leg_q_in, leg_q), (f_in, f_tab), (lat_in, lat), (w1_in, w1), (w2_in, w2)))]
    for c in loads + small[:3] + [load_k] + load_t + small[3:]:
        c.start()
    coming["k"] = load_k.wait
    coming["small"] = lambda: [c.wait() for c in small[3:]]
    coming.update({("t", b): load_t[b].wait for b in range(nb)})
    for ref in (ar, br, dar, dbr, st_s, gw, ls):
        ref[...] = jnp.zeros_like(ref)

    def settle(*keys):
        for key in keys or list(unsent):
            for wait in unsent.pop(key, []):
                wait()

    def along(axis, refs, sems, sent, key=None):
        size, index = {"dp": (dp_size, dp), "h": (h_size, h), "w": (w_size, w)}[axis]
        src, dst = refs(index)
        keep(src, dst, sems)

        def body(k, _):
            other = (index + k) % size
            src, dst = refs(other)
            push(src, dst, sems, {axis: other})
            return 0

        lax.fori_loop(1, size, body, 0)
        unsent.setdefault(key, []).append(lambda: drain(sent, sems.at[0]))

    def take(sem, count, counts):
        for n in counts:
            @pl.when(count == n)
            def _():
                drain(als.at[0, pl.ds(0, n * 8)], sem)

    n_groups = 2 * h_size
    last = n_groups - 1
    reach = 2 * h + 2
    low_h = (h // 2, (last - h) // 2)
    both_mine = last - h < reach
    n_met = (h_size + 1) * w_size
    assert l_own * w_size == 8 and all(2 * h_size - i // 2 - (last - i) // 2 == h_size + 1 for i in range(h_size))
    counts = [(2 * i + 2) * w_size for i in range(h_size)]
    back_counts = [n - 1 - int(last - i < 2 * i + 2) for i, n in enumerate(counts)]
    pairs = lambda k, parts: pl.ds(k * (ntp // parts), ntp // parts)

    def at_rows(i, k, parts):
        size = 16 * ntp // parts
        return pl.ds(pl.multiple_of(i * 16 * ntp + k * size, size), size)

    def send_home_rows(b, k, sem, name):
        along("w", lambda o: (pk.at[b, o, pairs(k, PARTS)], rows.at[b, pairs(k, PARTS), rows_at(w, npl)]), sem.at[b, k],
              pk.at[b, pl.ds(0, w_size - 1), pairs(k, PARTS)], ("pk", b, k))
        coming[name, b, k] = lambda: drain(rows.at[b, pairs(k, PARTS)], sem.at[b, k, 1])

    def send_rows_home(b, k, sem, name, parts):
        along("w", lambda o: (yrow.at[b, o, pairs(k, parts)], hy.at[b, w, pairs(k, parts)]), sem.at[b, k],
              yrow.at[b, pl.ds(0, w_size - 1), pairs(k, parts)], (name, "row", b, k))
        coming[name, b, k] = lambda: drain(hy.at[b, :, pairs(k, parts)], sem.at[b, k, 1])

    def send_orders(b, k, dst, sem, name):
        along("h", lambda o: (xs.at[b, o, at_rows(0, k, PARTS)], dst.at[b, at_rows(h, k, PARTS)]), sem.at[b, k],
              xs.at[b, pl.ds(0, h_size - 1), at_rows(0, k, PARTS)], ("xs", b, k))
        coming[name, b, k] = lambda: drain(xs.at[b, :, at_rows(0, k, PARTS)], sem.at[b, k, 1])

    def send_lats(b, dst, sem, name, parts):
        def one(k, _):
            keep(ys.at[b, at_rows(h, k, parts)], dst.at[b, h, at_rows(0, k, parts)], sem.at[b, k])

            def body(j, _):
                o = (h + j) % h_size
                push(ys.at[b, at_rows(o, k, parts)], dst.at[b, h, at_rows(0, k, parts)], sem.at[b, k], {"h": o})
                return 0

            return lax.fori_loop(1, h_size, body, 0)

        lax.fori_loop(0, parts, one, 0)
        for k in range(parts):
            unsent.setdefault(("ys", b), []).append(lambda k=k: drain(xs.at[b, pl.ds(0, h_size - 1), at_rows(0, k, parts)], sem.at[b, k, 0]))
            coming[name, b, k] = lambda k=k: drain(dst.at[b, :, at_rows(0, k, parts)], sem.at[b, k, 1])

    def send_owner(b, dst, sem, name):
        sems = sem.at[b]
        for g in range(2):
            tile = lambda h2, w2_, g=g: (als.at[b, rows_at((h2 * w_size + w2_) * 2 + g, 8)], dst.at[b, h, pl.ds(g * 8, 8), lanes_at(w)])

            def body(h2, _, tile=tile):
                for k in range(w_size):
                    w2_ = (w + k) % w_size
                    if k:
                        push(*tile(h2, w2_), sems, {"h": h2, "w": w2_})
                    else:
                        @pl.when(h2 != h)
                        def _():
                            push(*tile(h2, w2_), sems, {"h": h2, "w": w2_})
                return 0

            if g == 0:
                keep(*tile(h, w), sems)
            else:
                @pl.when(both_mine)
                def _():
                    keep(*tile(h, w), sems)
            lax.fori_loop(low_h[g], h_size, body, 0)
        unsent.setdefault(("als", b), []).append(lambda: take(sems.at[0], n_met - 1 - jnp.where(both_mine, 1, 0), [n_met - 1, n_met - 2]))
        coming[name, b] = lambda: take(sems.at[1], reach * w_size, counts)

    def send_back(b, dst, sem, name):
        sems = sem.at[b]
        tile = lambda h2, w2_, g: (bs.at[b, h2, w2_, rows_at(g, 8)], dst.at[b, rows_at(me * 2 + g, 8)])

        def body(n, _):
            g = n // h_size
            h2 = jnp.where(g == 0, n, last - n)
            for k in range(w_size):
                w2_ = (w + k) % w_size
                if k:
                    push(*tile(h2, w2_, g), sems, {"h": h2, "w": w2_})
                else:
                    @pl.when(h2 != h)
                    def _():
                        push(*tile(h2, w2_, g), sems, {"h": h2, "w": w2_})
            return 0

        keep(*tile(h, w, 0), sems)

        @pl.when(both_mine)
        def _():
            keep(*tile(h, w, 1), sems)

        lax.fori_loop(0, reach, body, 0)
        count = reach * w_size - 1 - jnp.where(both_mine, 1, 0)
        unsent.setdefault(("bs", b), []).append(
            lambda: take(sems.at[0], count, back_counts))
        coming[name, b] = lambda: drain(als.at[0, pl.ds(0, n_met * 8)], sems.at[1])

    def dft(b, k, table):
        settle(("xs", b, k))

        def body(n, _):
            i = 2 * n
            both = jnp.concatenate([rows[b, i], rows[b, i + 1]], axis=1)
            out = dot(table[...], both).reshape(h_size, 16, 2 * LANES)
            xs[b, :, rows_at(i, 16), :] = out[:, :, :LANES]
            xs[b, :, rows_at(i + 1, 16), :] = out[:, :, LANES:]
            return 0

        lax.fori_loop(k * ntp // PARTS // 2, (k + 1) * ntp // PARTS // 2, body, 0)

    def idft(b, k, table, src, parts):
        settle(*(("y", "row", b, j) for j in range(PARTS * k // parts, PARTS * (k + 1) // parts)))

        def body(n, _):
            i = 2 * n
            both = jnp.concatenate([src[b, :, rows_at(i + j, 16), :].reshape(-1, LANES) for j in range(2)], axis=1)
            out = dot(table[...], both)
            for j in range(2):
                yrow[b, :, i + j] = out[:, j * LANES:(j + 1) * LANES].reshape(w_size, npl, LANES)
            return 0

        lax.fori_loop(k * ntp // parts // 2, (k + 1) * ntp // parts // 2, body, 0)

    def level(v, here):
        mean = jnp.mean(v, axis=0, keepdims=True)
        mean = 0.5 * (mean + flip(mean))
        return v - jnp.where(jnp.logical_and(h == 0, here), mean, 0.0)

    def orders(body):
        def four(n, _):
            for i in range(4):
                body(4 * n + i, n == 0 if i == 0 else None, [pl.ds(8 * n + 4 * l + i, nl // 2, stride=16) for l in range(2)])
            return 0

        lax.fori_loop(0, 2, four, 0)

    def leg_down(b, table, src, fix):
        settle(("als", b))

        def one(m, here, at):
            re, im = (src[b, pl.ds(ri * 8 + m, ntp * h_size, stride=16), :] for ri in range(2))
            if fix and here is not None:
                re = level(re, here)
            out = dot(table[m], jnp.concatenate(weave(re, im), axis=0))
            for l in range(2):
                als[b, at[l], :] = out[l * (nl // 2):(l + 1) * (nl // 2)]

        orders(one)

    def leg_up(b, table, src, fix):
        settle(("ys", b))

        def one(m, here, at):
            out = dot(table[m], jnp.concatenate([src[b, at[l], :] for l in range(2)], axis=0))
            re, im = weave(out[:nlat // 2], out[nlat // 2:])
            if fix and here is not None:
                re = level(re, here)
            ys[b, pl.ds(m, ntp * h_size, stride=16), :] = re
            ys[b, pl.ds(8 + m, ntp * h_size, stride=16), :] = im

        orders(one)

    def halves(a, b):
        upper = lax.broadcasted_iota(jnp.int32, a.shape, 1) < 4
        turn = lambda v: jnp.concatenate([v[:, 4:], v[:, :4]], axis=1)
        return jnp.where(upper, a, turn(b)), jnp.where(upper, turn(a), b)

    def take_in(b, src):
        for j in range(w_size):
            lanes = slice(j * LANES, (j + 1) * LANES)
            for l, v in enumerate(halves(src[b, :, :8, lanes], src[b, :, 8:, lanes])):
                mix[l, j] = v.reshape(-1, LANES)

    def give_out(b):
        for j in range(w_size):
            for g, v in enumerate(halves(*(mix[l, j].reshape(h_size, 8, LANES) for l in range(2)))):
                bs[b, :, j, g * 8:(g + 1) * 8, :] = v

    def owned(l):
        return weave_wide([mix[l, j] for j in range(w_size)])

    def put_back(l, re, im):
        for j, tile in enumerate(weave_tiles(re, im)):
            mix[l, j] = tile

    def put_rows(b, i, v0, v1):
        for j, tile in enumerate(weave_tiles(v0, v1)):
            pk[b, j, i] = tile

    def get_rows(b, i):
        return weave_wide([hy[b, j, i] for j in range(w_size)])

    count = nt * npl
    n_tab = tab_s.shape[1] // dp_size

    def combine(stats, n):
        mean = jnp.mean(stats, axis=0)
        dev = stats - mean[None]
        dev2 = jnp.sum(dev * dev, axis=0)
        m2 = jnp.sum(stats, axis=0)
        return [(mean[2 * b:2 * b + 1], m2[2 * b + 1:2 * b + 2] + n * dev2[2 * b:2 * b + 1]) for b in range(nb)]

    sums = {}

    def pk_(b):
        loads[b].wait()

        def body(i, total):
            v0, v1 = xh[b, i], xh[b, i + ntp]
            put_rows(b, i, v0, v1)
            return total + jnp.sum(v0 + v1, axis=0, keepdims=True)

        sums[b] = lax.fori_loop(0, ntp, body, jnp.zeros((1, nc), F32))

    def go():
        for c in small[:3]:
            c.wait()
        for a, leg in enumerate((leg_p, leg_q)):
            for m in range(leg.shape[0]):
                tab_s[a, m // 2, :, m % 2 * nl:(m % 2 + 1) * nl] = leg[m]
        pl.semaphore_wait(barrier, ndev - 1 + dp_size - 1)
        along("w", lambda o: (tab_s.at[:, rows_at(dp, n_tab)], tab_w.at[:, w, rows_at(dp, n_tab)]), sem_tab.at[0],
              tab_w.at[:, pl.ds(0, w_size - 1), pl.ds(0, n_tab)])
        coming["tab"] = lambda: drain(tab_w.at[:, :, pl.ds(0, n_tab)], sem_tab.at[0, 1])

    def st1():
        for b in range(nb):
            mean = sums[b] / count

            def body(t, total, b=b, mean=mean):
                d = xh[b, t] - mean
                return total + jnp.sum(d * d, axis=0, keepdims=True)

            st_s[2 * b:2 * b + 1, :] = mean
            st_s[2 * b + 1:2 * b + 2, :] = lax.fori_loop(0, nt, body, jnp.zeros((1, nc), F32))
        along("w", lambda o: (st_s, st_w.at[w]), sem_st.at[0], st_w.at[pl.ds(0, w_size - 1)], "st")
        coming["st"] = lambda: drain(st_w, sem_st.at[0, 1])
        g_tab[...] = jnp.where(lax.broadcasted_iota(jnp.int32, f_tab.shape, 0) == 0, 1.0, 2.0) * f_tab[...]
        ft_tab[...] = f_tab[...].T
        gt_tab[...] = g_tab[...].T

    def st2():
        got("st")
        st_m[...] = jnp.zeros_like(st_m)
        for b, (mean, m2) in enumerate(combine(st_w[...], count)):
            st_m[2 * b:2 * b + 1, :] = mean
            st_m[2 * b + 1:2 * b + 2, :] = m2
        along("h", lambda o: (st_m, st_h.at[h]), sem_st.at[1], st_h.at[pl.ds(0, h_size - 1)], "st")
        coming["st2"] = lambda: drain(st_h, sem_st.at[1, 1])

    means, scales = [], []

    def st3():
        got("st2")
        for mean, m2 in combine(st_h[...], count * w_size):
            means.append(mean)
            scales.append(lax.rsqrt(m2 / (count * ndev) + NORM_EPS))

    def tb1():
        got("tab")
        for a in range(2):
            share = tab_w.at[a, :, rows_at(dp, n_tab)]
            for k in range(1, dp_size):
                push(share, share, sem_tab.at[1 + a], {"dp": (dp + k) % dp_size})
            others = tab_w.at[a, :, pl.ds(0, (dp_size - 1) * n_tab)]
            unsent.setdefault(None, []).append(lambda a=a, others=others: drain(others, sem_tab.at[1 + a, 0]))
            coming["tab1", a] = lambda a=a, others=others: drain(others, sem_tab.at[1 + a, 1])

    def table_out(a):
        got(("tab1", a))
        shards = w_size
        for g in range(2):
            def refs(o, g=g):
                group = o if g == 0 else last - o
                return tab_w.at[a, group // shards, rows_at(group % shards, 2)], tab.at[a, pl.ds(2 * g, 2), rows_at(h, nt)]

            along("h", refs, sem_tab.at[3 + a], tab.at[a, pl.ds(0, 2), pl.ds(0, nlat - nt)], ("table", a, g))
        for g in range(2):
            unsent.pop(("table", a, g))
        unsent.setdefault(None, []).append(lambda: drain(tab.at[a, :, pl.ds(0, nlat - nt)], sem_tab.at[3 + a, 0]))
        coming["tab2", a] = lambda: drain(tab.at[a], sem_tab.at[3 + a, 1])

    def table_in(a, down, up):
        got(("tab2", a))

        def body(n, _):
            both = tab[a, n].reshape(h_size, 2, ntp, 2 * nl)
            both = jnp.concatenate([both[:, j].reshape(-1, 2 * nl) for j in range(2)], axis=0)
            for j in range(2):
                turned[...] = both[:, j * nl:(j + 1) * nl].T
                t = jnp.concatenate([turned[pl.ds(l, nl // 2, stride=2), :] for l in range(2)], axis=0)
                down[2 * n + j] = t
                up[2 * n + j] = t.T
            return 0

        lax.fori_loop(0, tab.shape[1], body, 0)

    def tb2():
        table_out(0)

    def tb3():
        table_in(0, down_p, up_p)

    def tb4():
        table_out(1)

    def tb5():
        table_in(1, down_q, up_q)

    def sX(b, k):
        send_home_rows(b, k, sem_x, "x")

    def fd(b, k):
        got(("x", b, k))
        dft(b, k, f_tab)
        send_orders(b, k, sr, sem_s, "s")

    def fl(b):
        for k in range(PARTS):
            got(("s", b, k))
        leg_down(b, down_p, sr, True)
        send_owner(b, ar, sem_a, "a")

    def fo(b):
        if not scales:
            got("k")
            st3()
        got(("a", b))
        settle(("bs", b))

        def one(l, _):
            re, im = owned(l)
            a = jnp.concatenate([re, im], axis=0) * scales[b]
            asave[b, l] = a
            n = a.shape[0] // 2
            own, other = dot(a, ker[0, l]), dot(a, ker[1, l])
            put_back(l, own[:n] - other[n:], own[n:] + other[:n])
            return 0

        take_in(b, ar)
        lax.fori_loop(0, l_own, one, 0)
        give_out(b)
        send_back(b, br, sem_b, "b")
        along("dp", lambda o: (asave.at[b, o // 2], aall.at[dp, b]), sem_az.at[b], aall.at[pl.ds(0, dp_size - 1), b])
        coming["az", b] = lambda: drain(aall.at[:, b], sem_az.at[b, 1])

    def fu(b):
        got(("b", b))
        leg_up(b, up_q, br, False)
        send_lats(b, yr, sem_u, "u", PARTS)

    def fi(b, k):
        got(("u", b, k))
        idft(b, k, gt_tab, yr, PARTS)

    def sY(b, k):
        send_rows_home(b, k, sem_y, "y", PARTS)

    def pw(b, k):
        got(("y", b, k))
        if ("t", b) in coming:
            got(("t", b))
        if "small" in coming:
            got("small")
        settle(("pk", b, k))

        def body(n, _):
            lats = [n, n + ntp]
            y = jnp.concatenate(get_rows(b, n), axis=0)
            yb = y.astype(BF16)
            hid = bdot(yb, w1[...])
            th_ = jnp.tanh(GELU_C * (hid + GELU_A * (hid * hid * hid)))
            act = (hid * (0.5 * (1.0 + th_))).astype(BF16)
            resid = y + bdot(act, w2[...])
            parts = []
            for j, t in enumerate(lats):
                r = resid[j * npl:(j + 1) * npl] + xh[b, t] - th[b, t]
                d = lat[t] * r
                ls[...] += jnp.sum((d * r).reshape(-1, 8, nc), axis=0)
                dout[b, t] = d
                parts.append(d)
            d = jnp.concatenate(parts, axis=0)
            db = d.astype(BF16)
            gw[2 * nc:, :] += bdot(act, db, TN)
            slope = 0.5 * (1.0 + th_) + (0.5 * GELU_C) * hid * (1.0 - th_ * th_) * (1.0 + (3.0 * GELU_A) * (hid * hid))
            dh = (bdot(db, w2[...], NT) * slope).astype(BF16)
            gin = bdot(yb, dh, TN)
            gw[:nc, :] += gin[:, :nc]
            gw[nc:2 * nc, :] += gin[:, nc:]
            dy = d + bdot(dh, w1[...], NT)
            put_rows(b, n, dy[:npl], dy[npl:])
            return 0

        lax.fori_loop(k * ntp // PARTS, (k + 1) * ntp // PARTS, body, 0)

    def sD(b, k):
        send_home_rows(b, k, sem_d, "d")

    def bd(b, k):
        got(("d", b, k))
        dft(b, k, g_tab)
        send_orders(b, k, dsr, sem_ds, "ds")

    def bl(b):
        for k in range(PARTS):
            got(("ds", b, k))
        leg_down(b, down_q, dsr, False)
        send_owner(b, dar, sem_da, "da")

    def bo(b):
        got(("da", b))
        settle(("bs", b), "st")

        def one(l, s2):
            re, im = owned(l)
            d = jnp.concatenate([re, im], axis=0)
            dsave[b, l] = d
            n = d.shape[0] // 2
            own, other = dot(d, ker[0, l], NT), dot(d, ker[1, l], NT)
            re, im = own[:n] + other[n:], own[n:] - other[:n]
            put_back(l, re, im)
            return s2 + jnp.sum(re * asave[b, l, :n] + im * asave[b, l, n:], axis=0, keepdims=True)

        take_in(b, dar)
        s2 = lax.fori_loop(0, l_own, one, jnp.zeros((1, nc), F32))
        give_out(b)
        send_back(b, dbr, sem_db, "db")
        along("dp", lambda o: (dsave.at[b, o // 2, :, lanes_at(o % 2)], dall.at[dp, b]), sem_dz.at[b], dall.at[pl.ds(0, dp_size - 1), b])
        coming["dz", b] = lambda: drain(dall.at[:, b], sem_dz.at[b, 1])
        st_s[b:b + 1, :] = s2

    def bu(b):
        got(("db", b))
        leg_up(b, up_p, dbr, True)
        send_lats(b, dyr, sem_du, "du", N_PARTS)

    def bi(b, k):
        got(("du", b, k))
        idft(b, k, ft_tab, dyr, N_PARTS)

    def sN(b, k):
        send_rows_home(b, k, sem_n, "n", N_PARTS)

    def pj1():
        st_s[nb:, :] = jnp.zeros_like(st_s[nb:, :])
        along("w", lambda o: (st_s, st_w.at[w]), sem_st.at[2], st_w.at[pl.ds(0, w_size - 1)])
        coming["pj"] = lambda: drain(st_w, sem_st.at[2, 1])

    def pj2():
        got("pj")
        st_m[...] = jnp.sum(st_w[...], axis=0)
        along("h", lambda o: (st_m, st_h.at[h]), sem_st.at[3], st_h.at[pl.ds(0, h_size - 1)])
        coming["pj2"] = lambda: drain(st_h, sem_st.at[3, 1])

    proj = []

    def fn(b, k):
        if not proj:
            got("pj2")
            proj.append(jnp.sum(st_h[...], axis=0) / (count * ndev))
        got(("n", b, k))

        def body(i, _):
            for t, dn in zip((i, i + ntp), get_rows(b, i)):
                normed = (xh[b, t] - means[b]) * scales[b]
                dout[b, t] = dout[b, t] + scales[b] * (dn - normed * proj[0][b:b + 1])
            return 0

        lax.fori_loop(k * ntp // N_PARTS, (k + 1) * ntp // N_PARTS, body, 0)

    n_c, n_z, n_h, n_w = gw_a.shape[0], gw_zs.shape[0], gw_hs.shape[0], gw_ws.shape[0]
    chip, core = h // 2, h % 2
    chips = h_size // 2

    def over_chips(refs, sems, sent):
        src, dst = refs(chip)
        keep(src, dst, sems)
        for k in range(1, chips):
            o = (chip + k) % chips
            src, dst = refs(o)
            push(src, dst, sems, {"h": 2 * o + core})
        unsent.setdefault(None, []).append(lambda: drain(sent, sems.at[0]))

    def twin(src, dst, sems):
        push(src, dst, sems, {"h": h + 1 - 2 * core})
        unsent.setdefault(None, []).append(lambda: drain(dst, sems.at[0]))

    def gw1():
        twin(gw.at[rows_at(1 - core, n_c)], gw_p, sem_gw.at[0])
        twin(ls, ls_p, sem_ls.at[0])
        coming["gw1"] = lambda: (drain(gw_p, sem_gw.at[0, 1]), drain(ls_p, sem_ls.at[0, 1]))

    def gw2():
        got("gw1")
        gw_a[...] = gw[rows_at(core, n_c), :] + gw_p[...]
        ls_a[...] = ls[...] + ls_p[...]
        along("dp", lambda o: (gw_a.at[rows_at(o, n_z)], gw_z.at[dp]), sem_gw.at[1], gw_z.at[pl.ds(0, dp_size - 1)])
        along("dp", lambda o: (ls_a, ls_z.at[dp]), sem_ls.at[1], ls_z.at[pl.ds(0, dp_size - 1)])
        coming["gw2"] = lambda: (drain(gw_z, sem_gw.at[1, 1]), drain(ls_z, sem_ls.at[1, 1]))

    def gw3():
        got("gw2")
        gw_zs[...] = jnp.sum(gw_z[...], axis=0)
        ls_zs[...] = jnp.sum(ls_z[...], axis=0)
        over_chips(lambda o: (gw_zs.at[rows_at(o, n_h)], gw_h.at[chip]), sem_gw.at[2], gw_h.at[pl.ds(0, chips - 1)])
        over_chips(lambda o: (ls_zs, ls_h.at[chip]), sem_ls.at[2], ls_h.at[pl.ds(0, chips - 1)])
        coming["gw3"] = lambda: (drain(gw_h, sem_gw.at[2, 1]), drain(ls_h, sem_ls.at[2, 1]))

    def gw4():
        got("gw3")
        gw_hs[...] = jnp.sum(gw_h[...], axis=0)
        ls_hs[...] = jnp.sum(ls_h[...], axis=0)
        along("w", lambda o: (gw_hs.at[rows_at(o, n_w)], gw_w.at[w]), sem_gw.at[3], gw_w.at[pl.ds(0, w_size - 1)])
        along("w", lambda o: (ls_hs, ls_w.at[w]), sem_ls.at[3], ls_w.at[pl.ds(0, w_size - 1)])
        coming["gw4"] = lambda: (drain(gw_w, sem_gw.at[3, 1]), drain(ls_w, sem_ls.at[3, 1]))

    def gw5():
        got("gw4")
        gw_ws[...] = jnp.sum(gw_w[...], axis=0)
        loss_out[...] = jnp.sum(ls_w[...], keepdims=True).reshape(1, 1) / total_points
        along("w", lambda o: (gw_ws, gw_w2.at[rows_at(w, n_w)]), sem_gw.at[4], gw_w2.at[pl.ds(0, (w_size - 1) * n_w)])
        coming["gw5"] = lambda: drain(gw_w2, sem_gw.at[4, 1])

    def gw6():
        got("gw5")
        over_chips(lambda o: (gw_w2, gw_h2.at[rows_at(chip, n_h)]), sem_gw.at[5], gw_h2.at[pl.ds(0, (chips - 1) * n_h)])
        coming["gw6"] = lambda: drain(gw_h2, sem_gw.at[5, 1])

    def gw7():
        got("gw6")
        along("dp", lambda o: (gw_h2, gw_f.at[rows_at(dp, n_z)]), sem_gw.at[6], gw_f.at[pl.ds(0, (dp_size - 1) * n_z)])
        coming["gw7"] = lambda: drain(gw_f, sem_gw.at[6, 1])

    def gw8():
        got("gw7")
        twin(gw_f, gw_o, sem_gw.at[7])
        coming["gw8"] = lambda: drain(gw_o, sem_gw.at[7, 1])

    def end():
        got("gw8")
        for c, halves in enumerate(((gw_f, gw_o), (gw_o, gw_f))):
            @pl.when(core == c)
            def _():
                first, second = halves
                for i, (src, dst) in enumerate(((first.at[:nc], gin_out.at[:, :nc]), (first.at[nc:], gin_out.at[:, nc:]), (second, gout_out))):
                    pltpu.make_async_copy(src, dst, sem_fin.at[i]).start()
        for i, dst in enumerate((gin_out.at[:, :nc], gin_out.at[:, nc:], gout_out)):
            unsent.setdefault(None, []).append(lambda dst=dst, i=i: drain(dst, sem_fin.at[i]))

    gs_sum, gs_b = (gs_sum0, gs_sum1), (gs_b0, gs_b1)
    first_rows = (0, gs_sum0.shape[1])
    axes = (("w", "dp"), ("dp", "w"))
    place = {"w": (w, w_size), "dp": (dp, dp_size)}

    def next_to(axis, k):
        index, size = place[axis]
        return (index + k + size) % size

    def add_sample(b):
        got(("az", b))
        got(("dz", b))

        def body(n, _):
            d = dall[n, b]
            half = d.shape[0] // 2
            both = jnp.concatenate([d, jnp.concatenate([d[half:], -d[:half]], axis=0)], axis=1)
            gs_acc[...] += dot(aall[n, b], both, TN)
            return 0

        lax.fori_loop(0, dp_size, body, 0)

    def gsa():
        gs_acc[...] = jnp.zeros_like(gs_acc)
        add_sample(GS_FIRST[0])

    def gsb():
        add_sample(GS_FIRST[1])

    def gs1():
        add_sample(GS_FIRST[2])
        for q in range(2):
            rows_q = pl.ds(first_rows[q], gs_sum[q].shape[1])
            for p in range(2):
                gs_sum[q][p] = gs_acc[rows_q, p * LANES:(p + 1) * LANES]

    def once(key):
        if key in coming:
            got(key)

    def sent_later(ref, sem):
        unsent.setdefault(None, []).append(lambda: drain(ref, sem))

    def gs2(q):
        keep(gs_sum[q], gs_b[q].at[0], sem_gs.at[q, 0])
        for slot, k in ((1, 1), (3, -1)):
            push(gs_sum[q], gs_b[q].at[slot], sem_gs.at[q, slot], {axes[q][0]: next_to(axes[q][0], k)})
            sent_later(gs_sum[q], sem_gs.at[q, slot, 0])
        coming.update({("gs", q, k): lambda k=k: drain(gs_b[q].at[k], sem_gs.at[q, k, 1]) for k in (0, 1, 3)})

    def gs6(q):
        for slot, p, k, i in ((1, 0, 1, 2), (3, 1, -1, 4)):
            once(("gs", q, slot))
            push(gs_b[q].at[slot, p], gs_b[q].at[2, p], sem_gs.at[q, i], {axes[q][0]: next_to(axes[q][0], k)})
            sent_later(gs_b[q].at[2, p], sem_gs.at[q, i, 0])
        coming["gs", q, 2] = lambda: (drain(gs_b[q].at[2, 0], sem_gs.at[q, 2, 1]), drain(gs_b[q].at[2, 1], sem_gs.at[q, 4, 1]))

    def block_at(q, k, shift):
        at = {axes[q][0]: next_to(axes[q][0], -k), axes[q][1]: next_to(axes[q][1], shift)}
        return gs_out.at[:, l_own * at["w"] + at["dp"] // 2, pl.ds(first_rows[q], gs_sum[q].shape[1]), lanes_at(at["dp"] % 2)]

    def gs3(q, k):
        once(("gs", q, k))
        mine = block_at(q, k, 0)
        pltpu.make_async_copy(gs_b[q].at[k], mine, sem_gf.at[q, 3, k, 0]).start()
        for way, shift in ((0, 1), (1, -1)):
            push(gs_b[q].at[k], mine, sem_gf.at[q, way, k], {axes[q][1]: next_to(axes[q][1], shift)})

    def gs4(q, k):
        way, shift = (0, 1) if k < 2 else (1, -1)
        drain(gs_b[q].at[k], sem_gf.at[q, way, k, 1])
        block = block_at(q, k, -shift)
        push(block, block, sem_gf.at[q, 2, k], {axes[q][1]: next_to(axes[q][1], shift)})

    def gs5(q, k):
        drain(gs_b[q].at[k], sem_gf.at[q, 1 if k < 2 else 0, k, 1])
        drain(gs_b[q].at[k], sem_gf.at[q, 2, k, 1])
        for i in range(4):
            drain(gs_b[q].at[k], sem_gf.at[q, i, k, 0])

    scope = dict(locals())
    scope["pk"] = pk_
    for name in ORDER.split():
        call = name.rstrip("0123456789") or name
        if name in scope:
            scope[name]()
        elif name[:3] in scope:
            scope[name[:3]](*map(int, name[3:]))
        else:
            scope[call](*map(int, name[len(call):]))
    assert not coming
    settle()


def hand_on_kernel(*refs):
    n = len(refs) // 2
    pairs = []
    for src, dst in zip(refs[:n], refs[n:2 * n]):
        lead = [()] if len(src.shape) == 2 else [(i,) for i in range(src.shape[0])]
        pairs += [(src.at[i], dst.at[i]) if i else (src, dst) for i in lead]
    copies = [pltpu.make_async_copy(src, dst, refs[2 * n].at[i]) for i, (src, dst) in enumerate(pairs)]
    for c in copies:
        c.start()
    for c in copies:
        c.wait()


def hand_on(arrays):
    return pl.pallas_call(
        hand_on_kernel, name="hand_on",
        out_shape=[jax.ShapeDtypeStruct(a.shape, F32) for a in arrays],
        in_specs=[pl.BlockSpec(memory_space=pltpu.VMEM)] * len(arrays), out_specs=[pl.BlockSpec(memory_space=pl.ANY)] * len(arrays),
        scratch_shapes=[pltpu.SemaphoreType.DMA((32,))],
        compiler_params=pltpu.CompilerParams(vmem_limit_bytes=12 * 1024 * 1024),
    )(*[pltpu.with_memory_space_constraint(a, pltpu.VMEM) for a in arrays])


def solution(mesh):
    dp_size, w_size, h_size = mesh.shape["dp"], mesh.shape["w"], mesh.shape["h"]

    def local_step(field, target, lat_weight, leg_fwd, leg_inv, spec_w, w_in, w_out):
        nb, nc, nt, npl = field.shape
        nlon = npl * w_size
        ntp = nt // 2
        nm = leg_fwd.shape[0] * w_size
        ndev = h_size * w_size
        nlat = nt * h_size
        nl = leg_fwd.shape[1]
        lo = nl // ndev
        assert nm == 8 * h_size and nc == w_size * LANES // 2 and h_size == 2 * w_size and 2 * lo == dp_size and 2 * nl == LANES
        total_points = nb * dp_size * nc * nlat * nlon
        any_spec = pl.BlockSpec(memory_space=pl.ANY)
        vmem_spec = pl.BlockSpec(memory_space=pltpu.VMEM)
        sds = lambda *s: jax.ShapeDtypeStruct(s, F32)
        vm = lambda *s: pltpu.VMEM(s, F32)
        dma = lambda *s: pltpu.SemaphoreType.DMA(s)
        n_rows = 2 * nc + w_out.shape[0]
        n_z, n_h, n_w = n_rows // dp_size, n_rows // dp_size // h_size, n_rows // dp_size // h_size // w_size
        home = vm(nb, nt, npl, nc)
        woven = vm(nb, w_size, ntp, npl, LANES)
        order = vm(nb, 16 * nlat // 2, LANES)
        degree = vm(nb, 8 * nl, LANES)
        owner = vm(nb, h_size, 8 * lo, w_size * LANES)
        saved = vm(nb, lo, 2 * nm, nc)
        cut = GS_ROWS
        n_pairs = leg_fwd.shape[0] // 2
        n_c = n_rows // 2
        n_z, n_h, n_w = n_c // dp_size, n_c // dp_size // w_size, n_c // dp_size // w_size // w_size
        results = pl.pallas_call(
            functools.partial(block_kernel, (dp_size, h_size, w_size), total_points),
            name="block",
            out_shape=[vm(nb, nt, npl, nc), vm(2, lo * w_size, nc, nc), vm(nc, 2 * nc), vm(2 * nc, nc), sds(1, 1)],
            in_specs=[any_spec] * 9,
            out_specs=[vmem_spec] * 5,
            scratch_shapes=[
                vm(*leg_fwd.shape[:1], nt, nl), vm(*leg_fwd.shape[:1], nt, nl), pltpu.SMEM((nt,), F32), pltpu.VMEM(w_in.shape, BF16),
                pltpu.VMEM(w_out.shape, BF16), vm(2 * nm, nlon), vm(2 * nm, nlon), vm(nlon, 2 * nm), vm(nlon, 2 * nm),
                home, home, woven, vm(nb, ntp, nlon, LANES), woven, woven,
                vm(nb, h_size, 16 * ntp, LANES), order, order, order, vm(nb, h_size, 16 * ntp, LANES), vm(nb, h_size, 16 * ntp, LANES),
                degree, owner, owner, vm(nb, h_size, w_size, 8 * lo, LANES), degree, degree, saved, saved,
                vm(dp_size, nb, 2 * nm, nc), vm(dp_size, nb, 2 * nm, LANES), vm(lo, w_size, nm, LANES),
                vm(8, nc), vm(h_size, 8, nc), vm(8, nc), vm(w_size, 8, nc),
                vm(2, n_pairs, nt, 2 * nl), vm(2, w_size, n_pairs, nt, 2 * nl), vm(2, 4, nlat, 2 * nl), vm(nl, nlat),
                vm(8, nl, nlat), vm(8, nl, nlat), vm(8, nlat, nl), vm(8, nlat, nl),
                vm(2, lo, nc, nc),
                vm(n_rows, nc), vm(n_c, nc), vm(n_c, nc), vm(dp_size, n_z, nc), vm(n_z, nc), vm(w_size, n_h, nc), vm(n_h, nc),
                vm(w_size, n_w, nc), vm(n_w, nc), vm(n_h, nc), vm(n_z, nc), vm(n_c, nc), vm(n_c, nc),
                vm(8, nc), vm(8, nc), vm(8, nc), vm(dp_size, 8, nc), vm(8, nc), vm(w_size, 8, nc), vm(8, nc), vm(w_size, 8, nc),
                vm(nc, nc), vm(2, cut, LANES), vm(2, nc - cut, LANES), vm(4, 2, cut, LANES), vm(4, 2, nc - cut, LANES),
            ] + [dma(nb, PARTS, 2)] * 8 + [dma(nb, 2)] * 6 + [dma(nb, 2), dma(4, 2), dma(5, 2), dma(1), dma(8, 2), dma(4, 2),
                 dma(2, 5, 2), dma(2, 4, 4, 2), dma(3), dma(6)],
            compiler_params=pltpu.CompilerParams(collective_id=0, has_side_effects=True, vmem_limit_bytes=54 * 1024 * 1024),
        )(field.transpose(0, 2, 3, 1), target.transpose(0, 2, 3, 1), leg_fwd.transpose(0, 2, 1), leg_inv.transpose(0, 2, 1),
          spec_w, lat_weight, w_in, w_out, jnp.asarray(dft_table(nlon, nm, h_size)))
        d_x, g_spec, g_in, g_out = hand_on(results[:4])
        loss = results[4]
        return loss.reshape(()), d_x.transpose(0, 3, 1, 2), g_spec, g_in, g_out

    grid_spec = P("dp", None, "h", "w")
    table_spec = P("w", None, "h")
    kernel_spec = P(None, "h", None, None)
    return jax.shard_map(local_step, mesh=mesh, in_specs=(grid_spec, grid_spec, P("h"), table_spec, table_spec, P(), P(), P()), out_specs=(P(), grid_spec, kernel_spec, P(), P()), check_vma=False)
```

```python
import functools
import jax
import jax.numpy as jnp
import numpy as np
from jax import lax
from jax.experimental import pallas as pl
from jax.experimental.pallas import tpu as pltpu
from jax.sharding import PartitionSpec as P

NORM_EPS = 1e-5
PRECISE = lax.Precision.HIGHEST
MESH = pl.DeviceIdType.MESH
F32 = jnp.float32
BF16 = jnp.bfloat16
GELU_C = float(np.sqrt(2.0 / np.pi))
GELU_A = 0.044715
LANES = 128
NN = (((1,), (0,)), ((), ()))
NT = (((1,), (1,)), ((), ()))
TN = (((0,), (0,)), ((), ()))


def dot(a, b, dims=NN):
    return lax.dot_general(a, b, dims, precision=PRECISE, preferred_element_type=F32)


def bdot(a, b, dims=NN):
    return lax.dot_general(a, b, dims, preferred_element_type=F32)


def dft_table(lon_count, num_modes, h_size):
    modes, lons = np.arange(num_modes), np.arange(lon_count)
    angle = 2.0 * np.pi * ((modes[:, None] * lons[None, :]) % lon_count) / lon_count
    table = np.stack([np.cos(angle), -np.sin(angle)], 0) * lon_count ** -0.5
    table = table.reshape(2, h_size, num_modes // h_size, lon_count).transpose(1, 0, 2, 3)
    return table.reshape(2 * num_modes, lon_count).astype(np.float32)


def drain(ref, sem):
    pltpu.make_async_copy(ref, ref, sem).wait()


def rows_at(i, n):
    return pl.ds(pl.multiple_of(i * n, n), n)


def lanes_at(i):
    return pl.ds(pl.multiple_of(i * LANES, LANES), LANES)


def push(src, dst, sems, device):
    pltpu.make_async_remote_copy(src_ref=src, dst_ref=dst, send_sem=sems.at[0], recv_sem=sems.at[1],
                                 device_id=device, device_id_type=MESH).start()


def keep(src, dst, sems):
    pltpu.make_async_copy(src, dst, sems.at[1]).start()


def flip(v):
    return pltpu.roll(v, LANES // 2, 1)


def low(v):
    return lax.broadcasted_iota(jnp.int32, v.shape, 1) < LANES // 2


def weave(a, b):
    return jnp.where(low(a), a, flip(b)), jnp.where(low(a), flip(a), b)


def weave_wide(tiles):
    pairs = [weave(tiles[j], tiles[j + 1]) for j in range(0, len(tiles), 2)]
    return jnp.concatenate([p[0] for p in pairs], axis=1), jnp.concatenate([p[1] for p in pairs], axis=1)


def weave_tiles(a, b):
    out = []
    for j in range(0, a.shape[1], LANES):
        out.extend(weave(a[:, j:j + LANES], b[:, j:j + LANES]))
    return out


PARTS = 4
GS_ROWS = 176
GS_FIRST = (0, 1, 2)
ORDER = " ".join((
    'go', 'pk0', 'sX01', 'pk2', 'pk1', 'sX03', 'tb1', 'sX00', 'sX02', 'sX12',
    'fd01', 'fd03', 'sX10', 'tb2', 'fd00', 'fd02', 'tb4', 'st1', 'sX11', 'sX13',
    'tb3', 'fd12', 'fl0', 'st2', 'fd10', 'tb5', 'sX21', 'fd13', 'fd11', 'sX20',
    'fo0', 'fl1', 'sX23', 'sX22', 'fd20', 'fu0', 'fo1', 'fd23', 'fd21', 'fi00',
    'sY00', 'fi01', 'sY01', 'fi02', 'fd22', 'fi03', 'sY02', 'sY03', 'pw00', 'fu1',
    'sD00', 'fl2', 'pw02', 'sD02', 'pw01', 'pw03', 'sD03', 'sD01', 'fi12', 'bd02',
    'fi10', 'sY12', 'fi13', 'bd00', 'fo2', 'bd01', 'sY10', 'bd03', 'fi11', 'sY11',
    'pw12', 'sY13', 'fu2', 'pw10', 'sD12', 'bl0', 'sD10', 'pw11', 'fi21', 'fi20',
    'sY20', 'sY21', 'pw13', 'fi22', 'sD11', 'fi23', 'bd10', 'sD13', 'bo0', 'sY22',
    'pw21', 'bd12', 'sY23', 'sD21', 'bd13', 'pw20', 'sD20', 'bd11', 'bu0', 'pw22',
    'pw23', 'sD22', 'sD23', 'gw1', 'gsa', 'bd21', 'gw2', 'bl1', 'bi03', 'bi02',
    'bd22', 'sN02', 'bi01', 'sN01', 'bd20', 'bd23', 'gw3', 'bo1', 'bl2', 'bi00',
    'sN03', 'gw4', 'sN00', 'bu1', 'bo2', 'gw5', 'pj1', 'bi10', 'sN10', 'gsb',
    'bi11', 'sN11', 'pj2', 'gs1', 'gs20', 'gs21', 'bi13', 'sN13', 'gs300', 'gw6',
    'bu2', 'gs310', 'gs61', 'bi12', 'sN12', 'gs303', 'gw7', 'gs313', 'fn11', 'gs60',
    'bi20', 'gs311', 'fn12', 'bi23', 'fn10', 'fn02', 'gs312', 'gs403', 'gs301', 'gs413',
    'gs410', 'sN23', 'sN20', 'gs302', 'gs400', 'bi22', 'fn13', 'bi21', 'gw8', 'sN21',
    'sN22', 'fn00', 'gs503', 'gs412', 'gs401', 'fn20', 'gs402', 'fn01', 'gs411', 'end',
    'gs502', 'gs500', 'gs510', 'fn23', 'fn03', 'gs501', 'fn22', 'gs512', 'fn21', 'gs513',
    'gs511',
))


def block_kernel(sizes, total_points,
                 x, tgt, leg_p_in, leg_q_in, spec_w, lat_in, w1_in, w2_in, f_in,
                 dout, gs_out, gin_out, gout_out, loss_out,
                 leg_p, leg_q, lat, w1, w2, f_tab, g_tab, ft_tab, gt_tab,
                 xh, th, pk, rows, yrow, hy,
                 xs, sr, dsr, ys, yr, dyr, als, ar, dar, bs, br, dbr, asave, dsave, aall, dall,
                 st_s, st_h, st_m, st_w, tab_s, tab_w, tab, down_p, down_q, up_p, up_q, ker,
                 gw, gw_p, gw_a, gw_z, gw_zs, gw_h, gw_hs, gw_w, gw_ws, gw_w2, gw_h2, gw_f, gw_o,
                 ls, ls_p, ls_a, ls_z, ls_zs, ls_h, ls_hs, ls_w, gs_acc, gs_sum0, gs_sum1, gs_b0, gs_b1,
                 sem_x, sem_y, sem_d, sem_n, sem_s, sem_ds, sem_u, sem_du, sem_a, sem_da, sem_b, sem_db, sem_az, sem_dz,
                 sem_in, sem_st, sem_tab, sem_k, sem_gw, sem_ls, sem_gs, sem_gf, sem_fin, sem_small):
    dp_size, h_size, w_size = sizes
    dp, h, w = lax.axis_index("dp"), lax.axis_index("h"), lax.axis_index("w")
    ndev = h_size * w_size
    me = h * w_size + w
    nb, nt, npl, nc = x.shape
    ntp = nt // 2
    part = ntp // PARTS
    nlon = npl * w_size
    nlat = nt * h_size
    nl = als.shape[1] // 8
    l_own = nl // ndev
    piece = 8 * l_own
    unsent, coming = {}, {}

    def got(key):
        coming.pop(key)()

    def peer(k):
        return (h + k // w_size) % h_size, (w + k % w_size) % w_size

    barrier = pltpu.get_barrier_semaphore()

    def meet(k, _):
        h2, w2_ = peer(k)
        pl.semaphore_signal(barrier, inc=1, device_id={"h": h2, "w": w2_}, device_id_type=MESH)
        return 0

    def meet_dp(k, _):
        pl.semaphore_signal(barrier, inc=1, device_id={"dp": (dp + k) % dp_size}, device_id_type=MESH)
        return 0

    lax.fori_loop(1, ndev, meet, 0)
    lax.fori_loop(1, dp_size, meet_dp, 0)
    loads = [pltpu.make_async_copy(x.at[b], xh.at[b], sem_in.at[b, 0]) for b in range(nb)]
    load_t = [pltpu.make_async_copy(tgt.at[b], th.at[b], sem_in.at[b, 1]) for b in range(nb)]
    load_k = pltpu.make_async_copy(spec_w.at[:, pl.ds(me * l_own, l_own)], ker, sem_k.at[0])
    small = [pltpu.make_async_copy(src, dst, sem_small.at[i]) for i, (src, dst) in enumerate((
        (leg_p_in, leg_p), (leg_q_in, leg_q), (f_in, f_tab), (lat_in, lat), (w1_in, w1), (w2_in, w2)))]
    for c in loads + small[:3] + [load_k] + load_t + small[3:]:
        c.start()
    coming["k"] = load_k.wait
    coming["small"] = lambda: [c.wait() for c in small[3:]]
    coming.update({("t", b): load_t[b].wait for b in range(nb)})
    for ref in (ar, br, dar, dbr, st_s, gw, ls):
        ref[...] = jnp.zeros_like(ref)

    def settle(*keys):
        for key in keys or list(unsent):
            for wait in unsent.pop(key, []):
                wait()

    def along(axis, refs, sems, sent, key=None):
        size, index = {"dp": (dp_size, dp), "h": (h_size, h), "w": (w_size, w)}[axis]
        src, dst = refs(index)
        keep(src, dst, sems)

        def body(k, _):
            other = (index + k) % size
            src, dst = refs(other)
            push(src, dst, sems, {axis: other})
            return 0

        lax.fori_loop(1, size, body, 0)
        unsent.setdefault(key, []).append(lambda: drain(sent, sems.at[0]))

    def some(refs, sems, low_h, high_h, count, counts, key):
        src, dst = refs(h, w)
        keep(src, dst, sems)

        def one(h2, k):
            w2_ = (w + k) % w_size
            src, dst = refs(h2, w2_)
            push(src, dst, sems, {"h": h2, "w": w2_})

        for k in range(1, w_size):
            one(h, k)

        def body(h2, _):
            for k in range(w_size):
                one(h2, k)
            return 0

        lax.fori_loop(low_h, high_h, body, 0)
        unsent.setdefault(key, []).append(lambda: take(sems.at[0], count - 1, [n - 1 for n in counts]))

    def take(sem, count, counts):
        for n in counts:
            @pl.when(count == n)
            def _():
                drain(als.at[0, pl.ds(0, n * piece)], sem)

    n_orders, n_owners = (h + 1) * w_size, (h_size - h) * w_size
    counts = [w_size * n for n in range(1, h_size + 1)]
    pairs = lambda k: pl.ds(k * part, part)

    def at_rows(i, k):
        return pl.ds(pl.multiple_of(i * 16 * ntp + k * 16 * part, 16 * part), 16 * part)

    def send_home_rows(b, k, sem, name):
        along("w", lambda o: (pk.at[b, o, pairs(k)], rows.at[b, pairs(k), rows_at(w, npl)]), sem.at[b, k],
              pk.at[b, pl.ds(0, w_size - 1), pairs(k)], ("pk", b, k))
        coming[name, b, k] = lambda: drain(rows.at[b, pairs(k)], sem.at[b, k, 1])

    def send_rows_home(b, k, sem, name):
        along("w", lambda o: (yrow.at[b, o, pairs(k)], hy.at[b, w, pairs(k)]), sem.at[b, k],
              yrow.at[b, pl.ds(0, w_size - 1), pairs(k)], ("yrow", b, k))
        coming[name, b, k] = lambda: drain(hy.at[b, :, pairs(k)], sem.at[b, k, 1])

    def send_orders(b, k, dst, sem, name):
        along("h", lambda o: (xs.at[b, o, at_rows(0, k)], dst.at[b, at_rows(h, k)]), sem.at[b, k],
              xs.at[b, pl.ds(0, h_size - 1), at_rows(0, k)], ("xs", b, k))
        coming[name, b, k] = lambda: drain(xs.at[b, :, at_rows(0, k)], sem.at[b, k, 1])

    def send_lats(b, dst, sem, name):
        def one(k, _):
            keep(ys.at[b, at_rows(h, k)], dst.at[b, h, at_rows(0, k)], sem.at[b, k])

            def body(j, _):
                o = (h + j) % h_size
                push(ys.at[b, at_rows(o, k)], dst.at[b, h, at_rows(0, k)], sem.at[b, k], {"h": o})
                return 0

            return lax.fori_loop(1, h_size, body, 0)

        lax.fori_loop(0, PARTS, one, 0)
        for k in range(PARTS):
            unsent.setdefault(("ys", b), []).append(lambda k=k: drain(xs.at[b, pl.ds(0, h_size - 1), at_rows(0, k)], sem.at[b, k, 0]))
            coming[name, b, k] = lambda k=k: drain(dst.at[b, :, at_rows(0, k)], sem.at[b, k, 1])

    def send_owner(b, dst, sem, name):
        some(lambda h2, w2_: (als.at[b, rows_at(h2 * w_size + w2_, piece)], dst.at[b, h, :, lanes_at(w)]), sem.at[b],
             h + 1, h_size, n_owners, counts, ("als", b))
        coming[name, b] = lambda: take(sem.at[b, 1], n_orders, counts)

    def send_back(b, dst, sem, name):
        some(lambda h2, w2_: (bs.at[b, h2, w2_], dst.at[b, rows_at(me, piece)]), sem.at[b],
             0, h, n_orders, counts, ("bs", b))
        coming[name, b] = lambda: take(sem.at[b, 1], n_owners, counts)

    def dft(b, k, table):
        settle(("xs", b, k))

        def body(n, _):
            i = 2 * n
            both = jnp.concatenate([rows[b, i], rows[b, i + 1]], axis=1)
            out = dot(table[...], both).reshape(h_size, 16, 2 * LANES)
            xs[b, :, rows_at(i, 16), :] = out[:, :, :LANES]
            xs[b, :, rows_at(i + 1, 16), :] = out[:, :, LANES:]
            return 0

        lax.fori_loop(k * part // 2, (k + 1) * part // 2, body, 0)

    def idft(b, k, table, src):
        settle(("yrow", b, k))

        def body(n, _):
            i = 2 * n
            both = jnp.concatenate([src[b, :, rows_at(i + j, 16), :].reshape(-1, LANES) for j in range(2)], axis=1)
            out = dot(table[...], both)
            for j in range(2):
                yrow[b, :, i + j] = out[:, j * LANES:(j + 1) * LANES].reshape(w_size, npl, LANES)
            return 0

        lax.fori_loop(k * part // 2, (k + 1) * part // 2, body, 0)

    def level(v, here):
        mean = jnp.mean(v, axis=0, keepdims=True)
        mean = 0.5 * (mean + flip(mean))
        return v - jnp.where(jnp.logical_and(h == 0, here), mean, 0.0)

    def orders(body):
        def four(n, _):
            for i in range(4):
                body(4 * n + i, n == 0 if i == 0 else None)
            return 0

        lax.fori_loop(0, 2, four, 0)

    def leg_down(b, table, src, fix):
        settle(("als", b))

        def one(m, here):
            re, im = (src[b, pl.ds(ri * 8 + m, ntp * h_size, stride=16), :] for ri in range(2))
            if fix and here is not None:
                re = level(re, here)
            als[b, pl.ds(m, nl, stride=8), :] = dot(table[m], jnp.concatenate(weave(re, im), axis=0))

        orders(one)

    def leg_up(b, table, src, fix):
        settle(("ys", b))

        def one(m, here):
            out = dot(table[m], src[b, pl.ds(m, nl, stride=8), :])
            re, im = weave(out[:nlat // 2], out[nlat // 2:])
            if fix and here is not None:
                re = level(re, here)
            ys[b, pl.ds(m, ntp * h_size, stride=16), :] = re
            ys[b, pl.ds(8 + m, ntp * h_size, stride=16), :] = im

        orders(one)

    def owned(b, l, src):
        tiles = [src[b, :, rows_at(l, 8), j * LANES:(j + 1) * LANES].reshape(-1, LANES) for j in range(w_size)]
        return weave_wide(tiles)

    def put_back(b, l, re, im):
        for j, tile in enumerate(weave_tiles(re, im)):
            bs[b, :, j, rows_at(l, 8), :] = tile.reshape(h_size, 8, LANES)

    def put_rows(b, i, v0, v1):
        for j, tile in enumerate(weave_tiles(v0, v1)):
            pk[b, j, i] = tile

    def get_rows(b, i):
        return weave_wide([hy[b, j, i] for j in range(w_size)])

    count = nt * npl
    n_tab = tab_s.shape[1] // dp_size

    def combine(stats, n):
        mean = jnp.mean(stats, axis=0)
        dev = stats - mean[None]
        dev2 = jnp.sum(dev * dev, axis=0)
        m2 = jnp.sum(stats, axis=0)
        return [(mean[2 * b:2 * b + 1], m2[2 * b + 1:2 * b + 2] + n * dev2[2 * b:2 * b + 1]) for b in range(nb)]

    sums = {}

    def pk_(b):
        loads[b].wait()

        def body(i, total):
            v0, v1 = xh[b, i], xh[b, i + ntp]
            put_rows(b, i, v0, v1)
            return total + jnp.sum(v0 + v1, axis=0, keepdims=True)

        sums[b] = lax.fori_loop(0, ntp, body, jnp.zeros((1, nc), F32))

    def go():
        for c in small[:3]:
            c.wait()
        for a, leg in enumerate((leg_p, leg_q)):
            for m in range(leg.shape[0]):
                tab_s[a, m // 2, :, m % 2 * nl:(m % 2 + 1) * nl] = leg[m]
        pl.semaphore_wait(barrier, ndev - 1 + dp_size - 1)
        along("w", lambda o: (tab_s.at[:, rows_at(dp, n_tab)], tab_w.at[:, w, rows_at(dp, n_tab)]), sem_tab.at[0],
              tab_w.at[:, pl.ds(0, w_size - 1), pl.ds(0, n_tab)])
        coming["tab"] = lambda: drain(tab_w.at[:, :, pl.ds(0, n_tab)], sem_tab.at[0, 1])

    def st1():
        for b in range(nb):
            mean = sums[b] / count

            def body(t, total, b=b, mean=mean):
                d = xh[b, t] - mean
                return total + jnp.sum(d * d, axis=0, keepdims=True)

            st_s[2 * b:2 * b + 1, :] = mean
            st_s[2 * b + 1:2 * b + 2, :] = lax.fori_loop(0, nt, body, jnp.zeros((1, nc), F32))
        along("w", lambda o: (st_s, st_w.at[w]), sem_st.at[0], st_w.at[pl.ds(0, w_size - 1)], "st")
        coming["st"] = lambda: drain(st_w, sem_st.at[0, 1])
        g_tab[...] = jnp.where(lax.broadcasted_iota(jnp.int32, f_tab.shape, 0) == 0, 1.0, 2.0) * f_tab[...]
        ft_tab[...] = f_tab[...].T
        gt_tab[...] = g_tab[...].T

    def st2():
        got("st")
        st_m[...] = jnp.zeros_like(st_m)
        for b, (mean, m2) in enumerate(combine(st_w[...], count)):
            st_m[2 * b:2 * b + 1, :] = mean
            st_m[2 * b + 1:2 * b + 2, :] = m2
        along("h", lambda o: (st_m, st_h.at[h]), sem_st.at[1], st_h.at[pl.ds(0, h_size - 1)], "st")
        coming["st2"] = lambda: drain(st_h, sem_st.at[1, 1])

    means, scales = [], []

    def st3():
        got("st2")
        for mean, m2 in combine(st_h[...], count * w_size):
            means.append(mean)
            scales.append(lax.rsqrt(m2 / (count * ndev) + NORM_EPS))

    def tb1():
        got("tab")
        for a in range(2):
            share = tab_w.at[a, :, rows_at(dp, n_tab)]
            for k in range(1, dp_size):
                push(share, share, sem_tab.at[1 + a], {"dp": (dp + k) % dp_size})
            others = tab_w.at[a, :, pl.ds(0, (dp_size - 1) * n_tab)]
            unsent.setdefault(None, []).append(lambda a=a, others=others: drain(others, sem_tab.at[1 + a, 0]))
            coming["tab1", a] = lambda a=a, others=others: drain(others, sem_tab.at[1 + a, 1])

    def table_out(a):
        got(("tab1", a))
        along("h", lambda o: (tab_w.at[a, o // 2, rows_at(o % 2, 4)], tab.at[a, :, rows_at(h, nt)]), sem_tab.at[3 + a],
              tab.at[a, :, pl.ds(0, nlat - nt)])
        coming["tab2", a] = lambda: drain(tab.at[a], sem_tab.at[3 + a, 1])

    def table_in(a, down, up):
        got(("tab2", a))

        def body(n, _):
            both = tab[a, n].reshape(h_size, 2, ntp, 2 * nl)
            both = jnp.concatenate([both[:, j].reshape(-1, 2 * nl) for j in range(2)], axis=0)
            for j in range(2):
                t = both[:, j * nl:(j + 1) * nl]
                up[2 * n + j] = t
                down[2 * n + j] = t.T
            return 0

        lax.fori_loop(0, tab.shape[1], body, 0)

    def tb2():
        table_out(0)

    def tb3():
        table_in(0, down_p, up_p)

    def tb4():
        table_out(1)

    def tb5():
        table_in(1, down_q, up_q)

    def sX(b, k):
        send_home_rows(b, k, sem_x, "x")

    def fd(b, k):
        got(("x", b, k))
        dft(b, k, f_tab)
        send_orders(b, k, sr, sem_s, "s")

    def fl(b):
        for k in range(PARTS):
            got(("s", b, k))
        leg_down(b, down_p, sr, True)
        send_owner(b, ar, sem_a, "a")

    def fo(b):
        if not scales:
            got("k")
            st3()
        got(("a", b))
        settle(("bs", b))

        def one(l, _):
            re, im = owned(b, l, ar)
            a = jnp.concatenate([re, im], axis=0) * scales[b]
            asave[b, l] = a
            n = a.shape[0] // 2
            own, other = dot(a, ker[0, l]), dot(a, ker[1, l])
            put_back(b, l, own[:n] - other[n:], own[n:] + other[:n])
            return 0

        lax.fori_loop(0, l_own, one, 0)
        send_back(b, br, sem_b, "b")
        along("dp", lambda o: (asave.at[b, o // 2], aall.at[dp, b]), sem_az.at[b], aall.at[pl.ds(0, dp_size - 1), b])
        coming["az", b] = lambda: drain(aall.at[:, b], sem_az.at[b, 1])

    def fu(b):
        got(("b", b))
        leg_up(b, up_q, br, False)
        send_lats(b, yr, sem_u, "u")

    def fi(b, k):
        got(("u", b, k))
        idft(b, k, gt_tab, yr)

    def sY(b, k):
        send_rows_home(b, k, sem_y, "y")

    def pw(b, k):
        got(("y", b, k))
        if ("t", b) in coming:
            got(("t", b))
        if "small" in coming:
            got("small")
        settle(("pk", b, k))

        def body(n, _):
            lats = [n, n + ntp]
            y = jnp.concatenate(get_rows(b, n), axis=0)
            yb = y.astype(BF16)
            hid = bdot(yb, w1[...])
            th_ = jnp.tanh(GELU_C * (hid + GELU_A * (hid * hid * hid)))
            act = (hid * (0.5 * (1.0 + th_))).astype(BF16)
            resid = y + bdot(act, w2[...])
            parts = []
            for j, t in enumerate(lats):
                r = resid[j * npl:(j + 1) * npl] + xh[b, t] - th[b, t]
                d = lat[t] * r
                ls[...] += jnp.sum((d * r).reshape(-1, 8, nc), axis=0)
                dout[b, t] = d
                parts.append(d)
            d = jnp.concatenate(parts, axis=0)
            db = d.astype(BF16)
            gw[2 * nc:, :] += bdot(act, db, TN)
            slope = 0.5 * (1.0 + th_) + (0.5 * GELU_C) * hid * (1.0 - th_ * th_) * (1.0 + (3.0 * GELU_A) * (hid * hid))
            dh = (bdot(db, w2[...], NT) * slope).astype(BF16)
            gin = bdot(yb, dh, TN)
            gw[:nc, :] += gin[:, :nc]
            gw[nc:2 * nc, :] += gin[:, nc:]
            dy = d + bdot(dh, w1[...], NT)
            put_rows(b, n, dy[:npl], dy[npl:])
            return 0

        lax.fori_loop(k * part, (k + 1) * part, body, 0)

    def sD(b, k):
        send_home_rows(b, k, sem_d, "d")

    def bd(b, k):
        got(("d", b, k))
        dft(b, k, g_tab)
        send_orders(b, k, dsr, sem_ds, "ds")

    def bl(b):
        for k in range(PARTS):
            got(("ds", b, k))
        leg_down(b, down_q, dsr, False)
        send_owner(b, dar, sem_da, "da")

    def bo(b):
        got(("da", b))
        settle(("bs", b), "st")

        def one(l, s2):
            re, im = owned(b, l, dar)
            d = jnp.concatenate([re, im], axis=0)
            dsave[b, l] = d
            n = d.shape[0] // 2
            own, other = dot(d, ker[0, l], NT), dot(d, ker[1, l], NT)
            re, im = own[:n] + other[n:], own[n:] - other[:n]
            put_back(b, l, re, im)
            return s2 + jnp.sum(re * asave[b, l, :n] + im * asave[b, l, n:], axis=0, keepdims=True)

        s2 = lax.fori_loop(0, l_own, one, jnp.zeros((1, nc), F32))
        send_back(b, dbr, sem_db, "db")
        along("dp", lambda o: (dsave.at[b, o // 2, :, lanes_at(o % 2)], dall.at[dp, b]), sem_dz.at[b], dall.at[pl.ds(0, dp_size - 1), b])
        coming["dz", b] = lambda: drain(dall.at[:, b], sem_dz.at[b, 1])
        st_s[b:b + 1, :] = s2

    def bu(b):
        got(("db", b))
        leg_up(b, up_p, dbr, True)
        send_lats(b, dyr, sem_du, "du")

    def bi(b, k):
        got(("du", b, k))
        idft(b, k, ft_tab, dyr)

    def sN(b, k):
        send_rows_home(b, k, sem_n, "n")

    def pj1():
        st_s[nb:, :] = jnp.zeros_like(st_s[nb:, :])
        along("w", lambda o: (st_s, st_w.at[w]), sem_st.at[2], st_w.at[pl.ds(0, w_size - 1)])
        coming["pj"] = lambda: drain(st_w, sem_st.at[2, 1])

    def pj2():
        got("pj")
        st_m[...] = jnp.sum(st_w[...], axis=0)
        along("h", lambda o: (st_m, st_h.at[h]), sem_st.at[3], st_h.at[pl.ds(0, h_size - 1)])
        coming["pj2"] = lambda: drain(st_h, sem_st.at[3, 1])

    proj = []

    def fn(b, k):
        if not proj:
            got("pj2")
            proj.append(jnp.sum(st_h[...], axis=0) / (count * ndev))
        got(("n", b, k))

        def body(i, _):
            for t, dn in zip((i, i + ntp), get_rows(b, i)):
                normed = (xh[b, t] - means[b]) * scales[b]
                dout[b, t] = dout[b, t] + scales[b] * (dn - normed * proj[0][b:b + 1])
            return 0

        lax.fori_loop(k * part, (k + 1) * part, body, 0)

    n_c, n_z, n_h, n_w = gw_a.shape[0], gw_zs.shape[0], gw_hs.shape[0], gw_ws.shape[0]
    chip, core = h // 2, h % 2
    chips = h_size // 2

    def over_chips(refs, sems, sent):
        src, dst = refs(chip)
        keep(src, dst, sems)
        for k in range(1, chips):
            o = (chip + k) % chips
            src, dst = refs(o)
            push(src, dst, sems, {"h": 2 * o + core})
        unsent.setdefault(None, []).append(lambda: drain(sent, sems.at[0]))

    def twin(src, dst, sems):
        push(src, dst, sems, {"h": h + 1 - 2 * core})
        unsent.setdefault(None, []).append(lambda: drain(dst, sems.at[0]))

    def gw1():
        twin(gw.at[rows_at(1 - core, n_c)], gw_p, sem_gw.at[0])
        twin(ls, ls_p, sem_ls.at[0])
        coming["gw1"] = lambda: (drain(gw_p, sem_gw.at[0, 1]), drain(ls_p, sem_ls.at[0, 1]))

    def gw2():
        got("gw1")
        gw_a[...] = gw[rows_at(core, n_c), :] + gw_p[...]
        ls_a[...] = ls[...] + ls_p[...]
        along("dp", lambda o: (gw_a.at[rows_at(o, n_z)], gw_z.at[dp]), sem_gw.at[1], gw_z.at[pl.ds(0, dp_size - 1)])
        along("dp", lambda o: (ls_a, ls_z.at[dp]), sem_ls.at[1], ls_z.at[pl.ds(0, dp_size - 1)])
        coming["gw2"] = lambda: (drain(gw_z, sem_gw.at[1, 1]), drain(ls_z, sem_ls.at[1, 1]))

    def gw3():
        got("gw2")
        gw_zs[...] = jnp.sum(gw_z[...], axis=0)
        ls_zs[...] = jnp.sum(ls_z[...], axis=0)
        over_chips(lambda o: (gw_zs.at[rows_at(o, n_h)], gw_h.at[chip]), sem_gw.at[2], gw_h.at[pl.ds(0, chips - 1)])
        over_chips(lambda o: (ls_zs, ls_h.at[chip]), sem_ls.at[2], ls_h.at[pl.ds(0, chips - 1)])
        coming["gw3"] = lambda: (drain(gw_h, sem_gw.at[2, 1]), drain(ls_h, sem_ls.at[2, 1]))

    def gw4():
        got("gw3")
        gw_hs[...] = jnp.sum(gw_h[...], axis=0)
        ls_hs[...] = jnp.sum(ls_h[...], axis=0)
        along("w", lambda o: (gw_hs.at[rows_at(o, n_w)], gw_w.at[w]), sem_gw.at[3], gw_w.at[pl.ds(0, w_size - 1)])
        along("w", lambda o: (ls_hs, ls_w.at[w]), sem_ls.at[3], ls_w.at[pl.ds(0, w_size - 1)])
        coming["gw4"] = lambda: (drain(gw_w, sem_gw.at[3, 1]), drain(ls_w, sem_ls.at[3, 1]))

    def gw5():
        got("gw4")
        gw_ws[...] = jnp.sum(gw_w[...], axis=0)
        loss_out[...] = jnp.sum(ls_w[...], keepdims=True).reshape(1, 1) / total_points
        along("w", lambda o: (gw_ws, gw_w2.at[rows_at(w, n_w)]), sem_gw.at[4], gw_w2.at[pl.ds(0, (w_size - 1) * n_w)])
        coming["gw5"] = lambda: drain(gw_w2, sem_gw.at[4, 1])

    def gw6():
        got("gw5")
        over_chips(lambda o: (gw_w2, gw_h2.at[rows_at(chip, n_h)]), sem_gw.at[5], gw_h2.at[pl.ds(0, (chips - 1) * n_h)])
        coming["gw6"] = lambda: drain(gw_h2, sem_gw.at[5, 1])

    def gw7():
        got("gw6")
        along("dp", lambda o: (gw_h2, gw_f.at[rows_at(dp, n_z)]), sem_gw.at[6], gw_f.at[pl.ds(0, (dp_size - 1) * n_z)])
        coming["gw7"] = lambda: drain(gw_f, sem_gw.at[6, 1])

    def gw8():
        got("gw7")
        twin(gw_f, gw_o, sem_gw.at[7])
        coming["gw8"] = lambda: drain(gw_o, sem_gw.at[7, 1])

    def end():
        got("gw8")
        for c, halves in enumerate(((gw_f, gw_o), (gw_o, gw_f))):
            @pl.when(core == c)
            def _():
                first, second = halves
                for i, (src, dst) in enumerate(((first.at[:nc], gin_out.at[:, :nc]), (first.at[nc:], gin_out.at[:, nc:]), (second, gout_out))):
                    pltpu.make_async_copy(src, dst, sem_fin.at[i]).start()
        for i, dst in enumerate((gin_out.at[:, :nc], gin_out.at[:, nc:], gout_out)):
            unsent.setdefault(None, []).append(lambda dst=dst, i=i: drain(dst, sem_fin.at[i]))

    gs_sum, gs_b = (gs_sum0, gs_sum1), (gs_b0, gs_b1)
    first_rows = (0, gs_sum0.shape[1])
    axes = (("w", "dp"), ("dp", "w"))
    place = {"w": (w, w_size), "dp": (dp, dp_size)}

    def next_to(axis, k):
        index, size = place[axis]
        return (index + k + size) % size

    def add_sample(b):
        got(("az", b))
        got(("dz", b))

        def body(n, _):
            d = dall[n, b]
            half = d.shape[0] // 2
            both = jnp.concatenate([d, jnp.concatenate([d[half:], -d[:half]], axis=0)], axis=1)
            gs_acc[...] += dot(aall[n, b], both, TN)
            return 0

        lax.fori_loop(0, dp_size, body, 0)

    def gsa():
        gs_acc[...] = jnp.zeros_like(gs_acc)
        add_sample(GS_FIRST[0])

    def gsb():
        add_sample(GS_FIRST[1])

    def gs1():
        add_sample(GS_FIRST[2])
        for q in range(2):
            rows_q = pl.ds(first_rows[q], gs_sum[q].shape[1])
            for p in range(2):
                gs_sum[q][p] = gs_acc[rows_q, p * LANES:(p + 1) * LANES]

    def once(key):
        if key in coming:
            got(key)

    def sent_later(ref, sem):
        unsent.setdefault(None, []).append(lambda: drain(ref, sem))

    def gs2(q):
        keep(gs_sum[q], gs_b[q].at[0], sem_gs.at[q, 0])
        for slot, k in ((1, 1), (3, -1)):
            push(gs_sum[q], gs_b[q].at[slot], sem_gs.at[q, slot], {axes[q][0]: next_to(axes[q][0], k)})
            sent_later(gs_sum[q], sem_gs.at[q, slot, 0])
        coming.update({("gs", q, k): lambda k=k: drain(gs_b[q].at[k], sem_gs.at[q, k, 1]) for k in (0, 1, 3)})

    def gs6(q):
        for slot, p, k, i in ((1, 0, 1, 2), (3, 1, -1, 4)):
            once(("gs", q, slot))
            push(gs_b[q].at[slot, p], gs_b[q].at[2, p], sem_gs.at[q, i], {axes[q][0]: next_to(axes[q][0], k)})
            sent_later(gs_b[q].at[2, p], sem_gs.at[q, i, 0])
        coming["gs", q, 2] = lambda: (drain(gs_b[q].at[2, 0], sem_gs.at[q, 2, 1]), drain(gs_b[q].at[2, 1], sem_gs.at[q, 4, 1]))

    def block_at(q, k, shift):
        at = {axes[q][0]: next_to(axes[q][0], -k), axes[q][1]: next_to(axes[q][1], shift)}
        return gs_out.at[:, l_own * at["w"] + at["dp"] // 2, pl.ds(first_rows[q], gs_sum[q].shape[1]), lanes_at(at["dp"] % 2)]

    def gs3(q, k):
        once(("gs", q, k))
        mine = block_at(q, k, 0)
        pltpu.make_async_copy(gs_b[q].at[k], mine, sem_gf.at[q, 3, k, 0]).start()
        for way, shift in ((0, 1), (1, -1)):
            push(gs_b[q].at[k], mine, sem_gf.at[q, way, k], {axes[q][1]: next_to(axes[q][1], shift)})

    def gs4(q, k):
        way, shift = (0, 1) if k < 2 else (1, -1)
        drain(gs_b[q].at[k], sem_gf.at[q, way, k, 1])
        block = block_at(q, k, -shift)
        push(block, block, sem_gf.at[q, 2, k], {axes[q][1]: next_to(axes[q][1], shift)})

    def gs5(q, k):
        drain(gs_b[q].at[k], sem_gf.at[q, 1 if k < 2 else 0, k, 1])
        drain(gs_b[q].at[k], sem_gf.at[q, 2, k, 1])
        for i in range(4):
            drain(gs_b[q].at[k], sem_gf.at[q, i, k, 0])

    scope = dict(locals())
    scope["pk"] = pk_
    for name in ORDER.split():
        call = name.rstrip("0123456789") or name
        if name in scope:
            scope[name]()
        elif name[:3] in scope:
            scope[name[:3]](*map(int, name[3:]))
        else:
            scope[call](*map(int, name[len(call):]))
    assert not coming
    settle()


def hand_on_kernel(*refs):
    n = len(refs) // 2
    pairs = []
    for src, dst in zip(refs[:n], refs[n:2 * n]):
        lead = [()] if len(src.shape) == 2 else [(i,) for i in range(src.shape[0])]
        pairs += [(src.at[i], dst.at[i]) if i else (src, dst) for i in lead]
    copies = [pltpu.make_async_copy(src, dst, refs[2 * n].at[i]) for i, (src, dst) in enumerate(pairs)]
    for c in copies:
        c.start()
    for c in copies:
        c.wait()


def hand_on(arrays):
    return pl.pallas_call(
        hand_on_kernel, name="hand_on",
        out_shape=[jax.ShapeDtypeStruct(a.shape, F32) for a in arrays],
        in_specs=[pl.BlockSpec(memory_space=pltpu.VMEM)] * len(arrays), out_specs=[pl.BlockSpec(memory_space=pl.ANY)] * len(arrays),
        scratch_shapes=[pltpu.SemaphoreType.DMA((32,))],
        compiler_params=pltpu.CompilerParams(vmem_limit_bytes=12 * 1024 * 1024),
    )(*[pltpu.with_memory_space_constraint(a, pltpu.VMEM) for a in arrays])


def solution(mesh):
    dp_size, w_size, h_size = mesh.shape["dp"], mesh.shape["w"], mesh.shape["h"]

    def local_step(field, target, lat_weight, leg_fwd, leg_inv, spec_w, w_in, w_out):
        nb, nc, nt, npl = field.shape
        nlon = npl * w_size
        ntp = nt // 2
        nm = leg_fwd.shape[0] * w_size
        ndev = h_size * w_size
        nlat = nt * h_size
        nl = leg_fwd.shape[1]
        lo = nl // ndev
        assert nm == 8 * h_size and nc == w_size * LANES // 2 and h_size == 2 * w_size and 2 * lo == dp_size and 2 * nl == LANES
        total_points = nb * dp_size * nc * nlat * nlon
        any_spec = pl.BlockSpec(memory_space=pl.ANY)
        vmem_spec = pl.BlockSpec(memory_space=pltpu.VMEM)
        sds = lambda *s: jax.ShapeDtypeStruct(s, F32)
        vm = lambda *s: pltpu.VMEM(s, F32)
        dma = lambda *s: pltpu.SemaphoreType.DMA(s)
        n_rows = 2 * nc + w_out.shape[0]
        n_z, n_h, n_w = n_rows // dp_size, n_rows // dp_size // h_size, n_rows // dp_size // h_size // w_size
        home = vm(nb, nt, npl, nc)
        woven = vm(nb, w_size, ntp, npl, LANES)
        order = vm(nb, 16 * nlat // 2, LANES)
        degree = vm(nb, 8 * nl, LANES)
        owner = vm(nb, h_size, 8 * lo, w_size * LANES)
        saved = vm(nb, lo, 2 * nm, nc)
        cut = GS_ROWS
        n_pairs = leg_fwd.shape[0] // 2
        n_c = n_rows // 2
        n_z, n_h, n_w = n_c // dp_size, n_c // dp_size // w_size, n_c // dp_size // w_size // w_size
        results = pl.pallas_call(
            functools.partial(block_kernel, (dp_size, h_size, w_size), total_points),
            name="block",
            out_shape=[vm(nb, nt, npl, nc), vm(2, lo * w_size, nc, nc), vm(nc, 2 * nc), vm(2 * nc, nc), sds(1, 1)],
            in_specs=[any_spec] * 9,
            out_specs=[vmem_spec] * 5,
            scratch_shapes=[
                vm(*leg_fwd.shape[:1], nt, nl), vm(*leg_fwd.shape[:1], nt, nl), pltpu.SMEM((nt,), F32), pltpu.VMEM(w_in.shape, BF16),
                pltpu.VMEM(w_out.shape, BF16), vm(2 * nm, nlon), vm(2 * nm, nlon), vm(nlon, 2 * nm), vm(nlon, 2 * nm),
                home, home, woven, vm(nb, ntp, nlon, LANES), woven, woven,
                vm(nb, h_size, 16 * ntp, LANES), order, order, order, vm(nb, h_size, 16 * ntp, LANES), vm(nb, h_size, 16 * ntp, LANES),
                degree, owner, owner, vm(nb, h_size, w_size, 8 * lo, LANES), degree, degree, saved, saved,
                vm(dp_size, nb, 2 * nm, nc), vm(dp_size, nb, 2 * nm, LANES),
                vm(8, nc), vm(h_size, 8, nc), vm(8, nc), vm(w_size, 8, nc),
                vm(2, n_pairs, nt, 2 * nl), vm(2, w_size, n_pairs, nt, 2 * nl), vm(2, 4, nlat, 2 * nl),
                vm(8, nl, nlat), vm(8, nl, nlat), vm(8, nlat, nl), vm(8, nlat, nl),
                vm(2, lo, nc, nc),
                vm(n_rows, nc), vm(n_c, nc), vm(n_c, nc), vm(dp_size, n_z, nc), vm(n_z, nc), vm(w_size, n_h, nc), vm(n_h, nc),
                vm(w_size, n_w, nc), vm(n_w, nc), vm(n_h, nc), vm(n_z, nc), vm(n_c, nc), vm(n_c, nc),
                vm(8, nc), vm(8, nc), vm(8, nc), vm(dp_size, 8, nc), vm(8, nc), vm(w_size, 8, nc), vm(8, nc), vm(w_size, 8, nc),
                vm(nc, nc), vm(2, cut, LANES), vm(2, nc - cut, LANES), vm(4, 2, cut, LANES), vm(4, 2, nc - cut, LANES),
            ] + [dma(nb, PARTS, 2)] * 8 + [dma(nb, 2)] * 6 + [dma(nb, 2), dma(4, 2), dma(5, 2), dma(1), dma(8, 2), dma(4, 2),
                 dma(2, 5, 2), dma(2, 4, 4, 2), dma(3), dma(6)],
            compiler_params=pltpu.CompilerParams(collective_id=0, has_side_effects=True, vmem_limit_bytes=54 * 1024 * 1024),
        )(field.transpose(0, 2, 3, 1), target.transpose(0, 2, 3, 1), leg_fwd.transpose(0, 2, 1), leg_inv.transpose(0, 2, 1),
          spec_w, lat_weight, w_in, w_out, jnp.asarray(dft_table(nlon, nm, h_size)))
        d_x, g_spec, g_in, g_out = hand_on(results[:4])
        loss = results[4]
        return loss.reshape(()), d_x.transpose(0, 3, 1, 2), g_spec, g_in, g_out

    grid_spec = P("dp", None, "h", "w")
    table_spec = P("w", None, "h")
    kernel_spec = P(None, "h", None, None)
    return jax.shard_map(local_step, mesh=mesh, in_specs=(grid_spec, grid_spec, P("h"), table_spec, table_spec, P(), P(), P()), out_specs=(P(), grid_spec, kernel_spec, P(), P()), check_vma=False)
```

```python
import functools
import jax
import jax.numpy as jnp
import numpy as np
from jax import lax
from jax.experimental import pallas as pl
from jax.experimental.pallas import tpu as pltpu
from jax.sharding import PartitionSpec as P

NORM_EPS = 1e-5
PRECISE = lax.Precision.HIGHEST
MESH = pl.DeviceIdType.MESH
F32 = jnp.float32
BF16 = jnp.bfloat16
GELU_C = float(np.sqrt(2.0 / np.pi))
GELU_A = 0.044715
LANES = 128
NN = (((1,), (0,)), ((), ()))
NT = (((1,), (1,)), ((), ()))
TN = (((0,), (0,)), ((), ()))


def dot(a, b, dims=NN):
    return lax.dot_general(a, b, dims, precision=PRECISE, preferred_element_type=F32)


def bdot(a, b, dims=NN):
    return lax.dot_general(a, b, dims, preferred_element_type=F32)


def dft_table(lon_count, num_modes, h_size):
    modes, lons = np.arange(num_modes), np.arange(lon_count)
    angle = 2.0 * np.pi * ((modes[:, None] * lons[None, :]) % lon_count) / lon_count
    table = np.stack([np.cos(angle), -np.sin(angle)], 0) * lon_count ** -0.5
    table = table.reshape(2, h_size, num_modes // h_size, lon_count).transpose(1, 0, 2, 3)
    return table.reshape(2 * num_modes, lon_count).astype(np.float32)


def drain(ref, sem):
    pltpu.make_async_copy(ref, ref, sem).wait()


def rows_at(i, n):
    return pl.ds(pl.multiple_of(i * n, n), n)


def lanes_at(i):
    return pl.ds(pl.multiple_of(i * LANES, LANES), LANES)


def push(src, dst, sems, device):
    pltpu.make_async_remote_copy(src_ref=src, dst_ref=dst, send_sem=sems.at[0], recv_sem=sems.at[1],
                                 device_id=device, device_id_type=MESH).start()


def keep(src, dst, sems):
    pltpu.make_async_copy(src, dst, sems.at[1]).start()


def flip(v):
    return pltpu.roll(v, LANES // 2, 1)


def low(v):
    return lax.broadcasted_iota(jnp.int32, v.shape, 1) < LANES // 2


def weave(a, b):
    return jnp.where(low(a), a, flip(b)), jnp.where(low(a), flip(a), b)


def weave_wide(tiles):
    pairs = [weave(tiles[j], tiles[j + 1]) for j in range(0, len(tiles), 2)]
    return jnp.concatenate([p[0] for p in pairs], axis=1), jnp.concatenate([p[1] for p in pairs], axis=1)


def weave_tiles(a, b):
    out = []
    for j in range(0, a.shape[1], LANES):
        out.extend(weave(a[:, j:j + LANES], b[:, j:j + LANES]))
    return out


PARTS = 4
GS_ROWS = 176
GS_FIRST = (0, 1, 2)
ORDER = " ".join((
    'go', 'pk0', 'sX01', 'pk2', 'pk1', 'sX03', 'tb1', 'sX00', 'sX02', 'sX12',
    'fd01', 'fd03', 'sX10', 'tb2', 'fd00', 'fd02', 'tb4', 'st1', 'sX11', 'sX13',
    'tb3', 'fd12', 'fl0', 'st2', 'fd10', 'tb5', 'sX21', 'fd13', 'fd11', 'sX20',
    'fo0', 'fl1', 'sX23', 'sX22', 'fd20', 'fu0', 'fo1', 'fd23', 'fd21', 'fi00',
    'sY00', 'fi01', 'sY01', 'fi02', 'fd22', 'fi03', 'sY02', 'sY03', 'pw00', 'fu1',
    'sD00', 'fl2', 'pw02', 'sD02', 'pw01', 'pw03', 'sD03', 'sD01', 'fi12', 'bd02',
    'fi10', 'sY12', 'fi13', 'bd00', 'fo2', 'bd01', 'sY10', 'bd03', 'fi11', 'sY11',
    'pw12', 'sY13', 'fu2', 'pw10', 'sD12', 'bl0', 'sD10', 'pw11', 'fi21', 'fi20',
    'sY20', 'sY21', 'pw13', 'fi22', 'sD11', 'fi23', 'bd10', 'sD13', 'bo0', 'sY22',
    'pw21', 'bd12', 'sY23', 'sD21', 'bd13', 'pw20', 'sD20', 'bd11', 'bu0', 'pw22',
    'pw23', 'sD22', 'sD23', 'gw1', 'gsa', 'bd21', 'gw2', 'bl1', 'bi03', 'bi02',
    'bd22', 'sN02', 'bi01', 'sN01', 'bd20', 'bd23', 'gw3', 'bo1', 'bl2', 'bi00',
    'sN03', 'gw4', 'sN00', 'bu1', 'bo2', 'gw5', 'pj1', 'bi10', 'sN10', 'gsb',
    'bi11', 'sN11', 'pj2', 'gs1', 'gs20', 'gs21', 'bi13', 'sN13', 'gs300', 'gw6',
    'bu2', 'gs310', 'gs61', 'bi12', 'sN12', 'gs303', 'gw7', 'gs313', 'fn11', 'gs60',
    'bi20', 'gs311', 'fn12', 'bi23', 'fn10', 'fn02', 'gs312', 'gs403', 'gs301', 'gs413',
    'gs410', 'sN23', 'sN20', 'gs302', 'gs400', 'bi22', 'fn13', 'bi21', 'gw8', 'sN21',
    'sN22', 'fn00', 'gs503', 'gs412', 'gs401', 'fn20', 'gs402', 'fn01', 'gs411', 'end',
    'gs502', 'gs500', 'gs510', 'fn23', 'fn03', 'gs501', 'fn22', 'gs512', 'fn21', 'gs513',
    'gs511',
))


def block_kernel(sizes, total_points,
                 x, tgt, leg_p_in, leg_q_in, spec_w, lat_in, w1_in, w2_in, f_in,
                 dout, gs_out, gin_out, gout_out, loss_out,
                 leg_p, leg_q, lat, w1, w2, f_tab, g_tab, ft_tab, gt_tab,
                 xh, th, pk, rows, yrow, hy,
                 xs, sr, dsr, ys, yr, dyr, als, ar, dar, bs, br, dbr, asave, dsave, aall, dall,
                 st_s, st_h, st_m, st_w, tab_s, tab_w, tab, down_p, down_q, up_p, up_q, ker,
                 gw, gw_p, gw_a, gw_z, gw_zs, gw_h, gw_hs, gw_w, gw_ws, gw_w2, gw_h2, gw_f, gw_o,
                 ls, ls_p, ls_a, ls_z, ls_zs, ls_h, ls_hs, ls_w, gs_acc, gs_sum0, gs_sum1, gs_b0, gs_b1,
                 sem_x, sem_y, sem_d, sem_n, sem_s, sem_ds, sem_u, sem_du, sem_a, sem_da, sem_b, sem_db, sem_az, sem_dz,
                 sem_in, sem_st, sem_tab, sem_k, sem_gw, sem_ls, sem_gs, sem_gf, sem_fin, sem_small):
    dp_size, h_size, w_size = sizes
    dp, h, w = lax.axis_index("dp"), lax.axis_index("h"), lax.axis_index("w")
    ndev = h_size * w_size
    me = h * w_size + w
    nb, nt, npl, nc = x.shape
    ntp = nt // 2
    part = ntp // PARTS
    nlon = npl * w_size
    nlat = nt * h_size
    nl = als.shape[1] // 8
    l_own = nl // ndev
    piece = 8 * l_own
    unsent, coming = {}, {}

    def got(key):
        coming.pop(key)()

    def peer(k):
        return (h + k // w_size) % h_size, (w + k % w_size) % w_size

    barrier = pltpu.get_barrier_semaphore()

    def meet(k, _):
        h2, w2_ = peer(k)
        pl.semaphore_signal(barrier, inc=1, device_id={"h": h2, "w": w2_}, device_id_type=MESH)
        return 0

    def meet_dp(k, _):
        pl.semaphore_signal(barrier, inc=1, device_id={"dp": (dp + k) % dp_size}, device_id_type=MESH)
        return 0

    lax.fori_loop(1, ndev, meet, 0)
    lax.fori_loop(1, dp_size, meet_dp, 0)
    loads = [pltpu.make_async_copy(x.at[b], xh.at[b], sem_in.at[b, 0]) for b in range(nb)]
    load_t = [pltpu.make_async_copy(tgt.at[b], th.at[b], sem_in.at[b, 1]) for b in range(nb)]
    load_k = pltpu.make_async_copy(spec_w.at[:, pl.ds(me * l_own, l_own)], ker, sem_k.at[0])
    small = [pltpu.make_async_copy(src, dst, sem_small.at[i]) for i, (src, dst) in enumerate((
        (leg_p_in, leg_p), (leg_q_in, leg_q), (f_in, f_tab), (lat_in, lat), (w1_in, w1), (w2_in, w2)))]
    for c in loads + small[:3] + [load_k] + load_t + small[3:]:
        c.start()
    coming["k"] = load_k.wait
    coming["small"] = lambda: [c.wait() for c in small[3:]]
    coming.update({("t", b): load_t[b].wait for b in range(nb)})
    for ref in (ar, br, dar, dbr, st_s, gw, ls):
        ref[...] = jnp.zeros_like(ref)

    def settle(*keys):
        for key in keys or list(unsent):
            for wait in unsent.pop(key, []):
                wait()

    def along(axis, refs, sems, sent, key=None):
        size, index = {"dp": (dp_size, dp), "h": (h_size, h), "w": (w_size, w)}[axis]
        src, dst = refs(index)
        keep(src, dst, sems)

        def body(k, _):
            other = (index + k) % size
            src, dst = refs(other)
            push(src, dst, sems, {axis: other})
            return 0

        lax.fori_loop(1, size, body, 0)
        unsent.setdefault(key, []).append(lambda: drain(sent, sems.at[0]))

    def some(refs, sems, low_h, high_h, count, counts, key):
        src, dst = refs(h, w)
        keep(src, dst, sems)

        def one(h2, k):
            w2_ = (w + k) % w_size
            src, dst = refs(h2, w2_)
            push(src, dst, sems, {"h": h2, "w": w2_})

        for k in range(1, w_size):
            one(h, k)

        def body(h2, _):
            for k in range(w_size):
                one(h2, k)
            return 0

        lax.fori_loop(low_h, high_h, body, 0)
        unsent.setdefault(key, []).append(lambda: take(sems.at[0], count - 1, [n - 1 for n in counts]))

    def take(sem, count, counts):
        for n in counts:
            @pl.when(count == n)
            def _():
                drain(als.at[0, pl.ds(0, n * piece)], sem)

    n_orders, n_owners = (h + 1) * w_size, (h_size - h) * w_size
    counts = [w_size * n for n in range(1, h_size + 1)]
    pairs = lambda k: pl.ds(k * part, part)

    def at_rows(i, k):
        return pl.ds(pl.multiple_of(i * 16 * ntp + k * 16 * part, 16 * part), 16 * part)

    def send_home_rows(b, k, sem, name):
        along("w", lambda o: (pk.at[b, o, pairs(k)], rows.at[b, pairs(k), rows_at(w, npl)]), sem.at[b, k],
              pk.at[b, pl.ds(0, w_size - 1), pairs(k)], ("pk", b, k))
        coming[name, b, k] = lambda: drain(rows.at[b, pairs(k)], sem.at[b, k, 1])

    def send_rows_home(b, k, sem, name):
        along("w", lambda o: (yrow.at[b, o, pairs(k)], hy.at[b, w, pairs(k)]), sem.at[b, k],
              yrow.at[b, pl.ds(0, w_size - 1), pairs(k)], ("yrow", b, k))
        coming[name, b, k] = lambda: drain(hy.at[b, :, pairs(k)], sem.at[b, k, 1])

    def send_orders(b, k, dst, sem, name):
        along("h", lambda o: (xs.at[b, o, at_rows(0, k)], dst.at[b, at_rows(h, k)]), sem.at[b, k],
              xs.at[b, pl.ds(0, h_size - 1), at_rows(0, k)], ("xs", b, k))
        coming[name, b, k] = lambda: drain(xs.at[b, :, at_rows(0, k)], sem.at[b, k, 1])

    def send_lats(b, dst, sem, name):
        def one(k, _):
            keep(ys.at[b, at_rows(h, k)], dst.at[b, h, at_rows(0, k)], sem.at[b, k])

            def body(j, _):
                o = (h + j) % h_size
                push(ys.at[b, at_rows(o, k)], dst.at[b, h, at_rows(0, k)], sem.at[b, k], {"h": o})
                return 0

            return lax.fori_loop(1, h_size, body, 0)

        lax.fori_loop(0, PARTS, one, 0)
        for k in range(PARTS):
            unsent.setdefault(("ys", b), []).append(lambda k=k: drain(xs.at[b, pl.ds(0, h_size - 1), at_rows(0, k)], sem.at[b, k, 0]))
            coming[name, b, k] = lambda k=k: drain(dst.at[b, :, at_rows(0, k)], sem.at[b, k, 1])

    def send_owner(b, dst, sem, name):
        some(lambda h2, w2_: (als.at[b, rows_at(h2 * w_size + w2_, piece)], dst.at[b, h, :, lanes_at(w)]), sem.at[b],
             h + 1, h_size, n_owners, counts, ("als", b))
        coming[name, b] = lambda: take(sem.at[b, 1], n_orders, counts)

    def send_back(b, dst, sem, name):
        some(lambda h2, w2_: (bs.at[b, h2, w2_], dst.at[b, rows_at(me, piece)]), sem.at[b],
             0, h, n_orders, counts, ("bs", b))
        coming[name, b] = lambda: take(sem.at[b, 1], n_owners, counts)

    def dft(b, k, table):
        settle(("xs", b, k))

        def body(n, _):
            i = 2 * n
            both = jnp.concatenate([rows[b, i], rows[b, i + 1]], axis=1)
            out = dot(table[...], both).reshape(h_size, 16, 2 * LANES)
            xs[b, :, rows_at(i, 16), :] = out[:, :, :LANES]
            xs[b, :, rows_at(i + 1, 16), :] = out[:, :, LANES:]
            return 0

        lax.fori_loop(k * part // 2, (k + 1) * part // 2, body, 0)

    def idft(b, k, table, src):
        settle(("yrow", b, k))

        def body(n, _):
            i = 2 * n
            both = jnp.concatenate([src[b, :, rows_at(i + j, 16), :].reshape(-1, LANES) for j in range(2)], axis=1)
            out = dot(table[...], both)
            for j in range(2):
                yrow[b, :, i + j] = out[:, j * LANES:(j + 1) * LANES].reshape(w_size, npl, LANES)
            return 0

        lax.fori_loop(k * part // 2, (k + 1) * part // 2, body, 0)

    def level(v, here):
        mean = jnp.mean(v, axis=0, keepdims=True)
        mean = 0.5 * (mean + flip(mean))
        return v - jnp.where(jnp.logical_and(h == 0, here), mean, 0.0)

    def orders(body):
        def four(n, _):
            for i in range(4):
                body(4 * n + i, n == 0 if i == 0 else None)
            return 0

        lax.fori_loop(0, 2, four, 0)

    def leg_down(b, table, src, fix):
        settle(("als", b))

        def one(m, here):
            re, im = (src[b, pl.ds(ri * 8 + m, ntp * h_size, stride=16), :] for ri in range(2))
            if fix and here is not None:
                re = level(re, here)
            als[b, pl.ds(m, nl, stride=8), :] = dot(table[m], jnp.concatenate(weave(re, im), axis=0))

        orders(one)

    def leg_up(b, table, src, fix):
        settle(("ys", b))

        def one(m, here):
            out = dot(table[m], src[b, pl.ds(m, nl, stride=8), :])
            re, im = weave(out[:nlat // 2], out[nlat // 2:])
            if fix and here is not None:
                re = level(re, here)
            ys[b, pl.ds(m, ntp * h_size, stride=16), :] = re
            ys[b, pl.ds(8 + m, ntp * h_size, stride=16), :] = im

        orders(one)

    def owned(b, l, src):
        tiles = [src[b, :, rows_at(l, 8), j * LANES:(j + 1) * LANES].reshape(-1, LANES) for j in range(w_size)]
        return weave_wide(tiles)

    def put_back(b, l, re, im):
        for j, tile in enumerate(weave_tiles(re, im)):
            bs[b, :, j, rows_at(l, 8), :] = tile.reshape(h_size, 8, LANES)

    def put_rows(b, i, v0, v1):
        for j, tile in enumerate(weave_tiles(v0, v1)):
            pk[b, j, i] = tile

    def get_rows(b, i):
        return weave_wide([hy[b, j, i] for j in range(w_size)])

    count = nt * npl
    n_tab = tab_s.shape[1] // dp_size

    def combine(stats, n):
        mean = jnp.mean(stats, axis=0)
        dev = stats - mean[None]
        dev2 = jnp.sum(dev * dev, axis=0)
        m2 = jnp.sum(stats, axis=0)
        return [(mean[2 * b:2 * b + 1], m2[2 * b + 1:2 * b + 2] + n * dev2[2 * b:2 * b + 1]) for b in range(nb)]

    sums = {}

    def pk_(b):
        loads[b].wait()

        def body(i, total):
            v0, v1 = xh[b, i], xh[b, i + ntp]
            put_rows(b, i, v0, v1)
            return total + jnp.sum(v0 + v1, axis=0, keepdims=True)

        sums[b] = lax.fori_loop(0, ntp, body, jnp.zeros((1, nc), F32))

    def go():
        for c in small[:3]:
            c.wait()
        for a, leg in enumerate((leg_p, leg_q)):
            for m in range(leg.shape[0]):
                tab_s[a, m // 2, :, m % 2 * nl:(m % 2 + 1) * nl] = leg[m]
        pl.semaphore_wait(barrier, ndev - 1 + dp_size - 1)
        along("w", lambda o: (tab_s.at[:, rows_at(dp, n_tab)], tab_w.at[:, w, rows_at(dp, n_tab)]), sem_tab.at[0],
              tab_w.at[:, pl.ds(0, w_size - 1), pl.ds(0, n_tab)])
        coming["tab"] = lambda: drain(tab_w.at[:, :, pl.ds(0, n_tab)], sem_tab.at[0, 1])

    def st1():
        for b in range(nb):
            mean = sums[b] / count

            def body(t, total, b=b, mean=mean):
                d = xh[b, t] - mean
                return total + jnp.sum(d * d, axis=0, keepdims=True)

            st_s[2 * b:2 * b + 1, :] = mean
            st_s[2 * b + 1:2 * b + 2, :] = lax.fori_loop(0, nt, body, jnp.zeros((1, nc), F32))
        along("w", lambda o: (st_s, st_w.at[w]), sem_st.at[0], st_w.at[pl.ds(0, w_size - 1)], "st")
        coming["st"] = lambda: drain(st_w, sem_st.at[0, 1])
        g_tab[...] = jnp.where(lax.broadcasted_iota(jnp.int32, f_tab.shape, 0) == 0, 1.0, 2.0) * f_tab[...]
        ft_tab[...] = f_tab[...].T
        gt_tab[...] = g_tab[...].T

    def st2():
        got("st")
        st_m[...] = jnp.zeros_like(st_m)
        for b, (mean, m2) in enumerate(combine(st_w[...], count)):
            st_m[2 * b:2 * b + 1, :] = mean
            st_m[2 * b + 1:2 * b + 2, :] = m2
        along("h", lambda o: (st_m, st_h.at[h]), sem_st.at[1], st_h.at[pl.ds(0, h_size - 1)], "st")
        coming["st2"] = lambda: drain(st_h, sem_st.at[1, 1])

    means, scales = [], []

    def st3():
        got("st2")
        for mean, m2 in combine(st_h[...], count * w_size):
            means.append(mean)
            scales.append(lax.rsqrt(m2 / (count * ndev) + NORM_EPS))

    def tb1():
        got("tab")
        for a in range(2):
            share = tab_w.at[a, :, rows_at(dp, n_tab)]
            for k in range(1, dp_size):
                push(share, share, sem_tab.at[1 + a], {"dp": (dp + k) % dp_size})
            others = tab_w.at[a, :, pl.ds(0, (dp_size - 1) * n_tab)]
            unsent.setdefault(None, []).append(lambda a=a, others=others: drain(others, sem_tab.at[1 + a, 0]))
            coming["tab1", a] = lambda a=a, others=others: drain(others, sem_tab.at[1 + a, 1])

    def table_out(a):
        got(("tab1", a))
        along("h", lambda o: (tab_w.at[a, o // 2, rows_at(o % 2, 4)], tab.at[a, :, rows_at(h, nt)]), sem_tab.at[3 + a],
              tab.at[a, :, pl.ds(0, nlat - nt)])
        coming["tab2", a] = lambda: drain(tab.at[a], sem_tab.at[3 + a, 1])

    def table_in(a, down, up):
        got(("tab2", a))

        def body(n, _):
            both = tab[a, n].reshape(h_size, 2, ntp, 2 * nl)
            both = jnp.concatenate([both[:, j].reshape(-1, 2 * nl) for j in range(2)], axis=0)
            for j in range(2):
                t = both[:, j * nl:(j + 1) * nl]
                up[2 * n + j] = t
                down[2 * n + j] = t.T
            return 0

        lax.fori_loop(0, tab.shape[1], body, 0)

    def tb2():
        table_out(0)

    def tb3():
        table_in(0, down_p, up_p)

    def tb4():
        table_out(1)

    def tb5():
        table_in(1, down_q, up_q)

    def sX(b, k):
        send_home_rows(b, k, sem_x, "x")

    def fd(b, k):
        got(("x", b, k))
        dft(b, k, f_tab)
        send_orders(b, k, sr, sem_s, "s")

    def fl(b):
        for k in range(PARTS):
            got(("s", b, k))
        leg_down(b, down_p, sr, True)
        send_owner(b, ar, sem_a, "a")

    def fo(b):
        if not scales:
            got("k")
            st3()
        got(("a", b))
        settle(("bs", b))

        def one(l, _):
            re, im = owned(b, l, ar)
            a = jnp.concatenate([re, im], axis=0) * scales[b]
            asave[b, l] = a
            n = a.shape[0] // 2
            own, other = dot(a, ker[0, l]), dot(a, ker[1, l])
            put_back(b, l, own[:n] - other[n:], own[n:] + other[:n])
            return 0

        lax.fori_loop(0, l_own, one, 0)
        send_back(b, br, sem_b, "b")
        along("dp", lambda o: (asave.at[b, o // 2], aall.at[dp, b]), sem_az.at[b], aall.at[pl.ds(0, dp_size - 1), b])
        coming["az", b] = lambda: drain(aall.at[:, b], sem_az.at[b, 1])

    def fu(b):
        got(("b", b))
        leg_up(b, up_q, br, False)
        send_lats(b, yr, sem_u, "u")

    def fi(b, k):
        got(("u", b, k))
        idft(b, k, gt_tab, yr)

    def sY(b, k):
        send_rows_home(b, k, sem_y, "y")

    def pw(b, k):
        got(("y", b, k))
        if ("t", b) in coming:
            got(("t", b))
        if "small" in coming:
            got("small")
        settle(("pk", b, k))

        def body(n, _):
            lats = [n, n + ntp]
            y = jnp.concatenate(get_rows(b, n), axis=0)
            yb = y.astype(BF16)
            hid = bdot(yb, w1[...])
            th_ = jnp.tanh(GELU_C * (hid + GELU_A * (hid * hid * hid)))
            act = (hid * (0.5 * (1.0 + th_))).astype(BF16)
            resid = y + bdot(act, w2[...])
            parts = []
            for j, t in enumerate(lats):
                r = resid[j * npl:(j + 1) * npl] + xh[b, t] - th[b, t]
                d = lat[t] * r
                ls[...] += jnp.sum((d * r).reshape(-1, 8, nc), axis=0)
                dout[b, t] = d
                parts.append(d)
            d = jnp.concatenate(parts, axis=0)
            db = d.astype(BF16)
            gw[2 * nc:, :] += bdot(act, db, TN)
            slope = 0.5 * (1.0 + th_) + (0.5 * GELU_C) * hid * (1.0 - th_ * th_) * (1.0 + (3.0 * GELU_A) * (hid * hid))
            dh = (bdot(db, w2[...], NT) * slope).astype(BF16)
            gin = bdot(yb, dh, TN)
            gw[:nc, :] += gin[:, :nc]
            gw[nc:2 * nc, :] += gin[:, nc:]
            dy = d + bdot(dh, w1[...], NT)
            put_rows(b, n, dy[:npl], dy[npl:])
            return 0

        lax.fori_loop(k * part, (k + 1) * part, body, 0)

    def sD(b, k):
        send_home_rows(b, k, sem_d, "d")

    def bd(b, k):
        got(("d", b, k))
        dft(b, k, g_tab)
        send_orders(b, k, dsr, sem_ds, "ds")

    def bl(b):
        for k in range(PARTS):
            got(("ds", b, k))
        leg_down(b, down_q, dsr, False)
        send_owner(b, dar, sem_da, "da")

    def bo(b):
        got(("da", b))
        settle(("bs", b), "st")

        def one(l, s2):
            re, im = owned(b, l, dar)
            d = jnp.concatenate([re, im], axis=0)
            dsave[b, l] = d
            n = d.shape[0] // 2
            own, other = dot(d, ker[0, l], NT), dot(d, ker[1, l], NT)
            re, im = own[:n] + other[n:], own[n:] - other[:n]
            put_back(b, l, re, im)
            return s2 + jnp.sum(re * asave[b, l, :n] + im * asave[b, l, n:], axis=0, keepdims=True)

        s2 = lax.fori_loop(0, l_own, one, jnp.zeros((1, nc), F32))
        send_back(b, dbr, sem_db, "db")
        along("dp", lambda o: (dsave.at[b, o // 2, :, lanes_at(o % 2)], dall.at[dp, b]), sem_dz.at[b], dall.at[pl.ds(0, dp_size - 1), b])
        coming["dz", b] = lambda: drain(dall.at[:, b], sem_dz.at[b, 1])
        st_s[b:b + 1, :] = s2

    def bu(b):
        got(("db", b))
        leg_up(b, up_p, dbr, True)
        send_lats(b, dyr, sem_du, "du")

    def bi(b, k):
        got(("du", b, k))
        idft(b, k, ft_tab, dyr)

    def sN(b, k):
        send_rows_home(b, k, sem_n, "n")

    def pj1():
        st_s[nb:, :] = jnp.zeros_like(st_s[nb:, :])
        along("w", lambda o: (st_s, st_w.at[w]), sem_st.at[2], st_w.at[pl.ds(0, w_size - 1)])
        coming["pj"] = lambda: drain(st_w, sem_st.at[2, 1])

    def pj2():
        got("pj")
        st_m[...] = jnp.sum(st_w[...], axis=0)
        along("h", lambda o: (st_m, st_h.at[h]), sem_st.at[3], st_h.at[pl.ds(0, h_size - 1)])
        coming["pj2"] = lambda: drain(st_h, sem_st.at[3, 1])

    proj = []

    def fn(b, k):
        if not proj:
            got("pj2")
            proj.append(jnp.sum(st_h[...], axis=0) / (count * ndev))
        got(("n", b, k))

        def body(i, _):
            for t, dn in zip((i, i + ntp), get_rows(b, i)):
                normed = (xh[b, t] - means[b]) * scales[b]
                dout[b, t] = dout[b, t] + scales[b] * (dn - normed * proj[0][b:b + 1])
            return 0

        lax.fori_loop(k * part, (k + 1) * part, body, 0)

    n_c, n_z, n_h, n_w = gw_a.shape[0], gw_zs.shape[0], gw_hs.shape[0], gw_ws.shape[0]
    chip, core = h // 2, h % 2
    chips = h_size // 2

    def over_chips(refs, sems, sent):
        src, dst = refs(chip)
        keep(src, dst, sems)
        for k in range(1, chips):
            o = (chip + k) % chips
            src, dst = refs(o)
            push(src, dst, sems, {"h": 2 * o + core})
        unsent.setdefault(None, []).append(lambda: drain(sent, sems.at[0]))

    def twin(src, dst, sems):
        push(src, dst, sems, {"h": h + 1 - 2 * core})
        unsent.setdefault(None, []).append(lambda: drain(dst, sems.at[0]))

    def gw1():
        twin(gw.at[rows_at(1 - core, n_c)], gw_p, sem_gw.at[0])
        twin(ls, ls_p, sem_ls.at[0])
        coming["gw1"] = lambda: (drain(gw_p, sem_gw.at[0, 1]), drain(ls_p, sem_ls.at[0, 1]))

    def gw2():
        got("gw1")
        gw_a[...] = gw[rows_at(core, n_c), :] + gw_p[...]
        ls_a[...] = ls[...] + ls_p[...]
        along("dp", lambda o: (gw_a.at[rows_at(o, n_z)], gw_z.at[dp]), sem_gw.at[1], gw_z.at[pl.ds(0, dp_size - 1)])
        along("dp", lambda o: (ls_a, ls_z.at[dp]), sem_ls.at[1], ls_z.at[pl.ds(0, dp_size - 1)])
        coming["gw2"] = lambda: (drain(gw_z, sem_gw.at[1, 1]), drain(ls_z, sem_ls.at[1, 1]))

    def gw3():
        got("gw2")
        gw_zs[...] = jnp.sum(gw_z[...], axis=0)
        ls_zs[...] = jnp.sum(ls_z[...], axis=0)
        over_chips(lambda o: (gw_zs.at[rows_at(o, n_h)], gw_h.at[chip]), sem_gw.at[2], gw_h.at[pl.ds(0, chips - 1)])
        over_chips(lambda o: (ls_zs, ls_h.at[chip]), sem_ls.at[2], ls_h.at[pl.ds(0, chips - 1)])
        coming["gw3"] = lambda: (drain(gw_h, sem_gw.at[2, 1]), drain(ls_h, sem_ls.at[2, 1]))

    def gw4():
        got("gw3")
        gw_hs[...] = jnp.sum(gw_h[...], axis=0)
        ls_hs[...] = jnp.sum(ls_h[...], axis=0)
        along("w", lambda o: (gw_hs.at[rows_at(o, n_w)], gw_w.at[w]), sem_gw.at[3], gw_w.at[pl.ds(0, w_size - 1)])
        along("w", lambda o: (ls_hs, ls_w.at[w]), sem_ls.at[3], ls_w.at[pl.ds(0, w_size - 1)])
        coming["gw4"] = lambda: (drain(gw_w, sem_gw.at[3, 1]), drain(ls_w, sem_ls.at[3, 1]))

    def gw5():
        got("gw4")
        gw_ws[...] = jnp.sum(gw_w[...], axis=0)
        loss_out[...] = jnp.sum(ls_w[...], keepdims=True).reshape(1, 1) / total_points
        along("w", lambda o: (gw_ws, gw_w2.at[rows_at(w, n_w)]), sem_gw.at[4], gw_w2.at[pl.ds(0, (w_size - 1) * n_w)])
        coming["gw5"] = lambda: drain(gw_w2, sem_gw.at[4, 1])

    def gw6():
        got("gw5")
        over_chips(lambda o: (gw_w2, gw_h2.at[rows_at(chip, n_h)]), sem_gw.at[5], gw_h2.at[pl.ds(0, (chips - 1) * n_h)])
        coming["gw6"] = lambda: drain(gw_h2, sem_gw.at[5, 1])

    def gw7():
        got("gw6")
        along("dp", lambda o: (gw_h2, gw_f.at[rows_at(dp, n_z)]), sem_gw.at[6], gw_f.at[pl.ds(0, (dp_size - 1) * n_z)])
        coming["gw7"] = lambda: drain(gw_f, sem_gw.at[6, 1])

    def gw8():
        got("gw7")
        twin(gw_f, gw_o, sem_gw.at[7])
        coming["gw8"] = lambda: drain(gw_o, sem_gw.at[7, 1])

    def end():
        got("gw8")
        for c, halves in enumerate(((gw_f, gw_o), (gw_o, gw_f))):
            @pl.when(core == c)
            def _():
                first, second = halves
                for i, (src, dst) in enumerate(((first.at[:nc], gin_out.at[:, :nc]), (first.at[nc:], gin_out.at[:, nc:]), (second, gout_out))):
                    pltpu.make_async_copy(src, dst, sem_fin.at[i]).start()
        for i, dst in enumerate((gin_out.at[:, :nc], gin_out.at[:, nc:], gout_out)):
            unsent.setdefault(None, []).append(lambda dst=dst, i=i: drain(dst, sem_fin.at[i]))

    gs_sum, gs_b = (gs_sum0, gs_sum1), (gs_b0, gs_b1)
    first_rows = (0, gs_sum0.shape[1])
    axes = (("w", "dp"), ("dp", "w"))
    place = {"w": (w, w_size), "dp": (dp, dp_size)}

    def next_to(axis, k):
        index, size = place[axis]
        return (index + k + size) % size

    def add_sample(b):
        got(("az", b))
        got(("dz", b))

        def body(n, _):
            d = dall[n, b]
            half = d.shape[0] // 2
            both = jnp.concatenate([d, jnp.concatenate([d[half:], -d[:half]], axis=0)], axis=1)
            gs_acc[...] += dot(aall[n, b], both, TN)
            return 0

        lax.fori_loop(0, dp_size, body, 0)

    def gsa():
        gs_acc[...] = jnp.zeros_like(gs_acc)
        add_sample(GS_FIRST[0])

    def gsb():
        add_sample(GS_FIRST[1])

    def gs1():
        add_sample(GS_FIRST[2])
        for q in range(2):
            rows_q = pl.ds(first_rows[q], gs_sum[q].shape[1])
            for p in range(2):
                gs_sum[q][p] = gs_acc[rows_q, p * LANES:(p + 1) * LANES]

    def once(key):
        if key in coming:
            got(key)

    def sent_later(ref, sem):
        unsent.setdefault(None, []).append(lambda: drain(ref, sem))

    def gs2(q):
        keep(gs_sum[q], gs_b[q].at[0], sem_gs.at[q, 0])
        for slot, k in ((1, 1), (3, -1)):
            push(gs_sum[q], gs_b[q].at[slot], sem_gs.at[q, slot], {axes[q][0]: next_to(axes[q][0], k)})
            sent_later(gs_sum[q], sem_gs.at[q, slot, 0])
        coming.update({("gs", q, k): lambda k=k: drain(gs_b[q].at[k], sem_gs.at[q, k, 1]) for k in (0, 1, 3)})

    def gs6(q):
        for slot, p, k, i in ((1, 0, 1, 2), (3, 1, -1, 4)):
            once(("gs", q, slot))
            push(gs_b[q].at[slot, p], gs_b[q].at[2, p], sem_gs.at[q, i], {axes[q][0]: next_to(axes[q][0], k)})
            sent_later(gs_b[q].at[2, p], sem_gs.at[q, i, 0])
        coming["gs", q, 2] = lambda: (drain(gs_b[q].at[2, 0], sem_gs.at[q, 2, 1]), drain(gs_b[q].at[2, 1], sem_gs.at[q, 4, 1]))

    def block_at(q, k, shift):
        at = {axes[q][0]: next_to(axes[q][0], -k), axes[q][1]: next_to(axes[q][1], shift)}
        return gs_out.at[:, l_own * at["w"] + at["dp"] // 2, pl.ds(first_rows[q], gs_sum[q].shape[1]), lanes_at(at["dp"] % 2)]

    def gs3(q, k):
        once(("gs", q, k))
        mine = block_at(q, k, 0)
        pltpu.make_async_copy(gs_b[q].at[k], mine, sem_gf.at[q, 3, k, 0]).start()
        for way, shift in ((0, 1), (1, -1)):
            push(gs_b[q].at[k], mine, sem_gf.at[q, way, k], {axes[q][1]: next_to(axes[q][1], shift)})

    def gs4(q, k):
        way, shift = (0, 1) if k < 2 else (1, -1)
        drain(gs_b[q].at[k], sem_gf.at[q, way, k, 1])
        block = block_at(q, k, -shift)
        push(block, block, sem_gf.at[q, 2, k], {axes[q][1]: next_to(axes[q][1], shift)})

    def gs5(q, k):
        drain(gs_b[q].at[k], sem_gf.at[q, 1 if k < 2 else 0, k, 1])
        drain(gs_b[q].at[k], sem_gf.at[q, 2, k, 1])
        for i in range(4):
            drain(gs_b[q].at[k], sem_gf.at[q, i, k, 0])

    scope = dict(locals())
    scope["pk"] = pk_
    for name in ORDER.split():
        call = name.rstrip("0123456789") or name
        if name in scope:
            scope[name]()
        elif name[:3] in scope:
            scope[name[:3]](*map(int, name[3:]))
        else:
            scope[call](*map(int, name[len(call):]))
    assert not coming
    settle()


def hand_on_kernel(*refs):
    n = len(refs) // 2
    copies = [pltpu.make_async_copy(refs[i], refs[n + i], refs[2 * n].at[i]) for i in range(n)]
    for c in copies:
        c.start()
    for c in copies:
        c.wait()


def hand_on(arrays):
    return pl.pallas_call(
        hand_on_kernel, name="hand_on",
        out_shape=[jax.ShapeDtypeStruct(a.shape, F32) for a in arrays],
        in_specs=[pl.BlockSpec(memory_space=pltpu.VMEM)] * len(arrays), out_specs=[pl.BlockSpec(memory_space=pl.ANY)] * len(arrays),
        scratch_shapes=[pltpu.SemaphoreType.DMA((len(arrays),))],
        compiler_params=pltpu.CompilerParams(vmem_limit_bytes=12 * 1024 * 1024),
    )(*[pltpu.with_memory_space_constraint(a, pltpu.VMEM) for a in arrays])


def solution(mesh):
    dp_size, w_size, h_size = mesh.shape["dp"], mesh.shape["w"], mesh.shape["h"]

    def local_step(field, target, lat_weight, leg_fwd, leg_inv, spec_w, w_in, w_out):
        nb, nc, nt, npl = field.shape
        nlon = npl * w_size
        ntp = nt // 2
        nm = leg_fwd.shape[0] * w_size
        ndev = h_size * w_size
        nlat = nt * h_size
        nl = leg_fwd.shape[1]
        lo = nl // ndev
        assert nm == 8 * h_size and nc == w_size * LANES // 2 and h_size == 2 * w_size and 2 * lo == dp_size and 2 * nl == LANES
        total_points = nb * dp_size * nc * nlat * nlon
        any_spec = pl.BlockSpec(memory_space=pl.ANY)
        vmem_spec = pl.BlockSpec(memory_space=pltpu.VMEM)
        sds = lambda *s: jax.ShapeDtypeStruct(s, F32)
        vm = lambda *s: pltpu.VMEM(s, F32)
        dma = lambda *s: pltpu.SemaphoreType.DMA(s)
        n_rows = 2 * nc + w_out.shape[0]
        n_z, n_h, n_w = n_rows // dp_size, n_rows // dp_size // h_size, n_rows // dp_size // h_size // w_size
        home = vm(nb, nt, npl, nc)
        woven = vm(nb, w_size, ntp, npl, LANES)
        order = vm(nb, 16 * nlat // 2, LANES)
        degree = vm(nb, 8 * nl, LANES)
        owner = vm(nb, h_size, 8 * lo, w_size * LANES)
        saved = vm(nb, lo, 2 * nm, nc)
        cut = GS_ROWS
        n_pairs = leg_fwd.shape[0] // 2
        n_c = n_rows // 2
        n_z, n_h, n_w = n_c // dp_size, n_c // dp_size // w_size, n_c // dp_size // w_size // w_size
        results = pl.pallas_call(
            functools.partial(block_kernel, (dp_size, h_size, w_size), total_points),
            name="block",
            out_shape=[vm(nb, nt, npl, nc), vm(2, lo * w_size, nc, nc), vm(nc, 2 * nc), vm(2 * nc, nc), sds(1, 1)],
            in_specs=[any_spec] * 9,
            out_specs=[vmem_spec] * 5,
            scratch_shapes=[
                vm(*leg_fwd.shape[:1], nt, nl), vm(*leg_fwd.shape[:1], nt, nl), pltpu.SMEM((nt,), F32), pltpu.VMEM(w_in.shape, BF16),
                pltpu.VMEM(w_out.shape, BF16), vm(2 * nm, nlon), vm(2 * nm, nlon), vm(nlon, 2 * nm), vm(nlon, 2 * nm),
                home, home, woven, vm(nb, ntp, nlon, LANES), woven, woven,
                vm(nb, h_size, 16 * ntp, LANES), order, order, order, vm(nb, h_size, 16 * ntp, LANES), vm(nb, h_size, 16 * ntp, LANES),
                degree, owner, owner, vm(nb, h_size, w_size, 8 * lo, LANES), degree, degree, saved, saved,
                vm(dp_size, nb, 2 * nm, nc), vm(dp_size, nb, 2 * nm, LANES),
                vm(8, nc), vm(h_size, 8, nc), vm(8, nc), vm(w_size, 8, nc),
                vm(2, n_pairs, nt, 2 * nl), vm(2, w_size, n_pairs, nt, 2 * nl), vm(2, 4, nlat, 2 * nl),
                vm(8, nl, nlat), vm(8, nl, nlat), vm(8, nlat, nl), vm(8, nlat, nl),
                vm(2, lo, nc, nc),
                vm(n_rows, nc), vm(n_c, nc), vm(n_c, nc), vm(dp_size, n_z, nc), vm(n_z, nc), vm(w_size, n_h, nc), vm(n_h, nc),
                vm(w_size, n_w, nc), vm(n_w, nc), vm(n_h, nc), vm(n_z, nc), vm(n_c, nc), vm(n_c, nc),
                vm(8, nc), vm(8, nc), vm(8, nc), vm(dp_size, 8, nc), vm(8, nc), vm(w_size, 8, nc), vm(8, nc), vm(w_size, 8, nc),
                vm(nc, nc), vm(2, cut, LANES), vm(2, nc - cut, LANES), vm(4, 2, cut, LANES), vm(4, 2, nc - cut, LANES),
            ] + [dma(nb, PARTS, 2)] * 8 + [dma(nb, 2)] * 6 + [dma(nb, 2), dma(4, 2), dma(5, 2), dma(1), dma(8, 2), dma(4, 2),
                 dma(2, 5, 2), dma(2, 4, 4, 2), dma(3), dma(6)],
            compiler_params=pltpu.CompilerParams(collective_id=0, has_side_effects=True, vmem_limit_bytes=54 * 1024 * 1024),
        )(field.transpose(0, 2, 3, 1), target.transpose(0, 2, 3, 1), leg_fwd.transpose(0, 2, 1), leg_inv.transpose(0, 2, 1),
          spec_w, lat_weight, w_in, w_out, jnp.asarray(dft_table(nlon, nm, h_size)))
        d_x, g_spec, g_in, g_out = hand_on(results[:4])
        loss = results[4]
        return loss.reshape(()), d_x.transpose(0, 3, 1, 2), g_spec, g_in, g_out

    grid_spec = P("dp", None, "h", "w")
    table_spec = P("w", None, "h")
    kernel_spec = P(None, "h", None, None)
    return jax.shard_map(local_step, mesh=mesh, in_specs=(grid_spec, grid_spec, P("h"), table_spec, table_spec, P(), P(), P()), out_specs=(P(), grid_spec, kernel_spec, P(), P()), check_vma=False)
```

```python
import functools
import jax
import jax.numpy as jnp
import numpy as np
from jax import lax
from jax.experimental import pallas as pl
from jax.experimental.pallas import tpu as pltpu
from jax.sharding import PartitionSpec as P

NORM_EPS = 1e-5
PRECISE = lax.Precision.HIGHEST
MESH = pl.DeviceIdType.MESH
F32 = jnp.float32
BF16 = jnp.bfloat16
GELU_C = float(np.sqrt(2.0 / np.pi))
GELU_A = 0.044715
LANES = 128
NN = (((1,), (0,)), ((), ()))
NT = (((1,), (1,)), ((), ()))
TN = (((0,), (0,)), ((), ()))


def dot(a, b, dims=NN):
    return lax.dot_general(a, b, dims, precision=PRECISE, preferred_element_type=F32)


def bdot(a, b, dims=NN):
    return lax.dot_general(a, b, dims, preferred_element_type=F32)


def dft_table(lon_count, num_modes, h_size):
    modes, lons = np.arange(num_modes), np.arange(lon_count)
    angle = 2.0 * np.pi * ((modes[:, None] * lons[None, :]) % lon_count) / lon_count
    table = np.stack([np.cos(angle), -np.sin(angle)], 0) * lon_count ** -0.5
    table = table.reshape(2, h_size, num_modes // h_size, lon_count).transpose(1, 0, 2, 3)
    return table.reshape(2 * num_modes, lon_count).astype(np.float32)


def drain(ref, sem):
    pltpu.make_async_copy(ref, ref, sem).wait()


def rows_at(i, n):
    return pl.ds(pl.multiple_of(i * n, n), n)


def lanes_at(i):
    return pl.ds(pl.multiple_of(i * LANES, LANES), LANES)


def push(src, dst, sems, device):
    pltpu.make_async_remote_copy(src_ref=src, dst_ref=dst, send_sem=sems.at[0], recv_sem=sems.at[1],
                                 device_id=device, device_id_type=MESH).start()


def keep(src, dst, sems):
    pltpu.make_async_copy(src, dst, sems.at[1]).start()


def flip(v):
    return pltpu.roll(v, LANES // 2, 1)


def low(v):
    return lax.broadcasted_iota(jnp.int32, v.shape, 1) < LANES // 2


def weave(a, b):
    return jnp.where(low(a), a, flip(b)), jnp.where(low(a), flip(a), b)


def weave_wide(tiles):
    pairs = [weave(tiles[j], tiles[j + 1]) for j in range(0, len(tiles), 2)]
    return jnp.concatenate([p[0] for p in pairs], axis=1), jnp.concatenate([p[1] for p in pairs], axis=1)


def weave_tiles(a, b):
    out = []
    for j in range(0, a.shape[1], LANES):
        out.extend(weave(a[:, j:j + LANES], b[:, j:j + LANES]))
    return out


PARTS = 4
GS_ROWS = 176
GS_FIRST = (0, 1, 2)
ORDER = " ".join((
    'go', 'pk0', 'sX01', 'pk2', 'pk1', 'sX03', 'tb1', 'sX00', 'sX02', 'sX12',
    'fd01', 'fd03', 'sX10', 'tb2', 'fd00', 'fd02', 'tb4', 'st1', 'sX11', 'sX13',
    'tb3', 'fd12', 'fl0', 'st2', 'fd10', 'tb5', 'sX21', 'fd13', 'fd11', 'sX20',
    'fo0', 'fl1', 'sX23', 'sX22', 'fd20', 'fu0', 'fo1', 'fd23', 'fd21', 'fi00',
    'sY00', 'fi01', 'sY01', 'fi02', 'fd22', 'fi03', 'sY02', 'sY03', 'pw00', 'fu1',
    'sD00', 'fl2', 'pw02', 'sD02', 'pw01', 'pw03', 'sD03', 'sD01', 'fi12', 'bd02',
    'fi10', 'sY12', 'fi13', 'bd00', 'fo2', 'bd01', 'sY10', 'bd03', 'fi11', 'sY11',
    'pw12', 'sY13', 'fu2', 'pw10', 'sD12', 'bl0', 'sD10', 'pw11', 'fi21', 'fi20',
    'sY20', 'sY21', 'pw13', 'fi22', 'sD11', 'fi23', 'bd10', 'sD13', 'bo0', 'sY22',
    'pw21', 'bd12', 'sY23', 'sD21', 'bd13', 'pw20', 'sD20', 'bd11', 'bu0', 'pw22',
    'pw23', 'sD22', 'sD23', 'gw1', 'gsa', 'bd21', 'gw2', 'bl1', 'bi03', 'bi02',
    'bd22', 'sN02', 'bi01', 'sN01', 'bd20', 'bd23', 'gw3', 'bo1', 'bl2', 'bi00',
    'sN03', 'gw4', 'sN00', 'bu1', 'bo2', 'gw5', 'pj1', 'bi10', 'sN10', 'gsb',
    'bi11', 'sN11', 'pj2', 'gs1', 'gs20', 'gs21', 'bi13', 'sN13', 'gs300', 'gw6',
    'bu2', 'gs310', 'gs61', 'bi12', 'sN12', 'gs303', 'gw7', 'gs313', 'fn11', 'gs60',
    'bi20', 'gs311', 'fn12', 'bi23', 'fn10', 'fn02', 'gs312', 'gs403', 'gs301', 'gs413',
    'gs410', 'sN23', 'sN20', 'gs302', 'gs400', 'bi22', 'fn13', 'bi21', 'gw8', 'sN21',
    'sN22', 'fn00', 'gs503', 'gs412', 'gs401', 'fn20', 'gs402', 'fn01', 'gs411', 'end',
    'gs502', 'gs500', 'gs510', 'fn23', 'fn03', 'gs501', 'fn22', 'gs512', 'fn21', 'gs513',
    'gs511',
))


def block_kernel(sizes, total_points,
                 x, tgt, leg_p_in, leg_q_in, spec_w, lat_in, w1_in, w2_in, f_in,
                 dout, gs_out, gin_out, gout_out, loss_out,
                 leg_p, leg_q, lat, w1, w2, f_tab, g_tab, ft_tab, gt_tab,
                 xh, th, pk, rows, yrow, hy,
                 xs, sr, dsr, ys, yr, dyr, als, ar, dar, bs, br, dbr, asave, dsave, aall, dall,
                 st_s, st_h, st_m, st_w, tab_s, tab_w, tab, down_p, down_q, up_p, up_q, ker,
                 gw, gw_p, gw_a, gw_z, gw_zs, gw_h, gw_hs, gw_w, gw_ws, gw_w2, gw_h2, gw_f, gw_o,
                 ls, ls_p, ls_a, ls_z, ls_zs, ls_h, ls_hs, ls_w, gs_acc, gs_sum0, gs_sum1, gs_b0, gs_b1,
                 sem_x, sem_y, sem_d, sem_n, sem_s, sem_ds, sem_u, sem_du, sem_a, sem_da, sem_b, sem_db, sem_az, sem_dz,
                 sem_in, sem_st, sem_tab, sem_k, sem_gw, sem_ls, sem_gs, sem_gf, sem_fin, sem_small):
    dp_size, h_size, w_size = sizes
    dp, h, w = lax.axis_index("dp"), lax.axis_index("h"), lax.axis_index("w")
    ndev = h_size * w_size
    me = h * w_size + w
    nb, nt, npl, nc = x.shape
    ntp = nt // 2
    part = ntp // PARTS
    nlon = npl * w_size
    nlat = nt * h_size
    nl = als.shape[1] // 8
    l_own = nl // ndev
    piece = 8 * l_own
    unsent, coming = {}, {}

    def got(key):
        coming.pop(key)()

    def peer(k):
        return (h + k // w_size) % h_size, (w + k % w_size) % w_size

    barrier = pltpu.get_barrier_semaphore()

    def meet(k, _):
        h2, w2_ = peer(k)
        pl.semaphore_signal(barrier, inc=1, device_id={"h": h2, "w": w2_}, device_id_type=MESH)
        return 0

    def meet_dp(k, _):
        pl.semaphore_signal(barrier, inc=1, device_id={"dp": (dp + k) % dp_size}, device_id_type=MESH)
        return 0

    lax.fori_loop(1, ndev, meet, 0)
    lax.fori_loop(1, dp_size, meet_dp, 0)
    loads = [pltpu.make_async_copy(x.at[b], xh.at[b], sem_in.at[b, 0]) for b in range(nb)]
    load_t = [pltpu.make_async_copy(tgt.at[b], th.at[b], sem_in.at[b, 1]) for b in range(nb)]
    load_k = pltpu.make_async_copy(spec_w.at[:, pl.ds(me * l_own, l_own)], ker, sem_k.at[0])
    small = [pltpu.make_async_copy(src, dst, sem_small.at[i]) for i, (src, dst) in enumerate((
        (leg_p_in, leg_p), (leg_q_in, leg_q), (f_in, f_tab), (lat_in, lat), (w1_in, w1), (w2_in, w2)))]
    for c in loads + small[:3] + [load_k] + load_t + small[3:]:
        c.start()
    coming["k"] = load_k.wait
    coming["small"] = lambda: [c.wait() for c in small[3:]]
    coming.update({("t", b): load_t[b].wait for b in range(nb)})
    for ref in (ar, br, dar, dbr, st_s, gw, ls):
        ref[...] = jnp.zeros_like(ref)

    def settle(*keys):
        for key in keys or list(unsent):
            for wait in unsent.pop(key, []):
                wait()

    def far_first(k, size):
        j = k - 1
        return size // 2 + (j // 2) * (1 - j % 2) - ((j + 1) // 2) * (j % 2)

    def along(axis, refs, sems, sent, key=None):
        size, index = {"dp": (dp_size, dp), "h": (h_size, h), "w": (w_size, w)}[axis]
        src, dst = refs(index)
        keep(src, dst, sems)

        def body(k, _):
            other = (index + far_first(k, size)) % size
            src, dst = refs(other)
            push(src, dst, sems, {axis: other})
            return 0

        lax.fori_loop(1, size, body, 0)
        unsent.setdefault(key, []).append(lambda: drain(sent, sems.at[0]))

    def some(refs, sems, low_h, high_h, count, counts, key):
        src, dst = refs(h, w)
        keep(src, dst, sems)

        def one(h2, k):
            w2_ = (w + k) % w_size
            src, dst = refs(h2, w2_)
            push(src, dst, sems, {"h": h2, "w": w2_})

        def body(h2, _):
            for k in (2, 1, 3, 0):
                one(h2, k)
            return 0

        lax.fori_loop(low_h, high_h, body, 0)
        for k in (2, 1, 3):
            one(h, k)
        unsent.setdefault(key, []).append(lambda: take(sems.at[0], count - 1, [n - 1 for n in counts]))

    def take(sem, count, counts):
        for n in counts:
            @pl.when(count == n)
            def _():
                drain(als.at[0, pl.ds(0, n * piece)], sem)

    n_orders, n_owners = (h + 1) * w_size, (h_size - h) * w_size
    counts = [w_size * n for n in range(1, h_size + 1)]
    pairs = lambda k: pl.ds(k * part, part)

    def at_rows(i, k):
        return pl.ds(pl.multiple_of(i * 16 * ntp + k * 16 * part, 16 * part), 16 * part)

    def send_home_rows(b, k, sem, name):
        along("w", lambda o: (pk.at[b, o, pairs(k)], rows.at[b, pairs(k), rows_at(w, npl)]), sem.at[b, k],
              pk.at[b, pl.ds(0, w_size - 1), pairs(k)], ("pk", b, k))
        coming[name, b, k] = lambda: drain(rows.at[b, pairs(k)], sem.at[b, k, 1])

    def send_rows_home(b, k, sem, name):
        along("w", lambda o: (yrow.at[b, o, pairs(k)], hy.at[b, w, pairs(k)]), sem.at[b, k],
              yrow.at[b, pl.ds(0, w_size - 1), pairs(k)], ("yrow", b, k))
        coming[name, b, k] = lambda: drain(hy.at[b, :, pairs(k)], sem.at[b, k, 1])

    def send_orders(b, k, dst, sem, name):
        along("h", lambda o: (xs.at[b, o, at_rows(0, k)], dst.at[b, at_rows(h, k)]), sem.at[b, k],
              xs.at[b, pl.ds(0, h_size - 1), at_rows(0, k)], ("xs", b, k))
        coming[name, b, k] = lambda: drain(xs.at[b, :, at_rows(0, k)], sem.at[b, k, 1])

    def send_lats(b, dst, sem, name):
        def one(k, _):
            keep(ys.at[b, at_rows(h, k)], dst.at[b, h, at_rows(0, k)], sem.at[b, k])

            def body(j, _):
                o = (h + far_first(j, h_size)) % h_size
                push(ys.at[b, at_rows(o, k)], dst.at[b, h, at_rows(0, k)], sem.at[b, k], {"h": o})
                return 0

            return lax.fori_loop(1, h_size, body, 0)

        lax.fori_loop(0, PARTS, one, 0)
        for k in range(PARTS):
            unsent.setdefault(("ys", b), []).append(lambda k=k: drain(xs.at[b, pl.ds(0, h_size - 1), at_rows(0, k)], sem.at[b, k, 0]))
            coming[name, b, k] = lambda k=k: drain(dst.at[b, :, at_rows(0, k)], sem.at[b, k, 1])

    def send_owner(b, dst, sem, name):
        some(lambda h2, w2_: (als.at[b, rows_at(h2 * w_size + w2_, piece)], dst.at[b, h, :, lanes_at(w)]), sem.at[b],
             h + 1, h_size, n_owners, counts, ("als", b))
        coming[name, b] = lambda: take(sem.at[b, 1], n_orders, counts)

    def send_back(b, dst, sem, name):
        some(lambda h2, w2_: (bs.at[b, h2, w2_], dst.at[b, rows_at(me, piece)]), sem.at[b],
             0, h, n_orders, counts, ("bs", b))
        coming[name, b] = lambda: take(sem.at[b, 1], n_owners, counts)

    def dft(b, k, table):
        settle(("xs", b, k))

        def body(n, _):
            i = 2 * n
            both = jnp.concatenate([rows[b, i], rows[b, i + 1]], axis=1)
            out = dot(table[...], both).reshape(h_size, 16, 2 * LANES)
            xs[b, :, rows_at(i, 16), :] = out[:, :, :LANES]
            xs[b, :, rows_at(i + 1, 16), :] = out[:, :, LANES:]
            return 0

        lax.fori_loop(k * part // 2, (k + 1) * part // 2, body, 0)

    def idft(b, k, table, src):
        settle(("yrow", b, k))

        def body(n, _):
            i = 2 * n
            both = jnp.concatenate([src[b, :, rows_at(i + j, 16), :].reshape(-1, LANES) for j in range(2)], axis=1)
            out = dot(table[...], both)
            for j in range(2):
                yrow[b, :, i + j] = out[:, j * LANES:(j + 1) * LANES].reshape(w_size, npl, LANES)
            return 0

        lax.fori_loop(k * part // 2, (k + 1) * part // 2, body, 0)

    def level(v, here):
        mean = jnp.mean(v, axis=0, keepdims=True)
        mean = 0.5 * (mean + flip(mean))
        return v - jnp.where(jnp.logical_and(h == 0, here), mean, 0.0)

    def orders(body):
        def four(n, _):
            for i in range(4):
                body(4 * n + i, n == 0 if i == 0 else None)
            return 0

        lax.fori_loop(0, 2, four, 0)

    def leg_down(b, table, src, fix):
        settle(("als", b))

        def one(m, here):
            re, im = (src[b, pl.ds(ri * 8 + m, ntp * h_size, stride=16), :] for ri in range(2))
            if fix and here is not None:
                re = level(re, here)
            als[b, pl.ds(m, nl, stride=8), :] = dot(table[m], jnp.concatenate(weave(re, im), axis=0))

        orders(one)

    def leg_up(b, table, src, fix):
        settle(("ys", b))

        def one(m, here):
            out = dot(table[m], src[b, pl.ds(m, nl, stride=8), :])
            re, im = weave(out[:nlat // 2], out[nlat // 2:])
            if fix and here is not None:
                re = level(re, here)
            ys[b, pl.ds(m, ntp * h_size, stride=16), :] = re
            ys[b, pl.ds(8 + m, ntp * h_size, stride=16), :] = im

        orders(one)

    def owned(b, l, src):
        tiles = [src[b, :, rows_at(l, 8), j * LANES:(j + 1) * LANES].reshape(-1, LANES) for j in range(w_size)]
        return weave_wide(tiles)

    def put_back(b, l, re, im):
        for j, tile in enumerate(weave_tiles(re, im)):
            bs[b, :, j, rows_at(l, 8), :] = tile.reshape(h_size, 8, LANES)

    def put_rows(b, i, v0, v1):
        for j, tile in enumerate(weave_tiles(v0, v1)):
            pk[b, j, i] = tile

    def get_rows(b, i):
        return weave_wide([hy[b, j, i] for j in range(w_size)])

    count = nt * npl
    n_tab = tab_s.shape[1] // dp_size

    def combine(stats, n):
        mean = jnp.mean(stats, axis=0)
        dev = stats - mean[None]
        dev2 = jnp.sum(dev * dev, axis=0)
        m2 = jnp.sum(stats, axis=0)
        return [(mean[2 * b:2 * b + 1], m2[2 * b + 1:2 * b + 2] + n * dev2[2 * b:2 * b + 1]) for b in range(nb)]

    sums = {}

    def pk_(b):
        loads[b].wait()

        def body(i, total):
            v0, v1 = xh[b, i], xh[b, i + ntp]
            put_rows(b, i, v0, v1)
            return total + jnp.sum(v0 + v1, axis=0, keepdims=True)

        sums[b] = lax.fori_loop(0, ntp, body, jnp.zeros((1, nc), F32))

    def go():
        for c in small[:3]:
            c.wait()
        for a, leg in enumerate((leg_p, leg_q)):
            for m in range(leg.shape[0]):
                tab_s[a, m // 2, :, m % 2 * nl:(m % 2 + 1) * nl] = leg[m]
        pl.semaphore_wait(barrier, ndev - 1 + dp_size - 1)
        along("w", lambda o: (tab_s.at[:, rows_at(dp, n_tab)], tab_w.at[:, w, rows_at(dp, n_tab)]), sem_tab.at[0],
              tab_w.at[:, pl.ds(0, w_size - 1), pl.ds(0, n_tab)])
        coming["tab"] = lambda: drain(tab_w.at[:, :, pl.ds(0, n_tab)], sem_tab.at[0, 1])

    def st1():
        for b in range(nb):
            mean = sums[b] / count

            def body(t, total, b=b, mean=mean):
                d = xh[b, t] - mean
                return total + jnp.sum(d * d, axis=0, keepdims=True)

            st_s[2 * b:2 * b + 1, :] = mean
            st_s[2 * b + 1:2 * b + 2, :] = lax.fori_loop(0, nt, body, jnp.zeros((1, nc), F32))
        along("w", lambda o: (st_s, st_w.at[w]), sem_st.at[0], st_w.at[pl.ds(0, w_size - 1)], "st")
        coming["st"] = lambda: drain(st_w, sem_st.at[0, 1])
        g_tab[...] = jnp.where(lax.broadcasted_iota(jnp.int32, f_tab.shape, 0) == 0, 1.0, 2.0) * f_tab[...]
        ft_tab[...] = f_tab[...].T
        gt_tab[...] = g_tab[...].T

    def st2():
        got("st")
        st_m[...] = jnp.zeros_like(st_m)
        for b, (mean, m2) in enumerate(combine(st_w[...], count)):
            st_m[2 * b:2 * b + 1, :] = mean
            st_m[2 * b + 1:2 * b + 2, :] = m2
        along("h", lambda o: (st_m, st_h.at[h]), sem_st.at[1], st_h.at[pl.ds(0, h_size - 1)], "st")
        coming["st2"] = lambda: drain(st_h, sem_st.at[1, 1])

    means, scales = [], []

    def st3():
        got("st2")
        for mean, m2 in combine(st_h[...], count * w_size):
            means.append(mean)
            scales.append(lax.rsqrt(m2 / (count * ndev) + NORM_EPS))

    def tb1():
        got("tab")
        for a in range(2):
            share = tab_w.at[a, :, rows_at(dp, n_tab)]
            for k in range(1, dp_size):
                push(share, share, sem_tab.at[1 + a], {"dp": (dp + k) % dp_size})
            others = tab_w.at[a, :, pl.ds(0, (dp_size - 1) * n_tab)]
            unsent.setdefault(None, []).append(lambda a=a, others=others: drain(others, sem_tab.at[1 + a, 0]))
            coming["tab1", a] = lambda a=a, others=others: drain(others, sem_tab.at[1 + a, 1])

    def table_out(a):
        got(("tab1", a))
        along("h", lambda o: (tab_w.at[a, o // 2, rows_at(o % 2, 4)], tab.at[a, :, rows_at(h, nt)]), sem_tab.at[3 + a],
              tab.at[a, :, pl.ds(0, nlat - nt)])
        coming["tab2", a] = lambda: drain(tab.at[a], sem_tab.at[3 + a, 1])

    def table_in(a, down, up):
        got(("tab2", a))

        def body(n, _):
            both = tab[a, n].reshape(h_size, 2, ntp, 2 * nl)
            both = jnp.concatenate([both[:, j].reshape(-1, 2 * nl) for j in range(2)], axis=0)
            for j in range(2):
                t = both[:, j * nl:(j + 1) * nl]
                up[2 * n + j] = t
                down[2 * n + j] = t.T
            return 0

        lax.fori_loop(0, tab.shape[1], body, 0)

    def tb2():
        table_out(0)

    def tb3():
        table_in(0, down_p, up_p)

    def tb4():
        table_out(1)

    def tb5():
        table_in(1, down_q, up_q)

    def sX(b, k):
        send_home_rows(b, k, sem_x, "x")

    def fd(b, k):
        got(("x", b, k))
        dft(b, k, f_tab)
        send_orders(b, k, sr, sem_s, "s")

    def fl(b):
        for k in range(PARTS):
            got(("s", b, k))
        leg_down(b, down_p, sr, True)
        send_owner(b, ar, sem_a, "a")

    def fo(b):
        if not scales:
            got("k")
            st3()
        got(("a", b))
        settle(("bs", b))

        def one(l, _):
            re, im = owned(b, l, ar)
            a = jnp.concatenate([re, im], axis=0) * scales[b]
            asave[b, l] = a
            n = a.shape[0] // 2
            own, other = dot(a, ker[0, l]), dot(a, ker[1, l])
            put_back(b, l, own[:n] - other[n:], own[n:] + other[:n])
            return 0

        lax.fori_loop(0, l_own, one, 0)
        send_back(b, br, sem_b, "b")
        along("dp", lambda o: (asave.at[b, o // 2], aall.at[dp, b]), sem_az.at[b], aall.at[pl.ds(0, dp_size - 1), b])
        coming["az", b] = lambda: drain(aall.at[:, b], sem_az.at[b, 1])

    def fu(b):
        got(("b", b))
        leg_up(b, up_q, br, False)
        send_lats(b, yr, sem_u, "u")

    def fi(b, k):
        got(("u", b, k))
        idft(b, k, gt_tab, yr)

    def sY(b, k):
        send_rows_home(b, k, sem_y, "y")

    def pw(b, k):
        got(("y", b, k))
        if ("t", b) in coming:
            got(("t", b))
        if "small" in coming:
            got("small")
        settle(("pk", b, k))

        def body(n, _):
            lats = [n, n + ntp]
            y = jnp.concatenate(get_rows(b, n), axis=0)
            yb = y.astype(BF16)
            hid = bdot(yb, w1[...])
            th_ = jnp.tanh(GELU_C * (hid + GELU_A * (hid * hid * hid)))
            act = (hid * (0.5 * (1.0 + th_))).astype(BF16)
            resid = y + bdot(act, w2[...])
            parts = []
            for j, t in enumerate(lats):
                r = resid[j * npl:(j + 1) * npl] + xh[b, t] - th[b, t]
                d = lat[t] * r
                ls[...] += jnp.sum((d * r).reshape(-1, 8, nc), axis=0)
                dout[b, t] = d
                parts.append(d)
            d = jnp.concatenate(parts, axis=0)
            db = d.astype(BF16)
            gw[2 * nc:, :] += bdot(act, db, TN)
            slope = 0.5 * (1.0 + th_) + (0.5 * GELU_C) * hid * (1.0 - th_ * th_) * (1.0 + (3.0 * GELU_A) * (hid * hid))
            dh = (bdot(db, w2[...], NT) * slope).astype(BF16)
            gin = bdot(yb, dh, TN)
            gw[:nc, :] += gin[:, :nc]
            gw[nc:2 * nc, :] += gin[:, nc:]
            dy = d + bdot(dh, w1[...], NT)
            put_rows(b, n, dy[:npl], dy[npl:])
            return 0

        lax.fori_loop(k * part, (k + 1) * part, body, 0)

    def sD(b, k):
        send_home_rows(b, k, sem_d, "d")

    def bd(b, k):
        got(("d", b, k))
        dft(b, k, g_tab)
        send_orders(b, k, dsr, sem_ds, "ds")

    def bl(b):
        for k in range(PARTS):
            got(("ds", b, k))
        leg_down(b, down_q, dsr, False)
        send_owner(b, dar, sem_da, "da")

    def bo(b):
        got(("da", b))
        settle(("bs", b), "st")

        def one(l, s2):
            re, im = owned(b, l, dar)
            d = jnp.concatenate([re, im], axis=0)
            dsave[b, l] = d
            n = d.shape[0] // 2
            own, other = dot(d, ker[0, l], NT), dot(d, ker[1, l], NT)
            re, im = own[:n] + other[n:], own[n:] - other[:n]
            put_back(b, l, re, im)
            return s2 + jnp.sum(re * asave[b, l, :n] + im * asave[b, l, n:], axis=0, keepdims=True)

        s2 = lax.fori_loop(0, l_own, one, jnp.zeros((1, nc), F32))
        send_back(b, dbr, sem_db, "db")
        along("dp", lambda o: (dsave.at[b, o // 2, :, lanes_at(o % 2)], dall.at[dp, b]), sem_dz.at[b], dall.at[pl.ds(0, dp_size - 1), b])
        coming["dz", b] = lambda: drain(dall.at[:, b], sem_dz.at[b, 1])
        st_s[b:b + 1, :] = s2

    def bu(b):
        got(("db", b))
        leg_up(b, up_p, dbr, True)
        send_lats(b, dyr, sem_du, "du")

    def bi(b, k):
        got(("du", b, k))
        idft(b, k, ft_tab, dyr)

    def sN(b, k):
        send_rows_home(b, k, sem_n, "n")

    def pj1():
        st_s[nb:, :] = jnp.zeros_like(st_s[nb:, :])
        along("w", lambda o: (st_s, st_w.at[w]), sem_st.at[2], st_w.at[pl.ds(0, w_size - 1)])
        coming["pj"] = lambda: drain(st_w, sem_st.at[2, 1])

    def pj2():
        got("pj")
        st_m[...] = jnp.sum(st_w[...], axis=0)
        along("h", lambda o: (st_m, st_h.at[h]), sem_st.at[3], st_h.at[pl.ds(0, h_size - 1)])
        coming["pj2"] = lambda: drain(st_h, sem_st.at[3, 1])

    proj = []

    def fn(b, k):
        if not proj:
            got("pj2")
            proj.append(jnp.sum(st_h[...], axis=0) / (count * ndev))
        got(("n", b, k))

        def body(i, _):
            for t, dn in zip((i, i + ntp), get_rows(b, i)):
                normed = (xh[b, t] - means[b]) * scales[b]
                dout[b, t] = dout[b, t] + scales[b] * (dn - normed * proj[0][b:b + 1])
            return 0

        lax.fori_loop(k * part, (k + 1) * part, body, 0)

    n_c, n_z, n_h, n_w = gw_a.shape[0], gw_zs.shape[0], gw_hs.shape[0], gw_ws.shape[0]
    chip, core = h // 2, h % 2
    chips = h_size // 2

    def over_chips(refs, sems, sent):
        src, dst = refs(chip)
        keep(src, dst, sems)
        for k in range(1, chips):
            o = (chip + k) % chips
            src, dst = refs(o)
            push(src, dst, sems, {"h": 2 * o + core})
        unsent.setdefault(None, []).append(lambda: drain(sent, sems.at[0]))

    def twin(src, dst, sems):
        push(src, dst, sems, {"h": h + 1 - 2 * core})
        unsent.setdefault(None, []).append(lambda: drain(dst, sems.at[0]))

    def gw1():
        twin(gw.at[rows_at(1 - core, n_c)], gw_p, sem_gw.at[0])
        twin(ls, ls_p, sem_ls.at[0])
        coming["gw1"] = lambda: (drain(gw_p, sem_gw.at[0, 1]), drain(ls_p, sem_ls.at[0, 1]))

    def gw2():
        got("gw1")
        gw_a[...] = gw[rows_at(core, n_c), :] + gw_p[...]
        ls_a[...] = ls[...] + ls_p[...]
        along("dp", lambda o: (gw_a.at[rows_at(o, n_z)], gw_z.at[dp]), sem_gw.at[1], gw_z.at[pl.ds(0, dp_size - 1)])
        along("dp", lambda o: (ls_a, ls_z.at[dp]), sem_ls.at[1], ls_z.at[pl.ds(0, dp_size - 1)])
        coming["gw2"] = lambda: (drain(gw_z, sem_gw.at[1, 1]), drain(ls_z, sem_ls.at[1, 1]))

    def gw3():
        got("gw2")
        gw_zs[...] = jnp.sum(gw_z[...], axis=0)
        ls_zs[...] = jnp.sum(ls_z[...], axis=0)
        over_chips(lambda o: (gw_zs.at[rows_at(o, n_h)], gw_h.at[chip]), sem_gw.at[2], gw_h.at[pl.ds(0, chips - 1)])
        over_chips(lambda o: (ls_zs, ls_h.at[chip]), sem_ls.at[2], ls_h.at[pl.ds(0, chips - 1)])
        coming["gw3"] = lambda: (drain(gw_h, sem_gw.at[2, 1]), drain(ls_h, sem_ls.at[2, 1]))

    def gw4():
        got("gw3")
        gw_hs[...] = jnp.sum(gw_h[...], axis=0)
        ls_hs[...] = jnp.sum(ls_h[...], axis=0)
        along("w", lambda o: (gw_hs.at[rows_at(o, n_w)], gw_w.at[w]), sem_gw.at[3], gw_w.at[pl.ds(0, w_size - 1)])
        along("w", lambda o: (ls_hs, ls_w.at[w]), sem_ls.at[3], ls_w.at[pl.ds(0, w_size - 1)])
        coming["gw4"] = lambda: (drain(gw_w, sem_gw.at[3, 1]), drain(ls_w, sem_ls.at[3, 1]))

    def gw5():
        got("gw4")
        gw_ws[...] = jnp.sum(gw_w[...], axis=0)
        loss_out[...] = jnp.sum(ls_w[...], keepdims=True).reshape(1, 1) / total_points
        along("w", lambda o: (gw_ws, gw_w2.at[rows_at(w, n_w)]), sem_gw.at[4], gw_w2.at[pl.ds(0, (w_size - 1) * n_w)])
        coming["gw5"] = lambda: drain(gw_w2, sem_gw.at[4, 1])

    def gw6():
        got("gw5")
        over_chips(lambda o: (gw_w2, gw_h2.at[rows_at(chip, n_h)]), sem_gw.at[5], gw_h2.at[pl.ds(0, (chips - 1) * n_h)])
        coming["gw6"] = lambda: drain(gw_h2, sem_gw.at[5, 1])

    def gw7():
        got("gw6")
        along("dp", lambda o: (gw_h2, gw_f.at[rows_at(dp, n_z)]), sem_gw.at[6], gw_f.at[pl.ds(0, (dp_size - 1) * n_z)])
        coming["gw7"] = lambda: drain(gw_f, sem_gw.at[6, 1])

    def gw8():
        got("gw7")
        twin(gw_f, gw_o, sem_gw.at[7])
        coming["gw8"] = lambda: drain(gw_o, sem_gw.at[7, 1])

    def end():
        got("gw8")
        for c, halves in enumerate(((gw_f, gw_o), (gw_o, gw_f))):
            @pl.when(core == c)
            def _():
                first, second = halves
                for i, (src, dst) in enumerate(((first.at[:nc], gin_out.at[:, :nc]), (first.at[nc:], gin_out.at[:, nc:]), (second, gout_out))):
                    pltpu.make_async_copy(src, dst, sem_fin.at[i]).start()
        for i, dst in enumerate((gin_out.at[:, :nc], gin_out.at[:, nc:], gout_out)):
            unsent.setdefault(None, []).append(lambda dst=dst, i=i: drain(dst, sem_fin.at[i]))

    gs_sum, gs_b = (gs_sum0, gs_sum1), (gs_b0, gs_b1)
    first_rows = (0, gs_sum0.shape[1])
    axes = (("w", "dp"), ("dp", "w"))
    place = {"w": (w, w_size), "dp": (dp, dp_size)}

    def next_to(axis, k):
        index, size = place[axis]
        return (index + k + size) % size

    def add_sample(b):
        got(("az", b))
        got(("dz", b))

        def body(n, _):
            d = dall[n, b]
            half = d.shape[0] // 2
            both = jnp.concatenate([d, jnp.concatenate([d[half:], -d[:half]], axis=0)], axis=1)
            gs_acc[...] += dot(aall[n, b], both, TN)
            return 0

        lax.fori_loop(0, dp_size, body, 0)

    def gsa():
        gs_acc[...] = jnp.zeros_like(gs_acc)
        add_sample(GS_FIRST[0])

    def gsb():
        add_sample(GS_FIRST[1])

    def gs1():
        add_sample(GS_FIRST[2])
        for q in range(2):
            rows_q = pl.ds(first_rows[q], gs_sum[q].shape[1])
            for p in range(2):
                gs_sum[q][p] = gs_acc[rows_q, p * LANES:(p + 1) * LANES]

    def once(key):
        if key in coming:
            got(key)

    def sent_later(ref, sem):
        unsent.setdefault(None, []).append(lambda: drain(ref, sem))

    def gs2(q):
        keep(gs_sum[q], gs_b[q].at[0], sem_gs.at[q, 0])
        for slot, k in ((1, 1), (3, -1)):
            push(gs_sum[q], gs_b[q].at[slot], sem_gs.at[q, slot], {axes[q][0]: next_to(axes[q][0], k)})
            sent_later(gs_sum[q], sem_gs.at[q, slot, 0])
        coming.update({("gs", q, k): lambda k=k: drain(gs_b[q].at[k], sem_gs.at[q, k, 1]) for k in (0, 1, 3)})

    def gs6(q):
        for slot, p, k, i in ((1, 0, 1, 2), (3, 1, -1, 4)):
            once(("gs", q, slot))
            push(gs_b[q].at[slot, p], gs_b[q].at[2, p], sem_gs.at[q, i], {axes[q][0]: next_to(axes[q][0], k)})
            sent_later(gs_b[q].at[2, p], sem_gs.at[q, i, 0])
        coming["gs", q, 2] = lambda: (drain(gs_b[q].at[2, 0], sem_gs.at[q, 2, 1]), drain(gs_b[q].at[2, 1], sem_gs.at[q, 4, 1]))

    def block_at(q, k, shift):
        at = {axes[q][0]: next_to(axes[q][0], -k), axes[q][1]: next_to(axes[q][1], shift)}
        return gs_out.at[:, l_own * at["w"] + at["dp"] // 2, pl.ds(first_rows[q], gs_sum[q].shape[1]), lanes_at(at["dp"] % 2)]

    def gs3(q, k):
        once(("gs", q, k))
        mine = block_at(q, k, 0)
        pltpu.make_async_copy(gs_b[q].at[k], mine, sem_gf.at[q, 3, k, 0]).start()
        for way, shift in ((0, 1), (1, -1)):
            push(gs_b[q].at[k], mine, sem_gf.at[q, way, k], {axes[q][1]: next_to(axes[q][1], shift)})

    def gs4(q, k):
        way, shift = (0, 1) if k < 2 else (1, -1)
        drain(gs_b[q].at[k], sem_gf.at[q, way, k, 1])
        block = block_at(q, k, -shift)
        push(block, block, sem_gf.at[q, 2, k], {axes[q][1]: next_to(axes[q][1], shift)})

    def gs5(q, k):
        drain(gs_b[q].at[k], sem_gf.at[q, 1 if k < 2 else 0, k, 1])
        drain(gs_b[q].at[k], sem_gf.at[q, 2, k, 1])
        for i in range(4):
            drain(gs_b[q].at[k], sem_gf.at[q, i, k, 0])

    scope = dict(locals())
    scope["pk"] = pk_
    for name in ORDER.split():
        call = name.rstrip("0123456789") or name
        if name in scope:
            scope[name]()
        elif name[:3] in scope:
            scope[name[:3]](*map(int, name[3:]))
        else:
            scope[call](*map(int, name[len(call):]))
    assert not coming
    settle()


def hand_on_kernel(*refs):
    n = len(refs) // 2
    copies = [pltpu.make_async_copy(refs[i], refs[n + i], refs[2 * n].at[i]) for i in range(n)]
    for c in copies:
        c.start()
    for c in copies:
        c.wait()


def hand_on(arrays):
    return pl.pallas_call(
        hand_on_kernel, name="hand_on",
        out_shape=[jax.ShapeDtypeStruct(a.shape, F32) for a in arrays],
        in_specs=[pl.BlockSpec(memory_space=pltpu.VMEM)] * len(arrays), out_specs=[pl.BlockSpec(memory_space=pl.ANY)] * len(arrays),
        scratch_shapes=[pltpu.SemaphoreType.DMA((len(arrays),))],
        compiler_params=pltpu.CompilerParams(vmem_limit_bytes=12 * 1024 * 1024),
    )(*[pltpu.with_memory_space_constraint(a, pltpu.VMEM) for a in arrays])


def solution(mesh):
    dp_size, w_size, h_size = mesh.shape["dp"], mesh.shape["w"], mesh.shape["h"]

    def local_step(field, target, lat_weight, leg_fwd, leg_inv, spec_w, w_in, w_out):
        nb, nc, nt, npl = field.shape
        nlon = npl * w_size
        ntp = nt // 2
        nm = leg_fwd.shape[0] * w_size
        ndev = h_size * w_size
        nlat = nt * h_size
        nl = leg_fwd.shape[1]
        lo = nl // ndev
        assert nm == 8 * h_size and nc == w_size * LANES // 2 and h_size == 2 * w_size and 2 * lo == dp_size and 2 * nl == LANES
        total_points = nb * dp_size * nc * nlat * nlon
        any_spec = pl.BlockSpec(memory_space=pl.ANY)
        vmem_spec = pl.BlockSpec(memory_space=pltpu.VMEM)
        sds = lambda *s: jax.ShapeDtypeStruct(s, F32)
        vm = lambda *s: pltpu.VMEM(s, F32)
        dma = lambda *s: pltpu.SemaphoreType.DMA(s)
        n_rows = 2 * nc + w_out.shape[0]
        n_z, n_h, n_w = n_rows // dp_size, n_rows // dp_size // h_size, n_rows // dp_size // h_size // w_size
        home = vm(nb, nt, npl, nc)
        woven = vm(nb, w_size, ntp, npl, LANES)
        order = vm(nb, 16 * nlat // 2, LANES)
        degree = vm(nb, 8 * nl, LANES)
        owner = vm(nb, h_size, 8 * lo, w_size * LANES)
        saved = vm(nb, lo, 2 * nm, nc)
        cut = GS_ROWS
        n_pairs = leg_fwd.shape[0] // 2
        n_c = n_rows // 2
        n_z, n_h, n_w = n_c // dp_size, n_c // dp_size // w_size, n_c // dp_size // w_size // w_size
        results = pl.pallas_call(
            functools.partial(block_kernel, (dp_size, h_size, w_size), total_points),
            name="block",
            out_shape=[vm(nb, nt, npl, nc), vm(2, lo * w_size, nc, nc), vm(nc, 2 * nc), vm(2 * nc, nc), sds(1, 1)],
            in_specs=[any_spec] * 9,
            out_specs=[vmem_spec] * 5,
            scratch_shapes=[
                vm(*leg_fwd.shape[:1], nt, nl), vm(*leg_fwd.shape[:1], nt, nl), pltpu.SMEM((nt,), F32), pltpu.VMEM(w_in.shape, BF16),
                pltpu.VMEM(w_out.shape, BF16), vm(2 * nm, nlon), vm(2 * nm, nlon), vm(nlon, 2 * nm), vm(nlon, 2 * nm),
                home, home, woven, vm(nb, ntp, nlon, LANES), woven, woven,
                vm(nb, h_size, 16 * ntp, LANES), order, order, order, vm(nb, h_size, 16 * ntp, LANES), vm(nb, h_size, 16 * ntp, LANES),
                degree, owner, owner, vm(nb, h_size, w_size, 8 * lo, LANES), degree, degree, saved, saved,
                vm(dp_size, nb, 2 * nm, nc), vm(dp_size, nb, 2 * nm, LANES),
                vm(8, nc), vm(h_size, 8, nc), vm(8, nc), vm(w_size, 8, nc),
                vm(2, n_pairs, nt, 2 * nl), vm(2, w_size, n_pairs, nt, 2 * nl), vm(2, 4, nlat, 2 * nl),
                vm(8, nl, nlat), vm(8, nl, nlat), vm(8, nlat, nl), vm(8, nlat, nl),
                vm(2, lo, nc, nc),
                vm(n_rows, nc), vm(n_c, nc), vm(n_c, nc), vm(dp_size, n_z, nc), vm(n_z, nc), vm(w_size, n_h, nc), vm(n_h, nc),
                vm(w_size, n_w, nc), vm(n_w, nc), vm(n_h, nc), vm(n_z, nc), vm(n_c, nc), vm(n_c, nc),
                vm(8, nc), vm(8, nc), vm(8, nc), vm(dp_size, 8, nc), vm(8, nc), vm(w_size, 8, nc), vm(8, nc), vm(w_size, 8, nc),
                vm(nc, nc), vm(2, cut, LANES), vm(2, nc - cut, LANES), vm(4, 2, cut, LANES), vm(4, 2, nc - cut, LANES),
            ] + [dma(nb, PARTS, 2)] * 8 + [dma(nb, 2)] * 6 + [dma(nb, 2), dma(4, 2), dma(5, 2), dma(1), dma(8, 2), dma(4, 2),
                 dma(2, 5, 2), dma(2, 4, 4, 2), dma(3), dma(6)],
            compiler_params=pltpu.CompilerParams(collective_id=0, has_side_effects=True, vmem_limit_bytes=54 * 1024 * 1024),
        )(field.transpose(0, 2, 3, 1), target.transpose(0, 2, 3, 1), leg_fwd.transpose(0, 2, 1), leg_inv.transpose(0, 2, 1),
          spec_w, lat_weight, w_in, w_out, jnp.asarray(dft_table(nlon, nm, h_size)))
        d_x, g_spec, g_in, g_out = hand_on(results[:4])
        loss = results[4]
        return loss.reshape(()), d_x.transpose(0, 3, 1, 2), g_spec, g_in, g_out

    grid_spec = P("dp", None, "h", "w")
    table_spec = P("w", None, "h")
    kernel_spec = P(None, "h", None, None)
    return jax.shard_map(local_step, mesh=mesh, in_specs=(grid_spec, grid_spec, P("h"), table_spec, table_spec, P(), P(), P()), out_specs=(P(), grid_spec, kernel_spec, P(), P()), check_vma=False)
```
